128 devices in a mesh: rep: 4 (over z), ep: 4 (over y), dp: 8 (over x, core).
Axes of the slice: x: 4, y: 4, z: 4, core: 2. Of those that a mesh axis runs over, the one named last changes fastest.
Arguments:
- tok_in: bfloat16 [131072, 384], P(('rep', 'ep', 'dp'))
- tok_grad: bfloat16 [131072, 384], P(('rep', 'ep', 'dp'))
- route_ids: int32 [2, 131072, 2], P(None, ('rep', 'ep', 'dp'))
- gate_vals: float32 [2, 131072, 2], P(None, ('rep', 'ep', 'dp'))
- w_dense: bfloat16 [2, 384, 384], replicated
- w_gate: bfloat16 [2, 8, 384, 1024], P(None, 'ep')
- w_up: bfloat16 [2, 8, 384, 1024], P(None, 'ep')
- w_down: bfloat16 [2, 8, 1024, 384], P(None, 'ep')
Outputs:
- output 1: bfloat16 [131072, 384], P(('rep', 'ep', 'dp'))
- output 2: bfloat16 [131072, 384], P(('rep', 'ep', 'dp'))
- output 3: bfloat16 [2, 384, 384], replicated
- output 4: bfloat16 [2, 8, 384, 1024], P(None, 'ep')
- output 5: bfloat16 [2, 8, 384, 1024], P(None, 'ep')
- output 6: bfloat16 [2, 8, 1024, 384], P(None, 'ep')
All inputs are finite; a program needn't handle non-finite values.
Results may differ from the reference program's by a relative error of at most 0.02.
Values are sent between devices in bfloat16 or wider.
A program may use at most 1 GiB of HBM per device.

```python
import jax
import jax.numpy as jnp
from jax import lax

D = 384
FF = 1024
EXPERTS = 8
TOP = 2
TOKENS = 1024
DEVICES = 128
LAYERS = 2
CAPACITY = 2 * TOKENS * TOP // EXPERTS
ROWS = DEVICES * TOKENS


def draw_routes(route_key):
    half_cap = CAPACITY // 2
    key_pair, key_label, key_order = jax.random.split(route_key, 3)
    shifts = jax.random.randint(key_pair, (EXPERTS // 2,), -(half_cap - 2), half_cap - 1)
    shifts = shifts.at[0].set(half_cap - 1)
    counts = jnp.stack([half_cap + shifts, half_cap - shifts], axis=1).reshape(EXPERTS)
    counts = counts.at[0].add(1).at[2].add(-1)
    count_ends = jnp.cumsum(counts)
    positions = jnp.arange(TOKENS * TOP)
    labels = jnp.sum((positions[:, None] >= count_ends[None, :]).astype(jnp.int32), axis=1)
    relabel = jax.random.permutation(key_label, EXPERTS)
    choices = relabel[labels].reshape(TOP, TOKENS).T
    token_order = jax.random.permutation(key_order, TOKENS)
    return choices[token_order].astype(jnp.int32)


def setup_inputs(seed: int = 0) -> dict:
    base_key = jax.random.key(seed)
    key_list = jax.random.split(base_key, 8)
    route_ids = lax.map(draw_routes, jax.random.split(key_list[0], LAYERS * DEVICES)).reshape(LAYERS, ROWS, TOP)
    gate_vals = jax.random.uniform(key_list[1], (LAYERS, ROWS, TOP), jnp.float32, 0.25, 0.75) * TOP ** -0.5
    tok_in = jax.random.normal(key_list[2], (ROWS, D), jnp.float32).astype(jnp.bfloat16)
    tok_grad = jax.random.normal(key_list[3], (ROWS, D), jnp.float32).astype(jnp.bfloat16)
    w_dense = (jax.random.normal(key_list[4], (LAYERS, D, D), jnp.float32) * D ** -0.5).astype(jnp.bfloat16)
    w_gate = (jax.random.normal(key_list[5], (LAYERS, EXPERTS, D, FF), jnp.float32) * D ** -0.5).astype(jnp.bfloat16)
    w_up = (jax.random.normal(key_list[6], (LAYERS, EXPERTS, D, FF), jnp.float32) * D ** -0.5).astype(jnp.bfloat16)
    w_down = (jax.random.normal(key_list[7], (LAYERS, EXPERTS, FF, D), jnp.float32) * FF ** -0.5).astype(jnp.bfloat16)
    return {"tok_in": tok_in, "tok_grad": tok_grad, "route_ids": route_ids, "gate_vals": gate_vals, "w_dense": w_dense, "w_gate": w_gate, "w_up": w_up, "w_down": w_down}


def expert_block(mixed_blk, route_blk, gate_blk, gate_f32, up_f32, down_f32):
    flat_ids = route_blk.reshape(TOKENS * TOP)
    expert_hits = (flat_ids[:, None] == jnp.arange(EXPERTS, dtype=jnp.int32)[None, :]).astype(jnp.int32)
    slot_rank = jnp.sum((jnp.cumsum(expert_hits, axis=0) - 1) * expert_hits, axis=1)
    slot_of = flat_ids * CAPACITY + slot_rank
    copy_of = jnp.full((EXPERTS * CAPACITY,), TOKENS * TOP, jnp.int32).at[slot_of].set(jnp.arange(TOKENS * TOP, dtype=jnp.int32))
    padded = jnp.concatenate([mixed_blk, jnp.zeros((1, D), mixed_blk.dtype)], axis=0)
    rows_in = padded[copy_of // TOP].reshape(EXPERTS, CAPACITY, D).astype(jnp.float32)
    act_gate = jnp.einsum("ecd,edf->ecf", rows_in, gate_f32).astype(jnp.bfloat16)
    act_up = jnp.einsum("ecd,edf->ecf", rows_in, up_f32).astype(jnp.bfloat16)
    hidden = (jax.nn.silu(act_gate.astype(jnp.float32)) * act_up.astype(jnp.float32)).astype(jnp.bfloat16)
    rows_out = jnp.einsum("ecf,efd->ecd", hidden.astype(jnp.float32), down_f32).astype(jnp.bfloat16)
    per_copy = rows_out.reshape(EXPERTS * CAPACITY, D)[slot_of].reshape(TOKENS, TOP, D)
    return jnp.sum(gate_blk[:, :, None] * per_copy.astype(jnp.float32), axis=1)


expert_saved = jax.checkpoint(expert_block)


def layer_forward(tok_in, route_ids, gate_vals, dense_f32, gate_f32, up_f32, down_f32):
    mixed_val = (tok_in.astype(jnp.float32) + jnp.dot(tok_in.astype(jnp.float32), dense_f32)).astype(jnp.bfloat16)

    def block_fn(block_args):
        return expert_saved(block_args[0], block_args[1], block_args[2], gate_f32, up_f32, down_f32)

    mix_sum = lax.map(block_fn, (mixed_val.reshape(DEVICES, TOKENS, D), route_ids.reshape(DEVICES, TOKENS, TOP), gate_vals.reshape(DEVICES, TOKENS, TOP)))
    return (mixed_val.astype(jnp.float32) + mix_sum.reshape(ROWS, D)).astype(jnp.bfloat16)


def reference(tok_in, tok_grad, route_ids, gate_vals, w_dense, w_gate, w_up, w_down):
    def forward_all(tok_start, dense_f32, gate_f32, up_f32, down_f32):
        def layer_step(tok_carry, layer_args):
            return layer_forward(tok_carry, layer_args[0], layer_args[1], layer_args[2], layer_args[3], layer_args[4], layer_args[5]), None

        return lax.scan(layer_step, tok_start, (route_ids, gate_vals, dense_f32, gate_f32, up_f32, down_f32))[0]

    tok_out, pull_back = jax.vjp(forward_all, tok_in, w_dense.astype(jnp.float32), w_gate.astype(jnp.float32), w_up.astype(jnp.float32), w_down.astype(jnp.float32))
    grad_in, grad_dense, grad_gate, grad_up, grad_down = pull_back(tok_grad)
    return (tok_out, grad_in, grad_dense.astype(jnp.bfloat16), grad_gate.astype(jnp.bfloat16), grad_up.astype(jnp.bfloat16), grad_down.astype(jnp.bfloat16))
```

```python
import functools

import jax
import jax.numpy as jnp
from jax import lax
from jax.experimental import pallas as pl
from jax.experimental.pallas import tpu as pltpu
from jax.sharding import PartitionSpec as P

TOK_AXES = ("rep", "ep", "dp")
F32 = jnp.float32
BF16 = jnp.bfloat16
LANES = 128
SIDE = 4
WAYS = (1, -1)
BUFS = (0, 1)
LAYERS = (1, 0)
ARRAYS = range(3)
SLOTS = 8
MESH = pl.DeviceIdType.MESH
VMEM_LIMIT = 63 << 20


def dot(a, b):
    return jnp.dot(a, b, preferred_element_type=F32)


def dot_nt(a, b):
    return lax.dot_general(a, b, (((1,), (1,)), ((), ())), preferred_element_type=F32)


def dot_tn(a, b):
    return lax.dot_general(a, b, (((0,), (0,)), ((), ())), preferred_element_type=F32)


class Place:
    def __init__(self):
        self.z, self.y, dp = lax.axis_index("rep"), lax.axis_index("ep"), lax.axis_index("dp")
        self.x, self.c = dp // 2, dp % 2

    def at(self, axis, step):
        z, y, x, c = self.z, self.y, self.x, self.c
        if axis == "z":
            z = (z + step + SIDE) % SIDE
        elif axis == "y":
            y = (y + step + SIDE) % SIDE
        elif axis == "x":
            x = (x + step + SIDE) % SIDE
        else:
            c = 1 - c
        return (z, y, x * 2 + c)


class Copies:
    def __init__(self, place, send, recv):
        self.place, self.send, self.recv, self.made, self.number, self.count = place, send, recv, {}, {}, 0

    def add(self, key, src, dst, axis, step, like=None):
        if like is None:
            n, self.count = self.count, self.count + 1
        else:
            n = self.number[like]
        self.number[key] = n
        self.made[key] = pltpu.make_async_remote_copy(src_ref=src, dst_ref=dst, send_sem=self.send.at[n], recv_sem=self.recv.at[n], device_id=self.place.at(axis, step), device_id_type=MESH)

    def start(self, *keys):
        for key in keys:
            self.made[key].start()

    def arrive(self, *keys):
        for key in keys:
            self.made[key].wait_recv()

    def sent(self, *keys):
        for key in keys:
            self.made[key].wait_send()

    def drain(self):
        for copy in self.made.values():
            copy.wait_send()


def greet(place):
    barrier = pltpu.get_barrier_semaphore()
    peers = [(axis, step) for axis in "xyz" for step in WAYS] + [("c", 0)]
    for axis, step in peers:
        pl.semaphore_signal(barrier, inc=1, device_id=place.at(axis, step), device_id_type=MESH)
    pl.semaphore_wait(barrier, len(peers))


class Gather:
    FROM = {2: -1, 3: 1, 6: 2}
    PASS = {2: 4, 3: 5, 6: 7}

    def __init__(self, layer, copies, place, own, whole):
        self.layer, self.copies, self.place, self.own, self.whole = layer, copies, place, own, whole
        rows, ff = own[0].shape[2], own[2].shape[2]
        self.cut = {"x": ((0, 0, rows // SIDE), (2, 0, ff // 2 // SIDE)), "z": ((1, 0, rows // SIDE), (2, ff // 2, ff // 2 // SIDE))}
        mine = {"x": place.x, "z": place.z}
        for color in ("x", "z"):
            for part in BUFS:
                self._add(("y", 2, color, part), color, part, None, 2, mine[color], None, "y", 1)
                self._add(("y", 3, color, part), color, part, None, 3, mine[color], None, "y", -1)
                if color == "x":
                    self._add(("y", 6, color, part), color, part, 2, 6, mine[color], None, "y", 1)
                else:
                    self._add(("y", 6, color, part), color, part, 3, 6, mine[color], None, "y", -1)
                for slot in (2, 3, 6):
                    for step in WAYS:
                        self._add(("near", slot, color, part, step), color, part, slot, slot, mine[color], None, color, step)
                        behind = (mine[color] - step + SIDE) % SIDE
                        self._add(("far", slot, color, part, step), color, part, slot, slot, behind, (1 - step) // 2, color, step)
        for slot, to in self.PASS.items():
            for array in ARRAYS:
                copies.add((layer, "pass", slot, array), whole[array].at[layer, slot], whole[array].at[layer, to], "c", 0)

    def _view(self, refs, index, color, part, quarter, half):
        array, base, size = self.cut[color][part]
        start = base + quarter * size
        if half is not None:
            size = size // 2
            start = start + half * size
        return refs[array].at[self.layer, index, pl.ds(pl.multiple_of(start, 16), size)]

    def _add(self, key, color, part, src_slot, dst_slot, quarter, half, axis, step):
        src = self._view(self.own, self.place.c, color, part, quarter, half) if src_slot is None else self._view(self.whole, src_slot, color, part, quarter, half)
        self.copies.add((self.layer,) + key, src, self._view(self.whole, dst_slot, color, part, quarter, half), axis, step)

    def _keys(self, *key, extra=()):
        return [(self.layer,) + key + (part,) + extra for part in BUFS]

    def lead(self):
        self.spread(2, "x")
        self.spread(3, "z")

    def lead_onward(self):
        self.onward(2, "x")
        self.onward(3, "z")

    def follow(self):
        self.spread(2, "z")
        self.spread(3, "x")

    def follow_onward(self):
        self.onward(2, "z")
        self.onward(3, "x")

    def last(self):
        self.spread(6, "x")
        self.spread(6, "z")

    def last_onward(self):
        self.onward(6, "x")
        self.onward(6, "z")

    def complete_y(self):
        self.complete(2)
        self.complete(3)

    def complete_last(self):
        self.complete(6)

    def passed_left(self):
        self.passed(2)

    def passed_right(self):
        self.passed(3)

    def passed_last(self):
        self.passed(6)

    def begin(self):
        for slot, color in ((2, "x"), (3, "z"), (2, "z"), (3, "x")):
            self.copies.start(*self._keys("y", slot, color))

    def spread(self, slot, color):
        self.copies.arrive(*self._keys("y", slot, color))
        if (slot, color) in ((2, "x"), (3, "z")):
            self.copies.start(*self._keys("y", 6, color))
        for step in WAYS:
            self.copies.start(*self._keys("near", slot, color, extra=(step,)))

    def onward(self, slot, color):
        for step in WAYS:
            self.copies.arrive(*self._keys("near", slot, color, extra=(step,)))
            self.copies.start(*self._keys("far", slot, color, extra=(step,)))

    def complete(self, slot):
        for color in ("x", "z"):
            for step in WAYS:
                self.copies.arrive(*self._keys("far", slot, color, extra=(step,)))
        self.copies.start(*[(self.layer, "pass", slot, array) for array in ARRAYS])

    def passed(self, slot):
        self.copies.arrive(*[(self.layer, "pass", slot, array) for array in ARRAYS])


GATHER_COPIES = 2 * (2 * 2 * (3 + 3 * 4) + 9)


def route(layer, ids_ref, gate_ref, rank_ref, rank_t_ref, gmat_ref, place):
    tokens = ids_ref.shape[1]
    ids, gates = ids_ref[layer], gate_ref[layer]
    off = ((ids >> 1) - place.y) & (SIDE - 1)
    odd = (ids + place.c) & 1
    slot = jnp.where(off == 0, odd, jnp.where(off == SIDE - 1, 2 + 2 * odd, jnp.where(off == 1, 3 + 2 * odd, 6 + odd)))
    lane = lax.broadcasted_iota(jnp.int32, (tokens, LANES), 1)
    hit0 = slot[:, 0:1] == lane
    hit1 = slot[:, 1:2] == lane
    hit = hit0 | hit1
    gmat_ref[layer] = jnp.where(hit0, gates[:, 0:1], 0.0) + jnp.where(hit1, gates[:, 1:2], 0.0)
    row = lax.broadcasted_iota(jnp.int32, (tokens, tokens), 0)
    col = lax.broadcasted_iota(jnp.int32, (tokens, tokens), 1)
    below = jnp.where(col < row, 1.0, 0.0).astype(BF16)
    rank = jnp.where(hit, dot(below, jnp.where(hit, 1.0, 0.0).astype(BF16)), -1.0)
    rank_ref[layer] = rank.astype(jnp.int32)
    rank_t_ref[layer] = jnp.transpose(rank)[:SLOTS].astype(jnp.int32)


def one_hot(rank_t_ref, layer, slot, rows):
    tokens = rank_t_ref.shape[2]
    place = lax.broadcasted_iota(jnp.int32, (rows, tokens), 0)
    return jnp.where(rank_t_ref[layer, pl.ds(slot, 1), :] == place, 1.0, 0.0).astype(BF16)


def column(ref, layer, slot, zero):
    tokens = ref.shape[1]
    lane = lax.broadcasted_iota(jnp.int32, (tokens, LANES), 1)
    return jnp.sum(jnp.where(lane == slot, ref[layer], zero), axis=1, keepdims=True)


def one_hot_t(rank_ref, layer, slot, rows):
    tokens = rank_ref.shape[1]
    place = lax.broadcasted_iota(jnp.int32, (tokens, rows), 1)
    return jnp.where(column(rank_ref, layer, slot, jnp.int32(0)) == place, 1.0, 0.0).astype(BF16)


def fwd_kernel(cap, x_ref, ids_ref, gate_ref, wd_ref, o1_ref, o3_ref, o2_ref, y_ref, x1_ref, rank_ref, rank_t_ref, gmat_ref, g1_ref, g3_ref, g2_ref, z_ref, a_ref, b_ref, u_ref, acc_ref, b1_ref, b3_ref, b2_ref, load_sem, keep_sem, send_sem, recv_sem):
    s = pl.program_id(0)
    steps = pl.num_programs(0)
    layer, slot = s // SLOTS, s % SLOTS
    place = Place()
    copies = Copies(place, send_sem, recv_sem)
    own, whole, bufs = (o1_ref, o3_ref, o2_ref), (g1_ref, g3_ref, g2_ref), (b1_ref, b3_ref, b2_ref)
    g0, g1 = (Gather(l, copies, place, own, whole) for l in BUFS)

    def at(step, body):
        pl.when(s == step)(body)

    def loads(step, mine):
        l, k = step // SLOTS, step % SLOTS
        for n in ARRAYS:
            src = own[n].at[l, (place.c + k) % 2] if mine else whole[n].at[l, k]
            yield pltpu.make_async_copy(src, bufs[n].at[step % 2], load_sem.at[step % 2, n])

    def keeps(step):
        for n in ARRAYS:
            yield pltpu.make_async_copy(bufs[n].at[step % 2], whole[n].at[step // SLOTS, step % SLOTS], keep_sem.at[step % 2, n])

    def load(step):
        k = step % SLOTS

        @pl.when(k < 2)
        def _():
            for copy in loads(step, True):
                copy.start()

        @pl.when(k >= 2)
        def _():
            for copy in loads(step, False):
                copy.start()

    @pl.when(s == 0)
    def _():
        load(0)
        greet(place)
        g0.begin()
        for l in BUFS:
            route(l, ids_ref, gate_ref, rank_ref, rank_t_ref, gmat_ref, place)
        g0.lead()
        load(1)

    plan = [
        [],
        [g0.follow],
        [g0.lead_onward, g0.last, g1.begin, g0.follow_onward, g0.complete_y, lambda: load(s), g0.last_onward],
        [g0.passed_left],
        [g1.lead, g0.complete_last, g0.passed_right],
        [g1.follow],
        [g1.lead_onward, g0.passed_last],
        [g1.last],
        [g1.follow_onward],
        [g1.complete_y, g1.last_onward],
        [],
        [g1.passed_left],
        [g1.complete_last, g1.passed_right],
        [],
        [g1.passed_last],
    ]
    for step, parts in enumerate(plan):

        @pl.when(s == step)
        def _(parts=parts):
            for part in parts:
                part()

    for copy in loads(s, False):
        copy.wait()

    @pl.when((s > 0) & (s != 1) & (s < steps - 1))
    def _():
        load(s + 1)

    @pl.when(slot < 2)
    def _():
        for copy in keeps(s):
            copy.start()

    def enter(x):
        u_ref[...] = (x.astype(F32) + dot(x, wd_ref[layer])).astype(BF16)
        acc_ref[...] = jnp.zeros_like(acc_ref)

    at(0, lambda: enter(x_ref[...]))
    at(SLOTS, lambda: enter(x1_ref[...]))

    buf = s % 2
    z = dot(one_hot(rank_t_ref, layer, slot, cap), u_ref[...]).astype(BF16)
    z_ref[0, 0] = z
    a = dot(z, b1_ref[buf]).astype(BF16)
    b = dot(z, b3_ref[buf]).astype(BF16)
    a_ref[0, 0] = a
    b_ref[0, 0] = b
    h = (jax.nn.silu(a.astype(F32)) * b.astype(F32)).astype(BF16)
    o = dot(h, b2_ref[buf]).astype(BF16)
    acc_ref[...] += column(gmat_ref, layer, slot, 0.0) * dot(one_hot_t(rank_ref, layer, slot, cap), o)

    def leave(out_ref):
        out_ref[...] = (u_ref[...].astype(F32) + acc_ref[...]).astype(BF16)

    @pl.when(slot < 2)
    def _():
        for copy in keeps(s):
            copy.wait()

    at(SLOTS - 1, lambda: leave(x1_ref))

    @pl.when(s == steps - 1)
    def _():
        leave(y_ref)
        copies.drain()


def forward(cap, x, ids, gates, wd, w1, w3, w2):
    tokens, width = x.shape
    layers, _, ff = ids.shape[0], None, w1.shape[3]
    vmem = pl.BlockSpec(memory_space=pltpu.VMEM)
    hbm = pl.BlockSpec(memory_space=pl.ANY)

    def saved(n):
        return pl.BlockSpec((1, 1, cap, n), lambda s: (s // SLOTS, s % SLOTS, 0, 0))

    shape = jax.ShapeDtypeStruct
    return pl.pallas_call(
        functools.partial(fwd_kernel, cap),
        grid=(layers * SLOTS,),
        in_specs=[vmem] * 4 + [hbm] * 3,
        out_specs=[vmem] * 5 + [hbm] * 3 + [saved(width), saved(ff), saved(ff)],
        out_shape=[
            shape((tokens, width), BF16),
            shape((tokens, width), BF16),
            shape((layers, tokens, LANES), jnp.int32),
            shape((layers, SLOTS, tokens), jnp.int32),
            shape((layers, tokens, LANES), F32),
            shape((layers, SLOTS, width, ff), BF16),
            shape((layers, SLOTS, width, ff), BF16),
            shape((layers, SLOTS, ff, width), BF16),
            shape((layers, SLOTS, cap, width), BF16),
            shape((layers, SLOTS, cap, ff), BF16),
            shape((layers, SLOTS, cap, ff), BF16),
        ],
        scratch_shapes=[
            pltpu.VMEM((tokens, width), BF16),
            pltpu.VMEM((tokens, width), F32),
            pltpu.VMEM((2, width, ff), BF16),
            pltpu.VMEM((2, width, ff), BF16),
            pltpu.VMEM((2, ff, width), BF16),
            pltpu.SemaphoreType.DMA((2, 3)),
            pltpu.SemaphoreType.DMA((2, 3)),
            pltpu.SemaphoreType.DMA((GATHER_COPIES,)),
            pltpu.SemaphoreType.DMA((GATHER_COPIES,)),
        ],
        compiler_params=pltpu.CompilerParams(vmem_limit_bytes=VMEM_LIMIT, collective_id=0, has_side_effects=True),
        name="forward",
    )(x, ids, gates, wd, w1, w3, w2)


def add_to(dst, src):
    dst[...] = (dst[...].astype(F32) + src[...].astype(F32)).astype(BF16)


class RingSum:
    def __init__(self, copies, name, axis, block, first, second):
        self.copies, self.name, self.block, self.first, self.second = copies, name, block, first, second
        self.early, self.later = ([(name, when, step) for step in WAYS] for when in ("early", "later"))
        for half, step in enumerate(WAYS):
            copies.add(self.early[half], block(2, half), first.at[half], axis, step)
            copies.add(self.later[half], block(step, None), second.at[half], axis, step)

    def start(self):
        self.copies.start(*self.early)

    def onward(self):
        self.copies.arrive(*self.early)
        for half, step in enumerate(WAYS):
            add_to(self.block(step, half), self.first.at[half])
        self.copies.start(*self.later)

    def finish(self, out):
        self.copies.arrive(*self.later)
        out[...] = (self.block(0, None)[...].astype(F32) + self.second[0].astype(F32) + self.second[1].astype(F32)).astype(BF16)
        self.copies.sent(*self.early, *self.later)


class RingSpread:
    def __init__(self, copies, name, axis, me, block, source=None, like=None):
        self.copies = copies
        self.near, self.far = ([(name, when, step) for step in WAYS] for when in ("near", "far"))
        for half, step in enumerate(WAYS):
            behind = (me - step + SIDE) % SIDE
            near, far = (None, None) if like is None else (like.near[half], like.far[half])
            copies.add(self.near[half], block(me, None) if source is None else source, block(me, None), axis, step, near)
            copies.add(self.far[half], block(behind, half), block(behind, half), axis, step, far)

    def start(self):
        self.copies.start(*self.near)

    def onward(self):
        for near, far in zip(self.near, self.far):
            self.copies.arrive(near)
            self.copies.start(far)

    def finish(self):
        self.copies.arrive(*self.far)
        self.copies.sent(*self.near, *self.far)


def slices(ref, lead, base, size):
    def block(index, half):
        start, rows = base + index * size, size
        if half is not None:
            rows = size // 2
            start = start + half * rows
        return ref.at[(*lead, pl.ds(pl.multiple_of(start, 16), rows))]

    return block


def slabs(ref):
    def block(index, half):
        if half is None:
            return ref.at[index]
        rows = ref.shape[1] // 2
        return ref.at[index, pl.ds(half * rows, rows)]

    return block


def total(ref):
    return (ref[0].astype(F32) + ref[1].astype(F32) + ref[2].astype(F32) + ref[3].astype(F32)).astype(BF16)


OWN_STEPS = {1: 0, 4: 1, 5: 2, 7: 3}
REDUCE_COPIES = 107


def bwd_kernel(cap, dy_ref, x0_ref, x1_ref, wd_ref, rank_ref, rank_t_ref, gmat_ref, w1_ref, w3_ref, w2_ref, z_ref, a_ref, b_ref, dx_ref, gd_ref, g1_ref, g3_ref, g2_ref, acc_ref, cur_ref, m1_ref, m3_ref, m2_ref, d1_ref, d3_ref, d2_ref, s1_ref, s3_ref, s2_ref, r11_ref, r12_ref, r31_ref, r32_ref, t1_ref, t3_ref, y11_ref, y12_ref, y31_ref, y32_ref, y21_ref, y22_ref, u1_ref, u2_ref, l1_ref, l2_ref, c1_ref, c3_ref, cu_ref, cl_ref, f1_ref, f3_ref, fu_ref, fl_ref, dp_ref, dr_ref, dcx_ref, dcy_ref, dcz_ref, ds_ref, de_ref, put_sem, send_sem, recv_sem, credit):
    s = pl.program_id(0)
    steps = pl.num_programs(0)
    layer, slot, t = 1 - s // SLOTS, SLOTS - 1 - s % SLOTS, s % SLOTS
    group = t // 4 + t // 5 + t // 7
    into = (t // 2 + t // 3) % 2
    place = Place()
    copies = Copies(place, send_sem, recv_sem)
    rows, ff = s1_ref.shape[1], s2_ref.shape[1]
    quarter, part = rows // SIDE, ff // 2 // SIDE
    half_d = rows // 2

    stage, mate, own = (m1_ref, m3_ref, m2_ref), (d1_ref, d3_ref, d2_ref), (s1_ref, s3_ref, s2_ref)
    outs = (g1_ref, g3_ref, g2_ref)
    for buf in BUFS:
        for n in ARRAYS:
            copies.add(("pair", buf, n), stage[n], mate[n].at[buf], "c", 0)

    def ring_blocks(ref, q, me, base, size):
        block = slices(ref, (q,), base, size)
        return lambda offset, half: block((me + offset + SIDE) % SIDE, half)

    def group_blocks(ref):
        block = slabs(ref)
        return lambda offset, half: block({2: 0, 1: 1, -1: 2, 0: 3}[offset], half)

    first = {
        "x": [RingSum(copies, ("x", q), "x", ring_blocks(s1_ref, q, place.x, 0, quarter), r11_ref.at[q], r12_ref.at[q]) for q in range(SIDE)],
        "z": [RingSum(copies, ("z", q), "z", ring_blocks(s3_ref, q, place.z, 0, quarter), r31_ref.at[q], r32_ref.at[q]) for q in range(SIDE)],
    }
    mid = {"x": t1_ref, "z": t3_ref}
    on_y = {
        "x": RingSum(copies, "yx", "y", group_blocks(t1_ref), y11_ref, y12_ref),
        "z": RingSum(copies, "yz", "y", group_blocks(t3_ref), y31_ref, y32_ref),
        "w": RingSum(copies, "yw", "y", group_blocks(s2_ref), y21_ref, y22_ref),
    }
    inner = {
        "u": RingSum(copies, "u", "x", ring_blocks(s2_ref, 3, place.x, 0, part), u1_ref, u2_ref),
        "l": RingSum(copies, "l", "z", ring_blocks(s2_ref, 3, place.z, ff // 2, part), l1_ref, l2_ref),
    }
    ring_of = {"x": ("x", place.x), "u": ("x", place.x), "z": ("z", place.z), "l": ("z", place.z)}
    other_of = {"x": ("z", place.z), "u": ("z", place.z), "z": ("x", place.x), "l": ("x", place.x)}
    cross_ref = {"x": c1_ref, "z": c3_ref, "u": cu_ref, "l": cl_ref}
    done_ref = {"x": f1_ref, "z": f3_ref, "u": fu_ref, "l": fl_ref}
    out_of = {"x": (g1_ref, 0, quarter), "z": (g3_ref, 0, quarter), "u": (g2_ref, 0, part), "l": (g2_ref, ff // 2, part)}
    cross, final, puts = {}, {}, {}
    for i, k in enumerate(out_of):
        cross[k] = RingSpread(copies, ("cross", k), *other_of[k], slabs(cross_ref[k]))
        ref, base, size = out_of[k]
        for late in LAYERS:
            block = slices(ref, (late, place.c), base, size)
            final[k, late] = RingSpread(copies, ("final", k, late), *ring_of[k], block, source=done_ref[k], like=final.get((k, 1)))
            puts[k, late] = pltpu.make_async_copy(done_ref[k], block(ring_of[k][1], None), put_sem.at[i])
    mine, theirs = (pl.ds(pl.multiple_of(c * half_d, 16), half_d) for c in (place.c, 1 - place.c))
    for late in LAYERS:
        for n, out in enumerate(outs):
            copies.add(("pass", n, late), out.at[late, place.c], out.at[late, place.c], "c", 0, None if late else ("pass", n, 1))
    copies.add("dense pair", dp_ref.at[theirs], dr_ref, "c", 0)
    copies.add("dense pass", ds_ref, de_ref, "c", 0)
    dense_refs = {"y": dcy_ref, "x": dcx_ref, "z": dcz_ref}
    index_of = {"y": place.y, "x": place.x, "z": place.z}
    dense = {k: RingSpread(copies, ("dense", k), k, index_of[k], slabs(ref)) for k, ref in dense_refs.items()}

    def reduce_start(q):
        for k in ("x", "z"):
            first[k][q].start()

    def reduce_onward(q):
        for k in ("x", "z"):
            first[k][q].onward()

    def reduce_finish(q):
        for k in ("x", "z"):
            first[k][q].finish(mid[k].at[q])

    def y_start():
        for k in ("x", "z"):
            on_y[k].start()

    def y_onward():
        for k in ("x", "z"):
            on_y[k].onward()

    def y_finish():
        for k in ("x", "z"):
            on_y[k].finish(cross_ref[k].at[other_of[k][1]])
            cross[k].start()

    def w_finish():
        on_y["w"].finish(s2_ref.at[3])
        for k in ("u", "l"):
            inner[k].start()

    def inner_onward():
        for k in ("u", "l"):
            inner[k].onward()

    def inner_finish():
        for k in ("u", "l"):
            inner[k].finish(cross_ref[k].at[other_of[k][1]])
            cross[k].start()

    def cross_onward(*keys):
        for k in keys:
            cross[k].onward()

    def cross_finish(late, *keys):
        for k in keys:
            cross[k].finish()
            done_ref[k][...] = total(cross_ref[k])
            puts[k, late].start()
            final[k, late].start()

    def final_onward(late, *keys):
        for k in keys:
            final[k, late].onward()

    def final_finish(late, *keys):
        for k in keys:
            final[k, late].finish()
            puts[k, late].wait()
        copies.start(*[("pass", n, late) for n in ((0, 1) if "x" in keys else (2,))])

    def pass_finish(late):
        keys = [("pass", n, late) for n in ARRAYS]
        copies.arrive(*keys)
        copies.sent(*keys)

    def dense_sum():
        copies.arrive("dense pair")
        dcy_ref[place.y] = (dp_ref[mine].astype(F32) + dr_ref[...].astype(F32)).astype(BF16)
        copies.sent("dense pair")
        dense["y"].start()

    def dense_next(k, follow):
        dense[k].finish()
        dense_refs[follow][index_of[follow]] = total(dense_refs[k])
        dense[follow].start()

    def dense_pass(late):
        dense["z"].finish()
        ds_ref[...] = total(dcz_ref)
        gd_ref[late, mine] = ds_ref[...]
        copies.start("dense pass")

    def dense_finish(late):
        copies.arrive("dense pass")
        gd_ref[late, theirs] = de_ref[...]
        copies.sent("dense pass")

    spread = [
        lambda: (copies.start("dense pair"), reduce_onward(3), w_finish()),
        lambda: (dense_sum(), reduce_finish(3), y_finish(), inner_onward()),
        lambda: (inner_finish(), cross_onward("x", "z"), dense["y"].onward()),
        lambda: (cross_finish(1, "x", "z"), cross_onward("u", "l"), dense_next("y", "x")),
        lambda: (final_onward(1, "x", "z"), cross_finish(1, "u", "l"), dense["x"].onward()),
        lambda: (final_finish(1, "x", "z"), final_onward(1, "u", "l"), dense_next("x", "z")),
        lambda: (final_finish(1, "u", "l"), dense["z"].onward()),
        lambda: (pass_finish(1), dense_pass(1)),
    ]

    def ending():
        dense_finish(1)
        copies.start("dense pair")
        w_finish()
        reduce_onward(3)
        dense_sum()
        inner_onward()
        reduce_finish(3)
        y_finish()
        dense["y"].onward()
        inner_finish()
        cross_onward("x", "z")
        dense_next("y", "x")
        cross_onward("u", "l")
        cross_finish(0, "x", "z")
        dense["x"].onward()
        cross_finish(0, "u", "l")
        final_onward(0, "x", "z")
        dense_next("x", "z")
        final_onward(0, "u", "l")
        final_finish(0, "x", "z")
        dense["z"].onward()
        final_finish(0, "u", "l")
        dense_pass(0)
        pass_finish(0)
        dense_finish(0)

    def at(step, body):
        pl.when(s == step)(lambda: body() and None)

    def each(step, body):
        pl.when(t == step)(lambda: body() and None)

    def load_grad(x):
        acc_ref[...] = x.astype(F32)
        cur_ref[...] = x

    @pl.when(s == 0)
    def _():
        greet(place)
        load_grad(dy_ref[...])

    for step, body in enumerate(spread):
        at(step + SLOTS, body)
    each(2, lambda: reduce_onward(0))
    each(3, lambda: (reduce_finish(0), y_start()))
    each(5, lambda: reduce_onward(1))
    each(6, lambda: (reduce_onward(2), reduce_finish(1), on_y["w"].onward()))
    each(7, lambda: (reduce_finish(2), y_onward()))

    grad_gated = (column(gmat_ref, layer, slot, 0.0) * cur_ref[...].astype(F32)).astype(BF16)
    do = dot(one_hot(rank_t_ref, layer, slot, cap), grad_gated).astype(BF16)
    dh = dot_nt(do, w2_ref[0, 0])
    a = a_ref[0, 0].astype(F32)
    b = b_ref[0, 0].astype(F32)
    sig = jax.nn.sigmoid(a)
    act = a * sig
    h = (act * b).astype(BF16)
    db = (dh * act).astype(BF16)
    da = (dh * b * sig * (1.0 + a * (1.0 - sig))).astype(BF16)
    z = z_ref[0, 0]
    dz = (dot_nt(da, w1_ref[0, 0]) + dot_nt(db, w3_ref[0, 0])).astype(BF16)
    acc_ref[...] += dot(one_hot_t(rank_ref, layer, slot, cap), dz)

    def weight_grads():
        return dot_tn(z, da), dot_tn(z, db), dot_tn(h, do)

    is_own = functools.reduce(jnp.logical_or, [t == step for step in OWN_STEPS])

    @pl.when(jnp.logical_not(is_own))
    def _():
        for buf in BUFS:
            pl.when((s > 0) & (into == 1 - buf))(lambda buf=buf: copies.sent(*[("pair", buf, n) for n in ARRAYS]))

        for ref, grad in zip(stage, weight_grads()):
            ref[...] = grad.astype(BF16)

        pl.when(s >= 3)(lambda: pl.semaphore_wait(credit.at[into], 1))
        for buf in BUFS:
            pl.when(into == buf)(lambda buf=buf: copies.start(*[("pair", buf, n) for n in ARRAYS]))

    @pl.when(is_own)
    def _():
        for buf in BUFS:
            pl.when(group % 2 == buf)(lambda buf=buf: copies.arrive(*[("pair", buf, n) for n in ARRAYS]))

        for ref, add, grad in zip(own, mate, weight_grads()):
            ref[group] = (grad + add[group % 2].astype(F32)).astype(BF16)

        @pl.when(s < 13)
        def _():
            pl.semaphore_signal(credit.at[group % 2], inc=1, device_id=place.at("c", 0), device_id_type=MESH)

    def leave(x, out_ref):
        grad = acc_ref[...]
        grad_b = grad.astype(BF16)
        dp_ref[...] = dot_tn(x, grad_b).astype(BF16)
        out_ref[...] = (grad + dot_nt(grad_b, wd_ref[layer])).astype(BF16)

    for step, q in OWN_STEPS.items():
        each(step, lambda q=q: reduce_start(q))
    each(1, lambda: on_y["w"].start())

    @pl.when(s == SLOTS - 1)
    def _():
        leave(x1_ref[...], cur_ref)
        acc_ref[...] = cur_ref[...].astype(F32)

    @pl.when(s == steps - 1)
    def _():
        leave(x0_ref[...], dx_ref)
        ending()
        copies.sent(*[("pair", 1, n) for n in ARRAYS])


def backward(cap, dy, x0, x1, wd, rank, rank_t, gmat, w1, w3, w2, z, a, b):
    tokens, width = dy.shape
    layers, ff = w1.shape[0], w1.shape[3]
    local, quarter, part = SLOTS // SIDE, width // SIDE, ff // 2 // SIDE
    hbm = pl.BlockSpec(memory_space=pl.ANY)

    def fixed(shape):
        return pl.BlockSpec(shape, lambda s: (0,) * len(shape), pipeline_mode=pl.Buffered(1))

    def stream(*shape):
        return pl.BlockSpec((1, 1, *shape), lambda s: (1 - s // SLOTS, SLOTS - 1 - s % SLOTS, 0, 0))

    def buf(*shape):
        return pltpu.VMEM(shape, BF16)

    shape = jax.ShapeDtypeStruct
    ups, downs = [(width, ff), (width, ff), (ff, width)], [(quarter, ff), (part, width)]
    scratch = [pltpu.VMEM((tokens, width), F32), buf(tokens, width)]
    scratch += [buf(*u) for u in ups] + [buf(2, *u) for u in ups] + [buf(SIDE, *u) for u in ups]
    scratch += [buf(SIDE, 2, quarter // 2, ff), buf(SIDE, 2, quarter, ff)] * 2
    scratch += [buf(SIDE, quarter, ff)] * 2
    scratch += [buf(2, quarter // 2, ff), buf(2, quarter, ff)] * 2 + [buf(2, ff // 2, width), buf(2, ff, width)]
    scratch += [buf(2, part // 2, width), buf(2, part, width)] * 2
    scratch += [buf(SIDE, quarter, ff)] * 2 + [buf(SIDE, part, width)] * 2
    scratch += [buf(quarter, ff)] * 2 + [buf(part, width)] * 2
    scratch += [buf(width, width), buf(width // 2, width)] + [buf(SIDE, width // 2, width)] * 3 + [buf(width // 2, width)] * 2
    scratch += [pltpu.SemaphoreType.DMA((4,)), pltpu.SemaphoreType.DMA((REDUCE_COPIES,)), pltpu.SemaphoreType.DMA((REDUCE_COPIES,)), pltpu.SemaphoreType.REGULAR((2,))]
    return pl.pallas_call(
        functools.partial(bwd_kernel, cap),
        grid=(layers * SLOTS,),
        in_specs=[fixed(v.shape) for v in (dy, x0, x1, wd, rank, rank_t, gmat)] + [stream(*u) for u in ups] + [stream(cap, width), stream(cap, ff), stream(cap, ff)],
        out_specs=[fixed((tokens, width)), fixed((layers, width, width))] + [hbm] * 3,
        out_shape=[shape((tokens, width), BF16), shape((layers, width, width), BF16)] + [shape((layers, local, *u), BF16) for u in ups],
        scratch_shapes=scratch,
        compiler_params=pltpu.CompilerParams(vmem_limit_bytes=VMEM_LIMIT, collective_id=1, has_side_effects=True),
        name="backward",
    )(dy, x0, x1, wd, rank, rank_t, gmat, w1, w3, w2, z, a, b)


def solution(mesh):
    tok_spec = P(TOK_AXES, None)
    route_spec = P(None, TOK_AXES, None)
    expert_spec = P(None, "ep", None, None)
    whole_spec = P(None, None, None)

    def device_step(tok_in, tok_grad, route_ids, gate_vals, w_dense, w_gate, w_up, w_down):
        tokens, top_k = route_ids.shape[1:]
        cap = 2 * tokens * top_k // SLOTS
        y, x1, *kept = forward(cap, tok_in, route_ids, gate_vals, w_dense, w_gate, w_up, w_down)
        return (y, *backward(cap, tok_grad, tok_in, x1, w_dense, *kept))

    return jax.shard_map(device_step, mesh=mesh, in_specs=(tok_spec, tok_spec, route_spec, route_spec, whole_spec, expert_spec, expert_spec, expert_spec), out_specs=(tok_spec, tok_spec, whole_spec, expert_spec, expert_spec, expert_spec), check_vma=False)
```

```python
import functools

import jax
import jax.numpy as jnp
from jax import lax
from jax.experimental import pallas as pl
from jax.experimental.pallas import tpu as pltpu
from jax.sharding import PartitionSpec as P

TOK_AXES = ("rep", "ep", "dp")
F32 = jnp.float32
BF16 = jnp.bfloat16
LANES = 128
SIDE = 4
WAYS = (1, -1)
BUFS = (0, 1)
LAYERS = (1, 0)
ARRAYS = range(3)
SLOTS = 8
MESH = pl.DeviceIdType.MESH
VMEM_LIMIT = 63 << 20


def dot(a, b):
    return jnp.dot(a, b, preferred_element_type=F32)


def dot_nt(a, b):
    return lax.dot_general(a, b, (((1,), (1,)), ((), ())), preferred_element_type=F32)


def dot_tn(a, b):
    return lax.dot_general(a, b, (((0,), (0,)), ((), ())), preferred_element_type=F32)


class Place:
    def __init__(self):
        self.z, self.y, dp = lax.axis_index("rep"), lax.axis_index("ep"), lax.axis_index("dp")
        self.x, self.c = dp // 2, dp % 2

    def at(self, axis, step):
        z, y, x, c = self.z, self.y, self.x, self.c
        if axis == "z":
            z = (z + step + SIDE) % SIDE
        elif axis == "y":
            y = (y + step + SIDE) % SIDE
        elif axis == "x":
            x = (x + step + SIDE) % SIDE
        else:
            c = 1 - c
        return (z, y, x * 2 + c)


class Copies:
    def __init__(self, place, send, recv):
        self.place, self.send, self.recv, self.made, self.number, self.count = place, send, recv, {}, {}, 0

    def add(self, key, src, dst, axis, step, like=None):
        if like is None:
            n, self.count = self.count, self.count + 1
        else:
            n = self.number[like]
        self.number[key] = n
        self.made[key] = pltpu.make_async_remote_copy(src_ref=src, dst_ref=dst, send_sem=self.send.at[n], recv_sem=self.recv.at[n], device_id=self.place.at(axis, step), device_id_type=MESH)

    def start(self, *keys):
        for key in keys:
            self.made[key].start()

    def arrive(self, *keys):
        for key in keys:
            self.made[key].wait_recv()

    def sent(self, *keys):
        for key in keys:
            self.made[key].wait_send()

    def drain(self):
        for copy in self.made.values():
            copy.wait_send()


def greet(place):
    barrier = pltpu.get_barrier_semaphore()
    peers = [(axis, step) for axis in "xyz" for step in WAYS] + [("c", 0)]
    for axis, step in peers:
        pl.semaphore_signal(barrier, inc=1, device_id=place.at(axis, step), device_id_type=MESH)
    pl.semaphore_wait(barrier, len(peers))


class Gather:
    FROM = {2: -1, 3: 1, 6: 2}
    PASS = {2: 4, 3: 5, 6: 7}

    def __init__(self, layer, copies, place, own, whole):
        self.layer, self.copies, self.place, self.own, self.whole = layer, copies, place, own, whole
        rows, ff = own[0].shape[2], own[2].shape[2]
        self.cut = {"x": ((0, 0, rows // SIDE), (2, 0, ff // 2 // SIDE)), "z": ((1, 0, rows // SIDE), (2, ff // 2, ff // 2 // SIDE))}
        mine = {"x": place.x, "z": place.z}
        for color in ("x", "z"):
            for part in BUFS:
                self._add(("y", 2, color, part), color, part, None, 2, mine[color], None, "y", 1)
                self._add(("y", 3, color, part), color, part, None, 3, mine[color], None, "y", -1)
                if color == "x":
                    self._add(("y", 6, color, part), color, part, 2, 6, mine[color], None, "y", 1)
                else:
                    self._add(("y", 6, color, part), color, part, 3, 6, mine[color], None, "y", -1)
                for slot in (2, 3, 6):
                    for step in WAYS:
                        self._add(("near", slot, color, part, step), color, part, slot, slot, mine[color], None, color, step)
                        behind = (mine[color] - step + SIDE) % SIDE
                        self._add(("far", slot, color, part, step), color, part, slot, slot, behind, (1 - step) // 2, color, step)
        for slot, to in self.PASS.items():
            for array in ARRAYS:
                copies.add((layer, "pass", slot, array), whole[array].at[layer, slot], whole[array].at[layer, to], "c", 0)

    def _view(self, refs, index, color, part, quarter, half):
        array, base, size = self.cut[color][part]
        start = base + quarter * size
        if half is not None:
            size = size // 2
            start = start + half * size
        return refs[array].at[self.layer, index, pl.ds(pl.multiple_of(start, 16), size)]

    def _add(self, key, color, part, src_slot, dst_slot, quarter, half, axis, step):
        src = self._view(self.own, self.place.c, color, part, quarter, half) if src_slot is None else self._view(self.whole, src_slot, color, part, quarter, half)
        self.copies.add((self.layer,) + key, src, self._view(self.whole, dst_slot, color, part, quarter, half), axis, step)

    def _keys(self, *key, extra=()):
        return [(self.layer,) + key + (part,) + extra for part in BUFS]

    def lead(self):
        self.spread(2, "x")
        self.spread(3, "z")

    def lead_onward(self):
        self.onward(2, "x")
        self.onward(3, "z")

    def follow(self):
        self.spread(2, "z")
        self.spread(3, "x")

    def follow_onward(self):
        self.onward(2, "z")
        self.onward(3, "x")

    def last(self):
        self.spread(6, "x")
        self.spread(6, "z")

    def last_onward(self):
        self.onward(6, "x")
        self.onward(6, "z")

    def complete_y(self):
        self.complete(2)
        self.complete(3)

    def complete_last(self):
        self.complete(6)

    def passed_left(self):
        self.passed(2)

    def passed_right(self):
        self.passed(3)

    def passed_last(self):
        self.passed(6)

    def begin(self):
        for slot, color in ((2, "x"), (3, "z"), (2, "z"), (3, "x")):
            self.copies.start(*self._keys("y", slot, color))

    def spread(self, slot, color):
        self.copies.arrive(*self._keys("y", slot, color))
        if (slot, color) in ((2, "x"), (3, "z")):
            self.copies.start(*self._keys("y", 6, color))
        for step in WAYS:
            self.copies.start(*self._keys("near", slot, color, extra=(step,)))

    def onward(self, slot, color):
        for step in WAYS:
            self.copies.arrive(*self._keys("near", slot, color, extra=(step,)))
            self.copies.start(*self._keys("far", slot, color, extra=(step,)))

    def complete(self, slot):
        for color in ("x", "z"):
            for step in WAYS:
                self.copies.arrive(*self._keys("far", slot, color, extra=(step,)))
        self.copies.start(*[(self.layer, "pass", slot, array) for array in ARRAYS])

    def passed(self, slot):
        self.copies.arrive(*[(self.layer, "pass", slot, array) for array in ARRAYS])


GATHER_COPIES = 2 * (2 * 2 * (3 + 3 * 4) + 9)


def route(ids_ref, gate_ref, rank_ref, rank_t_ref, gmat_ref, place):
    layers, _, tokens = ids_ref.shape
    below = lax.broadcasted_iota(jnp.int32, (tokens, tokens), 0) < lax.broadcasted_iota(jnp.int32, (tokens, tokens), 1)
    below = jnp.where(below, 1.0, 0.0).astype(BF16)
    lead = lax.broadcasted_iota(jnp.int32, (LANES, tokens), 0)
    for layer in range(layers):
        ids, gates = ids_ref[layer], gate_ref[layer]
        off = ((ids >> 1) - place.y) & (SIDE - 1)
        odd = (ids + place.c) & 1
        slot = jnp.where(off == 0, odd, jnp.where(off == SIDE - 1, 2 + 2 * odd, jnp.where(off == 1, 3 + 2 * odd, 6 + odd)))
        hits = [slot[n : n + 1] == lead for n in BUFS]
        hit = hits[0] | hits[1]
        weight = jnp.where(hits[0], gates[0:1], 0.0) + jnp.where(hits[1], gates[1:2], 0.0)
        count = dot(jnp.where(hit, 1.0, 0.0)[: 2 * SLOTS].astype(BF16), below)
        rank = jnp.where(hit, jnp.concatenate([count, jnp.zeros((LANES - 2 * SLOTS, tokens), F32)], axis=0), -1.0)
        rank_t_ref[layer] = rank[:SLOTS].astype(jnp.int32)
        rank_ref[layer] = jnp.transpose(rank).astype(jnp.int32)
        gmat_ref[layer] = jnp.transpose(weight)


def one_hot(rank_t_ref, layer, slot, rows):
    tokens = rank_t_ref.shape[2]
    place = lax.broadcasted_iota(jnp.int32, (rows, tokens), 0)
    return jnp.where(rank_t_ref[layer, pl.ds(slot, 1), :] == place, 1.0, 0.0).astype(BF16)


def column(ref, layer, slot, zero):
    tokens = ref.shape[1]
    lane = lax.broadcasted_iota(jnp.int32, (tokens, LANES), 1)
    return jnp.sum(jnp.where(lane == slot, ref[layer], zero), axis=1, keepdims=True)


def one_hot_t(rank_ref, layer, slot, rows):
    tokens = rank_ref.shape[1]
    place = lax.broadcasted_iota(jnp.int32, (tokens, rows), 1)
    return jnp.where(column(rank_ref, layer, slot, jnp.int32(0)) == place, 1.0, 0.0).astype(BF16)


def fwd_kernel(cap, x_ref, ids_ref, gate_ref, wd_ref, o1_ref, o3_ref, o2_ref, y_ref, x1_ref, rank_ref, rank_t_ref, gmat_ref, g1_ref, g3_ref, g2_ref, z_ref, a_ref, b_ref, u_ref, acc_ref, b1_ref, b3_ref, b2_ref, load_sem, keep_sem, send_sem, recv_sem):
    s = pl.program_id(0)
    steps = pl.num_programs(0)
    layer, slot = s // SLOTS, s % SLOTS
    place = Place()
    copies = Copies(place, send_sem, recv_sem)
    own, whole, bufs = (o1_ref, o3_ref, o2_ref), (g1_ref, g3_ref, g2_ref), (b1_ref, b3_ref, b2_ref)
    g0, g1 = (Gather(l, copies, place, own, whole) for l in BUFS)

    def at(step, body):
        pl.when(s == step)(body)

    def loads(step, mine):
        l, k = step // SLOTS, step % SLOTS
        for n in ARRAYS:
            src = own[n].at[l, (place.c + k) % 2] if mine else whole[n].at[l, k]
            yield pltpu.make_async_copy(src, bufs[n].at[step % 2], load_sem.at[step % 2, n])

    def keeps(step):
        for n in ARRAYS:
            yield pltpu.make_async_copy(bufs[n].at[step % 2], whole[n].at[step // SLOTS, step % SLOTS], keep_sem.at[step % 2, n])

    def load(step):
        k = step % SLOTS

        @pl.when(k < 2)
        def _():
            for copy in loads(step, True):
                copy.start()

        @pl.when(k >= 2)
        def _():
            for copy in loads(step, False):
                copy.start()

    @pl.when(s == 0)
    def _():
        load(0)
        greet(place)
        g0.begin()
        load(1)
        route(ids_ref, gate_ref, rank_ref, rank_t_ref, gmat_ref, place)

    plan = [
        [],
        [g0.lead],
        [g0.follow, g0.lead_onward, g0.follow_onward, g0.last, g0.complete_y, lambda: load(s), g1.begin],
        [g0.passed_left],
        [g0.last_onward, g1.lead, g0.passed_right],
        [g1.follow, g0.complete_last],
        [g0.passed_last],
        [g1.lead_onward],
        [g1.follow_onward, g1.last],
        [g1.complete_y],
        [],
        [g1.last_onward, g1.passed_left],
        [g1.passed_right],
        [g1.complete_last],
        [g1.passed_last],
    ]
    for step, parts in enumerate(plan):

        @pl.when(s == step)
        def _(parts=parts):
            for part in parts:
                part()

    for copy in loads(s, False):
        copy.wait()

    @pl.when((s > 0) & (s != 1) & (s < steps - 1))
    def _():
        load(s + 1)

    @pl.when(slot < 2)
    def _():
        for copy in keeps(s):
            copy.start()

    def enter(x):
        u_ref[...] = (x.astype(F32) + dot(x, wd_ref[layer])).astype(BF16)
        acc_ref[...] = jnp.zeros_like(acc_ref)

    at(0, lambda: enter(x_ref[...]))
    at(SLOTS, lambda: enter(x1_ref[...]))

    buf = s % 2
    z = dot(one_hot(rank_t_ref, layer, slot, cap), u_ref[...]).astype(BF16)
    z_ref[0, 0] = z
    a = dot(z, b1_ref[buf]).astype(BF16)
    b = dot(z, b3_ref[buf]).astype(BF16)
    a_ref[0, 0] = a
    b_ref[0, 0] = b
    h = (jax.nn.silu(a.astype(F32)) * b.astype(F32)).astype(BF16)
    o = dot(h, b2_ref[buf]).astype(BF16)
    acc_ref[...] += column(gmat_ref, layer, slot, 0.0) * dot(one_hot_t(rank_ref, layer, slot, cap), o)

    def leave(out_ref):
        out_ref[...] = (u_ref[...].astype(F32) + acc_ref[...]).astype(BF16)

    @pl.when(slot < 2)
    def _():
        for copy in keeps(s):
            copy.wait()

    at(SLOTS - 1, lambda: leave(x1_ref))

    @pl.when(s == steps - 1)
    def _():
        leave(y_ref)
        copies.drain()


def forward(cap, x, ids, gates, wd, w1, w3, w2):
    tokens, width = x.shape
    layers, _, ff = ids.shape[0], None, w1.shape[3]
    vmem = pl.BlockSpec(memory_space=pltpu.VMEM)
    hbm = pl.BlockSpec(memory_space=pl.ANY)

    def saved(n):
        return pl.BlockSpec((1, 1, cap, n), lambda s: (s // SLOTS, s % SLOTS, 0, 0))

    shape = jax.ShapeDtypeStruct
    return pl.pallas_call(
        functools.partial(fwd_kernel, cap),
        grid=(layers * SLOTS,),
        in_specs=[vmem] * 4 + [hbm] * 3,
        out_specs=[vmem] * 5 + [hbm] * 3 + [saved(width), saved(ff), saved(ff)],
        out_shape=[
            shape((tokens, width), BF16),
            shape((tokens, width), BF16),
            shape((layers, tokens, LANES), jnp.int32),
            shape((layers, SLOTS, tokens), jnp.int32),
            shape((layers, tokens, LANES), F32),
            shape((layers, SLOTS, width, ff), BF16),
            shape((layers, SLOTS, width, ff), BF16),
            shape((layers, SLOTS, ff, width), BF16),
            shape((layers, SLOTS, cap, width), BF16),
            shape((layers, SLOTS, cap, ff), BF16),
            shape((layers, SLOTS, cap, ff), BF16),
        ],
        scratch_shapes=[
            pltpu.VMEM((tokens, width), BF16),
            pltpu.VMEM((tokens, width), F32),
            pltpu.VMEM((2, width, ff), BF16),
            pltpu.VMEM((2, width, ff), BF16),
            pltpu.VMEM((2, ff, width), BF16),
            pltpu.SemaphoreType.DMA((2, 3)),
            pltpu.SemaphoreType.DMA((2, 3)),
            pltpu.SemaphoreType.DMA((GATHER_COPIES,)),
            pltpu.SemaphoreType.DMA((GATHER_COPIES,)),
        ],
        compiler_params=pltpu.CompilerParams(vmem_limit_bytes=VMEM_LIMIT, collective_id=0, has_side_effects=True),
        name="forward",
    )(x, ids, gates, wd, w1, w3, w2)


def add_to(dst, src):
    dst[...] = (dst[...].astype(F32) + src[...].astype(F32)).astype(BF16)


class RingSum:
    def __init__(self, copies, name, axis, block, first, second):
        self.copies, self.name, self.block, self.first, self.second = copies, name, block, first, second
        self.early, self.later = ([(name, when, step) for step in WAYS] for when in ("early", "later"))
        for half, step in enumerate(WAYS):
            copies.add(self.early[half], block(2, half), first.at[half], axis, step)
            copies.add(self.later[half], block(step, None), second.at[half], axis, step)

    def start(self):
        self.copies.start(*self.early)

    def onward(self, *ways):
        for half in ways or BUFS:
            self.copies.arrive(self.early[half])
        for half in ways or BUFS:
            add_to(self.block(WAYS[half], half), self.first.at[half])
            self.copies.start(self.later[half])

    def finish(self, out):
        self.copies.arrive(*self.later)
        out[...] = (self.block(0, None)[...].astype(F32) + self.second[0].astype(F32) + self.second[1].astype(F32)).astype(BF16)
        self.copies.sent(*self.early, *self.later)


class RingSpread:
    def __init__(self, copies, name, axis, me, block, source=None, like=None):
        self.copies = copies
        self.near, self.far = ([(name, when, step) for step in WAYS] for when in ("near", "far"))
        for half, step in enumerate(WAYS):
            behind = (me - step + SIDE) % SIDE
            near, far = (None, None) if like is None else (like.near[half], like.far[half])
            copies.add(self.near[half], block(me, None) if source is None else source, block(me, None), axis, step, near)
            copies.add(self.far[half], block(behind, half), block(behind, half), axis, step, far)

    def start(self):
        self.copies.start(*self.near)

    def onward(self):
        for near, far in zip(self.near, self.far):
            self.copies.arrive(near)
            self.copies.start(far)

    def finish(self):
        self.copies.arrive(*self.far)
        self.copies.sent(*self.near, *self.far)


def slices(ref, lead, base, size):
    def block(index, half):
        start, rows = base + index * size, size
        if half is not None:
            rows = size // 2
            start = start + half * rows
        return ref.at[(*lead, pl.ds(pl.multiple_of(start, 16), rows))]

    return block


def slabs(ref):
    def block(index, half):
        if half is None:
            return ref.at[index]
        rows = ref.shape[1] // 2
        return ref.at[index, pl.ds(half * rows, rows)]

    return block


def total(ref):
    return (ref[0].astype(F32) + ref[1].astype(F32) + ref[2].astype(F32) + ref[3].astype(F32)).astype(BF16)


OWN_STEPS = {1: 0, 4: 1, 5: 2, 7: 3}
REDUCE_COPIES = 107


def bwd_kernel(cap, dy_ref, x0_ref, x1_ref, wd_ref, rank_ref, rank_t_ref, gmat_ref, w1_ref, w3_ref, w2_ref, z_ref, a_ref, b_ref, dx_ref, gd_ref, g1_ref, g3_ref, g2_ref, acc_ref, cur_ref, m1_ref, m3_ref, m2_ref, d1_ref, d3_ref, d2_ref, s1_ref, s3_ref, s2_ref, r11_ref, r12_ref, r31_ref, r32_ref, t1_ref, t3_ref, y11_ref, y12_ref, y31_ref, y32_ref, y21_ref, y22_ref, u1_ref, u2_ref, l1_ref, l2_ref, c1_ref, c3_ref, cu_ref, cl_ref, f1_ref, f3_ref, fu_ref, fl_ref, dp_ref, dr_ref, dcx_ref, dcy_ref, dcz_ref, ds_ref, de_ref, put_sem, send_sem, recv_sem, credit):
    s = pl.program_id(0)
    steps = pl.num_programs(0)
    layer, slot, t = 1 - s // SLOTS, SLOTS - 1 - s % SLOTS, s % SLOTS
    group = t // 4 + t // 5 + t // 7
    into = (t // 2 + t // 3) % 2
    place = Place()
    copies = Copies(place, send_sem, recv_sem)
    rows, ff = s1_ref.shape[1], s2_ref.shape[1]
    quarter, part = rows // SIDE, ff // 2 // SIDE
    half_d = rows // 2

    stage, mate, own = (m1_ref, m3_ref, m2_ref), (d1_ref, d3_ref, d2_ref), (s1_ref, s3_ref, s2_ref)
    outs = (g1_ref, g3_ref, g2_ref)
    for buf in BUFS:
        for n in ARRAYS:
            copies.add(("pair", buf, n), stage[n], mate[n].at[buf], "c", 0)

    def ring_blocks(ref, q, me, base, size):
        block = slices(ref, (q,), base, size)
        return lambda offset, half: block((me + offset + SIDE) % SIDE, half)

    def group_blocks(ref):
        block = slabs(ref)
        return lambda offset, half: block({2: 0, 1: 1, -1: 2, 0: 3}[offset], half)

    first = {
        "x": [RingSum(copies, ("x", q), "x", ring_blocks(s1_ref, q, place.x, 0, quarter), r11_ref.at[q], r12_ref.at[q]) for q in range(SIDE)],
        "z": [RingSum(copies, ("z", q), "z", ring_blocks(s3_ref, q, place.z, 0, quarter), r31_ref.at[q], r32_ref.at[q]) for q in range(SIDE)],
    }
    mid = {"x": t1_ref, "z": t3_ref}
    on_y = {
        "x": RingSum(copies, "yx", "y", group_blocks(t1_ref), y11_ref, y12_ref),
        "z": RingSum(copies, "yz", "y", group_blocks(t3_ref), y31_ref, y32_ref),
        "w": RingSum(copies, "yw", "y", group_blocks(s2_ref), y21_ref, y22_ref),
    }
    inner = {
        "u": RingSum(copies, "u", "x", ring_blocks(s2_ref, 3, place.x, 0, part), u1_ref, u2_ref),
        "l": RingSum(copies, "l", "z", ring_blocks(s2_ref, 3, place.z, ff // 2, part), l1_ref, l2_ref),
    }
    ring_of = {"x": ("x", place.x), "u": ("x", place.x), "z": ("z", place.z), "l": ("z", place.z)}
    other_of = {"x": ("z", place.z), "u": ("z", place.z), "z": ("x", place.x), "l": ("x", place.x)}
    cross_ref = {"x": c1_ref, "z": c3_ref, "u": cu_ref, "l": cl_ref}
    done_ref = {"x": f1_ref, "z": f3_ref, "u": fu_ref, "l": fl_ref}
    out_of = {"x": (g1_ref, 0, quarter), "z": (g3_ref, 0, quarter), "u": (g2_ref, 0, part), "l": (g2_ref, ff // 2, part)}
    cross, final, puts = {}, {}, {}
    for i, k in enumerate(out_of):
        cross[k] = RingSpread(copies, ("cross", k), *other_of[k], slabs(cross_ref[k]))
        ref, base, size = out_of[k]
        for late in LAYERS:
            block = slices(ref, (late, place.c), base, size)
            final[k, late] = RingSpread(copies, ("final", k, late), *ring_of[k], block, source=done_ref[k], like=final.get((k, 1)))
            puts[k, late] = pltpu.make_async_copy(done_ref[k], block(ring_of[k][1], None), put_sem.at[i])
    mine, theirs = (pl.ds(pl.multiple_of(c * half_d, 16), half_d) for c in (place.c, 1 - place.c))
    for late in LAYERS:
        for n, out in enumerate(outs):
            copies.add(("pass", n, late), out.at[late, place.c], out.at[late, place.c], "c", 0, None if late else ("pass", n, 1))
    copies.add("dense pair", dp_ref.at[theirs], dr_ref, "c", 0)
    copies.add("dense pass", ds_ref, de_ref, "c", 0)
    dense_refs = {"y": dcy_ref, "x": dcx_ref, "z": dcz_ref}
    index_of = {"y": place.y, "x": place.x, "z": place.z}
    dense = {k: RingSpread(copies, ("dense", k), k, index_of[k], slabs(ref)) for k, ref in dense_refs.items()}

    def reduce_start(q):
        for k in ("x", "z"):
            first[k][q].start()

    def reduce_onward(q):
        for k in ("x", "z"):
            first[k][q].onward()

    def reduce_finish(q):
        for k in ("x", "z"):
            first[k][q].finish(mid[k].at[q])

    def y_start():
        for k in ("x", "z"):
            on_y[k].start()

    def y_onward():
        for k in ("x", "z"):
            on_y[k].onward()

    def y_finish():
        for k in ("x", "z"):
            on_y[k].finish(cross_ref[k].at[other_of[k][1]])
            cross[k].start()

    def w_finish():
        on_y["w"].finish(s2_ref.at[3])
        for k in ("u", "l"):
            inner[k].start()

    def inner_onward():
        for k in ("u", "l"):
            inner[k].onward()

    def inner_finish():
        for k in ("u", "l"):
            inner[k].finish(cross_ref[k].at[other_of[k][1]])
            cross[k].start()

    def cross_onward(*keys):
        for k in keys:
            cross[k].onward()

    def cross_finish(late, *keys):
        for k in keys:
            cross[k].finish()
            done_ref[k][...] = total(cross_ref[k])
            puts[k, late].start()
            final[k, late].start()

    def final_onward(late, *keys):
        for k in keys:
            final[k, late].onward()

    def final_finish(late, *keys):
        for k in keys:
            final[k, late].finish()
            puts[k, late].wait()
        copies.start(*[("pass", n, late) for n in ARRAYS if ("xzu"[n] in keys)])

    def pass_finish(late):
        keys = [("pass", n, late) for n in ARRAYS]
        copies.arrive(*keys)
        copies.sent(*keys)

    def dense_sum():
        copies.arrive("dense pair")
        dcy_ref[place.y] = (dp_ref[mine].astype(F32) + dr_ref[...].astype(F32)).astype(BF16)
        copies.sent("dense pair")
        dense["y"].start()

    def dense_next(k, follow):
        dense[k].finish()
        dense_refs[follow][index_of[follow]] = total(dense_refs[k])
        dense[follow].start()

    def dense_pass(late):
        dense["z"].finish()
        ds_ref[...] = total(dcz_ref)
        gd_ref[late, mine] = ds_ref[...]
        copies.start("dense pass")

    def dense_finish(late):
        copies.arrive("dense pass")
        gd_ref[late, theirs] = de_ref[...]
        copies.sent("dense pass")

    before = {2: lambda: on_y["w"].start(), 3: lambda: reduce_onward(0), 5: lambda: (reduce_finish(0), y_start()), 6: lambda: reduce_onward(1), 7: lambda: reduce_onward(2)}
    middle = {7: lambda: reduce_finish(1)}
    after = {
        1: lambda: reduce_start(0),
        4: lambda: (reduce_start(1), on_y["w"].onward(0)),
        5: lambda: (reduce_start(2), on_y["w"].onward(1)),
        7: lambda: reduce_start(3),
    }
    late_before = [
        lambda: copies.start("dense pair"),
        lambda: reduce_onward(3),
        lambda: dense["y"].onward(),
        lambda: (reduce_finish(3), y_finish(), dense_next("y", "x")),
        lambda: dense["x"].onward(),
        lambda: dense_next("x", "z"),
        lambda: dense["z"].onward(),
        lambda: (final_onward(1, "x", "z", "u", "l"), dense_pass(1)),
    ]
    late_middle = [
        lambda: (dense_sum(), reduce_finish(2), y_onward()),
        lambda: w_finish(),
        lambda: inner_onward(),
        lambda: inner_finish(),
        lambda: cross_onward("x", "z", "u", "l"),
        lambda: cross_finish(1, "x", "z", "u", "l"),
        lambda: None,
        lambda: final_finish(1, "x", "z", "u", "l"),
    ]

    def ending():
        reduce_finish(2)
        y_onward()
        reduce_onward(3)
        dense_finish(1)
        pass_finish(1)
        copies.start("dense pair")
        w_finish()
        dense_sum()
        inner_onward()
        reduce_finish(3)
        dense["y"].onward()
        y_finish()
        inner_finish()
        dense_next("y", "x")
        cross_onward("x", "z")
        cross_onward("u", "l")
        cross_finish(0, "x", "z")
        dense["x"].onward()
        cross_finish(0, "u", "l")
        final_onward(0, "x", "z")
        dense_next("x", "z")
        final_onward(0, "u", "l")
        final_finish(0, "x", "z")
        dense["z"].onward()
        final_finish(0, "u", "l")
        dense_pass(0)
        pass_finish(0)
        dense_finish(0)

    def hook(index, step, body):
        pl.when(index == step)(lambda: body() and None)

    def hooks(late, always):
        for step, body in enumerate(late):
            hook(s, step + SLOTS, body)
        for step, body in always.items():
            hook(t, step, body)

    def load_grad(x):
        acc_ref[...] = x.astype(F32)
        cur_ref[...] = x

    @pl.when(s == 0)
    def _():
        greet(place)
        load_grad(dy_ref[...])

    hooks(late_before, before)

    grad_gated = (column(gmat_ref, layer, slot, 0.0) * cur_ref[...].astype(F32)).astype(BF16)
    do = dot(one_hot(rank_t_ref, layer, slot, cap), grad_gated).astype(BF16)
    dh = dot_nt(do, w2_ref[0, 0])
    a = a_ref[0, 0].astype(F32)
    b = b_ref[0, 0].astype(F32)
    sig = jax.nn.sigmoid(a)
    act = a * sig
    h = (act * b).astype(BF16)
    db = (dh * act).astype(BF16)
    da = (dh * b * sig * (1.0 + a * (1.0 - sig))).astype(BF16)
    z = z_ref[0, 0]
    dz = (dot_nt(da, w1_ref[0, 0]) + dot_nt(db, w3_ref[0, 0])).astype(BF16)
    acc_ref[...] += dot(one_hot_t(rank_ref, layer, slot, cap), dz)

    def weight_grads():
        return dot_tn(z, da), dot_tn(z, db), dot_tn(h, do)

    hooks(late_middle, middle)
    is_own = functools.reduce(jnp.logical_or, [t == step for step in OWN_STEPS])

    @pl.when(jnp.logical_not(is_own))
    def _():
        for buf in BUFS:
            pl.when((s > 0) & (into == 1 - buf))(lambda buf=buf: copies.sent(*[("pair", buf, n) for n in ARRAYS]))

        for ref, grad in zip(stage, weight_grads()):
            ref[...] = grad.astype(BF16)

        pl.when(s >= 3)(lambda: pl.semaphore_wait(credit.at[into], 1))
        for buf in BUFS:
            pl.when(into == buf)(lambda buf=buf: copies.start(*[("pair", buf, n) for n in ARRAYS]))

    @pl.when(is_own)
    def _():
        for buf in BUFS:
            pl.when(group % 2 == buf)(lambda buf=buf: copies.arrive(*[("pair", buf, n) for n in ARRAYS]))

        for ref, add, grad in zip(own, mate, weight_grads()):
            ref[group] = (grad + add[group % 2].astype(F32)).astype(BF16)

        @pl.when(s < 13)
        def _():
            pl.semaphore_signal(credit.at[group % 2], inc=1, device_id=place.at("c", 0), device_id_type=MESH)

    def leave(x, out_ref):
        grad = acc_ref[...]
        grad_b = grad.astype(BF16)
        dp_ref[...] = dot_tn(x, grad_b).astype(BF16)
        out_ref[...] = (grad + dot_nt(grad_b, wd_ref[layer])).astype(BF16)

    hooks([], after)

    @pl.when(s == SLOTS - 1)
    def _():
        leave(x1_ref[...], cur_ref)
        acc_ref[...] = cur_ref[...].astype(F32)

    @pl.when(s == steps - 1)
    def _():
        leave(x0_ref[...], dx_ref)
        ending()
        copies.sent(*[("pair", 1, n) for n in ARRAYS])


def backward(cap, dy, x0, x1, wd, rank, rank_t, gmat, w1, w3, w2, z, a, b):
    tokens, width = dy.shape
    layers, ff = w1.shape[0], w1.shape[3]
    local, quarter, part = SLOTS // SIDE, width // SIDE, ff // 2 // SIDE
    hbm = pl.BlockSpec(memory_space=pl.ANY)

    def fixed(shape):
        return pl.BlockSpec(shape, lambda s: (0,) * len(shape), pipeline_mode=pl.Buffered(1))

    def stream(*shape):
        return pl.BlockSpec((1, 1, *shape), lambda s: (1 - s // SLOTS, SLOTS - 1 - s % SLOTS, 0, 0))

    def buf(*shape):
        return pltpu.VMEM(shape, BF16)

    shape = jax.ShapeDtypeStruct
    ups, downs = [(width, ff), (width, ff), (ff, width)], [(quarter, ff), (part, width)]
    scratch = [pltpu.VMEM((tokens, width), F32), buf(tokens, width)]
    scratch += [buf(*u) for u in ups] + [buf(2, *u) for u in ups] + [buf(SIDE, *u) for u in ups]
    scratch += [buf(SIDE, 2, quarter // 2, ff), buf(SIDE, 2, quarter, ff)] * 2
    scratch += [buf(SIDE, quarter, ff)] * 2
    scratch += [buf(2, quarter // 2, ff), buf(2, quarter, ff)] * 2 + [buf(2, ff // 2, width), buf(2, ff, width)]
    scratch += [buf(2, part // 2, width), buf(2, part, width)] * 2
    scratch += [buf(SIDE, quarter, ff)] * 2 + [buf(SIDE, part, width)] * 2
    scratch += [buf(quarter, ff)] * 2 + [buf(part, width)] * 2
    scratch += [buf(width, width), buf(width // 2, width)] + [buf(SIDE, width // 2, width)] * 3 + [buf(width // 2, width)] * 2
    scratch += [pltpu.SemaphoreType.DMA((4,)), pltpu.SemaphoreType.DMA((REDUCE_COPIES,)), pltpu.SemaphoreType.DMA((REDUCE_COPIES,)), pltpu.SemaphoreType.REGULAR((2,))]
    return pl.pallas_call(
        functools.partial(bwd_kernel, cap),
        grid=(layers * SLOTS,),
        in_specs=[fixed(v.shape) for v in (dy, x0, x1, wd, rank, rank_t, gmat)] + [stream(*u) for u in ups] + [stream(cap, width), stream(cap, ff), stream(cap, ff)],
        out_specs=[fixed((tokens, width)), fixed((layers, width, width))] + [hbm] * 3,
        out_shape=[shape((tokens, width), BF16), shape((layers, width, width), BF16)] + [shape((layers, local, *u), BF16) for u in ups],
        scratch_shapes=scratch,
        compiler_params=pltpu.CompilerParams(vmem_limit_bytes=VMEM_LIMIT, collective_id=1, has_side_effects=True),
        name="backward",
    )(dy, x0, x1, wd, rank, rank_t, gmat, w1, w3, w2, z, a, b)


def solution(mesh):
    tok_spec = P(TOK_AXES, None)
    route_spec = P(None, TOK_AXES, None)
    expert_spec = P(None, "ep", None, None)
    whole_spec = P(None, None, None)

    def device_step(tok_in, tok_grad, route_ids, gate_vals, w_dense, w_gate, w_up, w_down):
        tokens, top_k = route_ids.shape[1:]
        cap = 2 * tokens * top_k // SLOTS
        y, x1, *kept = forward(cap, tok_in, jnp.swapaxes(route_ids, 1, 2), jnp.swapaxes(gate_vals, 1, 2), w_dense, w_gate, w_up, w_down)
        return (y, *backward(cap, tok_grad, tok_in, x1, w_dense, *kept))

    return jax.shard_map(device_step, mesh=mesh, in_specs=(tok_spec, tok_spec, route_spec, route_spec, whole_spec, expert_spec, expert_spec, expert_spec), out_specs=(tok_spec, tok_spec, whole_spec, expert_spec, expert_spec, expert_spec), check_vma=False)
```

```python
import functools

import jax
import jax.numpy as jnp
from jax import lax
from jax.experimental import pallas as pl
from jax.experimental.pallas import tpu as pltpu
from jax.sharding import PartitionSpec as P

TOK_AXES = ("rep", "ep", "dp")
F32 = jnp.float32
BF16 = jnp.bfloat16
LANES = 128
SIDE = 4
WAYS = (1, -1)
BUFS = (0, 1)
LAYERS = (1, 0)
ARRAYS = range(3)
SLOTS = 8
MESH = pl.DeviceIdType.MESH
VMEM_LIMIT = 63 << 20


def dot(a, b):
    return jnp.dot(a, b, preferred_element_type=F32)


def dot_nt(a, b):
    return lax.dot_general(a, b, (((1,), (1,)), ((), ())), preferred_element_type=F32)


def dot_tn(a, b):
    return lax.dot_general(a, b, (((0,), (0,)), ((), ())), preferred_element_type=F32)


class Place:
    def __init__(self):
        self.z, self.y, dp = lax.axis_index("rep"), lax.axis_index("ep"), lax.axis_index("dp")
        self.x, self.c = dp // 2, dp % 2

    def at(self, axis, step):
        z, y, x, c = self.z, self.y, self.x, self.c
        if axis == "z":
            z = (z + step + SIDE) % SIDE
        elif axis == "y":
            y = (y + step + SIDE) % SIDE
        elif axis == "x":
            x = (x + step + SIDE) % SIDE
        else:
            c = 1 - c
        return (z, y, x * 2 + c)


class Copies:
    def __init__(self, place, send, recv):
        self.place, self.send, self.recv, self.made, self.number, self.count = place, send, recv, {}, {}, 0

    def add(self, key, src, dst, axis, step, like=None):
        if like is None:
            n, self.count = self.count, self.count + 1
        else:
            n = self.number[like]
        self.number[key] = n
        self.made[key] = pltpu.make_async_remote_copy(src_ref=src, dst_ref=dst, send_sem=self.send.at[n], recv_sem=self.recv.at[n], device_id=self.place.at(axis, step), device_id_type=MESH)

    def start(self, *keys):
        for key in keys:
            self.made[key].start()

    def arrive(self, *keys):
        for key in keys:
            self.made[key].wait_recv()

    def sent(self, *keys):
        for key in keys:
            self.made[key].wait_send()


def greet(place):
    barrier = pltpu.get_barrier_semaphore()
    peers = [(axis, step) for axis in "xyz" for step in WAYS] + [("c", 0)]
    for axis, step in peers:
        pl.semaphore_signal(barrier, inc=1, device_id=place.at(axis, step), device_id_type=MESH)
    pl.semaphore_wait(barrier, len(peers))


class Gather:
    FROM = {2: -1, 3: 1, 6: 2}
    PASS = {2: 4, 3: 5, 6: 7}

    def __init__(self, layer, copies, place, own, whole):
        self.layer, self.copies, self.place, self.own, self.whole = layer, copies, place, own, whole
        rows, ff = own[0].shape[2], own[2].shape[2]
        self.cut = {"x": ((0, 0, rows // SIDE), (2, 0, ff // 2 // SIDE)), "z": ((1, 0, rows // SIDE), (2, ff // 2, ff // 2 // SIDE))}
        mine = {"x": place.x, "z": place.z}
        for color in ("x", "z"):
            for part in BUFS:
                self._add(("y", 2, color, part), color, part, None, 2, mine[color], None, "y", 1)
                self._add(("y", 3, color, part), color, part, None, 3, mine[color], None, "y", -1)
                if color == "x":
                    self._add(("y", 6, color, part), color, part, 2, 6, mine[color], None, "y", 1)
                else:
                    self._add(("y", 6, color, part), color, part, 3, 6, mine[color], None, "y", -1)
                for slot in (2, 3, 6):
                    for step in WAYS:
                        self._add(("near", slot, color, part, step), color, part, slot, slot, mine[color], None, color, step)
                        behind = (mine[color] - step + SIDE) % SIDE
                        self._add(("far", slot, color, part, step), color, part, slot, slot, behind, (1 - step) // 2, color, step)
        for slot, to in self.PASS.items():
            for array in ARRAYS:
                copies.add((layer, "pass", slot, array), whole[array].at[layer, slot], whole[array].at[layer, to], "c", 0)

    def _view(self, refs, index, color, part, quarter, half):
        array, base, size = self.cut[color][part]
        start = base + quarter * size
        if half is not None:
            size = size // 2
            start = start + half * size
        return refs[array].at[self.layer, index, pl.ds(pl.multiple_of(start, 16), size)]

    def _add(self, key, color, part, src_slot, dst_slot, quarter, half, axis, step):
        src = self._view(self.own, self.place.c, color, part, quarter, half) if src_slot is None else self._view(self.whole, src_slot, color, part, quarter, half)
        self.copies.add((self.layer,) + key, src, self._view(self.whole, dst_slot, color, part, quarter, half), axis, step)

    def _keys(self, *key, extra=()):
        return [(self.layer,) + key + (part,) + extra for part in BUFS]

    def lead(self):
        self.spread(2, "x")
        self.spread(3, "z")

    def lead_onward(self):
        self.onward(2, "x")
        self.onward(3, "z")

    def follow(self):
        self.spread(2, "z")
        self.spread(3, "x")

    def follow_onward(self):
        self.onward(2, "z")
        self.onward(3, "x")

    def last(self):
        self.spread(6, "x")
        self.spread(6, "z")

    def last_onward(self):
        self.onward(6, "x")
        self.onward(6, "z")

    def complete_y(self):
        self.complete(2)
        self.complete(3)

    def complete_last(self):
        self.complete(6)

    def passed_left(self):
        self.passed(2)

    def passed_right(self):
        self.passed(3)

    def passed_last(self):
        self.passed(6)

    def begin(self):
        for slot, color in ((2, "x"), (3, "z"), (2, "z"), (3, "x")):
            self.copies.start(*self._keys("y", slot, color))

    def spread(self, slot, color):
        self.copies.arrive(*self._keys("y", slot, color))
        if (slot, color) in ((2, "x"), (3, "z")):
            self.copies.start(*self._keys("y", 6, color))
        for step in WAYS:
            self.copies.start(*self._keys("near", slot, color, extra=(step,)))

    def onward(self, slot, color):
        for step in WAYS:
            self.copies.arrive(*self._keys("near", slot, color, extra=(step,)))
            self.copies.start(*self._keys("far", slot, color, extra=(step,)))

    def complete(self, slot):
        for color in ("x", "z"):
            for step in WAYS:
                self.copies.arrive(*self._keys("far", slot, color, extra=(step,)))
        self.copies.start(*[(self.layer, "pass", slot, array) for array in ARRAYS])

    def passed(self, slot):
        self.copies.arrive(*[(self.layer, "pass", slot, array) for array in ARRAYS])


GATHER_COPIES = 2 * (2 * 2 * (3 + 3 * 4) + 9)


def route(ids_ref, gate_ref, rows_ref, columns_ref, place):
    layers, _, tokens = ids_ref.shape
    below = lax.broadcasted_iota(jnp.int32, (tokens, tokens), 0) < lax.broadcasted_iota(jnp.int32, (tokens, tokens), 1)
    below = jnp.where(below, 1.0, 0.0).astype(BF16)
    lead = lax.broadcasted_iota(jnp.int32, (2 * SLOTS, tokens), 0)
    for layer in range(layers):
        ids, gates = ids_ref[layer], gate_ref[layer]
        off = ((ids >> 1) - place.y) & (SIDE - 1)
        odd = (ids + place.c) & 1
        slot = jnp.where(off == 0, odd, jnp.where(off == SIDE - 1, 2 + 2 * odd, jnp.where(off == 1, 3 + 2 * odd, 6 + odd)))
        hits = [slot[n : n + 1] == lead for n in BUFS]
        hit = hits[0] | hits[1]
        weight = jnp.where(hits[0], gates[0:1], 0.0) + jnp.where(hits[1], gates[1:2], 0.0)
        rank = jnp.where(hit, dot(jnp.where(hit, 1.0, 0.0).astype(BF16), below), -1.0)
        rows_ref[layer] = rank[:SLOTS].astype(jnp.int32)
        columns_ref[layer] = jnp.transpose(jnp.concatenate([rank[:SLOTS], weight[:SLOTS], jnp.zeros((LANES - 2 * SLOTS, tokens), F32)], axis=0))


def one_hot(rows_ref, layer, slot, cap):
    place = lax.broadcasted_iota(jnp.int32, (cap, rows_ref.shape[2]), 0)
    return jnp.where(rows_ref[layer, pl.ds(slot, 1), :] == place, 1.0, 0.0).astype(BF16)


def column(columns_ref, layer, index):
    lane = lax.broadcasted_iota(jnp.int32, columns_ref.shape[1:], 1)
    return jnp.sum(jnp.where(lane == index, columns_ref[layer], 0.0), axis=1, keepdims=True)


def one_hot_t(columns_ref, layer, slot, cap):
    place = lax.broadcasted_iota(jnp.int32, (columns_ref.shape[1], cap), 1)
    return jnp.where(column(columns_ref, layer, slot).astype(jnp.int32) == place, 1.0, 0.0).astype(BF16)


def add_to(dst, src):
    dst[...] = (dst[...].astype(F32) + src[...].astype(F32)).astype(BF16)


class RingSum:
    def __init__(self, copies, name, axis, block, first, second):
        self.copies, self.name, self.block, self.first, self.second = copies, name, block, first, second
        self.early, self.later = ([(name, when, step) for step in WAYS] for when in ("early", "later"))
        for half, step in enumerate(WAYS):
            copies.add(self.early[half], block(2, half), first.at[half], axis, step)
            copies.add(self.later[half], block(step, None), second.at[half], axis, step)

    def start(self):
        self.copies.start(*self.early)

    def onward(self):
        self.copies.arrive(*self.early)
        for half in BUFS:
            add_to(self.block(WAYS[half], half), self.first.at[half])
            self.copies.start(self.later[half])
        self.copies.sent(*self.early)

    def finish(self, out):
        self.copies.arrive(*self.later)
        out[...] = (self.block(0, None)[...].astype(F32) + self.second[0].astype(F32) + self.second[1].astype(F32)).astype(BF16)
        self.copies.sent(*self.later)


class RingSpread:
    def __init__(self, copies, name, axis, me, block, source=None, like=None):
        self.copies = copies
        self.near, self.far = ([(name, when, step) for step in WAYS] for when in ("near", "far"))
        for half, step in enumerate(WAYS):
            behind = (me - step + SIDE) % SIDE
            near, far = (None, None) if like is None else (like.near[half], like.far[half])
            copies.add(self.near[half], block(me, None) if source is None else source, block(me, None), axis, step, near)
            copies.add(self.far[half], block(behind, half), block(behind, half), axis, step, far)

    def start(self):
        self.copies.start(*self.near)

    def onward(self):
        for near, far in zip(self.near, self.far):
            self.copies.arrive(near)
            self.copies.start(far)

    def finish(self):
        self.copies.arrive(*self.far)
        self.copies.sent(*self.near, *self.far)


def slices(ref, lead, base, size):
    def block(index, half):
        start, rows = base + index * size, size
        if half is not None:
            rows = size // 2
            start = start + half * rows
        return ref.at[(*lead, pl.ds(pl.multiple_of(start, 16), rows))]

    return block


def slabs(ref):
    def block(index, half):
        if half is None:
            return ref.at[index]
        rows = ref.shape[1] // 2
        return ref.at[index, pl.ds(half * rows, rows)]

    return block


def total(ref):
    return (ref[0].astype(F32) + ref[1].astype(F32) + ref[2].astype(F32) + ref[3].astype(F32)).astype(BF16)


OWN_STEPS = {1: 0, 4: 1, 5: 2, 7: 3}
REDUCE_COPIES = 107
LAST, LATE, DEFER, STEPS = 2 * SLOTS, 3 * SLOTS, 4 * SLOTS, 5 * SLOTS


def kernel(cap, x0_ref, dy_ref, ids_ref, gate_ref, wd_ref, o1_ref, o3_ref, o2_ref, y_ref, dx_ref, gd_ref, g1_ref, g3_ref, g2_ref, h1_ref, h3_ref, h2_ref, kz_ref, ka_ref, kb_ref, kda_ref, kdb_ref, acc_ref, cur_ref, x1_ref, rows_ref, columns_ref, w1_ref, w3_ref, w2_ref, z_ref, a_ref, b_ref, m1_ref, m3_ref, m2_ref, d1_ref, d3_ref, d2_ref, s1_ref, s3_ref, s2_ref, r11_ref, r12_ref, r31_ref, r32_ref, t1_ref, t3_ref, y11_ref, y12_ref, y31_ref, y32_ref, y21_ref, y22_ref, u1_ref, u2_ref, l1_ref, l2_ref, c1_ref, c3_ref, cu_ref, cl_ref, f1_ref, f3_ref, fu_ref, fl_ref, dp_ref, dr_ref, dcx_ref, dcy_ref, dcz_ref, ds_ref, de_ref, put_sem, load_sem, keep_sem, save_sem, gsend_sem, grecv_sem, send_sem, recv_sem, credit):
    s = pl.program_id(0)
    place = Place()
    gathers = Copies(place, gsend_sem, grecv_sem)
    copies = Copies(place, send_sem, recv_sem)
    given, whole, bufs = (o1_ref, o3_ref, o2_ref), (h1_ref, h3_ref, h2_ref), (w1_ref, w3_ref, w2_ref)
    kept, acts = (kz_ref, ka_ref, kb_ref), (z_ref, a_ref, b_ref)
    deferred = (kda_ref, kdb_ref)
    g0, g1 = (Gather(l, gathers, place, given, whole) for l in BUFS)
    rows, ff = s1_ref.shape[1], s2_ref.shape[1]
    quarter, part = rows // SIDE, ff // 2 // SIDE
    half_d = rows // 2

    stage, mate, mine_of = (m1_ref, m3_ref, m2_ref), (d1_ref, d3_ref, d2_ref), (s1_ref, s3_ref, s2_ref)
    outs = (g1_ref, g3_ref, g2_ref)
    for buf in BUFS:
        for n in ARRAYS:
            copies.add(("pair", buf, n), stage[n], mate[n].at[buf], "c", 0)

    def ring_blocks(ref, q, me, base, size):
        block = slices(ref, (q,), base, size)
        return lambda offset, half: block((me + offset + SIDE) % SIDE, half)

    def group_blocks(ref):
        block = slabs(ref)
        return lambda offset, half: block({2: 0, 1: 1, -1: 2, 0: 3}[offset], half)

    first = {
        "x": [RingSum(copies, ("x", q), "x", ring_blocks(s1_ref, q, place.x, 0, quarter), r11_ref.at[q], r12_ref.at[q]) for q in range(SIDE)],
        "z": [RingSum(copies, ("z", q), "z", ring_blocks(s3_ref, q, place.z, 0, quarter), r31_ref.at[q], r32_ref.at[q]) for q in range(SIDE)],
    }
    mid = {"x": t1_ref, "z": t3_ref}
    on_y = {
        "x": RingSum(copies, "yx", "y", group_blocks(t1_ref), y11_ref, y12_ref),
        "z": RingSum(copies, "yz", "y", group_blocks(t3_ref), y31_ref, y32_ref),
        "w": RingSum(copies, "yw", "y", group_blocks(s2_ref), y21_ref, y22_ref),
    }
    inner = {
        "u": RingSum(copies, "u", "x", ring_blocks(s2_ref, 3, place.x, 0, part), u1_ref, u2_ref),
        "l": RingSum(copies, "l", "z", ring_blocks(s2_ref, 3, place.z, ff // 2, part), l1_ref, l2_ref),
    }
    ring_of = {"x": ("x", place.x), "u": ("x", place.x), "z": ("z", place.z), "l": ("z", place.z)}
    other_of = {"x": ("z", place.z), "u": ("z", place.z), "z": ("x", place.x), "l": ("x", place.x)}
    cross_ref = {"x": c1_ref, "z": c3_ref, "u": cu_ref, "l": cl_ref}
    done_ref = {"x": f1_ref, "z": f3_ref, "u": fu_ref, "l": fl_ref}
    out_of = {"x": (g1_ref, 0, quarter), "z": (g3_ref, 0, quarter), "u": (g2_ref, 0, part), "l": (g2_ref, ff // 2, part)}
    cross, final, puts = {}, {}, {}
    for i, k in enumerate(out_of):
        cross[k] = RingSpread(copies, ("cross", k), *other_of[k], slabs(cross_ref[k]))
        ref, base, size = out_of[k]
        for late in LAYERS:
            block = slices(ref, (late, place.c), base, size)
            final[k, late] = RingSpread(copies, ("final", k, late), *ring_of[k], block, source=done_ref[k], like=final.get((k, 1)))
            puts[k, late] = pltpu.make_async_copy(done_ref[k], block(ring_of[k][1], None), put_sem.at[i])
    mine, theirs = (pl.ds(pl.multiple_of(c * half_d, 16), half_d) for c in (place.c, 1 - place.c))
    for late in LAYERS:
        for n, out in enumerate(outs):
            copies.add(("pass", n, late), out.at[late, place.c], out.at[late, place.c], "c", 0, None if late else ("pass", n, 1))
    copies.add("dense pair", dp_ref.at[theirs], dr_ref, "c", 0)
    copies.add("dense pass", ds_ref, de_ref, "c", 0)
    dense_refs = {"y": dcy_ref, "x": dcx_ref, "z": dcz_ref}
    index_of = {"y": place.y, "x": place.x, "z": place.z}
    dense = {k: RingSpread(copies, ("dense", k), k, index_of[k], slabs(ref)) for k, ref in dense_refs.items()}

    def reduce_start(q):
        for k in ("x", "z"):
            first[k][q].start()

    def reduce_onward(q):
        for k in ("x", "z"):
            first[k][q].onward()

    def reduce_finish(q):
        for k in ("x", "z"):
            first[k][q].finish(mid[k].at[q])

    def y_start():
        for k in ("x", "z"):
            on_y[k].start()

    def y_onward():
        for k in ("x", "z"):
            on_y[k].onward()

    def y_finish():
        for k in ("x", "z"):
            on_y[k].finish(cross_ref[k].at[other_of[k][1]])
            cross[k].start()

    def w_finish():
        on_y["w"].finish(s2_ref.at[3])
        for k in ("u", "l"):
            inner[k].start()

    def inner_onward():
        for k in ("u", "l"):
            inner[k].onward()

    def inner_finish():
        for k in ("u", "l"):
            inner[k].finish(cross_ref[k].at[other_of[k][1]])
            cross[k].start()

    def cross_onward(*keys):
        for k in keys:
            cross[k].onward()

    def cross_finish(late, *keys):
        for k in keys:
            cross[k].finish()
            done_ref[k][...] = total(cross_ref[k])
            puts[k, late].start()
            final[k, late].start()

    def final_onward(late, *keys):
        for k in keys:
            final[k, late].onward()

    def final_finish(late, *keys):
        for k in keys:
            final[k, late].finish()
            puts[k, late].wait()
        copies.start(*[("pass", n, late) for n in ARRAYS if ("xzu"[n] in keys)])

    def pass_finish(late):
        keys = [("pass", n, late) for n in ARRAYS]
        copies.arrive(*keys)
        copies.sent(*keys)

    def dense_sum():
        copies.arrive("dense pair")
        dcy_ref[place.y] = (dp_ref[mine].astype(F32) + dr_ref[...].astype(F32)).astype(BF16)
        copies.sent("dense pair")
        dense["y"].start()

    def dense_next(k, follow):
        dense[k].finish()
        dense_refs[follow][index_of[follow]] = total(dense_refs[k])
        dense[follow].start()

    def dense_pass(late):
        dense["z"].finish()
        ds_ref[...] = total(dcz_ref)
        gd_ref[late, mine] = ds_ref[...]
        copies.start("dense pass")

    def dense_finish(late):
        copies.arrive("dense pass")
        gd_ref[late, theirs] = de_ref[...]
        copies.sent("dense pass")

    def copy(src, dst, sem):
        return pltpu.make_async_copy(src, dst, sem)

    def weights(step, layer, slot, arrays, buf, is_given=False):
        for n in arrays:
            src = given[n].at[layer, (place.c + slot) % 2] if is_given else whole[n].at[layer, slot]
            yield copy(src, bufs[n].at[buf], load_sem.at[buf, n])

    def saved(layer, slot, buf):
        for n in ARRAYS:
            yield copy(kept[n].at[layer, slot], acts[n].at[buf], load_sem.at[buf, 3 + n])

    def loads(step, do):
        forth, back = step % 2, (step + 1) % 2
        slot = step % SLOTS
        rest = SLOTS - 1 - slot

        def run(when, items):
            @pl.when(when)
            def _():
                for item in items():
                    do(item)

        run((step < LAST) & (slot < 2), lambda: weights(step, step // SLOTS, slot, ARRAYS, forth, True))
        run((step < LAST) & (slot >= 2), lambda: weights(step, step // SLOTS, slot, ARRAYS, forth))
        run((step > LAST) & (step < LATE), lambda: [*weights(step, 1, rest, ARRAYS, back), *saved(1, rest, back)])
        run((step >= LATE) & (step < DEFER), lambda: [*weights(step, 0, rest, [2], back), *saved(0, rest, back)])
        run((step >= DEFER) & (step < STEPS), lambda: [*weights(step, 0, rest, BUFS, back)] + [copy(deferred[n].at[rest], acts[n + 1].at[back], load_sem.at[back, 4 + n]) for n in BUFS])

    def load(step):
        loads(step, lambda item: item.start())

    def keeps(step):
        return [copy(bufs[n].at[step % 2], whole[n].at[step // SLOTS, step % SLOTS], keep_sem.at[step % 2, n]) for n in ARRAYS]

    def saves(step):
        return [copy(acts[n].at[step % 2], kept[n].at[step // SLOTS, step % SLOTS], save_sem.at[step % 2, n]) for n in ARRAYS]

    def defers(step):
        return [copy(acts[n + 1].at[2], deferred[n].at[SLOTS - 1 - step % SLOTS], save_sem.at[0, n]) for n in BUFS]

    def wait(items):
        for item in items:
            item.wait()

    def start(items):
        for item in items:
            item.start()

    def ending():
        inner_onward()
        dense_sum()
        inner_finish()
        y_finish()
        dense["y"].onward()
        pass_finish(1)
        pl.semaphore_signal(credit.at[2], inc=1, device_id=place.at("c", 0), device_id_type=MESH)
        cross_onward("u", "l")
        dense_next("y", "x")
        cross_onward("x", "z")
        cross_finish(0, "u", "l")
        dense["x"].onward()
        cross_finish(0, "x", "z")
        final_onward(0, "u", "l")
        dense_next("x", "z")
        final_onward(0, "x", "z")
        pl.semaphore_wait(credit.at[2], 1)
        final_finish(0, "u", "l")
        dense["z"].onward()
        final_finish(0, "x", "z")
        dense_pass(0)
        pass_finish(0)
        dense_finish(0)

    before, middle, after = {}, {}, {}

    def plan(table, first, *stages):
        for n, stage in enumerate(stages):
            table.setdefault(first + n, []).extend(stage)

    on, done = lambda q: lambda: reduce_onward(q), lambda q: lambda: reduce_finish(q)
    plan(before, 1, [g0.lead], [g0.follow, g0.lead_onward, g0.follow_onward, g0.last, g0.complete_y, lambda: load(s), g1.begin], [g0.passed_left])
    plan(before, 4, [g0.last_onward, g1.lead, g0.passed_right], [g1.follow, g0.complete_last], [g0.passed_last], [g1.lead_onward])
    plan(before, SLOTS, [g1.follow_onward, g1.last], [g1.complete_y], [], [g1.last_onward, g1.passed_left], [g1.passed_right], [g1.complete_last], [g1.passed_last])
    plan(before, LAST + 2, [on_y["w"].start], [on(0)], [], [done(0), y_start], [on(1), on_y["w"].onward], [on(2)])
    plan(middle, LATE - 1, [done(1)])
    plan(before, LATE, [lambda: copies.start("dense pair")], [on(3)], [dense["y"].onward], [], [inner_onward], [y_finish], [], [lambda: cross_onward("x", "z")])
    plan(middle, LATE, [dense_sum, done(2), y_onward], [], [w_finish], [done(3), lambda: dense_next("y", "x")], [], [inner_finish, dense["x"].onward], [], [lambda: cross_onward("u", "l"), lambda: dense_next("x", "z")])
    plan(before, DEFER + 1, [lambda: cross_finish(1, "x", "z", "u", "l")], [dense["z"].onward], [], [lambda: dense_pass(1)], [lambda: final_onward(1, "x", "z", "u", "l")], [], [lambda: final_finish(1, "x", "z", "u", "l"), lambda: dense_finish(1)])
    plan(after, LATE + 2, [on_y["w"].start])
    plan(before, LATE + 4, [on(0)], [], [done(0), y_start, on_y["w"].onward], [on(1)], [on(2)], [], [done(1)], [on(3)], [done(2), y_onward], [], [w_finish], [done(3)])
    for base in (LAST, LATE):
        for step, q in OWN_STEPS.items():
            plan(after, base + step, [lambda q=q: reduce_start(q)])

    def hooks(table):
        for step, stages in sorted(table.items()):

            @pl.when(s == step)
            def _(stages=stages):
                for stage in stages:
                    stage()

    is_forward, is_back = s < LAST, (s >= LAST) & (s < DEFER)
    forth, back = s % 2, (s + 1) % 2
    t = s % SLOTS

    @pl.when(s == 0)
    def _():
        load(0)
        greet(place)
        g0.begin()
        load(1)
        route(ids_ref, gate_ref, rows_ref, columns_ref, place)

    hooks(before)
    loads(s, lambda item: item.wait())
    pl.when((s > 1) & (s <= LAST))(lambda: wait(saves(s - 2)))
    pl.when((s > LATE) & (s <= DEFER))(lambda: wait(defers(s - 1)))
    pl.when((s > 0) & (s != 1) & (s != LAST - 1))(lambda: load(s + 1))
    pl.when(is_forward & (t < 2))(lambda: start(keeps(s)))

    def enter(x):
        cur_ref[...] = (x.astype(F32) + dot(x, wd_ref[s // SLOTS])).astype(BF16)
        acc_ref[...] = jnp.zeros_like(acc_ref)

    def enter_back(x):
        cur_ref[...] = x
        acc_ref[...] = x.astype(F32)

    pl.when(s == 0)(lambda: enter(x0_ref[...]))
    pl.when(s == SLOTS)(lambda: enter(x1_ref[...]))
    pl.when(s == LAST)(lambda: enter_back(dy_ref[...]))

    @pl.when(is_forward)
    def _():
        layer, slot = s // SLOTS, t
        z = dot(one_hot(rows_ref, layer, slot, cap), cur_ref[...]).astype(BF16)
        z_ref[forth] = z
        a = dot(z, w1_ref[forth]).astype(BF16)
        b = dot(z, w3_ref[forth]).astype(BF16)
        a_ref[forth] = a
        b_ref[forth] = b
        h = (jax.nn.silu(a.astype(F32)) * b.astype(F32)).astype(BF16)
        o = dot(h, w2_ref[forth]).astype(BF16)
        acc_ref[...] += column(columns_ref, layer, SLOTS + slot) * dot(one_hot_t(columns_ref, layer, slot, cap), o)
        pl.when(s < LAST - 1)(lambda: start(saves(s)))
        pl.when(t < 2)(lambda: wait(keeps(s)))

    def leave(out_ref):
        out_ref[...] = (cur_ref[...].astype(F32) + acc_ref[...]).astype(BF16)

    pl.when(s == SLOTS - 1)(lambda: leave(x1_ref))
    pl.when(s == LAST - 1)(lambda: leave(y_ref))

    @pl.when(is_back)
    def _():
        layer, slot = 1 - (s - LAST) // SLOTS, SLOTS - 1 - t
        grad_gated = (column(columns_ref, layer, SLOTS + slot) * cur_ref[...].astype(F32)).astype(BF16)
        do = dot(one_hot(rows_ref, layer, slot, cap), grad_gated).astype(BF16)
        dh = dot_nt(do, w2_ref[back])
        a = a_ref[back].astype(F32)
        b = b_ref[back].astype(F32)
        sig = jax.nn.sigmoid(a)
        act = a * sig
        h = (act * b).astype(BF16)
        db = (dh * act).astype(BF16)
        da = (dh * b * sig * (1.0 + a * (1.0 - sig))).astype(BF16)
        a_ref[2] = da
        b_ref[2] = db
        z = z_ref[back]
        pl.when(s >= LATE)(lambda: start(defers(s)))
        hooks(middle)

        def weight_grads():
            return dot_tn(z, da), dot_tn(z, db), dot_tn(h, do)

        is_own = functools.reduce(jnp.logical_or, [t == step for step in OWN_STEPS])
        group = t // 4 + t // 5 + t // 7
        into = (t // 2 + t // 3) % 2

        @pl.when(jnp.logical_not(is_own))
        def _():
            for buf in BUFS:
                pl.when((s > LAST) & (into == 1 - buf))(lambda buf=buf: copies.sent(*[("pair", buf, n) for n in ARRAYS]))

            for ref, grad in zip(stage, weight_grads()):
                ref[...] = grad.astype(BF16)

            pl.when(s >= LAST + 3)(lambda: pl.semaphore_wait(credit.at[into], 1))
            for buf in BUFS:
                pl.when(into == buf)(lambda buf=buf: copies.start(*[("pair", buf, n) for n in ARRAYS]))

        @pl.when(is_own)
        def _():
            for buf in BUFS:
                pl.when(group % 2 == buf)(lambda buf=buf: copies.arrive(*[("pair", buf, n) for n in ARRAYS]))

            for ref, add, grad in zip(mine_of, mate, weight_grads()):
                ref[group] = (grad + add[group % 2].astype(F32)).astype(BF16)

            @pl.when(s < DEFER - 3)
            def _():
                pl.semaphore_signal(credit.at[group % 2], inc=1, device_id=place.at("c", 0), device_id_type=MESH)

    @pl.when(((s >= LAST) & (s < LATE)) | (s >= DEFER))
    def _():
        layer, slot = s // LATE * -1 + 1, SLOTS - 1 - t
        src = back - (s // DEFER - 1) * (2 - back)
        dz = (dot_nt(a_ref[src], w1_ref[back]) + dot_nt(b_ref[src], w3_ref[back])).astype(BF16)
        acc_ref[...] += dot(one_hot_t(columns_ref, layer, slot, cap), dz)

    def leave_back(layer, x, out_ref):
        grad = acc_ref[...]
        grad_b = grad.astype(BF16)
        dp_ref[...] = dot_tn(x, grad_b).astype(BF16)
        out_ref[...] = (grad + dot_nt(grad_b, wd_ref[layer])).astype(BF16)

    @pl.when(s == LATE - 1)
    def _():
        leave_back(1, x1_ref[...], cur_ref)
        acc_ref[...] = cur_ref[...].astype(F32)

    hooks(after)

    @pl.when(s == STEPS - 1)
    def _():
        leave_back(0, x0_ref[...], dx_ref)
        copies.start("dense pair")
        ending()
        copies.sent(*[("pair", 1, n) for n in ARRAYS])
        gathers.sent(*gathers.made)


def step(cap, x0, dy, ids, gates, wd, w1, w3, w2):
    tokens, width = dy.shape
    layers, local, _, ff = w1.shape
    quarter, part = width // SIDE, ff // 2 // SIDE
    hbm = pl.BlockSpec(memory_space=pl.ANY)

    def fixed(shape):
        return pl.BlockSpec(shape, lambda s: (0,) * len(shape), pipeline_mode=pl.Buffered(1))

    def buf(*shape):
        return pltpu.VMEM(shape, BF16)

    def dma(*shape):
        return pltpu.SemaphoreType.DMA(shape)

    shape = jax.ShapeDtypeStruct
    ups, downs = [(width, ff), (width, ff), (ff, width)], [(quarter, ff), (part, width)]
    acts = [(cap, width), (cap, ff), (cap, ff)]
    scratch = [pltpu.VMEM((tokens, width), F32), buf(tokens, width), buf(tokens, width), pltpu.VMEM((layers, SLOTS, tokens), jnp.int32), pltpu.VMEM((layers, tokens, LANES), F32)]
    scratch += [buf(2, *u) for u in ups] + [buf(2, *acts[0]), buf(3, *acts[1]), buf(3, *acts[2])]
    scratch += [buf(*u) for u in ups] + [buf(2, *u) for u in ups] + [buf(SIDE, *u) for u in ups]
    scratch += [buf(SIDE, 2, quarter // 2, ff), buf(SIDE, 2, quarter, ff)] * 2
    scratch += [buf(SIDE, quarter, ff)] * 2
    scratch += [buf(2, quarter // 2, ff), buf(2, quarter, ff)] * 2 + [buf(2, ff // 2, width), buf(2, ff, width)]
    scratch += [buf(2, part // 2, width), buf(2, part, width)] * 2
    scratch += [buf(SIDE, quarter, ff)] * 2 + [buf(SIDE, part, width)] * 2
    scratch += [buf(quarter, ff)] * 2 + [buf(part, width)] * 2
    scratch += [buf(width, width), buf(width // 2, width)] + [buf(SIDE, width // 2, width)] * 3 + [buf(width // 2, width)] * 2
    scratch += [dma(4), dma(2, 6), dma(2, 3), dma(2, 3), dma(GATHER_COPIES), dma(GATHER_COPIES), dma(REDUCE_COPIES), dma(REDUCE_COPIES), pltpu.SemaphoreType.REGULAR((3,))]
    results = [(tokens, width), (tokens, width), (layers, width, width)]
    kept = [(layers, local, *u) for u in ups] + [(layers, SLOTS, *u) for u in ups + acts] + [(SLOTS, cap, ff)] * 2
    return pl.pallas_call(
        functools.partial(kernel, cap),
        grid=(STEPS,),
        in_specs=[fixed(v.shape) for v in (x0, dy, ids, gates, wd)] + [hbm] * 3,
        out_specs=[fixed(r) for r in results] + [hbm] * len(kept),
        out_shape=[shape(r, BF16) for r in results + kept],
        scratch_shapes=scratch,
        compiler_params=pltpu.CompilerParams(vmem_limit_bytes=VMEM_LIMIT, collective_id=0, has_side_effects=True),
        name="step",
    )(x0, dy, ids, gates, wd, w1, w3, w2)[:6]


def solution(mesh):
    tok_spec = P(TOK_AXES, None)
    route_spec = P(None, TOK_AXES, None)
    expert_spec = P(None, "ep", None, None)
    whole_spec = P(None, None, None)

    def device_step(tok_in, tok_grad, route_ids, gate_vals, *weights):
        tokens, top_k = route_ids.shape[1:]
        return tuple(step(2 * tokens * top_k // SLOTS, tok_in, tok_grad, jnp.swapaxes(route_ids, 1, 2), jnp.swapaxes(gate_vals, 1, 2), *weights))

    return jax.shard_map(device_step, mesh=mesh, in_specs=(tok_spec, tok_spec, route_spec, route_spec, whole_spec, expert_spec, expert_spec, expert_spec), out_specs=(tok_spec, tok_spec, whole_spec, expert_spec, expert_spec, expert_spec), check_vma=False)
```

```python
import functools

import jax
import jax.numpy as jnp
from jax import lax
from jax.experimental import pallas as pl
from jax.experimental.pallas import tpu as pltpu
from jax.sharding import PartitionSpec as P

TOK_AXES = ("rep", "ep", "dp")
F32 = jnp.float32
BF16 = jnp.bfloat16
LANES = 128
SIDE = 4
WAYS = (1, -1)
BUFS = (0, 1)
LAYERS = (1, 0)
ARRAYS = range(3)
SLOTS = 8
MESH = pl.DeviceIdType.MESH
VMEM_LIMIT = 63 << 20


def dot(a, b):
    return jnp.dot(a, b, preferred_element_type=F32)


def dot_nt(a, b):
    return lax.dot_general(a, b, (((1,), (1,)), ((), ())), preferred_element_type=F32)


def dot_tn(a, b):
    return lax.dot_general(a, b, (((0,), (0,)), ((), ())), preferred_element_type=F32)


class Place:
    def __init__(self):
        self.z, self.y, dp = lax.axis_index("rep"), lax.axis_index("ep"), lax.axis_index("dp")
        self.x, self.c = dp // 2, dp % 2

    def at(self, axis, step):
        z, y, x, c = self.z, self.y, self.x, self.c
        if axis == "z":
            z = (z + step + SIDE) % SIDE
        elif axis == "y":
            y = (y + step + SIDE) % SIDE
        elif axis == "x":
            x = (x + step + SIDE) % SIDE
        else:
            c = 1 - c
        return (z, y, x * 2 + c)


class Copies:
    def __init__(self, place, send, recv):
        self.place, self.send, self.recv, self.made, self.number, self.count = place, send, recv, {}, {}, 0

    def add(self, key, src, dst, axis, step, like=None):
        if like is None:
            n, self.count = self.count, self.count + 1
        else:
            n = self.number[like]
        self.number[key] = n
        self.made[key] = pltpu.make_async_remote_copy(src_ref=src, dst_ref=dst, send_sem=self.send.at[n], recv_sem=self.recv.at[n], device_id=self.place.at(axis, step), device_id_type=MESH)

    def start(self, *keys):
        for key in keys:
            self.made[key].start()

    def arrive(self, *keys):
        for key in keys:
            self.made[key].wait_recv()

    def sent(self, *keys):
        for key in keys:
            self.made[key].wait_send()


def greet(place):
    barrier = pltpu.get_barrier_semaphore()
    peers = [(axis, step) for axis in "xyz" for step in WAYS] + [("c", 0)]
    for axis, step in peers:
        pl.semaphore_signal(barrier, inc=1, device_id=place.at(axis, step), device_id_type=MESH)
    pl.semaphore_wait(barrier, len(peers))


class Gather:
    FROM = {2: -1, 3: 1, 6: 2}
    PASS = {2: 4, 3: 5, 6: 7}

    def __init__(self, layer, copies, place, own, whole):
        self.layer, self.copies, self.place, self.own, self.whole = layer, copies, place, own, whole
        rows, ff = own[0].shape[2], own[2].shape[2]
        self.cut = {"x": ((0, 0, rows // SIDE), (2, 0, ff // 2 // SIDE)), "z": ((1, 0, rows // SIDE), (2, ff // 2, ff // 2 // SIDE))}
        mine = {"x": place.x, "z": place.z}
        for color in ("x", "z"):
            for part in BUFS:
                self._add(("y", 2, color, part), color, part, None, 2, mine[color], None, "y", 1)
                self._add(("y", 3, color, part), color, part, None, 3, mine[color], None, "y", -1)
                if color == "x":
                    self._add(("y", 6, color, part), color, part, 2, 6, mine[color], None, "y", 1)
                else:
                    self._add(("y", 6, color, part), color, part, 3, 6, mine[color], None, "y", -1)
                for slot in (2, 3, 6):
                    for step in WAYS:
                        self._add(("near", slot, color, part, step), color, part, slot, slot, mine[color], None, color, step)
                        behind = (mine[color] - step + SIDE) % SIDE
                        self._add(("far", slot, color, part, step), color, part, slot, slot, behind, (1 - step) // 2, color, step)
        for slot, to in self.PASS.items():
            for array in ARRAYS:
                copies.add((layer, "pass", slot, array), whole[array].at[layer, slot], whole[array].at[layer, to], "c", 0)

    def _view(self, refs, index, color, part, quarter, half):
        array, base, size = self.cut[color][part]
        start = base + quarter * size
        if half is not None:
            size = size // 2
            start = start + half * size
        return refs[array].at[self.layer, index, pl.ds(pl.multiple_of(start, 16), size)]

    def _add(self, key, color, part, src_slot, dst_slot, quarter, half, axis, step):
        src = self._view(self.own, self.place.c, color, part, quarter, half) if src_slot is None else self._view(self.whole, src_slot, color, part, quarter, half)
        self.copies.add((self.layer,) + key, src, self._view(self.whole, dst_slot, color, part, quarter, half), axis, step)

    def _keys(self, *key, extra=()):
        return [(self.layer,) + key + (part,) + extra for part in BUFS]

    def lead(self):
        self.spread(2, "x")
        self.spread(3, "z")

    def lead_onward(self):
        self.onward(2, "x")
        self.onward(3, "z")

    def follow(self):
        self.spread(2, "z")
        self.spread(3, "x")

    def follow_onward(self):
        self.onward(2, "z")
        self.onward(3, "x")

    def last(self):
        self.spread(6, "x")
        self.spread(6, "z")

    def last_onward(self):
        self.onward(6, "x")
        self.onward(6, "z")

    def complete_y(self):
        self.complete(2)
        self.complete(3)

    def complete_last(self):
        self.complete(6)

    def passed_left(self):
        self.passed(2)

    def passed_right(self):
        self.passed(3)

    def passed_last(self):
        self.passed(6)

    def begin(self):
        for slot, color in ((2, "x"), (3, "z"), (2, "z"), (3, "x")):
            self.copies.start(*self._keys("y", slot, color))

    def spread(self, slot, color):
        self.copies.arrive(*self._keys("y", slot, color))
        if (slot, color) in ((2, "x"), (3, "z")):
            self.copies.start(*self._keys("y", 6, color))
        for step in WAYS:
            self.copies.start(*self._keys("near", slot, color, extra=(step,)))

    def onward(self, slot, color):
        for step in WAYS:
            self.copies.arrive(*self._keys("near", slot, color, extra=(step,)))
            self.copies.start(*self._keys("far", slot, color, extra=(step,)))

    def complete(self, slot):
        for color in ("x", "z"):
            for step in WAYS:
                self.copies.arrive(*self._keys("far", slot, color, extra=(step,)))
        self.copies.start(*[(self.layer, "pass", slot, array) for array in ARRAYS])

    def passed(self, slot):
        self.copies.arrive(*[(self.layer, "pass", slot, array) for array in ARRAYS])


GATHER_COPIES = 2 * (2 * 2 * (3 + 3 * 4) + 9)


def route(ids_ref, gate_ref, rows_ref, columns_ref, place):
    layers, _, tokens = ids_ref.shape
    below = lax.broadcasted_iota(jnp.int32, (tokens, tokens), 0) < lax.broadcasted_iota(jnp.int32, (tokens, tokens), 1)
    below = jnp.where(below, 1.0, 0.0).astype(BF16)
    lead = lax.broadcasted_iota(jnp.int32, (2 * SLOTS, tokens), 0)
    for layer in range(layers):
        ids, gates = ids_ref[layer], gate_ref[layer]
        off = ((ids >> 1) - place.y) & (SIDE - 1)
        odd = (ids + place.c) & 1
        slot = jnp.where(off == 0, odd, jnp.where(off == SIDE - 1, 2 + 2 * odd, jnp.where(off == 1, 3 + 2 * odd, 6 + odd)))
        hits = [slot[n : n + 1] == lead for n in BUFS]
        hit = hits[0] | hits[1]
        weight = jnp.where(hits[0], gates[0:1], 0.0) + jnp.where(hits[1], gates[1:2], 0.0)
        rank = jnp.where(hit, dot(jnp.where(hit, 1.0, 0.0).astype(BF16), below), -1.0)
        rows_ref[layer] = rank[:SLOTS].astype(jnp.int32)
        columns_ref[layer] = jnp.transpose(jnp.concatenate([rank[:SLOTS], weight[:SLOTS], jnp.zeros((LANES - 2 * SLOTS, tokens), F32)], axis=0))


def one_hot(rows_ref, layer, slot, cap):
    place = lax.broadcasted_iota(jnp.int32, (cap, rows_ref.shape[2]), 0)
    return jnp.where(rows_ref[layer, pl.ds(slot, 1), :] == place, 1.0, 0.0).astype(BF16)


def column(columns_ref, layer, index):
    lane = lax.broadcasted_iota(jnp.int32, columns_ref.shape[1:], 1)
    return jnp.sum(jnp.where(lane == index, columns_ref[layer], 0.0), axis=1, keepdims=True)


def one_hot_t(columns_ref, layer, slot, cap):
    place = lax.broadcasted_iota(jnp.int32, (columns_ref.shape[1], cap), 1)
    return jnp.where(column(columns_ref, layer, slot).astype(jnp.int32) == place, 1.0, 0.0).astype(BF16)


def add_to(dst, src):
    dst[...] = (dst[...].astype(F32) + src[...].astype(F32)).astype(BF16)


class RingSum:
    def __init__(self, copies, name, axis, block, first, second):
        self.copies, self.name, self.block, self.first, self.second = copies, name, block, first, second
        self.early, self.later = ([(name, when, step) for step in WAYS] for when in ("early", "later"))
        for half, step in enumerate(WAYS):
            copies.add(self.early[half], block(2, half), first.at[half], axis, step)
            copies.add(self.later[half], block(step, None), second.at[half], axis, step)

    def start(self):
        self.copies.start(*self.early)

    def onward(self):
        self.copies.arrive(*self.early)
        for half in BUFS:
            add_to(self.block(WAYS[half], half), self.first.at[half])
            self.copies.start(self.later[half])
        self.copies.sent(*self.early)

    def finish(self, out):
        self.copies.arrive(*self.later)
        out[...] = (self.block(0, None)[...].astype(F32) + self.second[0].astype(F32) + self.second[1].astype(F32)).astype(BF16)
        self.copies.sent(*self.later)


class RingSpread:
    def __init__(self, copies, name, axis, me, block, source=None, like=None):
        self.copies = copies
        self.near, self.far = ([(name, when, step) for step in WAYS] for when in ("near", "far"))
        for half, step in enumerate(WAYS):
            behind = (me - step + SIDE) % SIDE
            near, far = (None, None) if like is None else (like.near[half], like.far[half])
            copies.add(self.near[half], block(me, None) if source is None else source, block(me, None), axis, step, near)
            copies.add(self.far[half], block(behind, half), block(behind, half), axis, step, far)

    def start(self):
        self.copies.start(*self.near)

    def onward(self):
        for near, far in zip(self.near, self.far):
            self.copies.arrive(near)
            self.copies.start(far)

    def finish(self):
        self.copies.arrive(*self.far)
        self.copies.sent(*self.near, *self.far)


def slices(ref, lead, base, size):
    def block(index, half):
        start, rows = base + index * size, size
        if half is not None:
            rows = size // 2
            start = start + half * rows
        return ref.at[(*lead, pl.ds(pl.multiple_of(start, 16), rows))]

    return block


def slabs(ref):
    def block(index, half):
        if half is None:
            return ref.at[index]
        rows = ref.shape[1] // 2
        return ref.at[index, pl.ds(half * rows, rows)]

    return block


def total(ref):
    return (ref[0].astype(F32) + ref[1].astype(F32) + ref[2].astype(F32) + ref[3].astype(F32)).astype(BF16)


OWN_STEPS = {1: 0, 4: 1, 5: 2, 7: 3}
REDUCE_COPIES = 107
WEIGHTS1, INPUTS1, WEIGHTS0, INPUTS0, STEPS = (n * SLOTS for n in range(2, 7))


def kernel(cap, x0_ref, dy_ref, ids_ref, gate_ref, wd_ref, o1_ref, o3_ref, o2_ref, y_ref, dx_ref, gd_ref, g1_ref, g3_ref, g2_ref, h1_ref, h3_ref, h2_ref, kz_ref, ka_ref, kb_ref, kda_ref, kdb_ref, acc_ref, cur_ref, x1_ref, rows_ref, columns_ref, w1_ref, w3_ref, w2_ref, z_ref, a_ref, b_ref, m1_ref, m3_ref, m2_ref, d1_ref, d3_ref, d2_ref, s1_ref, s3_ref, s2_ref, r11_ref, r12_ref, r31_ref, r32_ref, t1_ref, t3_ref, y11_ref, y12_ref, y31_ref, y32_ref, y21_ref, y22_ref, u1_ref, u2_ref, l1_ref, l2_ref, c1_ref, c3_ref, cu_ref, cl_ref, f1_ref, f3_ref, fu_ref, fl_ref, dp_ref, dr_ref, dcx_ref, dcy_ref, dcz_ref, ds_ref, de_ref, put_sem, load_sem, keep_sem, save_sem, gsend_sem, grecv_sem, send_sem, recv_sem, credit):
    s = pl.program_id(0)
    place = Place()
    gathers = Copies(place, gsend_sem, grecv_sem)
    copies = Copies(place, send_sem, recv_sem)
    given, whole, bufs = (o1_ref, o3_ref, o2_ref), (h1_ref, h3_ref, h2_ref), (w1_ref, w3_ref, w2_ref)
    kept, acts = (kz_ref, ka_ref, kb_ref), (z_ref, a_ref, b_ref)
    deferred = (kda_ref, kdb_ref)
    g0, g1 = (Gather(l, gathers, place, given, whole) for l in BUFS)
    rows, ff = s1_ref.shape[1], s2_ref.shape[1]
    quarter, part = rows // SIDE, ff // 2 // SIDE
    half_d = rows // 2

    stage, mate, mine_of = (m1_ref, m3_ref, m2_ref), (d1_ref, d3_ref, d2_ref), (s1_ref, s3_ref, s2_ref)
    outs = (g1_ref, g3_ref, g2_ref)
    for buf in BUFS:
        for n in ARRAYS:
            copies.add(("pair", buf, n), stage[n], mate[n].at[buf], "c", 0)

    def ring_blocks(ref, q, me, base, size):
        block = slices(ref, (q,), base, size)
        return lambda offset, half: block((me + offset + SIDE) % SIDE, half)

    def group_blocks(ref):
        block = slabs(ref)
        return lambda offset, half: block({2: 0, 1: 1, -1: 2, 0: 3}[offset], half)

    first = {
        "x": [RingSum(copies, ("x", q), "x", ring_blocks(s1_ref, q, place.x, 0, quarter), r11_ref.at[q], r12_ref.at[q]) for q in range(SIDE)],
        "z": [RingSum(copies, ("z", q), "z", ring_blocks(s3_ref, q, place.z, 0, quarter), r31_ref.at[q], r32_ref.at[q]) for q in range(SIDE)],
    }
    mid = {"x": t1_ref, "z": t3_ref}
    on_y = {
        "x": RingSum(copies, "yx", "y", group_blocks(t1_ref), y11_ref, y12_ref),
        "z": RingSum(copies, "yz", "y", group_blocks(t3_ref), y31_ref, y32_ref),
        "w": RingSum(copies, "yw", "y", group_blocks(s2_ref), y21_ref, y22_ref),
    }
    inner = {
        "u": RingSum(copies, "u", "x", ring_blocks(s2_ref, 3, place.x, 0, part), u1_ref, u2_ref),
        "l": RingSum(copies, "l", "z", ring_blocks(s2_ref, 3, place.z, ff // 2, part), l1_ref, l2_ref),
    }
    ring_of = {"x": ("x", place.x), "u": ("x", place.x), "z": ("z", place.z), "l": ("z", place.z)}
    other_of = {"x": ("z", place.z), "u": ("z", place.z), "z": ("x", place.x), "l": ("x", place.x)}
    cross_ref = {"x": c1_ref, "z": c3_ref, "u": cu_ref, "l": cl_ref}
    done_ref = {"x": f1_ref, "z": f3_ref, "u": fu_ref, "l": fl_ref}
    out_of = {"x": (g1_ref, 0, quarter), "z": (g3_ref, 0, quarter), "u": (g2_ref, 0, part), "l": (g2_ref, ff // 2, part)}
    cross, final, puts = {}, {}, {}
    for i, k in enumerate(out_of):
        cross[k] = RingSpread(copies, ("cross", k), *other_of[k], slabs(cross_ref[k]))
        ref, base, size = out_of[k]
        for late in LAYERS:
            block = slices(ref, (late, place.c), base, size)
            final[k, late] = RingSpread(copies, ("final", k, late), *ring_of[k], block, source=done_ref[k], like=final.get((k, 1)))
            puts[k, late] = pltpu.make_async_copy(done_ref[k], block(ring_of[k][1], None), put_sem.at[i])
    mine, theirs = (pl.ds(pl.multiple_of(c * half_d, 16), half_d) for c in (place.c, 1 - place.c))
    for late in LAYERS:
        for n, out in enumerate(outs):
            copies.add(("pass", n, late), out.at[late, place.c], out.at[late, place.c], "c", 0, None if late else ("pass", n, 1))
    copies.add("dense pair", dp_ref.at[theirs], dr_ref, "c", 0)
    copies.add("dense pass", ds_ref, de_ref, "c", 0)
    dense_refs = {"y": dcy_ref, "x": dcx_ref, "z": dcz_ref}
    index_of = {"y": place.y, "x": place.x, "z": place.z}
    dense = {k: RingSpread(copies, ("dense", k), k, index_of[k], slabs(ref)) for k, ref in dense_refs.items()}

    def reduce_start(q):
        for k in ("x", "z"):
            first[k][q].start()

    def reduce_onward(q):
        for k in ("x", "z"):
            first[k][q].onward()

    def reduce_finish(q):
        for k in ("x", "z"):
            first[k][q].finish(mid[k].at[q])

    def y_start():
        for k in ("x", "z"):
            on_y[k].start()

    def y_onward():
        for k in ("x", "z"):
            on_y[k].onward()

    def y_finish():
        for k in ("x", "z"):
            on_y[k].finish(cross_ref[k].at[other_of[k][1]])
            cross[k].start()

    def w_finish():
        on_y["w"].finish(s2_ref.at[3])
        for k in ("u", "l"):
            inner[k].start()

    def inner_onward():
        for k in ("u", "l"):
            inner[k].onward()

    def inner_finish():
        for k in ("u", "l"):
            inner[k].finish(cross_ref[k].at[other_of[k][1]])
            cross[k].start()

    def cross_onward(*keys):
        for k in keys:
            cross[k].onward()

    def cross_finish(late, *keys):
        for k in keys:
            cross[k].finish()
            done_ref[k][...] = total(cross_ref[k])
            puts[k, late].start()
            final[k, late].start()

    def final_onward(late, *keys):
        for k in keys:
            final[k, late].onward()

    def final_finish(late, *keys):
        for k in keys:
            final[k, late].finish()
            puts[k, late].wait()
        copies.start(*[("pass", n, late) for n in ARRAYS if ("xzu"[n] in keys)])

    def pass_finish(late):
        keys = [("pass", n, late) for n in ARRAYS]
        copies.arrive(*keys)
        copies.sent(*keys)

    def dense_sum():
        copies.arrive("dense pair")
        dcy_ref[place.y] = (dp_ref[mine].astype(F32) + dr_ref[...].astype(F32)).astype(BF16)
        copies.sent("dense pair")
        dense["y"].start()

    def dense_next(k, follow):
        dense[k].finish()
        dense_refs[follow][index_of[follow]] = total(dense_refs[k])
        dense[follow].start()

    def dense_pass(late):
        dense["z"].finish()
        ds_ref[...] = total(dcz_ref)
        gd_ref[late, mine] = ds_ref[...]
        copies.start("dense pass")

    def dense_finish(late):
        copies.arrive("dense pass")
        gd_ref[late, theirs] = de_ref[...]
        copies.sent("dense pass")

    def copy(src, dst, sem):
        return pltpu.make_async_copy(src, dst, sem)

    def weights(layer, slot, arrays, buf, is_given=False):
        for n in arrays:
            src = given[n].at[layer, (place.c + slot) % 2] if is_given else whole[n].at[layer, slot]
            yield copy(src, bufs[n].at[buf], load_sem.at[buf, n])

    def saved(layer, slot, buf):
        for n in ARRAYS:
            yield copy(kept[n].at[layer, slot], acts[n].at[buf], load_sem.at[buf, 3 + n])

    def forward_loads(step, do):
        buf, slot = step % 2, step % SLOTS
        for is_given in (True, False):

            @pl.when((slot < 2) == is_given)
            def _():
                for item in weights(step // SLOTS, slot, ARRAYS, buf, is_given):
                    do(item)

    def weights_loads(step):
        layer, slot, buf = layer_of(step), SLOTS - 1 - step % SLOTS, (step + 1) % 2
        return [*weights(layer, slot, [2], buf), *saved(layer, slot, buf)]

    def inputs_loads(step):
        layer, slot, buf = layer_of(step), SLOTS - 1 - step % SLOTS, (step + 1) % 2
        return [*weights(layer, slot, BUFS, buf)] + [copy(deferred[n].at[slot], acts[n + 1].at[buf], load_sem.at[buf, 4 + n]) for n in BUFS]

    def load(step):
        forward_loads(step, lambda item: item.start())

    def layer_of(step):
        return 1 - (step - WEIGHTS1) // (2 * SLOTS)

    def keeps(step):
        return [copy(bufs[n].at[step % 2], whole[n].at[step // SLOTS, step % SLOTS], keep_sem.at[step % 2, n]) for n in ARRAYS]

    def saves(step):
        return [copy(acts[n].at[step % 2], kept[n].at[step // SLOTS, step % SLOTS], save_sem.at[step % 2, n]) for n in ARRAYS]

    def defers(step):
        return [copy(acts[n + 1].at[2], deferred[n].at[SLOTS - 1 - step % SLOTS], save_sem.at[0, n]) for n in BUFS]

    def wait(items):
        for item in items:
            item.wait()

    def start(items):
        for item in items:
            item.start()

    def ending():
        dense_sum()
        y_finish()
        inner_finish()
        dense["y"].onward()
        cross_onward("x", "z")
        dense_next("y", "x")
        cross_onward("u", "l")
        cross_finish(0, "x", "z")
        dense["x"].onward()
        cross_finish(0, "u", "l")
        final_onward(0, "x", "z")
        dense_next("x", "z")
        final_onward(0, "u", "l")
        final_finish(0, "x", "z")
        dense["z"].onward()
        final_finish(0, "u", "l")
        dense_pass(0)
        pass_finish(0)
        dense_finish(0)

    before, middle, after = {}, {}, {}

    def plan(table, first, *stages):
        for n, stage in enumerate(stages):
            table.setdefault(first + n, []).extend(stage)

    on, done = lambda q: lambda: reduce_onward(q), lambda q: lambda: reduce_finish(q)
    plan(before, 1, [g0.lead], [g0.follow, g0.lead_onward, g0.follow_onward, g0.last, g0.complete_y, lambda: load(s), g1.begin], [g0.passed_left])
    plan(before, 4, [g0.last_onward, g1.lead, g0.passed_right], [g1.follow, g0.complete_last], [g0.passed_last], [g1.lead_onward])
    plan(before, SLOTS, [g1.follow_onward, g1.last], [g1.complete_y], [], [g1.last_onward, g1.passed_left], [g1.passed_right], [g1.complete_last], [g1.passed_last])
    late = ("x", "z", "u", "l")
    plan(before, WEIGHTS0, [lambda: copies.start("dense pair")], [inner_finish], [dense["y"].onward], [lambda: cross_onward(*late), lambda: dense_next("y", "x")])
    plan(before, WEIGHTS0 + 5, [dense["x"].onward], [lambda: dense_next("x", "z")], [lambda: final_onward(1, *late)])
    plan(middle, WEIGHTS0, [dense_sum, y_finish], [], [], [], [lambda: cross_finish(1, *late)], [], [], [dense["z"].onward])
    plan(before, INPUTS0 + 1, [lambda: dense_pass(1), lambda: final_finish(1, *late)], [], [lambda: dense_finish(1)], [], [lambda: pass_finish(1)])
    for base in (WEIGHTS1, WEIGHTS0):
        plan(before, base + 2, [on_y["w"].start], [], [], [], [on_y["w"].onward])
        plan(middle, base + 3, [on(0)], [], [done(0), y_start], [on(1)], [on(2)])
        plan(before, base + SLOTS, [done(1)], [], [done(2), y_onward], [on(3)], [], [w_finish], [done(3)], [inner_onward])
        for step, q in OWN_STEPS.items():
            plan(after, base + step, [lambda q=q: reduce_start(q)])

    def hooks(table, *phases):
        for phase in phases:
            mine = {step: stages for step, stages in sorted(table.items()) if phase <= step < phase + SLOTS}
            if mine:

                @pl.when(s // SLOTS == phase // SLOTS)
                def _(mine=mine):
                    for step, stages in mine.items():

                        @pl.when(s == step)
                        def _(stages=stages):
                            for stage in stages:
                                stage()

    phase, t = s // SLOTS, s % SLOTS
    forth, back = s % 2, (s + 1) % 2

    @pl.when(s == 0)
    def _():
        load(0)
        greet(place)
        g0.begin()
        load(1)
        route(ids_ref, gate_ref, rows_ref, columns_ref, place)

    def enter(x):
        cur_ref[...] = (x.astype(F32) + dot(x, wd_ref[phase])).astype(BF16)
        acc_ref[...] = jnp.zeros_like(acc_ref)

    def leave(out_ref):
        out_ref[...] = (cur_ref[...].astype(F32) + acc_ref[...]).astype(BF16)

    @pl.when(s < WEIGHTS1)
    def _():
        hooks(before, 0, SLOTS)
        forward_loads(s, lambda item: item.wait())
        pl.when(s > 1)(lambda: wait(saves(s - 2)))
        pl.when((s > 0) & (s != 1) & (s < WEIGHTS1 - 1))(lambda: load(s + 1))

        @pl.when(t < 2)
        def _():
            start(keeps(s))
            pl.when(s == 0)(lambda: enter(x0_ref[...]))
            pl.when(s == SLOTS)(lambda: enter(x1_ref[...]))

        layer, slot = phase, t
        z = dot(one_hot(rows_ref, layer, slot, cap), cur_ref[...]).astype(BF16)
        z_ref[forth] = z
        a = dot(z, w1_ref[forth]).astype(BF16)
        b = dot(z, w3_ref[forth]).astype(BF16)
        a_ref[forth] = a
        b_ref[forth] = b
        h = (jax.nn.silu(a.astype(F32)) * b.astype(F32)).astype(BF16)
        o = dot(h, w2_ref[forth]).astype(BF16)
        acc_ref[...] += column(columns_ref, layer, SLOTS + slot) * dot(one_hot_t(columns_ref, layer, slot, cap), o)
        pl.when(s < WEIGHTS1 - 1)(lambda: start(saves(s)))
        pl.when(t < 2)(lambda: wait(keeps(s)))

        @pl.when(t == SLOTS - 1)
        def _():
            pl.when(s == SLOTS - 1)(lambda: leave(x1_ref))
            pl.when(s == WEIGHTS1 - 1)(lambda: leave(y_ref))

    @pl.when((phase == WEIGHTS1 // SLOTS) | (phase == WEIGHTS0 // SLOTS))
    def _():
        layer, slot = layer_of(s), SLOTS - 1 - t
        hooks(before, WEIGHTS1, WEIGHTS0)

        @pl.when(s == WEIGHTS1)
        def _():
            wait(saves(s - 2))
            cur_ref[...] = dy_ref[...]
            acc_ref[...] = dy_ref[...].astype(F32)

        pl.when(s > WEIGHTS1)(lambda: wait(weights_loads(s)))
        pl.when(t > 0)(lambda: wait(defers(s - 1)))
        pl.when(t < SLOTS - 1)(lambda: start(weights_loads(s + 1)))
        pl.when(t == SLOTS - 1)(lambda: start(inputs_loads(s + 1)))

        grad_gated = (column(columns_ref, layer, SLOTS + slot) * cur_ref[...].astype(F32)).astype(BF16)
        do = dot(one_hot(rows_ref, layer, slot, cap), grad_gated).astype(BF16)
        dh = dot_nt(do, w2_ref[back])
        a = a_ref[back].astype(F32)
        b = b_ref[back].astype(F32)
        sig = jax.nn.sigmoid(a)
        act = a * sig
        h = (act * b).astype(BF16)
        db = (dh * act).astype(BF16)
        da = (dh * b * sig * (1.0 + a * (1.0 - sig))).astype(BF16)
        a_ref[2] = da
        b_ref[2] = db
        z = z_ref[back]
        start(defers(s))
        hooks(middle, WEIGHTS1, WEIGHTS0)

        def weight_grads():
            return dot_tn(z, da), dot_tn(z, db), dot_tn(h, do)

        is_own = functools.reduce(jnp.logical_or, [t == step for step in OWN_STEPS])
        group = t // 4 + t // 5 + t // 7
        into = (t // 2 + t // 3) % 2
        turn = t + (1 - layer) * SLOTS

        @pl.when(jnp.logical_not(is_own))
        def _():
            for buf in BUFS:
                pl.when((turn > 0) & (into == 1 - buf))(lambda buf=buf: copies.sent(*[("pair", buf, n) for n in ARRAYS]))

            for ref, grad in zip(stage, weight_grads()):
                ref[...] = grad.astype(BF16)

            pl.when(turn >= 3)(lambda: pl.semaphore_wait(credit.at[into], 1))
            for buf in BUFS:
                pl.when(into == buf)(lambda buf=buf: copies.start(*[("pair", buf, n) for n in ARRAYS]))

        @pl.when(is_own)
        def _():
            for buf in BUFS:
                pl.when(group % 2 == buf)(lambda buf=buf: copies.arrive(*[("pair", buf, n) for n in ARRAYS]))

            for ref, add, grad in zip(mine_of, mate, weight_grads()):
                ref[group] = (grad + add[group % 2].astype(F32)).astype(BF16)

            @pl.when(turn < 2 * SLOTS - 3)
            def _():
                pl.semaphore_signal(credit.at[group % 2], inc=1, device_id=place.at("c", 0), device_id_type=MESH)

            hooks(after, WEIGHTS1, WEIGHTS0)

    def leave_back(layer, x, out_ref):
        grad = acc_ref[...]
        grad_b = grad.astype(BF16)
        dp_ref[...] = dot_tn(x, grad_b).astype(BF16)
        out_ref[...] = (grad + dot_nt(grad_b, wd_ref[layer])).astype(BF16)

    @pl.when((phase == INPUTS1 // SLOTS) | (phase == INPUTS0 // SLOTS))
    def _():
        layer, slot = layer_of(s), SLOTS - 1 - t
        hooks(before, INPUTS1, INPUTS0)
        wait(inputs_loads(s))
        pl.when(t == 0)(lambda: wait(defers(s - 1)))
        pl.when(t < SLOTS - 1)(lambda: start(inputs_loads(s + 1)))
        pl.when(s == WEIGHTS0 - 1)(lambda: start(weights_loads(s + 1)))
        dz = (dot_nt(a_ref[back], w1_ref[back]) + dot_nt(b_ref[back], w3_ref[back])).astype(BF16)
        acc_ref[...] += dot(one_hot_t(columns_ref, layer, slot, cap), dz)

        @pl.when(s == WEIGHTS0 - 1)
        def _():
            leave_back(1, x1_ref[...], cur_ref)
            acc_ref[...] = cur_ref[...].astype(F32)

        @pl.when(s == STEPS - 1)
        def _():
            leave_back(0, x0_ref[...], dx_ref)
            copies.start("dense pair")
            ending()
            copies.sent(*[("pair", 1, n) for n in ARRAYS])
            gathers.sent(*gathers.made)


def step(cap, x0, dy, ids, gates, wd, w1, w3, w2):
    tokens, width = dy.shape
    layers, local, _, ff = w1.shape
    quarter, part = width // SIDE, ff // 2 // SIDE
    hbm = pl.BlockSpec(memory_space=pl.ANY)

    def fixed(shape):
        return pl.BlockSpec(shape, lambda s: (0,) * len(shape), pipeline_mode=pl.Buffered(1))

    def buf(*shape):
        return pltpu.VMEM(shape, BF16)

    def dma(*shape):
        return pltpu.SemaphoreType.DMA(shape)

    shape = jax.ShapeDtypeStruct
    ups, downs = [(width, ff), (width, ff), (ff, width)], [(quarter, ff), (part, width)]
    acts = [(cap, width), (cap, ff), (cap, ff)]
    scratch = [pltpu.VMEM((tokens, width), F32), buf(tokens, width), buf(tokens, width), pltpu.VMEM((layers, SLOTS, tokens), jnp.int32), pltpu.VMEM((layers, tokens, LANES), F32)]
    scratch += [buf(2, *u) for u in ups] + [buf(2, *acts[0]), buf(3, *acts[1]), buf(3, *acts[2])]
    scratch += [buf(*u) for u in ups] + [buf(2, *u) for u in ups] + [buf(SIDE, *u) for u in ups]
    scratch += [buf(SIDE, 2, quarter // 2, ff), buf(SIDE, 2, quarter, ff)] * 2
    scratch += [buf(SIDE, quarter, ff)] * 2
    scratch += [buf(2, quarter // 2, ff), buf(2, quarter, ff)] * 2 + [buf(2, ff // 2, width), buf(2, ff, width)]
    scratch += [buf(2, part // 2, width), buf(2, part, width)] * 2
    scratch += [buf(SIDE, quarter, ff)] * 2 + [buf(SIDE, part, width)] * 2
    scratch += [buf(quarter, ff)] * 2 + [buf(part, width)] * 2
    scratch += [buf(width, width), buf(width // 2, width)] + [buf(SIDE, width // 2, width)] * 3 + [buf(width // 2, width)] * 2
    scratch += [dma(4), dma(2, 6), dma(2, 3), dma(2, 3), dma(GATHER_COPIES), dma(GATHER_COPIES), dma(REDUCE_COPIES), dma(REDUCE_COPIES), pltpu.SemaphoreType.REGULAR((2,))]
    results = [(tokens, width), (tokens, width), (layers, width, width)]
    kept = [(layers, local, *u) for u in ups] + [(layers, SLOTS, *u) for u in ups + acts] + [(SLOTS, cap, ff)] * 2
    return pl.pallas_call(
        functools.partial(kernel, cap),
        grid=(STEPS,),
        in_specs=[fixed(v.shape) for v in (x0, dy, ids, gates, wd)] + [hbm] * 3,
        out_specs=[fixed(r) for r in results] + [hbm] * len(kept),
        out_shape=[shape(r, BF16) for r in results + kept],
        scratch_shapes=scratch,
        compiler_params=pltpu.CompilerParams(vmem_limit_bytes=VMEM_LIMIT, collective_id=0, has_side_effects=True),
        name="step",
    )(x0, dy, ids, gates, wd, w1, w3, w2)[:6]


def solution(mesh):
    tok_spec = P(TOK_AXES, None)
    route_spec = P(None, TOK_AXES, None)
    expert_spec = P(None, "ep", None, None)
    whole_spec = P(None, None, None)

    def device_step(tok_in, tok_grad, route_ids, gate_vals, *weights):
        tokens, top_k = route_ids.shape[1:]
        return tuple(step(2 * tokens * top_k // SLOTS, tok_in, tok_grad, jnp.swapaxes(route_ids, 1, 2), jnp.swapaxes(gate_vals, 1, 2), *weights))

    return jax.shard_map(device_step, mesh=mesh, in_specs=(tok_spec, tok_spec, route_spec, route_spec, whole_spec, expert_spec, expert_spec, expert_spec), out_specs=(tok_spec, tok_spec, whole_spec, expert_spec, expert_spec, expert_spec), check_vma=False)
```

```python
import functools

import jax
import jax.numpy as jnp
from jax import lax
from jax.experimental import pallas as pl
from jax.experimental.pallas import tpu as pltpu
from jax.sharding import PartitionSpec as P

TOK_AXES = ("rep", "ep", "dp")
F32 = jnp.float32
BF16 = jnp.bfloat16
LANES = 128
SIDE = 4
WAYS = (1, -1)
BUFS = (0, 1)
LAYERS = (1, 0)
ARRAYS = range(3)
SLOTS = 8
MESH = pl.DeviceIdType.MESH
VMEM_LIMIT = 63 << 20


def dot(a, b):
    return jnp.dot(a, b, preferred_element_type=F32)


def dot_nt(a, b):
    return lax.dot_general(a, b, (((1,), (1,)), ((), ())), preferred_element_type=F32)


def dot_tn(a, b):
    return lax.dot_general(a, b, (((0,), (0,)), ((), ())), preferred_element_type=F32)


class Place:
    def __init__(self):
        self.z, self.y, dp = lax.axis_index("rep"), lax.axis_index("ep"), lax.axis_index("dp")
        self.x, self.c = dp // 2, dp % 2

    def at(self, axis, step):
        z, y, x, c = self.z, self.y, self.x, self.c
        if axis == "z":
            z = (z + step + SIDE) % SIDE
        elif axis == "y":
            y = (y + step + SIDE) % SIDE
        elif axis == "x":
            x = (x + step + SIDE) % SIDE
        else:
            c = 1 - c
        return (z, y, x * 2 + c)


class Copies:
    def __init__(self, place, send, recv):
        self.place, self.send, self.recv, self.made, self.number, self.count, self.over = place, send, recv, {}, {}, 0, set()

    def add(self, key, src, dst, axis, step, like=None):
        if like is None:
            n, self.count = self.count, self.count + 1
        else:
            n = self.number[like]
        self.number[key] = n
        self.made[key] = pltpu.make_async_remote_copy(src_ref=src, dst_ref=dst, send_sem=self.send.at[n], recv_sem=self.recv.at[n], device_id=self.place.at(axis, step), device_id_type=MESH)

    def start(self, *keys):
        for key in keys:
            self.made[key].start()

    def arrive(self, *keys):
        for key in keys:
            self.made[key].wait_recv()

    def sent(self, *keys):
        for key in keys:
            self.made[key].wait_send()
            self.over.add(key)

    def drain(self):
        self.sent(*[key for key in self.made if key not in self.over])


def greet(place):
    barrier = pltpu.get_barrier_semaphore()
    peers = [(axis, step) for axis in "xyz" for step in WAYS] + [("c", 0)]
    for axis, step in peers:
        pl.semaphore_signal(barrier, inc=1, device_id=place.at(axis, step), device_id_type=MESH)
    pl.semaphore_wait(barrier, len(peers))


class Gather:
    FROM = {2: -1, 3: 1, 6: 2}
    PASS = {2: 4, 3: 5, 6: 7}

    def __init__(self, layer, copies, place, own, whole):
        self.layer, self.copies, self.place, self.own, self.whole = layer, copies, place, own, whole
        rows, ff = own[0].shape[2], own[2].shape[2]
        self.cut = {"x": ((0, 0, rows // SIDE), (2, 0, ff // 2 // SIDE)), "z": ((1, 0, rows // SIDE), (2, ff // 2, ff // 2 // SIDE))}
        mine = {"x": place.x, "z": place.z}
        for color in ("x", "z"):
            for part in BUFS:
                self._add(("y", 2, color, part), color, part, None, 2, mine[color], None, "y", 1)
                self._add(("y", 3, color, part), color, part, None, 3, mine[color], None, "y", -1)
                if color == "x":
                    self._add(("y", 6, color, part), color, part, 2, 6, mine[color], None, "y", 1)
                else:
                    self._add(("y", 6, color, part), color, part, 3, 6, mine[color], None, "y", -1)
                for slot in (2, 3, 6):
                    for step in WAYS:
                        self._add(("near", slot, color, part, step), color, part, slot, slot, mine[color], None, color, step)
                        behind = (mine[color] - step + SIDE) % SIDE
                        self._add(("far", slot, color, part, step), color, part, slot, slot, behind, (1 - step) // 2, color, step)
        for slot, to in self.PASS.items():
            for array in ARRAYS:
                copies.add((layer, "pass", slot, array), whole[array].at[layer, slot], whole[array].at[layer, to], "c", 0)

    def _view(self, refs, index, color, part, quarter, half):
        array, base, size = self.cut[color][part]
        start = base + quarter * size
        if half is not None:
            size = size // 2
            start = start + half * size
        return refs[array].at[self.layer, index, pl.ds(pl.multiple_of(start, 16), size)]

    def _add(self, key, color, part, src_slot, dst_slot, quarter, half, axis, step):
        src = self._view(self.own, self.place.c, color, part, quarter, half) if src_slot is None else self._view(self.whole, src_slot, color, part, quarter, half)
        self.copies.add((self.layer,) + key, src, self._view(self.whole, dst_slot, color, part, quarter, half), axis, step)

    def _keys(self, *key, extra=()):
        return [(self.layer,) + key + (part,) + extra for part in BUFS]

    def lead(self):
        self.spread(2, "x")
        self.spread(3, "z")

    def lead_onward(self):
        self.onward(2, "x")
        self.onward(3, "z")

    def follow(self):
        self.spread(2, "z")
        self.spread(3, "x")

    def follow_onward(self):
        self.onward(2, "z")
        self.onward(3, "x")

    def last(self):
        self.spread(6, "x")
        self.spread(6, "z")

    def last_onward(self):
        self.onward(6, "x")
        self.onward(6, "z")

    def complete_y(self):
        self.complete(2)
        self.complete(3)

    def complete_last(self):
        self.complete(6)

    def passed_left(self):
        self.passed(2)

    def passed_right(self):
        self.passed(3)

    def passed_last(self):
        self.passed(6)

    def begin(self):
        self.copies.start(*self._keys("y", 2, "x"), *self._keys("y", 3, "z"))

    def second(self):
        self.copies.sent(*self._keys("y", 2, "x"), *self._keys("y", 3, "z"))
        self.copies.start(*self._keys("y", 2, "z"), *self._keys("y", 3, "x"))

    def third(self):
        self.copies.sent(*self._keys("y", 2, "z"), *self._keys("y", 3, "x"))
        self.copies.start(*self._keys("y", 6, "x"), *self._keys("y", 6, "z"))

    def spread(self, slot, color):
        self.copies.arrive(*self._keys("y", slot, color))
        for step in WAYS:
            self.copies.start(*self._keys("near", slot, color, extra=(step,)))

    def onward(self, slot, color):
        for step in WAYS:
            self.copies.arrive(*self._keys("near", slot, color, extra=(step,)))
            self.copies.start(*self._keys("far", slot, color, extra=(step,)))

    def complete(self, slot):
        for color in ("x", "z"):
            for step in WAYS:
                self.copies.arrive(*self._keys("far", slot, color, extra=(step,)))
        self.copies.start(*[(self.layer, "pass", slot, array) for array in ARRAYS])

    def passed(self, slot):
        self.copies.arrive(*[(self.layer, "pass", slot, array) for array in ARRAYS])


GATHER_COPIES = 2 * (2 * 2 * (3 + 3 * 4) + 9)


def route(ids_ref, gate_ref, rows_ref, columns_ref, place):
    layers, _, tokens = ids_ref.shape
    below = lax.broadcasted_iota(jnp.int32, (tokens, tokens), 0) < lax.broadcasted_iota(jnp.int32, (tokens, tokens), 1)
    below = jnp.where(below, 1.0, 0.0).astype(BF16)
    lead = lax.broadcasted_iota(jnp.int32, (2 * SLOTS, tokens), 0)
    for layer in range(layers):
        ids, gates = ids_ref[layer], gate_ref[layer]
        off = ((ids >> 1) - place.y) & (SIDE - 1)
        odd = (ids + place.c) & 1
        slot = jnp.where(off == 0, odd, jnp.where(off == SIDE - 1, 2 + 2 * odd, jnp.where(off == 1, 3 + 2 * odd, 6 + odd)))
        hits = [slot[n : n + 1] == lead for n in BUFS]
        hit = hits[0] | hits[1]
        weight = jnp.where(hits[0], gates[0:1], 0.0) + jnp.where(hits[1], gates[1:2], 0.0)
        rank = jnp.where(hit, dot(jnp.where(hit, 1.0, 0.0).astype(BF16), below), -1.0)
        rows_ref[layer] = rank[:SLOTS].astype(jnp.int32)
        columns_ref[layer] = jnp.transpose(jnp.concatenate([rank[:SLOTS], weight[:SLOTS], jnp.zeros((LANES - 2 * SLOTS, tokens), F32)], axis=0))


def one_hot(rows_ref, layer, slot, cap):
    place = lax.broadcasted_iota(jnp.int32, (cap, rows_ref.shape[2]), 0)
    return jnp.where(rows_ref[layer, pl.ds(slot, 1), :] == place, 1.0, 0.0).astype(BF16)


def column(columns_ref, layer, index):
    lane = lax.broadcasted_iota(jnp.int32, columns_ref.shape[1:], 1)
    return jnp.sum(jnp.where(lane == index, columns_ref[layer], 0.0), axis=1, keepdims=True)


def one_hot_t(columns_ref, layer, slot, cap):
    place = lax.broadcasted_iota(jnp.int32, (columns_ref.shape[1], cap), 1)
    return jnp.where(column(columns_ref, layer, slot).astype(jnp.int32) == place, 1.0, 0.0).astype(BF16)


def add_to(dst, src):
    dst[...] = (dst[...].astype(F32) + src[...].astype(F32)).astype(BF16)


class RingSum:
    def __init__(self, copies, name, axis, block, first, second):
        self.copies, self.name, self.block, self.first, self.second = copies, name, block, first, second
        self.early, self.later = ([(name, when, step) for step in WAYS] for when in ("early", "later"))
        for half, step in enumerate(WAYS):
            copies.add(self.early[half], block(2, half), first.at[half], axis, step)
            copies.add(self.later[half], block(step, None), second.at[half], axis, step)

    def start(self):
        self.copies.start(*self.early)

    def onward(self):
        self.copies.arrive(*self.early)
        for half in BUFS:
            add_to(self.block(WAYS[half], half), self.first.at[half])
            self.copies.start(self.later[half])
        self.copies.sent(*self.early)

    def finish(self, out):
        self.copies.arrive(*self.later)
        out[...] = (self.block(0, None)[...].astype(F32) + self.second[0].astype(F32) + self.second[1].astype(F32)).astype(BF16)
        self.copies.sent(*self.later)


class RingSpread:
    def __init__(self, copies, name, axis, me, block, source=None, like=None):
        self.copies = copies
        self.near, self.far = ([(name, when, step) for step in WAYS] for when in ("near", "far"))
        for half, step in enumerate(WAYS):
            behind = (me - step + SIDE) % SIDE
            near, far = (None, None) if like is None else (like.near[half], like.far[half])
            copies.add(self.near[half], block(me, None) if source is None else source, block(me, None), axis, step, near)
            copies.add(self.far[half], block(behind, half), block(behind, half), axis, step, far)

    def start(self):
        self.copies.start(*self.near)

    def onward(self):
        for near, far in zip(self.near, self.far):
            self.copies.arrive(near)
            self.copies.start(far)

    def finish(self):
        self.copies.arrive(*self.far)
        self.copies.sent(*self.near, *self.far)


def slices(ref, lead, base, size):
    def block(index, half):
        start, rows = base + index * size, size
        if half is not None:
            rows = size // 2
            start = start + half * rows
        return ref.at[(*lead, pl.ds(pl.multiple_of(start, 16), rows))]

    return block


def slabs(ref):
    def block(index, half):
        if half is None:
            return ref.at[index]
        rows = ref.shape[1] // 2
        return ref.at[index, pl.ds(half * rows, rows)]

    return block


def total(ref):
    return (ref[0].astype(F32) + ref[1].astype(F32) + ref[2].astype(F32) + ref[3].astype(F32)).astype(BF16)


OWN_STEPS = {1: 0, 4: 1, 5: 2, 7: 3}
REDUCE_COPIES = 107
WEIGHTS1, INPUTS1, WEIGHTS0, INPUTS0, STEPS = (n * SLOTS for n in range(2, 7))


def kernel(cap, x0_ref, dy_ref, ids_ref, gate_ref, wd_ref, o1_ref, o3_ref, o2_ref, y_ref, dx_ref, gdense_ref, g1_ref, g3_ref, g2_ref, h1_ref, h3_ref, h2_ref, kz_ref, ka_ref, kb_ref, kda_ref, kdb_ref, acc_ref, cur_ref, x1_ref, hold_ref, gd_ref, rows_ref, columns_ref, w1_ref, w3_ref, w2_ref, z_ref, a_ref, b_ref, m1_ref, m3_ref, m2_ref, d1_ref, d3_ref, d2_ref, s1_ref, s3_ref, s2_ref, r11_ref, r12_ref, r31_ref, r32_ref, t1_ref, t3_ref, y11_ref, y12_ref, y31_ref, y32_ref, y21_ref, y22_ref, u1_ref, u2_ref, l1_ref, l2_ref, c1_ref, c3_ref, cu_ref, cl_ref, f1_ref, f3_ref, fu_ref, fl_ref, dp_ref, dr_ref, dcx_ref, dcy_ref, dcz_ref, ds_ref, de_ref, put_sem, load_sem, keep_sem, save_sem, gsend_sem, grecv_sem, send_sem, recv_sem, credit):
    s = pl.program_id(0)
    place = Place()
    gathers = Copies(place, gsend_sem, grecv_sem)
    copies = Copies(place, send_sem, recv_sem)
    given, whole, bufs = (o1_ref, o3_ref, o2_ref), (h1_ref, h3_ref, h2_ref), (w1_ref, w3_ref, w2_ref)
    kept, acts = (kz_ref, ka_ref, kb_ref), (z_ref, a_ref, b_ref)
    deferred = (kda_ref, kdb_ref)
    g0, g1 = (Gather(l, gathers, place, given, whole) for l in BUFS)
    rows, ff = s1_ref.shape[1], s2_ref.shape[1]
    quarter, part = rows // SIDE, ff // 2 // SIDE
    half_d = rows // 2

    stage, mate, mine_of = (m1_ref, m3_ref, m2_ref), (d1_ref, d3_ref, d2_ref), (s1_ref, s3_ref, s2_ref)
    outs = (g1_ref, g3_ref, g2_ref)
    for buf in BUFS:
        for n in ARRAYS:
            copies.add(("pair", buf, n), stage[n], mate[n].at[buf], "c", 0)

    def ring_blocks(ref, q, me, base, size):
        block = slices(ref, (q,), base, size)
        return lambda offset, half: block((me + offset + SIDE) % SIDE, half)

    def group_blocks(ref):
        block = slabs(ref)
        return lambda offset, half: block({2: 0, 1: 1, -1: 2, 0: 3}[offset], half)

    first = {
        "x": [RingSum(copies, ("x", q), "x", ring_blocks(s1_ref, q, place.x, 0, quarter), r11_ref.at[q], r12_ref.at[q]) for q in range(SIDE)],
        "z": [RingSum(copies, ("z", q), "z", ring_blocks(s3_ref, q, place.z, 0, quarter), r31_ref.at[q], r32_ref.at[q]) for q in range(SIDE)],
    }
    mid = {"x": t1_ref, "z": t3_ref}
    on_y = {
        "x": RingSum(copies, "yx", "y", group_blocks(t1_ref), y11_ref, y12_ref),
        "z": RingSum(copies, "yz", "y", group_blocks(t3_ref), y31_ref, y32_ref),
        "w": RingSum(copies, "yw", "y", group_blocks(s2_ref), y21_ref, y22_ref),
    }
    inner = {
        "u": RingSum(copies, "u", "x", ring_blocks(s2_ref, 3, place.x, 0, part), u1_ref, u2_ref),
        "l": RingSum(copies, "l", "z", ring_blocks(s2_ref, 3, place.z, ff // 2, part), l1_ref, l2_ref),
    }
    ring_of = {"x": ("x", place.x), "u": ("x", place.x), "z": ("z", place.z), "l": ("z", place.z)}
    other_of = {"x": ("z", place.z), "u": ("z", place.z), "z": ("x", place.x), "l": ("x", place.x)}
    cross_ref = {"x": c1_ref, "z": c3_ref, "u": cu_ref, "l": cl_ref}
    done_ref = {"x": f1_ref, "z": f3_ref, "u": fu_ref, "l": fl_ref}
    out_of = {"x": (g1_ref, 0, quarter), "z": (g3_ref, 0, quarter), "u": (g2_ref, 0, part), "l": (g2_ref, ff // 2, part)}
    cross, final, puts = {}, {}, {}
    for i, k in enumerate(out_of):
        cross[k] = RingSpread(copies, ("cross", k), *other_of[k], slabs(cross_ref[k]))
        ref, base, size = out_of[k]
        for late in LAYERS:
            block = slices(ref, (late, place.c), base, size)
            final[k, late] = RingSpread(copies, ("final", k, late), *ring_of[k], block, source=done_ref[k], like=final.get((k, 1)))
            puts[k, late] = pltpu.make_async_copy(done_ref[k], block(ring_of[k][1], None), put_sem.at[i])
    mine, theirs = (pl.ds(pl.multiple_of(c * half_d, 16), half_d) for c in (place.c, 1 - place.c))
    for late in LAYERS:
        for n, out in enumerate(outs):
            copies.add(("pass", n, late), out.at[late, place.c], out.at[late, place.c], "c", 0, None if late else ("pass", n, 1))
    copies.add("dense pair", dp_ref.at[theirs], dr_ref, "c", 0)
    copies.add("dense pass", ds_ref, de_ref, "c", 0)
    dense_refs = {"y": dcy_ref, "x": dcx_ref, "z": dcz_ref}
    index_of = {"y": place.y, "x": place.x, "z": place.z}
    dense = {k: RingSpread(copies, ("dense", k), k, index_of[k], slabs(ref)) for k, ref in dense_refs.items()}

    def reduce_start(q):
        for k in ("x", "z"):
            first[k][q].start()

    def reduce_onward(q):
        for k in ("x", "z"):
            first[k][q].onward()

    def reduce_finish(q):
        for k in ("x", "z"):
            first[k][q].finish(mid[k].at[q])

    def y_start():
        for k in ("x", "z"):
            on_y[k].start()

    def y_onward():
        for k in ("x", "z"):
            on_y[k].onward()

    def y_finish():
        for k in ("x", "z"):
            on_y[k].finish(cross_ref[k].at[other_of[k][1]])
            cross[k].start()

    def w_finish():
        on_y["w"].finish(s2_ref.at[3])
        for k in ("u", "l"):
            inner[k].start()

    def inner_onward():
        for k in ("u", "l"):
            inner[k].onward()

    def inner_finish():
        for k in ("u", "l"):
            inner[k].finish(cross_ref[k].at[other_of[k][1]])
            cross[k].start()

    def cross_onward(*keys):
        for k in keys:
            cross[k].onward()

    def cross_finish(late, *keys):
        for k in keys:
            cross[k].finish()
            done_ref[k][...] = total(cross_ref[k])
            puts[k, late].start()
            final[k, late].start()

    def final_onward(late, *keys):
        for k in keys:
            final[k, late].onward()

    def final_finish(late, *keys):
        for k in keys:
            final[k, late].finish()
            puts[k, late].wait()
        copies.start(*[("pass", n, late) for n in ARRAYS if ("xzu"[n] in keys)])

    def pass_finish(late):
        keys = [("pass", n, late) for n in ARRAYS]
        copies.arrive(*keys)
        copies.sent(*keys)

    def dense_sum():
        copies.arrive("dense pair")
        dcy_ref[place.y] = (dp_ref[mine].astype(F32) + dr_ref[...].astype(F32)).astype(BF16)
        copies.sent("dense pair")
        dense["y"].start()

    def dense_next(k, follow):
        dense[k].finish()
        dense_refs[follow][index_of[follow]] = total(dense_refs[k])
        dense[follow].start()

    def dense_pass(late):
        dense["z"].finish()
        ds_ref[...] = total(dcz_ref)
        gd_ref[late, mine] = ds_ref[...]
        copies.start("dense pass")

    def dense_finish(late):
        copies.arrive("dense pass")
        gd_ref[late, theirs] = de_ref[...]
        copies.sent("dense pass")

    def copy(src, dst, sem):
        return pltpu.make_async_copy(src, dst, sem)

    def weights(layer, slot, arrays, buf, is_given=False):
        for n in arrays:
            src = given[n].at[layer, (place.c + slot) % 2] if is_given else whole[n].at[layer, slot]
            yield copy(src, bufs[n].at[buf], load_sem.at[buf, n])

    def saved(layer, slot, buf):
        for n in ARRAYS:
            yield copy(kept[n].at[layer, slot], acts[n].at[buf], load_sem.at[buf, 3 + n])

    def forward_loads(step, do):
        buf, slot = step % 2, step % SLOTS
        for is_given in (True, False):

            @pl.when((slot < 2) == is_given)
            def _():
                for item in weights(step // SLOTS, slot, ARRAYS, buf, is_given):
                    do(item)

    def weights_loads(step):
        layer, slot, buf = layer_of(step), SLOTS - 1 - step % SLOTS, (step + 1) % 2
        return [*weights(layer, slot, [2], buf), *saved(layer, slot, buf)]

    def inputs_loads(step):
        layer, slot, buf = layer_of(step), SLOTS - 1 - step % SLOTS, (step + 1) % 2
        return [*weights(layer, slot, BUFS, buf)] + [copy(deferred[n].at[slot], acts[n + 1].at[buf], load_sem.at[buf, 4 + n]) for n in BUFS]

    def load(step):
        forward_loads(step, lambda item: item.start())

    def layer_of(step):
        return 1 - (step - WEIGHTS1) // (2 * SLOTS)

    def keeps(step):
        return [copy(bufs[n].at[step % 2], whole[n].at[step // SLOTS, step % SLOTS], keep_sem.at[step % 2, n]) for n in ARRAYS]

    def saves(step):
        return [copy(acts[n].at[step % 2], kept[n].at[step // SLOTS, step % SLOTS], save_sem.at[step % 2, n]) for n in ARRAYS]

    def defers(step):
        return [copy(acts[n + 1].at[2], deferred[n].at[SLOTS - 1 - step % SLOTS], save_sem.at[0, n]) for n in BUFS]

    def wait(items):
        for item in items:
            item.wait()

    def start(items):
        for item in items:
            item.start()

    def ending():
        y_finish()
        inner_finish()
        dense_finish(1)
        copies.start("dense pair")
        dense_sum()
        cross_onward("x", "z")
        cross_onward("u", "l")
        dense["y"].onward()
        cross_finish(0, "x", "z")
        cross_finish(0, "u", "l")
        dense_next("y", "x")
        final_onward(0, "x", "z")
        dense["x"].onward()
        final_onward(0, "u", "l")
        dense_next("x", "z")
        final_finish(0, "x", "z")
        final_finish(0, "u", "l")
        dense["z"].onward()
        dense_pass(0)
        pass_finish(0)
        dense_finish(0)

    before, middle, after = {}, {}, {}

    def plan(table, first, *stages):
        for n, stage in enumerate(stages):
            table.setdefault(first + n, []).extend(stage)

    on, done = lambda q: lambda: reduce_onward(q), lambda q: lambda: reduce_finish(q)
    now = lambda: load(s)
    plan(before, 0, [g0.second, g0.lead], [g0.third, g0.follow, g0.lead_onward], [g1.begin, g0.follow_onward, g0.complete_y, now, g0.last])
    plan(before, 3, [g0.passed_left, g1.second], [g0.passed_right, g0.last_onward, g1.lead], [g1.third], [g0.complete_last, now, g1.follow], [g0.passed_last, now, g1.lead_onward])
    plan(before, SLOTS + 1, [g1.follow_onward], [g1.complete_y, now, g1.last], [g1.passed_left], [g1.passed_right], [g1.last_onward], [g1.complete_last, now], [g1.passed_last, now])
    unready = (1, 5, 6, SLOTS + 1, SLOTS + 5, SLOTS + 6)
    late = ("x", "z", "u", "l")
    plan(before, WEIGHTS0, [lambda: copies.start("dense pair")], [inner_finish], [], [lambda: cross_onward(*late), dense["y"].onward], [], [], [lambda: dense_next("y", "x")])
    plan(middle, WEIGHTS0, [dense_sum, y_finish], [], [], [], [lambda: cross_finish(1, *late)], [], [], [lambda: final_onward(1, *late)])
    plan(before, INPUTS0 + 1, [dense["x"].onward], [lambda: final_finish(1, *late)], [lambda: dense_next("x", "z")], [], [dense["z"].onward], [lambda: pass_finish(1)], [lambda: dense_pass(1)])
    for base in (WEIGHTS1, WEIGHTS0):
        plan(before, base + 2, [on_y["w"].start], [], [], [], [on_y["w"].onward])
        plan(middle, base + 3, [on(0)], [], [done(0), y_start], [on(1)], [on(2)])
        plan(before, base + SLOTS, [done(1)], [], [done(2), y_onward], [on(3)], [w_finish], [], [done(3), inner_onward])
        for step, q in OWN_STEPS.items():
            plan(after, base + step, [lambda q=q: reduce_start(q)])

    def hooks(table, *phases):
        for phase in phases:
            mine = {step: stages for step, stages in sorted(table.items()) if phase <= step < phase + SLOTS}
            if mine:

                @pl.when(s // SLOTS == phase // SLOTS)
                def _(mine=mine):
                    for step, stages in mine.items():

                        @pl.when(s == step)
                        def _(stages=stages):
                            for stage in stages:
                                stage()

    phase, t = s // SLOTS, s % SLOTS
    forth, back = s % 2, (s + 1) % 2

    @pl.when(s == 0)
    def _():
        load(0)
        greet(place)
        g0.begin()
        load(1)
        route(ids_ref, gate_ref, rows_ref, columns_ref, place)

    def enter(x):
        cur_ref[...] = (x.astype(F32) + dot(x, wd_ref[phase])).astype(BF16)
        acc_ref[...] = jnp.zeros_like(acc_ref)

    def leave(out_ref):
        out_ref[...] = (cur_ref[...].astype(F32) + acc_ref[...]).astype(BF16)

    @pl.when(s < WEIGHTS1)
    def _():
        hooks(before, 0, SLOTS)
        forward_loads(s, lambda item: item.wait())
        pl.when(s > 1)(lambda: wait(saves(s - 2)))
        ahead = functools.reduce(jnp.logical_and, [s != step for step in unready], (s > 0) & (s < WEIGHTS1 - 1))
        pl.when(ahead)(lambda: load(s + 1))

        @pl.when(t < 2)
        def _():
            start(keeps(s))
            pl.when(s == 0)(lambda: enter(x0_ref[...]))
            pl.when(s == SLOTS)(lambda: enter(x1_ref[...]))

        layer, slot = phase, t
        z = dot(one_hot(rows_ref, layer, slot, cap), cur_ref[...]).astype(BF16)
        z_ref[forth] = z
        a = dot(z, w1_ref[forth]).astype(BF16)
        b = dot(z, w3_ref[forth]).astype(BF16)
        a_ref[forth] = a
        b_ref[forth] = b
        h = (jax.nn.silu(a.astype(F32)) * b.astype(F32)).astype(BF16)
        o = dot(h, w2_ref[forth]).astype(BF16)
        acc_ref[...] += column(columns_ref, layer, SLOTS + slot) * dot(one_hot_t(columns_ref, layer, slot, cap), o)
        pl.when(s < WEIGHTS1 - 1)(lambda: start(saves(s)))
        pl.when(t < 2)(lambda: wait(keeps(s)))

        @pl.when(t == SLOTS - 1)
        def _():
            pl.when(s == SLOTS - 1)(lambda: leave(x1_ref))
            pl.when(s == WEIGHTS1 - 1)(lambda: leave(hold_ref))

    @pl.when((phase == WEIGHTS1 // SLOTS) | (phase == WEIGHTS0 // SLOTS))
    def _():
        layer, slot = layer_of(s), SLOTS - 1 - t
        hooks(before, WEIGHTS1, WEIGHTS0)

        @pl.when(s == WEIGHTS1)
        def _():
            moved = copy(hold_ref, y_ref, keep_sem.at[0, 0])
            moved.start()
            wait(saves(s - 2))
            gathers.drain()
            moved.wait()
            cur_ref[...] = dy_ref[...]
            acc_ref[...] = dy_ref[...].astype(F32)

        pl.when(s > WEIGHTS1)(lambda: wait(weights_loads(s)))
        pl.when(t > 0)(lambda: wait(defers(s - 1)))
        pl.when(t < SLOTS - 1)(lambda: start(weights_loads(s + 1)))
        pl.when(t == SLOTS - 1)(lambda: start(inputs_loads(s + 1)))

        grad_gated = (column(columns_ref, layer, SLOTS + slot) * cur_ref[...].astype(F32)).astype(BF16)
        do = dot(one_hot(rows_ref, layer, slot, cap), grad_gated).astype(BF16)
        dh = dot_nt(do, w2_ref[back])
        a = a_ref[back].astype(F32)
        b = b_ref[back].astype(F32)
        sig = jax.nn.sigmoid(a)
        act = a * sig
        h = (act * b).astype(BF16)
        db = (dh * act).astype(BF16)
        da = (dh * b * sig * (1.0 + a * (1.0 - sig))).astype(BF16)
        a_ref[2] = da
        b_ref[2] = db
        z = z_ref[back]
        start(defers(s))
        hooks(middle, WEIGHTS1, WEIGHTS0)

        def weight_grad(n):
            return dot_tn(*((z, da), (z, db), (h, do))[n])

        is_own = functools.reduce(jnp.logical_or, [t == step for step in OWN_STEPS])
        group = t // 4 + t // 5 + t // 7
        into = (t // 2 + t // 3) % 2
        turn = t + (1 - layer) * SLOTS

        @pl.when(jnp.logical_not(is_own))
        def _():
            pl.when(turn >= 3)(lambda: pl.semaphore_wait(credit.at[into], 1))
            for n, ref in enumerate(stage):
                for buf in BUFS:
                    pl.when((turn > 0) & (into == 1 - buf))(lambda: copies.sent(("pair", buf, n)))
                ref[...] = weight_grad(n).astype(BF16)
                for buf in BUFS:
                    pl.when(into == buf)(lambda: copies.start(("pair", buf, n)))

        @pl.when(is_own)
        def _():
            for n, ref in enumerate(mine_of):
                for buf in BUFS:
                    pl.when(group % 2 == buf)(lambda: copies.arrive(("pair", buf, n)))
                ref[group] = (weight_grad(n) + mate[n][group % 2].astype(F32)).astype(BF16)

            @pl.when(turn < 2 * SLOTS - 3)
            def _():
                pl.semaphore_signal(credit.at[group % 2], inc=1, device_id=place.at("c", 0), device_id_type=MESH)

            hooks(after, WEIGHTS1, WEIGHTS0)

    def leave_back(layer, x, out_ref):
        grad = acc_ref[...]
        grad_b = grad.astype(BF16)
        dp_ref[...] = dot_tn(x, grad_b).astype(BF16)
        out_ref[...] = (grad + dot_nt(grad_b, wd_ref[layer])).astype(BF16)

    @pl.when((phase == INPUTS1 // SLOTS) | (phase == INPUTS0 // SLOTS))
    def _():
        layer, slot = layer_of(s), SLOTS - 1 - t
        hooks(before, INPUTS1, INPUTS0)
        wait(inputs_loads(s))
        pl.when(t == 0)(lambda: wait(defers(s - 1)))
        pl.when(t < SLOTS - 1)(lambda: start(inputs_loads(s + 1)))
        pl.when(s == WEIGHTS0 - 1)(lambda: start(weights_loads(s + 1)))
        dz = (dot_nt(a_ref[back], w1_ref[back]) + dot_nt(b_ref[back], w3_ref[back])).astype(BF16)
        acc_ref[...] += dot(one_hot_t(columns_ref, layer, slot, cap), dz)

        @pl.when(s == WEIGHTS0 - 1)
        def _():
            leave_back(1, x1_ref[...], cur_ref)
            acc_ref[...] = cur_ref[...].astype(F32)

        @pl.when(s == STEPS - 1)
        def _():
            leave_back(0, x0_ref[...], hold_ref)
            moved = copy(hold_ref, dx_ref, keep_sem.at[0, 0])
            moved.start()
            ending()
            dense_out = copy(gd_ref, gdense_ref, keep_sem.at[0, 1])
            dense_out.start()
            copies.sent(*[("pair", 1, n) for n in ARRAYS])
            moved.wait()
            dense_out.wait()


def step(cap, x0, dy, ids, gates, wd, w1, w3, w2):
    tokens, width = dy.shape
    layers, local, _, ff = w1.shape
    quarter, part = width // SIDE, ff // 2 // SIDE
    hbm = pl.BlockSpec(memory_space=pl.ANY)

    def fixed(shape):
        return pl.BlockSpec(shape, lambda s: (0,) * len(shape), pipeline_mode=pl.Buffered(1))

    def buf(*shape):
        return pltpu.VMEM(shape, BF16)

    def dma(*shape):
        return pltpu.SemaphoreType.DMA(shape)

    shape = jax.ShapeDtypeStruct
    ups, downs = [(width, ff), (width, ff), (ff, width)], [(quarter, ff), (part, width)]
    acts = [(cap, width), (cap, ff), (cap, ff)]
    scratch = [pltpu.VMEM((tokens, width), F32)] + [buf(tokens, width)] * 3 + [buf(layers, width, width), pltpu.VMEM((layers, SLOTS, tokens), jnp.int32), pltpu.VMEM((layers, tokens, LANES), F32)]
    scratch += [buf(2, *u) for u in ups] + [buf(2, *acts[0]), buf(3, *acts[1]), buf(3, *acts[2])]
    scratch += [buf(*u) for u in ups] + [buf(2, *u) for u in ups] + [buf(SIDE, *u) for u in ups]
    scratch += [buf(SIDE, 2, quarter // 2, ff), buf(SIDE, 2, quarter, ff)] * 2
    scratch += [buf(SIDE, quarter, ff)] * 2
    scratch += [buf(2, quarter // 2, ff), buf(2, quarter, ff)] * 2 + [buf(2, ff // 2, width), buf(2, ff, width)]
    scratch += [buf(2, part // 2, width), buf(2, part, width)] * 2
    scratch += [buf(SIDE, quarter, ff)] * 2 + [buf(SIDE, part, width)] * 2
    scratch += [buf(quarter, ff)] * 2 + [buf(part, width)] * 2
    scratch += [buf(width, width), buf(width // 2, width)] + [buf(SIDE, width // 2, width)] * 3 + [buf(width // 2, width)] * 2
    scratch += [dma(4), dma(2, 6), dma(2, 3), dma(2, 3), dma(GATHER_COPIES), dma(GATHER_COPIES), dma(REDUCE_COPIES), dma(REDUCE_COPIES), pltpu.SemaphoreType.REGULAR((2,))]
    results = [(tokens, width), (tokens, width), (layers, width, width)]
    kept = [(layers, local, *u) for u in ups] + [(layers, SLOTS, *u) for u in ups + acts] + [(SLOTS, cap, ff)] * 2
    return pl.pallas_call(
        functools.partial(kernel, cap),
        grid=(STEPS,),
        in_specs=[fixed(v.shape) for v in (x0, dy, ids, gates, wd)] + [hbm] * 3,
        out_specs=[hbm] * len(results + kept),
        out_shape=[shape(r, BF16) for r in results + kept],
        scratch_shapes=scratch,
        compiler_params=pltpu.CompilerParams(vmem_limit_bytes=VMEM_LIMIT, collective_id=0, has_side_effects=True),
        name="step",
    )(x0, dy, ids, gates, wd, w1, w3, w2)[:6]


def take_kernel(count, *refs):
    sources, targets, holds, (come, go) = refs[:count], refs[count : 2 * count], refs[2 * count : 3 * count], refs[3 * count :]
    comes = [pltpu.make_async_copy(a, b, come.at[n]) for n, (a, b) in enumerate(zip(sources, holds))]
    goes = [pltpu.make_async_copy(a, b, go.at[n]) for n, (a, b) in enumerate(zip(holds, targets))]
    for item in comes:
        item.start()
    for first, then in zip(comes, goes):
        first.wait()
        then.start()
    for item in goes:
        item.wait()


def take(arrays):
    count = len(arrays)
    hbm = pl.BlockSpec(memory_space=pl.ANY)
    return pl.pallas_call(
        functools.partial(take_kernel, count),
        in_specs=[hbm] * count,
        out_specs=[hbm] * count,
        out_shape=[jax.ShapeDtypeStruct(a.shape, a.dtype) for a in arrays],
        scratch_shapes=[pltpu.VMEM(a.shape, a.dtype) for a in arrays] + [pltpu.SemaphoreType.DMA((count,))] * 2,
        compiler_params=pltpu.CompilerParams(vmem_limit_bytes=VMEM_LIMIT),
        name="take",
    )(*arrays)


def solution(mesh):
    tok_spec = P(TOK_AXES, None)
    route_spec = P(None, TOK_AXES, None)
    expert_spec = P(None, "ep", None, None)
    whole_spec = P(None, None, None)

    def device_step(tok_in, tok_grad, route_ids, gate_vals, *weights):
        tokens, top_k = route_ids.shape[1:]
        return tuple(take(step(2 * tokens * top_k // SLOTS, tok_in, tok_grad, jnp.swapaxes(route_ids, 1, 2), jnp.swapaxes(gate_vals, 1, 2), *weights)))

    return jax.shard_map(device_step, mesh=mesh, in_specs=(tok_spec, tok_spec, route_spec, route_spec, whole_spec, expert_spec, expert_spec, expert_spec), out_specs=(tok_spec, tok_spec, whole_spec, expert_spec, expert_spec, expert_spec), check_vma=False)
```

```python
import functools

import jax
import jax.numpy as jnp
from jax import lax
from jax.experimental import pallas as pl
from jax.experimental.pallas import tpu as pltpu
from jax.sharding import PartitionSpec as P

TOK_AXES = ("rep", "ep", "dp")
F32 = jnp.float32
BF16 = jnp.bfloat16
LANES = 128
SIDE = 4
WAYS = (1, -1)
BUFS = (0, 1)
LAYERS = (1, 0)
ARRAYS = range(3)
SLOTS = 8
MESH = pl.DeviceIdType.MESH
VMEM_LIMIT = 67_043_328


def dot(a, b):
    return jnp.dot(a, b, preferred_element_type=F32)


def dot_nt(a, b):
    return lax.dot_general(a, b, (((1,), (1,)), ((), ())), preferred_element_type=F32)


def dot_tn(a, b):
    return lax.dot_general(a, b, (((0,), (0,)), ((), ())), preferred_element_type=F32)


class Place:
    def __init__(self):
        self.z, self.y, dp = lax.axis_index("rep"), lax.axis_index("ep"), lax.axis_index("dp")
        self.x, self.c = dp // 2, dp % 2

    def at(self, axis, step):
        z, y, x, c = self.z, self.y, self.x, self.c
        if axis == "z":
            z = (z + step + SIDE) % SIDE
        elif axis == "y":
            y = (y + step + SIDE) % SIDE
        elif axis == "x":
            x = (x + step + SIDE) % SIDE
        else:
            c = 1 - c
        return (z, y, x * 2 + c)


class Copies:
    def __init__(self, place, send, recv):
        self.place, self.send, self.recv, self.made, self.number, self.count, self.over = place, send, recv, {}, {}, 0, set()

    def add(self, key, src, dst, axis, step, like=None):
        if like is None:
            n, self.count = self.count, self.count + 1
        else:
            n = self.number[like]
        self.number[key] = n
        self.made[key] = pltpu.make_async_remote_copy(src_ref=src, dst_ref=dst, send_sem=self.send.at[n], recv_sem=self.recv.at[n], device_id=self.place.at(axis, step), device_id_type=MESH)

    def start(self, *keys):
        for key in keys:
            self.made[key].start()

    def arrive(self, *keys):
        for key in keys:
            self.made[key].wait_recv()

    def sent(self, *keys):
        for key in keys:
            self.made[key].wait_send()
            self.over.add(key)

    def drain(self):
        self.sent(*[key for key in self.made if key not in self.over])


def greet(place):
    barrier = pltpu.get_barrier_semaphore()
    peers = [(axis, step) for axis in "xyz" for step in WAYS] + [("c", 0)]
    for axis, step in peers:
        pl.semaphore_signal(barrier, inc=1, device_id=place.at(axis, step), device_id_type=MESH)
    pl.semaphore_wait(barrier, len(peers))


class Gather:
    PASS = {2: 4, 3: 6, 5: 7}

    def __init__(self, layer, copies, place, own, whole):
        self.layer, self.copies, self.place, self.own, self.whole = layer, copies, place, own, whole
        rows, ff = own[0].shape[2], own[2].shape[2]
        self.cut = {"x": ((0, 0, rows // SIDE), (2, 0, ff // 2 // SIDE)), "z": ((1, 0, rows // SIDE), (2, ff // 2, ff // 2 // SIDE))}
        mine = {"x": place.x, "z": place.z}
        for color in ("x", "z"):
            for part in BUFS:
                self._add(("y", 2, color, part), color, part, None, 2, mine[color], None, "y", 1)
                self._add(("y", 3, color, part), color, part, None, 3, mine[color], None, "y", -1)
                if color == "x":
                    self._add(("y", 5, color, part), color, part, 2, 5, mine[color], None, "y", 1)
                else:
                    self._add(("y", 5, color, part), color, part, 3, 5, mine[color], None, "y", -1)
                for slot in (2, 3, 5):
                    for step in WAYS:
                        self._add(("near", slot, color, part, step), color, part, slot, slot, mine[color], None, color, step)
                        behind = (mine[color] - step + SIDE) % SIDE
                        self._add(("far", slot, color, part, step), color, part, slot, slot, behind, (1 - step) // 2, color, step)
        for slot, to in self.PASS.items():
            for array in ARRAYS:
                copies.add((layer, "pass", slot, array), whole[array].at[layer, slot], whole[array].at[layer, to], "c", 0)

    def _view(self, refs, index, color, part, quarter, half):
        array, base, size = self.cut[color][part]
        start = base + quarter * size
        if half is not None:
            size = size // 2
            start = start + half * size
        return refs[array].at[self.layer, index, pl.ds(pl.multiple_of(start, 16), size)]

    def _add(self, key, color, part, src_slot, dst_slot, quarter, half, axis, step):
        src = self._view(self.own, self.place.c, color, part, quarter, half) if src_slot is None else self._view(self.whole, src_slot, color, part, quarter, half)
        self.copies.add((self.layer,) + key, src, self._view(self.whole, dst_slot, color, part, quarter, half), axis, step)

    def _keys(self, *key, extra=()):
        return [(self.layer,) + key + (part,) + extra for part in BUFS]

    def lead(self):
        self.spread(2, "x")
        self.spread(3, "z")

    def lead_onward(self):
        self.onward(2, "x")
        self.onward(3, "z")

    def follow(self):
        self.spread(2, "z")
        self.spread(3, "x")

    def follow_onward(self):
        self.onward(2, "z")
        self.onward(3, "x")

    def last(self):
        self.spread(5, "x")
        self.spread(5, "z")

    def last_onward(self):
        self.onward(5, "x")
        self.onward(5, "z")

    def complete_y(self):
        self.complete(2)
        self.complete(3)

    def complete_last(self):
        self.complete(5)

    def passed_left(self):
        self.passed(2)

    def passed_right(self):
        self.passed(3)

    def passed_last(self):
        self.passed(5)

    def begin(self):
        self.copies.start(*self._keys("y", 2, "x"), *self._keys("y", 3, "z"))

    def second(self):
        self.copies.sent(*self._keys("y", 2, "x"), *self._keys("y", 3, "z"))
        self.copies.start(*self._keys("y", 2, "z"), *self._keys("y", 3, "x"))

    def third(self):
        self.copies.sent(*self._keys("y", 2, "z"), *self._keys("y", 3, "x"))
        self.copies.start(*self._keys("y", 5, "x"), *self._keys("y", 5, "z"))

    def spread(self, slot, color):
        self.copies.arrive(*self._keys("y", slot, color))
        for step in WAYS:
            self.copies.start(*self._keys("near", slot, color, extra=(step,)))

    def onward(self, slot, color):
        for step in WAYS:
            self.copies.arrive(*self._keys("near", slot, color, extra=(step,)))
            self.copies.start(*self._keys("far", slot, color, extra=(step,)))

    def complete(self, slot):
        for color in ("x", "z"):
            for step in WAYS:
                self.copies.arrive(*self._keys("far", slot, color, extra=(step,)))
        self.copies.start(*[(self.layer, "pass", slot, array) for array in ARRAYS])

    def passed(self, slot):
        self.copies.arrive(*[(self.layer, "pass", slot, array) for array in ARRAYS])


GATHER_COPIES = 2 * (2 * 2 * (3 + 3 * 4) + 9)


def route(ids_ref, gate_ref, rows_ref, columns_ref, place):
    layers, _, tokens = ids_ref.shape
    below = lax.broadcasted_iota(jnp.int32, (tokens, tokens), 0) < lax.broadcasted_iota(jnp.int32, (tokens, tokens), 1)
    below = jnp.where(below, 1.0, 0.0).astype(BF16)
    lead = lax.broadcasted_iota(jnp.int32, (2 * SLOTS, tokens), 0)
    for layer in range(layers):
        ids, gates = ids_ref[layer], gate_ref[layer]
        off = ((ids >> 1) - place.y) & (SIDE - 1)
        odd = (ids + place.c) & 1
        slot = jnp.where(off == 0, odd, jnp.where(off == SIDE - 1, 2 + 2 * odd, jnp.where(off == 1, 3 + 3 * odd, 5 + 2 * odd)))
        hits = [slot[n : n + 1] == lead for n in BUFS]
        hit = hits[0] | hits[1]
        weight = jnp.where(hits[0], gates[0:1], 0.0) + jnp.where(hits[1], gates[1:2], 0.0)
        rank = jnp.where(hit, dot(jnp.where(hit, 1.0, 0.0).astype(BF16), below), -1.0)
        rows_ref[layer] = rank[:SLOTS].astype(jnp.int32)
        columns_ref[layer] = jnp.transpose(jnp.concatenate([rank[:SLOTS], weight[:SLOTS], jnp.zeros((LANES - 2 * SLOTS, tokens), F32)], axis=0))


def one_hot(rows_ref, layer, slot, cap):
    place = lax.broadcasted_iota(jnp.int32, (cap, rows_ref.shape[2]), 0)
    return jnp.where(rows_ref[layer, pl.ds(slot, 1), :] == place, 1.0, 0.0).astype(BF16)


def column(columns_ref, layer, index):
    lane = lax.broadcasted_iota(jnp.int32, columns_ref.shape[1:], 1)
    return jnp.sum(jnp.where(lane == index, columns_ref[layer], 0.0), axis=1, keepdims=True)


def one_hot_t(columns_ref, layer, slot, cap):
    place = lax.broadcasted_iota(jnp.int32, (columns_ref.shape[1], cap), 1)
    return jnp.where(column(columns_ref, layer, slot).astype(jnp.int32) == place, 1.0, 0.0).astype(BF16)


def add_to(dst, src):
    dst[...] = (dst[...].astype(F32) + src[...].astype(F32)).astype(BF16)


class RingSum:
    def __init__(self, copies, name, axis, block, first, second):
        self.copies, self.name, self.block, self.first, self.second = copies, name, block, first, second
        self.early, self.later = ([(name, when, step) for step in WAYS] for when in ("early", "later"))
        for half, step in enumerate(WAYS):
            copies.add(self.early[half], block(2, half), first.at[half], axis, step)
            copies.add(self.later[half], block(step, None), second.at[half], axis, step)

    def start(self):
        self.copies.start(*self.early)

    def onward(self):
        self.copies.arrive(*self.early)
        for half in BUFS:
            add_to(self.block(WAYS[half], half), self.first.at[half])
            self.copies.start(self.later[half])
        self.copies.sent(*self.early)

    def finish(self, out):
        self.copies.arrive(*self.later)
        out[...] = (self.block(0, None)[...].astype(F32) + self.second[0].astype(F32) + self.second[1].astype(F32)).astype(BF16)
        self.copies.sent(*self.later)


class RingSpread:
    def __init__(self, copies, name, axis, me, block, source=None, like=None):
        self.copies = copies
        self.near, self.far = ([(name, when, step) for step in WAYS] for when in ("near", "far"))
        for half, step in enumerate(WAYS):
            behind = (me - step + SIDE) % SIDE
            near, far = (None, None) if like is None else (like.near[half], like.far[half])
            copies.add(self.near[half], block(me, None) if source is None else source, block(me, None), axis, step, near)
            copies.add(self.far[half], block(behind, half), block(behind, half), axis, step, far)

    def start(self):
        self.copies.start(*self.near)

    def onward(self):
        for near, far in zip(self.near, self.far):
            self.copies.arrive(near)
            self.copies.start(far)

    def finish(self):
        self.copies.arrive(*self.far)
        self.copies.sent(*self.near, *self.far)


def slices(ref, lead, base, size):
    def block(index, half):
        start, rows = base + index * size, size
        if half is not None:
            rows = size // 2
            start = start + half * rows
        return ref.at[(*lead, pl.ds(pl.multiple_of(start, 16), rows))]

    return block


def slabs(ref):
    def block(index, half):
        if half is None:
            return ref.at[index]
        rows = ref.shape[1] // 2
        return ref.at[index, pl.ds(half * rows, rows)]

    return block


def total(ref):
    return (ref[0].astype(F32) + ref[1].astype(F32) + ref[2].astype(F32) + ref[3].astype(F32)).astype(BF16)


OWN_STEPS = {2: 0, 4: 1, 5: 2, 7: 3}
REDUCE_COPIES = 107
WEIGHTS1, INPUTS1, WEIGHTS0, INPUTS0, STEPS = (n * SLOTS for n in range(2, 7))


def kernel(cap, x0_ref, dy_ref, ids_ref, gate_ref, wd_ref, o1_ref, o3_ref, o2_ref, y_ref, dx_ref, gdense_ref, g1_ref, g3_ref, g2_ref, h1_ref, h3_ref, h2_ref, kz_ref, kp_ref, kq_ref, kh_ref, kda_ref, kdb_ref, acc_ref, cur_ref, x1_ref, hold_ref, gd_ref, rows_ref, columns_ref, w1_ref, w3_ref, w2_ref, z_ref, p_ref, q_ref, h_ref, m1_ref, m3_ref, m2_ref, d1_ref, d3_ref, d2_ref, s1_ref, s3_ref, s2_ref, r11_ref, r12_ref, r31_ref, r32_ref, t1_ref, t3_ref, y11_ref, y12_ref, y31_ref, y32_ref, y21_ref, y22_ref, u1_ref, u2_ref, l1_ref, l2_ref, c1_ref, c3_ref, cu_ref, cl_ref, f1_ref, f3_ref, fu_ref, fl_ref, dp_ref, dr_ref, dcx_ref, dcy_ref, dcz_ref, ds_ref, de_ref, put_sem, load_sem, keep_sem, save_sem, gsend_sem, grecv_sem, send_sem, recv_sem, credit):
    s = pl.program_id(0)
    place = Place()
    gathers = Copies(place, gsend_sem, grecv_sem)
    copies = Copies(place, send_sem, recv_sem)
    given, whole, bufs = (o1_ref, o3_ref, o2_ref), (h1_ref, h3_ref, h2_ref), (w1_ref, w3_ref, w2_ref)
    kept, acts = (kz_ref, kp_ref, kq_ref, kh_ref), (z_ref, p_ref, q_ref, h_ref)
    deferred = (kda_ref, kdb_ref)
    g0, g1 = (Gather(l, gathers, place, given, whole) for l in BUFS)
    rows, ff = s1_ref.shape[1], s2_ref.shape[1]
    quarter, part = rows // SIDE, ff // 2 // SIDE
    half_d = rows // 2

    stage, mate, mine_of = (m1_ref, m3_ref, m2_ref), (d1_ref, d3_ref, d2_ref), (s1_ref, s3_ref, s2_ref)
    outs = (g1_ref, g3_ref, g2_ref)
    for buf in BUFS:
        for n in ARRAYS:
            copies.add(("pair", buf, n), stage[n].at[buf], mate[n].at[buf], "c", 0)

    def ring_blocks(ref, q, me, base, size):
        block = slices(ref, (q,), base, size)
        return lambda offset, half: block((me + offset + SIDE) % SIDE, half)

    def group_blocks(ref):
        block = slabs(ref)
        return lambda offset, half: block({2: 0, 1: 1, -1: 2, 0: 3}[offset], half)

    first = {
        "x": [RingSum(copies, ("x", q), "x", ring_blocks(s1_ref, q, place.x, 0, quarter), r11_ref.at[q], r12_ref.at[q]) for q in range(SIDE)],
        "z": [RingSum(copies, ("z", q), "z", ring_blocks(s3_ref, q, place.z, 0, quarter), r31_ref.at[q], r32_ref.at[q]) for q in range(SIDE)],
    }
    mid = {"x": t1_ref, "z": t3_ref}
    on_y = {
        "x": RingSum(copies, "yx", "y", group_blocks(t1_ref), y11_ref, y12_ref),
        "z": RingSum(copies, "yz", "y", group_blocks(t3_ref), y31_ref, y32_ref),
        "w": RingSum(copies, "yw", "y", group_blocks(s2_ref), y21_ref, y22_ref),
    }
    inner = {
        "u": RingSum(copies, "u", "x", ring_blocks(s2_ref, 3, place.x, 0, part), u1_ref, u2_ref),
        "l": RingSum(copies, "l", "z", ring_blocks(s2_ref, 3, place.z, ff // 2, part), l1_ref, l2_ref),
    }
    ring_of = {"x": ("x", place.x), "u": ("x", place.x), "z": ("z", place.z), "l": ("z", place.z)}
    other_of = {"x": ("z", place.z), "u": ("z", place.z), "z": ("x", place.x), "l": ("x", place.x)}
    cross_ref = {"x": c1_ref, "z": c3_ref, "u": cu_ref, "l": cl_ref}
    done_ref = {"x": f1_ref, "z": f3_ref, "u": fu_ref, "l": fl_ref}
    out_of = {"x": (g1_ref, 0, quarter), "z": (g3_ref, 0, quarter), "u": (g2_ref, 0, part), "l": (g2_ref, ff // 2, part)}
    cross, final, puts = {}, {}, {}
    for i, k in enumerate(out_of):
        cross[k] = RingSpread(copies, ("cross", k), *other_of[k], slabs(cross_ref[k]))
        ref, base, size = out_of[k]
        for late in LAYERS:
            block = slices(ref, (late, place.c), base, size)
            final[k, late] = RingSpread(copies, ("final", k, late), *ring_of[k], block, source=done_ref[k], like=final.get((k, 1)))
            puts[k, late] = pltpu.make_async_copy(done_ref[k], block(ring_of[k][1], None), put_sem.at[i])
    mine, theirs = (pl.ds(pl.multiple_of(c * half_d, 16), half_d) for c in (place.c, 1 - place.c))
    for late in LAYERS:
        for n, out in enumerate(outs):
            copies.add(("pass", n, late), out.at[late, place.c], out.at[late, place.c], "c", 0, None if late else ("pass", n, 1))
    copies.add("dense pair", dp_ref.at[theirs], dr_ref, "c", 0)
    copies.add("dense pass", ds_ref, de_ref, "c", 0)
    dense_refs = {"y": dcy_ref, "x": dcx_ref, "z": dcz_ref}
    index_of = {"y": place.y, "x": place.x, "z": place.z}
    dense = {k: RingSpread(copies, ("dense", k), k, index_of[k], slabs(ref)) for k, ref in dense_refs.items()}

    def reduce_start(q):
        for k in ("x", "z"):
            first[k][q].start()

    def reduce_onward(q):
        for k in ("x", "z"):
            first[k][q].onward()

    def reduce_finish(q):
        for k in ("x", "z"):
            first[k][q].finish(mid[k].at[q])

    def y_start():
        for k in ("x", "z"):
            on_y[k].start()

    def y_onward():
        for k in ("x", "z"):
            on_y[k].onward()

    def y_finish():
        for k in ("x", "z"):
            on_y[k].finish(cross_ref[k].at[other_of[k][1]])
            cross[k].start()

    def w_finish():
        on_y["w"].finish(s2_ref.at[3])
        for k in ("u", "l"):
            inner[k].start()

    def inner_onward():
        for k in ("u", "l"):
            inner[k].onward()

    def inner_finish():
        for k in ("u", "l"):
            inner[k].finish(cross_ref[k].at[other_of[k][1]])
            cross[k].start()

    def cross_onward(*keys):
        for k in keys:
            cross[k].onward()

    def cross_finish(late, *keys):
        for k in keys:
            cross[k].finish()
            done_ref[k][...] = total(cross_ref[k])
            puts[k, late].start()
            final[k, late].start()

    def final_onward(late, *keys):
        for k in keys:
            final[k, late].onward()

    def final_finish(late, *keys):
        for k in keys:
            final[k, late].finish()
            puts[k, late].wait()
        copies.start(*[("pass", n, late) for n in ARRAYS if ("xzu"[n] in keys)])

    def pass_finish(late):
        keys = [("pass", n, late) for n in ARRAYS]
        copies.arrive(*keys)
        copies.sent(*keys)

    def dense_sum():
        copies.arrive("dense pair")
        dcy_ref[place.y] = (dp_ref[mine].astype(F32) + dr_ref[...].astype(F32)).astype(BF16)
        copies.sent("dense pair")
        dense["y"].start()

    def dense_next(k, follow):
        dense[k].finish()
        dense_refs[follow][index_of[follow]] = total(dense_refs[k])
        dense[follow].start()

    def dense_out(late):
        return pltpu.make_async_copy(gd_ref, gdense_ref.at[late], keep_sem.at[0, 1])

    def dense_pass(late):
        dense["z"].finish()
        ds_ref[...] = total(dcz_ref)
        if late == 0:
            dense_out(1).wait()
        gd_ref[mine] = ds_ref[...]
        copies.start("dense pass")

    def dense_finish(late):
        copies.arrive("dense pass")
        gd_ref[theirs] = de_ref[...]
        copies.sent("dense pass")
        dense_out(late).start()

    def copy(src, dst, sem):
        return pltpu.make_async_copy(src, dst, sem)

    def weights(layer, slot, arrays, buf, is_given=False):
        for n in arrays:
            src = given[n].at[layer, (place.c + slot) % 2] if is_given else whole[n].at[layer, slot]
            yield copy(src, bufs[n].at[buf], load_sem.at[buf, n])

    def saved(layer, slot, buf):
        for n, (src, dst) in enumerate(zip(kept, acts)):
            yield copy(src.at[layer, slot], dst.at[buf], load_sem.at[buf, 3 + n])

    def forward_loads(step, do):
        buf, slot = step % 2, step % SLOTS
        for is_given in (True, False):

            @pl.when((slot < 2) == is_given)
            def _():
                for item in weights(step // SLOTS, slot, ARRAYS, buf, is_given):
                    do(item)

    def weights_loads(step):
        layer, slot, buf = layer_of(step), SLOTS - 1 - step % SLOTS, (step + 1) % 2
        return [*weights(layer, slot, [2], buf), *saved(layer, slot, buf)]

    def inputs_loads(step):
        layer, slot, buf = layer_of(step), SLOTS - 1 - step % SLOTS, (step + 1) % 2
        return [*weights(layer, slot, BUFS, buf)] + [copy(deferred[n].at[slot], acts[n + 1].at[buf], load_sem.at[buf, 4 + n]) for n in BUFS]

    def load(step):
        forward_loads(step, lambda item: item.start())

    def layer_of(step):
        return 1 - (step - WEIGHTS1) // (2 * SLOTS)

    def keeps(step):
        return [copy(bufs[n].at[step % 2], whole[n].at[step // SLOTS, step % SLOTS], keep_sem.at[step % 2, n]) for n in ARRAYS]

    def saves(step):
        return [copy(src.at[step % 2], dst.at[step // SLOTS, step % SLOTS], save_sem.at[step % 2, n]) for n, (src, dst) in enumerate(zip(acts, kept))]

    def defers(step):
        return [copy(acts[n + 1].at[2], deferred[n].at[SLOTS - 1 - step % SLOTS], save_sem.at[0, n]) for n in BUFS]

    def wait(items):
        for item in items:
            item.wait()

    def start(items):
        for item in items:
            item.start()

    def ending():
        y_finish()
        inner_finish()
        dense_finish(1)
        copies.start("dense pair")
        dense_sum()
        cross_onward("x", "z")
        cross_onward("u", "l")
        dense["y"].onward()
        cross_finish(0, "x", "z")
        cross_finish(0, "u", "l")
        dense_next("y", "x")
        final_onward(0, "x", "z")
        dense["x"].onward()
        final_onward(0, "u", "l")
        dense_next("x", "z")
        final_finish(0, "x", "z")
        final_finish(0, "u", "l")
        dense["z"].onward()
        dense_pass(0)
        pass_finish(0)
        dense_finish(0)

    before, middle, after = {}, {}, {}

    def plan(table, first, *stages):
        for n, stage in enumerate(stages):
            table.setdefault(first + n, []).extend(stage)

    on, done = lambda q: lambda: reduce_onward(q), lambda q: lambda: reduce_finish(q)
    now = lambda: load(s)
    plan(before, 0, [g0.second, g0.lead], [g0.third, g0.follow, g0.lead_onward], [g1.begin, g0.follow_onward, g0.complete_y, now, g0.last])
    plan(before, 3, [g0.passed_left, g1.second], [g0.last_onward, g1.lead], [g0.complete_last, now, g1.third, g0.passed_right], [g1.follow], [g0.passed_last, now, g1.lead_onward])
    plan(before, SLOTS + 1, [g1.follow_onward], [g1.complete_y, now, g1.last], [g1.passed_left], [g1.last_onward], [g1.complete_last, now, g1.passed_right], [], [g1.passed_last, now])
    unready = (1, 4, 6, SLOTS + 1, SLOTS + 4, SLOTS + 6)
    late = ("x", "z", "u", "l")
    plan(before, WEIGHTS0, [lambda: copies.start("dense pair")], [inner_finish], [], [lambda: cross_onward(*late), dense["y"].onward], [], [], [lambda: dense_next("y", "x")])
    plan(middle, WEIGHTS0, [dense_sum, y_finish], [], [], [], [lambda: cross_finish(1, *late)], [], [], [lambda: final_onward(1, *late)])
    plan(before, INPUTS0 + 1, [dense["x"].onward], [lambda: final_finish(1, *late)], [lambda: dense_next("x", "z")], [], [dense["z"].onward], [lambda: pass_finish(1)], [lambda: dense_pass(1)])
    for base in (WEIGHTS1, WEIGHTS0):
        plan(before, base + 3, [on_y["w"].start], [], [], [done(0), y_start, on_y["w"].onward])
        plan(middle, base + 4, [on(0)], [], [on(1)], [on(2)])
        plan(before, base + SLOTS, [], [done(1)], [done(2), y_onward], [on(3)], [], [w_finish], [done(3)], [inner_onward])
        for step, q in OWN_STEPS.items():
            plan(after, base + step, [lambda q=q: reduce_start(q)])

    def hooks(table, *phases):
        for phase in phases:
            mine = {step: stages for step, stages in sorted(table.items()) if phase <= step < phase + SLOTS}
            if mine:

                @pl.when(s // SLOTS == phase // SLOTS)
                def _(mine=mine):
                    for step, stages in mine.items():

                        @pl.when(s == step)
                        def _(stages=stages):
                            for stage in stages:
                                stage()

    phase, t = s // SLOTS, s % SLOTS
    forth, back = s % 2, (s + 1) % 2

    def bring(ref, hold):
        return copy(ref, hold, keep_sem.at[1, 0])

    @pl.when(s == 0)
    def _():
        bring(x0_ref, hold_ref).start()
        load(0)
        greet(place)
        g0.begin()
        load(1)
        route(ids_ref, gate_ref, rows_ref, columns_ref, place)
        bring(x0_ref, hold_ref).wait()

    def enter(x):
        cur_ref[...] = (x.astype(F32) + dot(x, wd_ref[phase])).astype(BF16)
        acc_ref[...] = jnp.zeros_like(acc_ref)

    def leave(out_ref):
        out_ref[...] = (cur_ref[...].astype(F32) + acc_ref[...]).astype(BF16)

    @pl.when(s < WEIGHTS1)
    def _():
        hooks(before, 0, SLOTS)
        forward_loads(s, lambda item: item.wait())
        pl.when(s > 1)(lambda: wait(saves(s - 2)))
        ahead = functools.reduce(jnp.logical_and, [s != step for step in unready], (s > 0) & (s < WEIGHTS1 - 1))
        pl.when(ahead)(lambda: load(s + 1))

        @pl.when(t < 2)
        def _():
            start(keeps(s))
            pl.when(s == 0)(lambda: enter(hold_ref[...]))
            pl.when(s == SLOTS)(lambda: enter(x1_ref[...]))

        layer, slot = phase, t
        z = dot(one_hot(rows_ref, layer, slot, cap), cur_ref[...]).astype(BF16)
        z_ref[forth] = z
        a = dot(z, w1_ref[forth]).astype(BF16)
        b = dot(z, w3_ref[forth]).astype(BF16)
        a, b = a.astype(F32), b.astype(F32)
        sig = jax.nn.sigmoid(a)
        act = a * sig
        h = (act * b).astype(BF16)
        p_ref[forth] = act.astype(BF16)
        q_ref[forth] = (b * (sig + act * (1.0 - sig))).astype(BF16)
        h_ref[forth] = h
        o = dot(h, w2_ref[forth]).astype(BF16)
        acc_ref[...] += column(columns_ref, layer, SLOTS + slot) * dot(one_hot_t(columns_ref, layer, slot, cap), o)
        pl.when(s < WEIGHTS1 - 1)(lambda: start(saves(s)))
        pl.when(t < 2)(lambda: wait(keeps(s)))

        @pl.when(t == SLOTS - 1)
        def _():
            pl.when(s == SLOTS - 1)(lambda: leave(x1_ref))
            pl.when(s == WEIGHTS1 - 1)(lambda: leave(hold_ref))

    @pl.when((phase == WEIGHTS1 // SLOTS) | (phase == WEIGHTS0 // SLOTS))
    def _():
        layer, slot = layer_of(s), SLOTS - 1 - t
        hooks(before, WEIGHTS1, WEIGHTS0)

        @pl.when(s == WEIGHTS1)
        def _():
            moved = copy(hold_ref, y_ref, keep_sem.at[0, 0])
            moved.start()
            bring(dy_ref, cur_ref).start()
            wait(saves(s - 2))
            gathers.drain()
            bring(dy_ref, cur_ref).wait()
            moved.wait()
            acc_ref[...] = cur_ref[...].astype(F32)

        pl.when(s > WEIGHTS1)(lambda: wait(weights_loads(s)))
        pl.when(t > 0)(lambda: wait(defers(s - 1)))
        pl.when(t < SLOTS - 1)(lambda: start(weights_loads(s + 1)))
        pl.when(t == SLOTS - 1)(lambda: start(inputs_loads(s + 1)))

        grad_gated = (column(columns_ref, layer, SLOTS + slot) * cur_ref[...].astype(F32)).astype(BF16)
        do = dot(one_hot(rows_ref, layer, slot, cap), grad_gated).astype(BF16)
        dh = dot_nt(do, w2_ref[back])
        db = (dh * p_ref[back].astype(F32)).astype(BF16)
        da = (dh * q_ref[back].astype(F32)).astype(BF16)
        p_ref[2] = da
        q_ref[2] = db
        z, h = z_ref[back], h_ref[back]
        start(defers(s))
        hooks(middle, WEIGHTS1, WEIGHTS0)

        def weight_grads():
            return dot_tn(z, da), dot_tn(z, db), dot_tn(h, do)

        is_own = functools.reduce(jnp.logical_or, [t == step for step in OWN_STEPS])
        group = t // 4 + t // 5 + t // 7
        into = (t + t // 3 + t // 6) % 2
        turn = t + (1 - layer) * SLOTS

        @pl.when(jnp.logical_not(is_own))
        def _():
            for buf in BUFS:
                pl.when((turn >= 3) & (into == buf))(lambda: copies.sent(*[("pair", buf, n) for n in ARRAYS]))

            for ref, grad in zip(stage, weight_grads()):
                ref[into] = grad.astype(BF16)

            pl.when(turn >= 3)(lambda: pl.semaphore_wait(credit.at[into], 1))
            for buf in BUFS:
                pl.when(into == buf)(lambda: copies.start(*[("pair", buf, n) for n in ARRAYS]))

        @pl.when(is_own)
        def _():
            for buf in BUFS:
                pl.when(group % 2 == buf)(lambda: copies.arrive(*[("pair", buf, n) for n in ARRAYS]))

            for ref, add, grad in zip(mine_of, mate, weight_grads()):
                ref[group] = (grad + add[group % 2].astype(F32)).astype(BF16)

            @pl.when(turn < 2 * SLOTS - 3)
            def _():
                pl.semaphore_signal(credit.at[group % 2], inc=1, device_id=place.at("c", 0), device_id_type=MESH)

            hooks(after, WEIGHTS1, WEIGHTS0)

    def leave_back(layer, x, out_ref):
        grad = acc_ref[...]
        grad_b = grad.astype(BF16)
        dp_ref[...] = dot_tn(x, grad_b).astype(BF16)
        out_ref[...] = (grad + dot_nt(grad_b, wd_ref[layer])).astype(BF16)

    @pl.when((phase == INPUTS1 // SLOTS) | (phase == INPUTS0 // SLOTS))
    def _():
        layer, slot = layer_of(s), SLOTS - 1 - t
        hooks(before, INPUTS1, INPUTS0)
        wait(inputs_loads(s))
        pl.when(t == 0)(lambda: wait(defers(s - 1)))
        pl.when(t < SLOTS - 1)(lambda: start(inputs_loads(s + 1)))
        pl.when(s == WEIGHTS0 - 1)(lambda: start(weights_loads(s + 1)))
        dz = (dot_nt(p_ref[back], w1_ref[back]) + dot_nt(q_ref[back], w3_ref[back])).astype(BF16)
        acc_ref[...] += dot(one_hot_t(columns_ref, layer, slot, cap), dz)

        @pl.when(s == WEIGHTS0 - 1)
        def _():
            leave_back(1, x1_ref[...], cur_ref)
            acc_ref[...] = cur_ref[...].astype(F32)
            bring(x0_ref, x1_ref).start()
            bring(x0_ref, x1_ref).wait()

        @pl.when(s == STEPS - 1)
        def _():
            leave_back(0, x1_ref[...], hold_ref)
            moved = copy(hold_ref, dx_ref, keep_sem.at[0, 0])
            moved.start()
            ending()
            copies.sent(*[("pair", buf, n) for buf in BUFS for n in ARRAYS])
            moved.wait()
            dense_out(0).wait()


def step(cap, x0, dy, ids, gates, wd, w1, w3, w2):
    tokens, width = dy.shape
    layers, local, _, ff = w1.shape
    quarter, part = width // SIDE, ff // 2 // SIDE
    hbm = pl.BlockSpec(memory_space=pl.ANY)

    def fixed(shape):
        return pl.BlockSpec(shape, lambda s: (0,) * len(shape), pipeline_mode=pl.Buffered(1))

    def buf(*shape):
        return pltpu.VMEM(shape, BF16)

    def dma(*shape):
        return pltpu.SemaphoreType.DMA(shape)

    shape = jax.ShapeDtypeStruct
    ups, downs = [(width, ff), (width, ff), (ff, width)], [(quarter, ff), (part, width)]
    acts = [(cap, width), (cap, ff), (cap, ff), (cap, ff)]
    scratch = [pltpu.VMEM((tokens, width), F32)] + [buf(tokens, width)] * 3 + [buf(width, width), pltpu.VMEM((layers, SLOTS, tokens), jnp.int32), pltpu.VMEM((layers, tokens, LANES), F32)]
    scratch += [buf(2, *u) for u in ups] + [buf(n, *a) for n, a in zip((2, 3, 3, 2), acts)]
    scratch += [buf(2, *u) for u in ups] * 2 + [buf(SIDE, *u) for u in ups]
    scratch += [buf(SIDE, 2, quarter // 2, ff), buf(SIDE, 2, quarter, ff)] * 2
    scratch += [buf(SIDE, quarter, ff)] * 2
    scratch += [buf(2, quarter // 2, ff), buf(2, quarter, ff)] * 2 + [buf(2, ff // 2, width), buf(2, ff, width)]
    scratch += [buf(2, part // 2, width), buf(2, part, width)] * 2
    scratch += [buf(SIDE, quarter, ff)] * 2 + [buf(SIDE, part, width)] * 2
    scratch += [buf(quarter, ff)] * 2 + [buf(part, width)] * 2
    scratch += [buf(width, width), buf(width // 2, width)] + [buf(SIDE, width // 2, width)] * 3 + [buf(width // 2, width)] * 2
    scratch += [dma(4), dma(2, 7), dma(2, 3), dma(2, 4), dma(GATHER_COPIES), dma(GATHER_COPIES), dma(REDUCE_COPIES), dma(REDUCE_COPIES), pltpu.SemaphoreType.REGULAR((2,))]
    results = [(tokens, width), (tokens, width), (layers, width, width)]
    kept = [(layers, local, *u) for u in ups] + [(layers, SLOTS, *u) for u in ups + acts] + [(SLOTS, cap, ff)] * 2
    return pl.pallas_call(
        functools.partial(kernel, cap),
        grid=(STEPS,),
        in_specs=[hbm] * 2 + [fixed(v.shape) for v in (ids, gates, wd)] + [hbm] * 3,
        out_specs=[hbm] * len(results + kept),
        out_shape=[shape(r, BF16) for r in results + kept],
        scratch_shapes=scratch,
        compiler_params=pltpu.CompilerParams(vmem_limit_bytes=VMEM_LIMIT, collective_id=0, has_side_effects=True),
        name="step",
    )(x0, dy, ids, gates, wd, w1, w3, w2)[:6]


def take_kernel(count, *refs):
    sources, targets, holds, (come, go) = refs[:count], refs[count : 2 * count], refs[2 * count : 3 * count], refs[3 * count :]
    comes = [pltpu.make_async_copy(a, b, come.at[n]) for n, (a, b) in enumerate(zip(sources, holds))]
    goes = [pltpu.make_async_copy(a, b, go.at[n]) for n, (a, b) in enumerate(zip(holds, targets))]
    for item in comes:
        item.start()
    for first, then in zip(comes, goes):
        first.wait()
        then.start()
    for item in goes:
        item.wait()


def take(arrays):
    count = len(arrays)
    hbm = pl.BlockSpec(memory_space=pl.ANY)
    return pl.pallas_call(
        functools.partial(take_kernel, count),
        in_specs=[hbm] * count,
        out_specs=[hbm] * count,
        out_shape=[jax.ShapeDtypeStruct(a.shape, a.dtype) for a in arrays],
        scratch_shapes=[pltpu.VMEM(a.shape, a.dtype) for a in arrays] + [pltpu.SemaphoreType.DMA((count,))] * 2,
        compiler_params=pltpu.CompilerParams(vmem_limit_bytes=VMEM_LIMIT),
        name="take",
    )(*arrays)


def solution(mesh):
    tok_spec = P(TOK_AXES, None)
    route_spec = P(None, TOK_AXES, None)
    expert_spec = P(None, "ep", None, None)
    whole_spec = P(None, None, None)

    def device_step(tok_in, tok_grad, route_ids, gate_vals, *weights):
        tokens, top_k = route_ids.shape[1:]
        return tuple(take(step(2 * tokens * top_k // SLOTS, tok_in, tok_grad, jnp.swapaxes(route_ids, 1, 2), jnp.swapaxes(gate_vals, 1, 2), *weights)))

    return jax.shard_map(device_step, mesh=mesh, in_specs=(tok_spec, tok_spec, route_spec, route_spec, whole_spec, expert_spec, expert_spec, expert_spec), out_specs=(tok_spec, tok_spec, whole_spec, expert_spec, expert_spec, expert_spec), check_vma=False)
```

```python
import functools

import jax
import jax.numpy as jnp
from jax import lax
from jax.experimental import pallas as pl
from jax.experimental.pallas import tpu as pltpu
from jax.sharding import PartitionSpec as P

TOK_AXES = ("rep", "ep", "dp")
F32 = jnp.float32
BF16 = jnp.bfloat16
LANES = 128
SIDE = 4
WAYS = (1, -1)
BUFS = (0, 1)
LAYERS = (1, 0)
ARRAYS = range(3)
SLOTS = 8
MESH = pl.DeviceIdType.MESH
VMEM_LIMIT = 67_043_328


def dot(a, b):
    return jnp.dot(a, b, preferred_element_type=F32)


def dot_nt(a, b):
    return lax.dot_general(a, b, (((1,), (1,)), ((), ())), preferred_element_type=F32)


def dot_tn(a, b):
    return lax.dot_general(a, b, (((0,), (0,)), ((), ())), preferred_element_type=F32)


class Place:
    def __init__(self):
        self.z, self.y, dp = lax.axis_index("rep"), lax.axis_index("ep"), lax.axis_index("dp")
        self.x, self.c = dp // 2, dp % 2

    def at(self, axis, step):
        z, y, x, c = self.z, self.y, self.x, self.c
        if axis == "z":
            z = (z + step + SIDE) % SIDE
        elif axis == "y":
            y = (y + step + SIDE) % SIDE
        elif axis == "x":
            x = (x + step + SIDE) % SIDE
        else:
            c = 1 - c
        return (z, y, x * 2 + c)


class Copies:
    def __init__(self, place, send, recv):
        self.place, self.send, self.recv, self.made, self.number, self.count, self.over = place, send, recv, {}, {}, 0, set()

    def add(self, key, src, dst, axis, step, like=None):
        if like is None:
            n, self.count = self.count, self.count + 1
        else:
            n = self.number[like]
        self.number[key] = n
        self.made[key] = pltpu.make_async_remote_copy(src_ref=src, dst_ref=dst, send_sem=self.send.at[n], recv_sem=self.recv.at[n], device_id=self.place.at(axis, step), device_id_type=MESH)

    def start(self, *keys):
        for key in keys:
            self.made[key].start()

    def arrive(self, *keys):
        for key in keys:
            self.made[key].wait_recv()

    def sent(self, *keys):
        for key in keys:
            self.made[key].wait_send()
            self.over.add(key)

    def drain(self):
        self.sent(*[key for key in self.made if key not in self.over])


def greet(place):
    barrier = pltpu.get_barrier_semaphore()
    peers = [(axis, step) for axis in "xyz" for step in WAYS] + [("c", 0)]
    for axis, step in peers:
        pl.semaphore_signal(barrier, inc=1, device_id=place.at(axis, step), device_id_type=MESH)
    pl.semaphore_wait(barrier, len(peers))


class Gather:
    PASS = {2: 4, 3: 6, 5: 7}

    def __init__(self, layer, copies, place, own, whole):
        self.layer, self.copies, self.place, self.own, self.whole = layer, copies, place, own, whole
        rows, ff = own[0].shape[2], own[2].shape[2]
        self.cut = {"x": ((0, 0, rows // SIDE), (2, 0, ff // 2 // SIDE)), "z": ((1, 0, rows // SIDE), (2, ff // 2, ff // 2 // SIDE))}
        mine = {"x": place.x, "z": place.z}
        for color in ("x", "z"):
            for part in BUFS:
                self._add(("y", 2, color, part), color, part, None, 2, mine[color], None, "y", 1)
                self._add(("y", 3, color, part), color, part, None, 3, mine[color], None, "y", -1)
                if color == "x":
                    self._add(("y", 5, color, part), color, part, 2, 5, mine[color], None, "y", 1)
                else:
                    self._add(("y", 5, color, part), color, part, 3, 5, mine[color], None, "y", -1)
                for slot in (2, 3, 5):
                    for step in WAYS:
                        self._add(("near", slot, color, part, step), color, part, slot, slot, mine[color], None, color, step)
                        behind = (mine[color] - step + SIDE) % SIDE
                        self._add(("far", slot, color, part, step), color, part, slot, slot, behind, (1 - step) // 2, color, step)
        for slot, to in self.PASS.items():
            for array in ARRAYS:
                copies.add((layer, "pass", slot, array), whole[array].at[layer, slot], whole[array].at[layer, to], "c", 0)

    def _view(self, refs, index, color, part, quarter, half):
        array, base, size = self.cut[color][part]
        start = base + quarter * size
        if half is not None:
            size = size // 2
            start = start + half * size
        return refs[array].at[self.layer, index, pl.ds(pl.multiple_of(start, 16), size)]

    def _add(self, key, color, part, src_slot, dst_slot, quarter, half, axis, step):
        src = self._view(self.own, self.place.c, color, part, quarter, half) if src_slot is None else self._view(self.whole, src_slot, color, part, quarter, half)
        self.copies.add((self.layer,) + key, src, self._view(self.whole, dst_slot, color, part, quarter, half), axis, step)

    def _keys(self, *key, extra=()):
        return [(self.layer,) + key + (part,) + extra for part in BUFS]

    def lead(self):
        self.spread(2, "x")
        self.spread(3, "z")

    def lead_onward(self):
        self.onward(2, "x")
        self.onward(3, "z")

    def follow(self):
        self.spread(2, "z")
        self.spread(3, "x")

    def follow_onward(self):
        self.onward(2, "z")
        self.onward(3, "x")

    def last(self):
        self.spread(5, "x")
        self.spread(5, "z")

    def last_onward(self):
        self.onward(5, "x")
        self.onward(5, "z")

    def complete_y(self):
        self.complete(2)
        self.complete(3)

    def complete_last(self):
        self.complete(5)

    def passed_left(self):
        self.passed(2)

    def passed_right(self):
        self.passed(3)

    def passed_last(self):
        self.passed(5)

    def begin(self):
        self.copies.start(*self._keys("y", 2, "x"), *self._keys("y", 3, "z"))

    def second(self):
        self.copies.sent(*self._keys("y", 2, "x"), *self._keys("y", 3, "z"))
        self.copies.start(*self._keys("y", 2, "z"), *self._keys("y", 3, "x"))

    def third(self):
        self.copies.sent(*self._keys("y", 2, "z"), *self._keys("y", 3, "x"))
        self.copies.start(*self._keys("y", 5, "x"), *self._keys("y", 5, "z"))

    def spread(self, slot, color):
        self.copies.arrive(*self._keys("y", slot, color))
        for step in WAYS:
            self.copies.start(*self._keys("near", slot, color, extra=(step,)))

    def onward(self, slot, color):
        for step in WAYS:
            self.copies.arrive(*self._keys("near", slot, color, extra=(step,)))
            self.copies.start(*self._keys("far", slot, color, extra=(step,)))

    def complete(self, slot):
        for color in ("x", "z"):
            for step in WAYS:
                self.copies.arrive(*self._keys("far", slot, color, extra=(step,)))
        self.copies.start(*[(self.layer, "pass", slot, array) for array in ARRAYS])

    def passed(self, slot):
        self.copies.arrive(*[(self.layer, "pass", slot, array) for array in ARRAYS])


GATHER_COPIES = 2 * (2 * 2 * (3 + 3 * 4) + 9)


def route(ids_ref, gate_ref, rows_ref, columns_ref, place):
    layers, _, tokens = ids_ref.shape
    below = lax.broadcasted_iota(jnp.int32, (tokens, tokens), 0) < lax.broadcasted_iota(jnp.int32, (tokens, tokens), 1)
    below = jnp.where(below, 1.0, 0.0).astype(BF16)
    lead = lax.broadcasted_iota(jnp.int32, (2 * SLOTS, tokens), 0)
    for layer in range(layers):
        ids, gates = ids_ref[layer], gate_ref[layer]
        off = ((ids >> 1) - place.y) & (SIDE - 1)
        odd = (ids + place.c) & 1
        slot = jnp.where(off == 0, odd, jnp.where(off == SIDE - 1, 2 + 2 * odd, jnp.where(off == 1, 3 + 3 * odd, 5 + 2 * odd)))
        hits = [slot[n : n + 1] == lead for n in BUFS]
        hit = hits[0] | hits[1]
        weight = jnp.where(hits[0], gates[0:1], 0.0) + jnp.where(hits[1], gates[1:2], 0.0)
        rank = jnp.where(hit, dot(jnp.where(hit, 1.0, 0.0).astype(BF16), below), -1.0)
        rows_ref[layer] = rank[:SLOTS].astype(jnp.int32)
        columns_ref[layer] = jnp.transpose(jnp.concatenate([rank[:SLOTS], weight[:SLOTS], jnp.zeros((LANES - 2 * SLOTS, tokens), F32)], axis=0))


def one_hot(rows_ref, layer, slot, cap):
    place = lax.broadcasted_iota(jnp.int32, (cap, rows_ref.shape[2]), 0)
    return jnp.where(rows_ref[layer, pl.ds(slot, 1), :] == place, 1.0, 0.0).astype(BF16)


def column(columns_ref, layer, index):
    lane = lax.broadcasted_iota(jnp.int32, columns_ref.shape[1:], 1)
    return jnp.sum(jnp.where(lane == index, columns_ref[layer], 0.0), axis=1, keepdims=True)


def one_hot_t(columns_ref, layer, slot, cap):
    place = lax.broadcasted_iota(jnp.int32, (columns_ref.shape[1], cap), 1)
    return jnp.where(column(columns_ref, layer, slot).astype(jnp.int32) == place, 1.0, 0.0).astype(BF16)


def add_to(dst, src):
    dst[...] = (dst[...].astype(F32) + src[...].astype(F32)).astype(BF16)


def cut(rows, half):
    first = (rows // 2 + 15) // 16 * 16
    return (half * first, first + half * (rows - 2 * first))


class RingSum:
    def __init__(self, copies, name, axis, block, first, second):
        self.copies, self.block, self.second = copies, block, second
        self.first = [first.at[half, pl.ds(0, block(2, half).shape[0])] for half in BUFS]
        self.early, self.later = ([(name, when, step) for step in WAYS] for when in ("early", "later"))
        for half, step in enumerate(WAYS):
            copies.add(self.early[half], block(2, half), self.first[half], axis, step)
            copies.add(self.later[half], block(step, None), second.at[half], axis, step)

    def start(self):
        self.copies.start(*self.early)

    def onward(self):
        self.copies.arrive(*self.early)
        for half in BUFS:
            add_to(self.block(WAYS[half], half), self.first[half])
            self.copies.start(self.later[half])
        self.copies.sent(*self.early)

    def finish(self, out):
        self.copies.arrive(*self.later)
        out[...] = (self.block(0, None)[...].astype(F32) + self.second[0].astype(F32) + self.second[1].astype(F32)).astype(BF16)
        self.copies.sent(*self.later)


class RingSpread:
    def __init__(self, copies, name, axis, me, block, source=None, like=None):
        self.copies = copies
        self.near, self.far = ([(name, when, step) for step in WAYS] for when in ("near", "far"))
        for half, step in enumerate(WAYS):
            behind = (me - step + SIDE) % SIDE
            near, far = (None, None) if like is None else (like.near[half], like.far[half])
            copies.add(self.near[half], block(me, None) if source is None else source, block(me, None), axis, step, near)
            copies.add(self.far[half], block(behind, half), block(behind, half), axis, step, far)

    def start(self):
        self.copies.start(*self.near)

    def onward(self):
        for near, far in zip(self.near, self.far):
            self.copies.arrive(near)
            self.copies.start(far)

    def finish(self):
        self.copies.arrive(*self.far)
        self.copies.sent(*self.near, *self.far)


def slices(ref, lead, base, size):
    def block(index, half):
        start, rows = base + index * size, size
        if half is not None:
            skip, rows = cut(size, half)
            start = start + skip
        return ref.at[(*lead, pl.ds(pl.multiple_of(start, 16), rows))]

    return block


def slabs(ref):
    def block(index, half):
        if half is None:
            return ref.at[index]
        return ref.at[index, pl.ds(*cut(ref.shape[1], half))]

    return block


def total(ref):
    return (ref[0].astype(F32) + ref[1].astype(F32) + ref[2].astype(F32) + ref[3].astype(F32)).astype(BF16)


OWN_STEPS = {2: 0, 4: 1, 5: 2, 7: 3}
REDUCE_COPIES = 111
WEIGHTS1, INPUTS1, WEIGHTS0, INPUTS0, STEPS = (n * SLOTS for n in range(2, 7))


def kernel(cap, x0_ref, dy_ref, ids_ref, gate_ref, wd_ref, o1_ref, o3_ref, o2_ref, y_ref, dx_ref, gdense_ref, g1_ref, g3_ref, g2_ref, h1_ref, h3_ref, h2_ref, kz_ref, ka_ref, kb_ref, kda_ref, kdb_ref, acc_ref, cur_ref, x1_ref, hold_ref, gd_ref, rows_ref, columns_ref, w1_ref, w3_ref, w2_ref, z_ref, a_ref, b_ref, m1_ref, m3_ref, m2_ref, d1_ref, d3_ref, d2_ref, s1_ref, s3_ref, s2_ref, r11_ref, r12_ref, r31_ref, r32_ref, t1_ref, t3_ref, y11_ref, y12_ref, y31_ref, y32_ref, y21_ref, y22_ref, u1_ref, u2_ref, l1_ref, l2_ref, c1_ref, c3_ref, cu_ref, cl_ref, f1_ref, f3_ref, fu_ref, fl_ref, dp_ref, dr_ref, ds_ref, e1_ref, e2_ref, dcx_ref, dcz_ref, dcy_ref, de_ref, put_sem, load_sem, keep_sem, save_sem, gsend_sem, grecv_sem, send_sem, recv_sem, credit):
    s = pl.program_id(0)
    place = Place()
    gathers = Copies(place, gsend_sem, grecv_sem)
    copies = Copies(place, send_sem, recv_sem)
    given, whole, bufs = (o1_ref, o3_ref, o2_ref), (h1_ref, h3_ref, h2_ref), (w1_ref, w3_ref, w2_ref)
    kept, acts = (kz_ref, ka_ref, kb_ref), (z_ref, a_ref, b_ref)
    deferred = (kda_ref, kdb_ref)
    g0, g1 = (Gather(l, gathers, place, given, whole) for l in BUFS)
    rows, ff = s1_ref.shape[1], s2_ref.shape[1]
    quarter, part = rows // SIDE, ff // 2 // SIDE
    half_d = rows // 2

    stage, mate, mine_of = (m1_ref, m3_ref, m2_ref), (d1_ref, d3_ref, d2_ref), (s1_ref, s3_ref, s2_ref)
    outs = (g1_ref, g3_ref, g2_ref)
    for buf in BUFS:
        for n in ARRAYS:
            copies.add(("pair", buf, n), stage[n].at[buf], mate[n].at[buf], "c", 0)

    def ring_blocks(ref, q, me, base, size):
        block = slices(ref, (q,), base, size)
        return lambda offset, half: block((me + offset + SIDE) % SIDE, half)

    def group_blocks(ref):
        block = slabs(ref)
        return lambda offset, half: block({2: 0, 1: 1, -1: 2, 0: 3}[offset], half)

    first = {
        "x": [RingSum(copies, ("x", q), "x", ring_blocks(s1_ref, q, place.x, 0, quarter), r11_ref.at[q], r12_ref.at[q]) for q in range(SIDE)],
        "z": [RingSum(copies, ("z", q), "z", ring_blocks(s3_ref, q, place.z, 0, quarter), r31_ref.at[q], r32_ref.at[q]) for q in range(SIDE)],
    }
    mid = {"x": t1_ref, "z": t3_ref}
    on_y = {
        "x": RingSum(copies, "yx", "y", group_blocks(t1_ref), y11_ref, y12_ref),
        "z": RingSum(copies, "yz", "y", group_blocks(t3_ref), y31_ref, y32_ref),
        "w": RingSum(copies, "yw", "y", group_blocks(s2_ref), y21_ref, y22_ref),
    }
    inner = {
        "u": RingSum(copies, "u", "x", ring_blocks(s2_ref, 3, place.x, 0, part), u1_ref, u2_ref),
        "l": RingSum(copies, "l", "z", ring_blocks(s2_ref, 3, place.z, ff // 2, part), l1_ref, l2_ref),
    }
    ring_of = {"x": ("x", place.x), "u": ("x", place.x), "z": ("z", place.z), "l": ("z", place.z)}
    other_of = {"x": ("z", place.z), "u": ("z", place.z), "z": ("x", place.x), "l": ("x", place.x)}
    cross_ref = {"x": c1_ref, "z": c3_ref, "u": cu_ref, "l": cl_ref}
    done_ref = {"x": f1_ref, "z": f3_ref, "u": fu_ref, "l": fl_ref}
    out_of = {"x": (g1_ref, 0, quarter), "z": (g3_ref, 0, quarter), "u": (g2_ref, 0, part), "l": (g2_ref, ff // 2, part)}
    cross, final, puts = {}, {}, {}
    for i, k in enumerate(out_of):
        cross[k] = RingSpread(copies, ("cross", k), *other_of[k], slabs(cross_ref[k]))
        ref, base, size = out_of[k]
        for late in LAYERS:
            block = slices(ref, (late, place.c), base, size)
            final[k, late] = RingSpread(copies, ("final", k, late), *ring_of[k], block, source=done_ref[k], like=final.get((k, 1)))
            puts[k, late] = pltpu.make_async_copy(done_ref[k], block(ring_of[k][1], None), put_sem.at[i])
    mine, theirs = (pl.ds(pl.multiple_of(c * half_d, 16), half_d) for c in (place.c, 1 - place.c))
    for late in LAYERS:
        for n, out in enumerate(outs):
            copies.add(("pass", n, late), out.at[late, place.c], out.at[late, place.c], "c", 0, None if late else ("pass", n, 1))
    copies.add("dense pair", dp_ref.at[theirs], dr_ref, "c", 0)
    copies.add("dense pass", dcy_ref, de_ref, "c", 0)
    piece = half_d // SIDE
    dense_block = slices(ds_ref, (), 0, piece)
    dense_sums = RingSum(copies, "dense sums", "y", lambda offset, half: dense_block((place.y + offset + SIDE) % SIDE, half), e1_ref, e2_ref)
    dense = {k: RingSpread(copies, ("dense", k), k, me, block) for k, me, block in (("x", place.x, slabs(dcx_ref)), ("z", place.z, slabs(dcz_ref)), ("y", place.y, slices(dcy_ref, (), 0, piece)))}

    def reduce_start(q):
        for k in ("x", "z"):
            first[k][q].start()

    def reduce_onward(q):
        for k in ("x", "z"):
            first[k][q].onward()

    def reduce_finish(q):
        for k in ("x", "z"):
            first[k][q].finish(mid[k].at[q])

    def y_start():
        for k in ("x", "z"):
            on_y[k].start()

    def y_onward():
        for k in ("x", "z"):
            on_y[k].onward()

    def y_finish():
        for k in ("x", "z"):
            on_y[k].finish(cross_ref[k].at[other_of[k][1]])
            cross[k].start()

    def w_finish():
        on_y["w"].finish(s2_ref.at[3])
        for k in ("u", "l"):
            inner[k].start()

    def inner_onward():
        for k in ("u", "l"):
            inner[k].onward()

    def inner_finish():
        for k in ("u", "l"):
            inner[k].finish(cross_ref[k].at[other_of[k][1]])
            cross[k].start()

    def cross_onward(*keys):
        for k in keys:
            cross[k].onward()

    def cross_finish(late, *keys):
        for k in keys:
            cross[k].finish()
            done_ref[k][...] = total(cross_ref[k])
            puts[k, late].start()
            final[k, late].start()

    def final_onward(late, *keys):
        for k in keys:
            final[k, late].onward()

    def final_finish(late, *keys):
        for k in keys:
            final[k, late].finish()
            puts[k, late].wait()
        copies.start(*[("pass", n, late) for n in ARRAYS if ("xzu"[n] in keys)])

    def pass_finish(late):
        keys = [("pass", n, late) for n in ARRAYS]
        copies.arrive(*keys)
        copies.sent(*keys)

    def dense_sum():
        copies.arrive("dense pair")
        ds_ref[...] = (dp_ref[mine].astype(F32) + dr_ref[...].astype(F32)).astype(BF16)
        copies.sent("dense pair")
        dense_sums.start()

    def dense_to_x():
        dense_sums.finish(dcx_ref.at[place.x])
        dense["x"].start()

    def dense_to_z():
        dense["x"].finish()
        dcz_ref[place.z] = total(dcx_ref)
        dense["z"].start()

    def dense_to_y():
        dense["z"].finish()
        dcy_ref[pl.ds(pl.multiple_of(place.y * piece, 16), piece)] = total(dcz_ref)
        dense["y"].start()

    def dense_out(late):
        return pltpu.make_async_copy(gd_ref, gdense_ref.at[late], keep_sem.at[0, 1])

    def dense_pass(late):
        dense["y"].finish()
        if late == 0:
            dense_out(1).wait()
        gd_ref[mine] = dcy_ref[...]
        copies.start("dense pass")

    def dense_finish(late):
        copies.arrive("dense pass")
        gd_ref[theirs] = de_ref[...]
        copies.sent("dense pass")
        dense_out(late).start()

    def copy(src, dst, sem):
        return pltpu.make_async_copy(src, dst, sem)

    def weights(layer, slot, arrays, buf, is_given=False):
        for n in arrays:
            src = given[n].at[layer, (place.c + slot) % 2] if is_given else whole[n].at[layer, slot]
            yield copy(src, bufs[n].at[buf], load_sem.at[buf, n])

    def saved(layer, slot, buf):
        for n, (src, dst) in enumerate(zip(kept, acts)):
            yield copy(src.at[layer, slot], dst.at[buf], load_sem.at[buf, 3 + n])

    def weights_loads(step):
        layer, slot, buf = layer_of(step), SLOTS - 1 - step % SLOTS, (step + 1) % 2
        return [*weights(layer, slot, [2], buf), *saved(layer, slot, buf)]

    def inputs_loads(step):
        layer, slot, buf = layer_of(step), SLOTS - 1 - step % SLOTS, (step + 1) % 2
        return [*weights(layer, slot, BUFS, buf)] + [copy(deferred[n].at[slot], acts[n + 1].at[buf], load_sem.at[buf, 4 + n]) for n in BUFS]

    def load(step):
        slot = step % SLOTS
        for is_given in (True, False):
            pl.when((slot < 2) == is_given)(lambda: start(weights(step // SLOTS, slot, ARRAYS, step % 2, is_given)))

    def layer_of(step):
        return 1 - (step - WEIGHTS1) // (2 * SLOTS)

    def keeps(step):
        return [copy(bufs[n].at[step % 2], whole[n].at[step // SLOTS, step % SLOTS], keep_sem.at[step % 2, n]) for n in ARRAYS]

    def saves(step):
        return [copy(src.at[step % 2], dst.at[step // SLOTS, step % SLOTS], save_sem.at[step % 2, n]) for n, (src, dst) in enumerate(zip(acts, kept))]

    def defers(step):
        return [copy(acts[n + 1].at[2], deferred[n].at[SLOTS - 1 - step % SLOTS], save_sem.at[0, n]) for n in BUFS]

    def wait(items):
        for item in items:
            item.wait()

    def start(items):
        for item in items:
            item.start()

    def ending():
        dense_finish(1)
        copies.start("dense pair")
        y_finish()
        inner_finish()
        dense_sum()
        dense_sums.onward()
        cross_onward("x", "z")
        dense_to_x()
        cross_onward("u", "l")
        dense["x"].onward()
        cross_finish(0, "x", "z")
        dense_to_z()
        cross_finish(0, "u", "l")
        dense["z"].onward()
        dense_to_y()
        final_onward(0, "x", "z")
        dense["y"].onward()
        final_onward(0, "u", "l")
        dense_pass(0)
        final_finish(0, "x", "z")
        final_finish(0, "u", "l")
        dense_finish(0)
        pass_finish(0)

    before, middle, after = {}, {}, {}

    def plan(table, first, *stages):
        for n, stage in enumerate(stages):
            table.setdefault(first + n, []).extend(stage)

    on, done = lambda q: lambda: reduce_onward(q), lambda q: lambda: reduce_finish(q)
    now = lambda: load(s)
    plan(before, 0, [g0.second, g0.lead], [g0.third, g0.follow, g0.lead_onward], [g1.begin, g0.follow_onward, g0.complete_y, now, g0.last])
    plan(before, 3, [g0.passed_left, g1.second], [g0.last_onward, g1.lead], [g0.complete_last, now, g1.third, g0.passed_right], [g1.follow], [g0.passed_last, now, g1.lead_onward])
    plan(before, SLOTS + 1, [g1.follow_onward], [g1.complete_y, now, g1.last], [g1.passed_left], [g1.last_onward], [g1.complete_last, now, g1.passed_right], [], [g1.passed_last, now])
    unready = (1, 4, 6, SLOTS + 1, SLOTS + 4, SLOTS + 6)
    late = ("x", "z", "u", "l")
    plan(before, WEIGHTS0, [lambda: copies.start("dense pair"), inner_onward], [], [inner_finish, dense_sums.onward], [lambda: cross_onward("x", "z"), dense_to_x], [lambda: cross_onward("u", "l")])
    plan(middle, WEIGHTS0, [dense_sum, y_finish], [], [], [], [dense["x"].onward], [lambda: cross_finish(1, *late)], [dense_to_z])
    plan(before, INPUTS0, [dense["z"].onward], [lambda: final_onward(1, *late)], [dense_to_y], [lambda: final_finish(1, *late)], [dense["y"].onward], [], [lambda: dense_pass(1)], [lambda: pass_finish(1)])
    plan(before, INPUTS1 + 6, [w_finish])
    plan(before, INPUTS0 + 5, [w_finish], [], [inner_onward])
    for base in (WEIGHTS1, WEIGHTS0):
        plan(before, base + 3, [on_y["w"].start], [], [], [on_y["w"].onward])
        plan(middle, base + 4, [on(0)], [], [done(0), y_start, on(1)], [on(2)])
        plan(before, base + SLOTS, [], [done(1)], [done(2), y_onward], [on(3)], [], [], [done(3)])
        for step, q in OWN_STEPS.items():
            plan(after, base + step, [lambda q=q: reduce_start(q)])

    def hooks(table, *phases):
        for phase in phases:
            mine = {step: stages for step, stages in sorted(table.items()) if phase <= step < phase + SLOTS}
            if mine:

                @pl.when(s // SLOTS == phase // SLOTS)
                def _(mine=mine):
                    for step, stages in mine.items():

                        @pl.when(s == step)
                        def _(stages=stages):
                            for stage in stages:
                                stage()

    phase, t = s // SLOTS, s % SLOTS
    forth, back = s % 2, (s + 1) % 2

    def bring(ref, hold):
        return copy(ref, hold, keep_sem.at[1, 0])

    @pl.when(s == 0)
    def _():
        bring(x0_ref, hold_ref).start()
        load(0)
        greet(place)
        g0.begin()
        load(1)
        route(ids_ref, gate_ref, rows_ref, columns_ref, place)
        bring(x0_ref, hold_ref).wait()

    def enter(x):
        cur_ref[...] = (x.astype(F32) + dot(x, wd_ref[phase])).astype(BF16)
        acc_ref[...] = jnp.zeros_like(acc_ref)

    def leave(out_ref):
        out_ref[...] = (cur_ref[...].astype(F32) + acc_ref[...]).astype(BF16)

    @pl.when(s < WEIGHTS1)
    def _():
        hooks(before, 0, SLOTS)
        pl.when(s > 1)(lambda: wait(saves(s - 2)))
        ahead = functools.reduce(jnp.logical_and, [s != step for step in unready], (s > 0) & (s < WEIGHTS1 - 1))
        pl.when(ahead)(lambda: load(s + 1))

        @pl.when(t < 2)
        def _():
            pl.when(s == 0)(lambda: enter(hold_ref[...]))
            pl.when(s == SLOTS)(lambda: enter(x1_ref[...]))

        layer, slot = phase, t
        z = dot(one_hot(rows_ref, layer, slot, cap), cur_ref[...]).astype(BF16)
        z_ref[forth] = z
        come = list(weights(layer, slot, ARRAYS, forth))
        wait(come[:2])
        a = dot(z, w1_ref[forth]).astype(BF16)
        b = dot(z, w3_ref[forth]).astype(BF16)
        a_ref[forth] = a
        b_ref[forth] = b
        h = (jax.nn.silu(a.astype(F32)) * b.astype(F32)).astype(BF16)
        wait(come[2:])
        pl.when(t < 2)(lambda: start(keeps(s)))
        o = dot(h, w2_ref[forth]).astype(BF16)
        acc_ref[...] += column(columns_ref, layer, SLOTS + slot) * dot(one_hot_t(columns_ref, layer, slot, cap), o)
        pl.when(s < WEIGHTS1 - 1)(lambda: start(saves(s)))
        pl.when(t < 2)(lambda: wait(keeps(s)))

        @pl.when(t == SLOTS - 1)
        def _():
            pl.when(s == SLOTS - 1)(lambda: leave(x1_ref))
            pl.when(s == WEIGHTS1 - 1)(lambda: leave(hold_ref))

    @pl.when((phase == WEIGHTS1 // SLOTS) | (phase == WEIGHTS0 // SLOTS))
    def _():
        layer, slot = layer_of(s), SLOTS - 1 - t
        hooks(before, WEIGHTS1, WEIGHTS0)

        @pl.when(s == WEIGHTS1)
        def _():
            moved = copy(hold_ref, y_ref, keep_sem.at[0, 0])
            moved.start()
            bring(dy_ref, cur_ref).start()
            wait(saves(s - 2))
            gathers.drain()
            bring(dy_ref, cur_ref).wait()
            moved.wait()
            acc_ref[...] = cur_ref[...].astype(F32)

        pl.when(s > WEIGHTS1)(lambda: wait(weights_loads(s)))
        pl.when(t > 0)(lambda: wait(defers(s - 1)))
        pl.when(t < SLOTS - 1)(lambda: start(weights_loads(s + 1)))
        pl.when(t == SLOTS - 1)(lambda: start(inputs_loads(s + 1)))

        grad_gated = (column(columns_ref, layer, SLOTS + slot) * cur_ref[...].astype(F32)).astype(BF16)
        do = dot(one_hot(rows_ref, layer, slot, cap), grad_gated).astype(BF16)
        dh = dot_nt(do, w2_ref[back])
        a = a_ref[back].astype(F32)
        b = b_ref[back].astype(F32)
        sig = jax.nn.sigmoid(a)
        act = a * sig
        h = (act * b).astype(BF16)
        db = (dh * act).astype(BF16)
        da = (dh * b * (sig + act * (1.0 - sig))).astype(BF16)
        a_ref[2] = da
        b_ref[2] = db
        z = z_ref[back]
        start(defers(s))
        hooks(middle, WEIGHTS1, WEIGHTS0)

        def weight_grads():
            return dot_tn(z, da), dot_tn(z, db), dot_tn(h, do)

        is_own = functools.reduce(jnp.logical_or, [t == step for step in OWN_STEPS])
        group = t // 4 + t // 5 + t // 7
        into = (t + t // 3 + t // 6) % 2
        turn = t + (1 - layer) * SLOTS

        @pl.when(jnp.logical_not(is_own))
        def _():
            for buf in BUFS:
                pl.when((turn >= 3) & (into == buf))(lambda: copies.sent(*[("pair", buf, n) for n in ARRAYS]))

            for ref, grad in zip(stage, weight_grads()):
                ref[into] = grad.astype(BF16)

            pl.when(turn >= 3)(lambda: pl.semaphore_wait(credit.at[into], 1))
            for buf in BUFS:
                pl.when(into == buf)(lambda: copies.start(*[("pair", buf, n) for n in ARRAYS]))

        @pl.when(is_own)
        def _():
            for buf in BUFS:
                pl.when(group % 2 == buf)(lambda: copies.arrive(*[("pair", buf, n) for n in ARRAYS]))

            for ref, add, grad in zip(mine_of, mate, weight_grads()):
                ref[group] = (grad + add[group % 2].astype(F32)).astype(BF16)

            @pl.when(turn < 2 * SLOTS - 3)
            def _():
                pl.semaphore_signal(credit.at[group % 2], inc=1, device_id=place.at("c", 0), device_id_type=MESH)

            hooks(after, WEIGHTS1, WEIGHTS0)

    def leave_back(layer, x, out_ref):
        grad = acc_ref[...]
        grad_b = grad.astype(BF16)
        dp_ref[...] = dot_tn(x, grad_b).astype(BF16)
        out_ref[...] = (grad + dot_nt(grad_b, wd_ref[layer])).astype(BF16)

    @pl.when((phase == INPUTS1 // SLOTS) | (phase == INPUTS0 // SLOTS))
    def _():
        layer, slot = layer_of(s), SLOTS - 1 - t
        hooks(before, INPUTS1, INPUTS0)
        wait(inputs_loads(s))
        pl.when(t == 0)(lambda: wait(defers(s - 1)))
        pl.when(t < SLOTS - 1)(lambda: start(inputs_loads(s + 1)))
        pl.when(s == WEIGHTS0 - 1)(lambda: start(weights_loads(s + 1)))
        dz = (dot_nt(a_ref[back], w1_ref[back]) + dot_nt(b_ref[back], w3_ref[back])).astype(BF16)
        acc_ref[...] += dot(one_hot_t(columns_ref, layer, slot, cap), dz)

        @pl.when(s == WEIGHTS0 - 1)
        def _():
            leave_back(1, x1_ref[...], cur_ref)
            acc_ref[...] = cur_ref[...].astype(F32)
            bring(x0_ref, x1_ref).start()
            bring(x0_ref, x1_ref).wait()

        @pl.when(s == STEPS - 1)
        def _():
            leave_back(0, x1_ref[...], hold_ref)
            moved = copy(hold_ref, dx_ref, keep_sem.at[0, 0])
            moved.start()
            ending()
            copies.sent(*[("pair", buf, n) for buf in BUFS for n in ARRAYS])
            moved.wait()
            dense_out(0).wait()


def step(cap, x0, dy, ids, gates, wd, w1, w3, w2):
    tokens, width = dy.shape
    layers, local, _, ff = w1.shape
    quarter, part, piece = width // SIDE, ff // 2 // SIDE, width // 2 // SIDE
    hbm = pl.BlockSpec(memory_space=pl.ANY)

    def fixed(shape):
        return pl.BlockSpec(shape, lambda s: (0,) * len(shape), pipeline_mode=pl.Buffered(1))

    def buf(*shape):
        return pltpu.VMEM(shape, BF16)

    def dma(*shape):
        return pltpu.SemaphoreType.DMA(shape)

    shape = jax.ShapeDtypeStruct
    ups, downs = [(width, ff), (width, ff), (ff, width)], [(quarter, ff), (part, width)]
    acts = [(cap, width), (cap, ff), (cap, ff)]
    scratch = [pltpu.VMEM((tokens, width), F32)] + [buf(tokens, width)] * 3 + [buf(width, width), pltpu.VMEM((layers, SLOTS, tokens), jnp.int32), pltpu.VMEM((layers, tokens, LANES), F32)]
    scratch += [buf(2, *u) for u in ups] + [buf(n, *a) for n, a in zip((2, 3, 3), acts)]
    scratch += [buf(2, *u) for u in ups] * 2 + [buf(SIDE, *u) for u in ups]
    scratch += [buf(SIDE, 2, quarter // 2, ff), buf(SIDE, 2, quarter, ff)] * 2
    scratch += [buf(SIDE, quarter, ff)] * 2
    scratch += [buf(2, quarter // 2, ff), buf(2, quarter, ff)] * 2 + [buf(2, ff // 2, width), buf(2, ff, width)]
    scratch += [buf(2, part // 2, width), buf(2, part, width)] * 2
    scratch += [buf(SIDE, quarter, ff)] * 2 + [buf(SIDE, part, width)] * 2
    scratch += [buf(quarter, ff)] * 2 + [buf(part, width)] * 2
    scratch += [buf(width, width)] + [buf(width // 2, width)] * 2 + [buf(2, piece, width)] * 2 + [buf(SIDE, piece, width)] * 2 + [buf(width // 2, width)] * 2
    scratch += [dma(4), dma(2, 6), dma(2, 3), dma(2, 3), dma(GATHER_COPIES), dma(GATHER_COPIES), dma(REDUCE_COPIES), dma(REDUCE_COPIES), pltpu.SemaphoreType.REGULAR((2,))]
    results = [(tokens, width), (tokens, width), (layers, width, width)]
    kept = [(layers, local, *u) for u in ups] + [(layers, SLOTS, *u) for u in ups + acts] + [(SLOTS, cap, ff)] * 2
    return pl.pallas_call(
        functools.partial(kernel, cap),
        grid=(STEPS,),
        in_specs=[hbm] * 2 + [fixed(v.shape) for v in (ids, gates, wd)] + [hbm] * 3,
        out_specs=[hbm] * len(results + kept),
        out_shape=[shape(r, BF16) for r in results + kept],
        scratch_shapes=scratch,
        compiler_params=pltpu.CompilerParams(vmem_limit_bytes=VMEM_LIMIT, collective_id=0, has_side_effects=True),
        name="step",
    )(x0, dy, ids, gates, wd, w1, w3, w2)[:6]


def take_kernel(count, *refs):
    sources, targets, holds, (come, go) = refs[:count], refs[count : 2 * count], refs[2 * count : 3 * count], refs[3 * count :]
    comes = [pltpu.make_async_copy(a, b, come.at[n]) for n, (a, b) in enumerate(zip(sources, holds))]
    goes = [pltpu.make_async_copy(a, b, go.at[n]) for n, (a, b) in enumerate(zip(holds, targets))]
    for item in comes:
        item.start()
    for first, then in zip(comes, goes):
        first.wait()
        then.start()
    for item in goes:
        item.wait()


def take(arrays):
    count = len(arrays)
    hbm = pl.BlockSpec(memory_space=pl.ANY)
    return pl.pallas_call(
        functools.partial(take_kernel, count),
        in_specs=[hbm] * count,
        out_specs=[hbm] * count,
        out_shape=[jax.ShapeDtypeStruct(a.shape, a.dtype) for a in arrays],
        scratch_shapes=[pltpu.VMEM(a.shape, a.dtype) for a in arrays] + [pltpu.SemaphoreType.DMA((count,))] * 2,
        compiler_params=pltpu.CompilerParams(vmem_limit_bytes=VMEM_LIMIT),
        name="take",
    )(*arrays)


def solution(mesh):
    tok_spec = P(TOK_AXES, None)
    route_spec = P(None, TOK_AXES, None)
    expert_spec = P(None, "ep", None, None)
    whole_spec = P(None, None, None)

    def device_step(tok_in, tok_grad, route_ids, gate_vals, *weights):
        tokens, top_k = route_ids.shape[1:]
        return tuple(take(step(2 * tokens * top_k // SLOTS, tok_in, tok_grad, jnp.swapaxes(route_ids, 1, 2), jnp.swapaxes(gate_vals, 1, 2), *weights)))

    return jax.shard_map(device_step, mesh=mesh, in_specs=(tok_spec, tok_spec, route_spec, route_spec, whole_spec, expert_spec, expert_spec, expert_spec), out_specs=(tok_spec, tok_spec, whole_spec, expert_spec, expert_spec, expert_spec), check_vma=False)
```

```python
import functools

import jax
import jax.numpy as jnp
from jax import lax
from jax.experimental import pallas as pl
from jax.experimental.pallas import tpu as pltpu
from jax.sharding import PartitionSpec as P

TOK_AXES = ("rep", "ep", "dp")
F32 = jnp.float32
BF16 = jnp.bfloat16
LANES = 128
SIDE = 4
WAYS = (1, -1)
BUFS = (0, 1)
LAYERS = (1, 0)
ARRAYS = range(3)
SLOTS = 8
MESH = pl.DeviceIdType.MESH
VMEM_LIMIT = 67_043_328


def dot(a, b):
    return jnp.dot(a, b, preferred_element_type=F32)


def dot_nt(a, b):
    return lax.dot_general(a, b, (((1,), (1,)), ((), ())), preferred_element_type=F32)


def dot_tn(a, b):
    return lax.dot_general(a, b, (((0,), (0,)), ((), ())), preferred_element_type=F32)


class Place:
    def __init__(self):
        self.z, self.y, dp = lax.axis_index("rep"), lax.axis_index("ep"), lax.axis_index("dp")
        self.x, self.c = dp // 2, dp % 2

    def at(self, axis, step):
        z, y, x, c = self.z, self.y, self.x, self.c
        if axis == "z":
            z = (z + step + SIDE) % SIDE
        elif axis == "y":
            y = (y + step + SIDE) % SIDE
        elif axis == "x":
            x = (x + step + SIDE) % SIDE
        else:
            c = 1 - c
        return (z, y, x * 2 + c)


class Copies:
    def __init__(self, place, send, recv):
        self.place, self.send, self.recv, self.made, self.number, self.count, self.over = place, send, recv, {}, {}, 0, set()

    def add(self, key, src, dst, axis, step, like=None):
        if like is None:
            n, self.count = self.count, self.count + 1
        else:
            n = self.number[like]
        self.number[key] = n
        self.made[key] = pltpu.make_async_remote_copy(src_ref=src, dst_ref=dst, send_sem=self.send.at[n], recv_sem=self.recv.at[n], device_id=self.place.at(axis, step), device_id_type=MESH)

    def start(self, *keys):
        for key in keys:
            self.made[key].start()

    def arrive(self, *keys):
        for key in keys:
            self.made[key].wait_recv()

    def sent(self, *keys):
        for key in keys:
            self.made[key].wait_send()
            self.over.add(key)

    def drain(self):
        self.sent(*[key for key in self.made if key not in self.over])


def greet(place):
    barrier = pltpu.get_barrier_semaphore()
    peers = [(axis, step) for axis in "xyz" for step in range(1, SIDE)] + [("c", 0)]
    for axis, step in peers:
        pl.semaphore_signal(barrier, inc=1, device_id=place.at(axis, step), device_id_type=MESH)
    pl.semaphore_wait(barrier, len(peers))


class Gather:
    PASS = {2: 4, 3: 6, 5: 7}

    def __init__(self, layer, copies, place, own, whole):
        self.layer, self.copies, self.place, self.own, self.whole = layer, copies, place, own, whole
        rows, ff = own[0].shape[2], own[2].shape[2]
        self.cut = {"x": ((0, 0, rows // SIDE), (2, 0, ff // 2 // SIDE)), "z": ((1, 0, rows // SIDE), (2, ff // 2, ff // 2 // SIDE))}
        mine = {"x": place.x, "z": place.z}
        for color in ("x", "z"):
            for part in BUFS:
                self._add(("y", 2, color, part), color, part, None, 2, mine[color], None, "y", 1)
                self._add(("y", 3, color, part), color, part, None, 3, mine[color], None, "y", -1)
                if color == "x":
                    self._add(("y", 5, color, part), color, part, 2, 5, mine[color], None, "y", 1)
                else:
                    self._add(("y", 5, color, part), color, part, 3, 5, mine[color], None, "y", -1)
                for slot in (2, 3, 5):
                    for step in WAYS:
                        self._add(("near", slot, color, part, step), color, part, slot, slot, mine[color], None, color, step)
                        behind = (mine[color] - step + SIDE) % SIDE
                        self._add(("far", slot, color, part, step), color, part, slot, slot, behind, (1 - step) // 2, color, step)
        for slot, to in self.PASS.items():
            for array in ARRAYS:
                copies.add((layer, "pass", slot, array), whole[array].at[layer, slot], whole[array].at[layer, to], "c", 0)

    def _view(self, refs, index, color, part, quarter, half):
        array, base, size = self.cut[color][part]
        start = base + quarter * size
        if half is not None:
            size = size // 2
            start = start + half * size
        return refs[array].at[self.layer, index, pl.ds(pl.multiple_of(start, 16), size)]

    def _add(self, key, color, part, src_slot, dst_slot, quarter, half, axis, step):
        src = self._view(self.own, self.place.c, color, part, quarter, half) if src_slot is None else self._view(self.whole, src_slot, color, part, quarter, half)
        self.copies.add((self.layer,) + key, src, self._view(self.whole, dst_slot, color, part, quarter, half), axis, step)

    def _keys(self, *key, extra=()):
        return [(self.layer,) + key + (part,) + extra for part in BUFS]

    def lead(self):
        self.spread(2, "x")
        self.spread(3, "z")

    def lead_onward(self):
        self.onward(2, "x")
        self.onward(3, "z")

    def follow(self):
        self.spread(2, "z")
        self.spread(3, "x")

    def follow_onward(self):
        self.onward(2, "z")
        self.onward(3, "x")

    def last(self):
        self.spread(5, "x")
        self.spread(5, "z")

    def last_onward(self):
        self.onward(5, "x")
        self.onward(5, "z")

    def complete_y(self):
        self.complete(2)
        self.complete(3)

    def complete_last(self):
        self.complete(5)

    def passed_left(self):
        self.passed(2)

    def passed_right(self):
        self.passed(3)

    def passed_last(self):
        self.passed(5)

    def begin(self):
        for slot, color in ((2, "x"), (3, "z"), (2, "z"), (3, "x")):
            self.copies.start(*self._keys("y", slot, color))

    def spread(self, slot, color):
        for part in BUFS:
            self.copies.arrive((self.layer, "y", slot, color, part))
            self.copies.start(*[(self.layer, "near", slot, color, part, step) for step in WAYS])
        if (slot, color) in ((2, "x"), (3, "z")):
            self.copies.start(*self._keys("y", 5, color))

    def onward(self, slot, color):
        for part in BUFS:
            for step in WAYS:
                self.copies.arrive((self.layer, "near", slot, color, part, step))
                self.copies.start((self.layer, "far", slot, color, part, step))

    def complete(self, slot):
        for color in ("x", "z"):
            for step in WAYS:
                self.copies.arrive(*self._keys("far", slot, color, extra=(step,)))
        self.copies.start(*[(self.layer, "pass", slot, array) for array in ARRAYS])

    def passed(self, slot):
        self.copies.arrive(*[(self.layer, "pass", slot, array) for array in ARRAYS])


GATHER_COPIES = 2 * (2 * 2 * (3 + 3 * 4) + 9)


def route(ids_ref, gate_ref, rows_ref, columns_ref, place):
    layers, _, tokens = ids_ref.shape
    below = lax.broadcasted_iota(jnp.int32, (tokens, tokens), 0) < lax.broadcasted_iota(jnp.int32, (tokens, tokens), 1)
    below = jnp.where(below, 1.0, 0.0).astype(BF16)
    lead = lax.broadcasted_iota(jnp.int32, (2 * SLOTS, tokens), 0)
    for layer in range(layers):
        ids, gates = ids_ref[layer], gate_ref[layer]
        off = ((ids >> 1) - place.y) & (SIDE - 1)
        odd = (ids + place.c) & 1
        slot = jnp.where(off == 0, odd, jnp.where(off == SIDE - 1, 2 + 2 * odd, jnp.where(off == 1, 3 + 3 * odd, 5 + 2 * odd)))
        hits = [slot[n : n + 1] == lead for n in BUFS]
        hit = hits[0] | hits[1]
        weight = jnp.where(hits[0], gates[0:1], 0.0) + jnp.where(hits[1], gates[1:2], 0.0)
        rank = jnp.where(hit, dot(jnp.where(hit, 1.0, 0.0).astype(BF16), below), -1.0)
        rows_ref[layer] = rank[:SLOTS].astype(jnp.int32)
        columns_ref[layer] = jnp.transpose(jnp.concatenate([rank[:SLOTS], weight[:SLOTS], jnp.zeros((LANES - 2 * SLOTS, tokens), F32)], axis=0))


def one_hot(rows_ref, layer, slot, cap):
    place = lax.broadcasted_iota(jnp.int32, (cap, rows_ref.shape[2]), 0)
    return jnp.where(rows_ref[layer, pl.ds(slot, 1), :] == place, 1.0, 0.0).astype(BF16)


def column(columns_ref, layer, index):
    lane = lax.broadcasted_iota(jnp.int32, columns_ref.shape[1:], 1)
    return jnp.sum(jnp.where(lane == index, columns_ref[layer], 0.0), axis=1, keepdims=True)


def one_hot_t(columns_ref, layer, slot, cap):
    place = lax.broadcasted_iota(jnp.int32, (columns_ref.shape[1], cap), 1)
    return jnp.where(column(columns_ref, layer, slot).astype(jnp.int32) == place, 1.0, 0.0).astype(BF16)


def add_to(dst, src):
    dst[...] = (dst[...].astype(F32) + src[...].astype(F32)).astype(BF16)


def cut(rows, half):
    first = (rows // 2 + 15) // 16 * 16
    return (half * first, first + half * (rows - 2 * first))


class RingSum:
    def __init__(self, copies, name, axis, block, first, second):
        self.copies, self.block, self.second = copies, block, second
        self.first = [first.at[half, pl.ds(0, block(2, half).shape[0])] for half in BUFS]
        self.early, self.later = ([(name, when, step) for step in WAYS] for when in ("early", "later"))
        for half, step in enumerate(WAYS):
            copies.add(self.early[half], block(2, half), self.first[half], axis, step)
            copies.add(self.later[half], block(step, None), second.at[half], axis, step)

    def start(self):
        self.copies.start(*self.early)

    def onward(self):
        self.copies.arrive(*self.early)
        for half in BUFS:
            add_to(self.block(WAYS[half], half), self.first[half])
            self.copies.start(self.later[half])
        self.copies.sent(*self.early)

    def finish(self, out):
        self.copies.arrive(*self.later)
        out[...] = (self.block(0, None)[...].astype(F32) + self.second[0].astype(F32) + self.second[1].astype(F32)).astype(BF16)
        self.copies.sent(*self.later)


class RingSpread:
    def __init__(self, copies, name, axis, me, block, source=None, like=None):
        self.copies = copies
        self.near, self.far = ([(name, when, step) for step in WAYS] for when in ("near", "far"))
        for half, step in enumerate(WAYS):
            behind = (me - step + SIDE) % SIDE
            near, far = (None, None) if like is None else (like.near[half], like.far[half])
            copies.add(self.near[half], block(me, None) if source is None else source, block(me, None), axis, step, near)
            copies.add(self.far[half], block(behind, half), block(behind, half), axis, step, far)

    def start(self):
        self.copies.start(*self.near)

    def onward(self):
        for near, far in zip(self.near, self.far):
            self.copies.arrive(near)
            self.copies.start(far)

    def finish(self):
        self.copies.arrive(*self.far)
        self.copies.sent(*self.near, *self.far)


class Direct:
    def __init__(self, copies, name, axis, source, target):
        self.copies, self.keys = copies, [(name, step) for step in range(1, SIDE)]
        for name, step in self.keys:
            copies.add((name, step), source(step), target(step), axis, step)

    def start(self):
        self.copies.start(*self.keys)

    def finish(self):
        self.copies.arrive(*self.keys)
        self.copies.sent(*self.keys)


def slices(ref, lead, base, size):
    def block(index, half):
        start, rows = base + index * size, size
        if half is not None:
            skip, rows = cut(size, half)
            start = start + skip
        return ref.at[(*lead, pl.ds(pl.multiple_of(start, 16), rows))]

    return block


def slabs(ref):
    def block(index, half):
        if half is None:
            return ref.at[index]
        return ref.at[index, pl.ds(*cut(ref.shape[1], half))]

    return block


def total(ref):
    return (ref[0].astype(F32) + ref[1].astype(F32) + ref[2].astype(F32) + ref[3].astype(F32)).astype(BF16)


OWN_STEPS = {2: 0, 4: 1, 5: 2, 7: 3}
REDUCE_COPIES = 107
WEIGHTS1, INPUTS1, WEIGHTS0, INPUTS0, STEPS = (n * SLOTS for n in range(2, 7))


def kernel(cap, x0_ref, dy_ref, ids_ref, gate_ref, wd_ref, o1_ref, o3_ref, o2_ref, y_ref, dx_ref, gdense_ref, g1_ref, g3_ref, g2_ref, h1_ref, h3_ref, h2_ref, kz_ref, ka_ref, kb_ref, kda_ref, kdb_ref, acc_ref, cur_ref, x1_ref, hold_ref, gd_ref, rows_ref, columns_ref, w1_ref, w3_ref, w2_ref, z_ref, a_ref, b_ref, m1_ref, m3_ref, m2_ref, d1_ref, d3_ref, d2_ref, s1_ref, s3_ref, s2_ref, r11_ref, r12_ref, r31_ref, r32_ref, t1_ref, t3_ref, y11_ref, y12_ref, y31_ref, y32_ref, y21_ref, y22_ref, u1_ref, u2_ref, l1_ref, l2_ref, c1_ref, c3_ref, cu_ref, cl_ref, f1_ref, f3_ref, fu_ref, fl_ref, dp_ref, dr_ref, ds_ref, e_ref, dcx_ref, dcz_ref, dcy_ref, de_ref, put_sem, load_sem, keep_sem, save_sem, gsend_sem, grecv_sem, send_sem, recv_sem, credit):
    s = pl.program_id(0)
    place = Place()
    gathers = Copies(place, gsend_sem, grecv_sem)
    copies = Copies(place, send_sem, recv_sem)
    given, whole, bufs = (o1_ref, o3_ref, o2_ref), (h1_ref, h3_ref, h2_ref), (w1_ref, w3_ref, w2_ref)
    kept, acts = (kz_ref, ka_ref, kb_ref), (z_ref, a_ref, b_ref)
    deferred = (kda_ref, kdb_ref)
    g0, g1 = (Gather(l, gathers, place, given, whole) for l in BUFS)
    rows, ff = s1_ref.shape[1], s2_ref.shape[1]
    quarter, part = rows // SIDE, ff // 2 // SIDE
    half_d = rows // 2

    stage, mate, mine_of = (m1_ref, m3_ref, m2_ref), (d1_ref, d3_ref, d2_ref), (s1_ref, s3_ref, s2_ref)
    outs = (g1_ref, g3_ref, g2_ref)
    for buf in BUFS:
        for n in ARRAYS:
            copies.add(("pair", buf, n), stage[n].at[buf], mate[n].at[buf], "c", 0)

    def ring_blocks(ref, q, me, base, size):
        block = slices(ref, (q,), base, size)
        return lambda offset, half: block((me + offset + SIDE) % SIDE, half)

    def group_blocks(ref):
        block = slabs(ref)
        return lambda offset, half: block({2: 0, 1: 1, -1: 2, 0: 3}[offset], half)

    first = {
        "x": [RingSum(copies, ("x", q), "x", ring_blocks(s1_ref, q, place.x, 0, quarter), r11_ref.at[q], r12_ref.at[q]) for q in range(SIDE)],
        "z": [RingSum(copies, ("z", q), "z", ring_blocks(s3_ref, q, place.z, 0, quarter), r31_ref.at[q], r32_ref.at[q]) for q in range(SIDE)],
    }
    mid = {"x": t1_ref, "z": t3_ref}
    on_y = {
        "x": RingSum(copies, "yx", "y", group_blocks(t1_ref), y11_ref, y12_ref),
        "z": RingSum(copies, "yz", "y", group_blocks(t3_ref), y31_ref, y32_ref),
        "w": RingSum(copies, "yw", "y", group_blocks(s2_ref), y21_ref, y22_ref),
    }
    inner = {
        "u": RingSum(copies, "u", "x", ring_blocks(s2_ref, 3, place.x, 0, part), u1_ref, u2_ref),
        "l": RingSum(copies, "l", "z", ring_blocks(s2_ref, 3, place.z, ff // 2, part), l1_ref, l2_ref),
    }
    ring_of = {"x": ("x", place.x), "u": ("x", place.x), "z": ("z", place.z), "l": ("z", place.z)}
    other_of = {"x": ("z", place.z), "u": ("z", place.z), "z": ("x", place.x), "l": ("x", place.x)}
    cross_ref = {"x": c1_ref, "z": c3_ref, "u": cu_ref, "l": cl_ref}
    done_ref = {"x": f1_ref, "z": f3_ref, "u": fu_ref, "l": fl_ref}
    out_of = {"x": (g1_ref, 0, quarter), "z": (g3_ref, 0, quarter), "u": (g2_ref, 0, part), "l": (g2_ref, ff // 2, part)}
    cross, final, puts = {}, {}, {}
    for i, k in enumerate(out_of):
        cross[k] = RingSpread(copies, ("cross", k), *other_of[k], slabs(cross_ref[k]))
        ref, base, size = out_of[k]
        for late in LAYERS:
            block = slices(ref, (late, place.c), base, size)
            final[k, late] = RingSpread(copies, ("final", k, late), *ring_of[k], block, source=done_ref[k], like=final.get((k, 1)))
            puts[k, late] = pltpu.make_async_copy(done_ref[k], block(ring_of[k][1], None), put_sem.at[i])
    mine, theirs = (pl.ds(pl.multiple_of(c * half_d, 16), half_d) for c in (place.c, 1 - place.c))
    for late in LAYERS:
        for n, out in enumerate(outs):
            copies.add(("pass", n, late), out.at[late, place.c], out.at[late, place.c], "c", 0, None if late else ("pass", n, 1))
    copies.add("dense pair", dp_ref.at[theirs], dr_ref, "c", 0)
    copies.add("dense pass", dcy_ref, de_ref, "c", 0)
    piece = half_d // SIDE
    dense_block = slices(ds_ref, (), 0, piece)
    dense_sums = Direct(copies, "dense sums", "y", lambda step: dense_block((place.y + step) % SIDE, None), lambda step: e_ref.at[step - 1])
    gather_block = slices(dcy_ref, (), 0, piece)(place.y, None)
    own_piece = {"x": dcx_ref.at[place.x], "z": dcz_ref.at[place.z], "y": gather_block}
    dense = {k: Direct(copies, ("dense", k), k, lambda step, k=k: own_piece[k], lambda step, k=k: own_piece[k]) for k in own_piece}

    def reduce_start(q):
        for k in ("x", "z"):
            first[k][q].start()

    def reduce_onward(q):
        for k in ("x", "z"):
            first[k][q].onward()

    def reduce_finish(q):
        for k in ("x", "z"):
            first[k][q].finish(mid[k].at[q])

    def y_start():
        for k in ("x", "z"):
            on_y[k].start()

    def y_onward():
        for k in ("x", "z"):
            on_y[k].onward()

    def y_finish():
        for k in ("x", "z"):
            on_y[k].finish(cross_ref[k].at[other_of[k][1]])
            cross[k].start()

    def w_finish():
        on_y["w"].finish(s2_ref.at[3])
        for k in ("u", "l"):
            inner[k].start()

    def inner_onward():
        for k in ("u", "l"):
            inner[k].onward()

    def inner_finish():
        for k in ("u", "l"):
            inner[k].finish(cross_ref[k].at[other_of[k][1]])
            cross[k].start()

    def cross_onward(*keys):
        for k in keys:
            cross[k].onward()

    def cross_finish(late, *keys):
        for k in keys:
            cross[k].finish()
            done_ref[k][...] = total(cross_ref[k])
            puts[k, late].start()
            final[k, late].start()

    def final_onward(late, *keys):
        for k in keys:
            final[k, late].onward()

    def final_finish(late, *keys):
        for k in keys:
            final[k, late].finish()
            puts[k, late].wait()
        copies.start(*[("pass", n, late) for n in ARRAYS if ("xzu"[n] in keys)])

    def pass_finish(late):
        keys = [("pass", n, late) for n in ARRAYS]
        copies.arrive(*keys)
        copies.sent(*keys)

    def dense_sum():
        copies.arrive("dense pair")
        ds_ref[...] = (dp_ref[mine].astype(F32) + dr_ref[...].astype(F32)).astype(BF16)
        copies.sent("dense pair")
        dense_sums.start()

    def dense_to_x():
        dense_sums.finish()
        mine = dense_block(place.y, None)[...].astype(F32)
        own_piece["x"][...] = (mine + e_ref[0].astype(F32) + e_ref[1].astype(F32) + e_ref[2].astype(F32)).astype(BF16)
        dense["x"].start()

    def dense_next(k, ref, follow):
        dense[k].finish()
        own_piece[follow][...] = total(ref)
        dense[follow].start()

    def dense_to_z():
        dense_next("x", dcx_ref, "z")

    def dense_to_y():
        dense_next("z", dcz_ref, "y")

    def dense_out(late):
        return pltpu.make_async_copy(gd_ref, gdense_ref.at[late], keep_sem.at[0, 1])

    def dense_pass(late):
        dense["y"].finish()
        if late == 0:
            dense_out(1).wait()
        gd_ref[mine] = dcy_ref[...]
        copies.start("dense pass")

    def dense_finish(late):
        copies.arrive("dense pass")
        gd_ref[theirs] = de_ref[...]
        copies.sent("dense pass")
        dense_out(late).start()

    def copy(src, dst, sem):
        return pltpu.make_async_copy(src, dst, sem)

    def weights(layer, slot, arrays, buf, is_given=False):
        for n in arrays:
            src = given[n].at[layer, (place.c + slot) % 2] if is_given else whole[n].at[layer, slot]
            yield copy(src, bufs[n].at[buf], load_sem.at[buf, n])

    def saved(layer, slot, buf):
        for n, (src, dst) in enumerate(zip(kept, acts)):
            yield copy(src.at[layer, slot], dst.at[buf], load_sem.at[buf, 3 + n])

    def weights_loads(step):
        layer, slot, buf = layer_of(step), SLOTS - 1 - step % SLOTS, (step + 1) % 2
        return [*weights(layer, slot, [2], buf), *saved(layer, slot, buf)]

    def inputs_loads(step):
        layer, slot, buf = layer_of(step), SLOTS - 1 - step % SLOTS, (step + 1) % 2
        return [*weights(layer, slot, BUFS, buf)] + [copy(deferred[n].at[slot], acts[n + 1].at[buf], load_sem.at[buf, 4 + n]) for n in BUFS]

    def load(step):
        slot = step % SLOTS
        for is_given in (True, False):
            pl.when((slot < 2) == is_given)(lambda: start(weights(step // SLOTS, slot, ARRAYS, step % 2, is_given)))

    def layer_of(step):
        return 1 - (step - WEIGHTS1) // (2 * SLOTS)

    def keeps(step):
        return [copy(bufs[n].at[step % 2], whole[n].at[step // SLOTS, step % SLOTS], keep_sem.at[step % 2, n]) for n in ARRAYS]

    def saves(step):
        return [copy(src.at[step % 2], dst.at[step // SLOTS, step % SLOTS], save_sem.at[step % 2, n]) for n, (src, dst) in enumerate(zip(acts, kept))]

    def defers(step):
        return [copy(acts[n + 1].at[2], deferred[n].at[SLOTS - 1 - step % SLOTS], save_sem.at[0, n]) for n in BUFS]

    def wait(items):
        for item in items:
            item.wait()

    def start(items):
        for item in items:
            item.start()

    def ending():
        dense_finish(1)
        copies.start("dense pair")
        y_finish()
        inner_finish()
        dense_sum()
        dense_to_x()
        cross_onward("x", "z")
        pass_finish(1)
        pl.semaphore_signal(credit.at[2], inc=1, device_id=place.at("c", 0), device_id_type=MESH)
        cross_onward("u", "l")
        dense_to_z()
        cross_finish(0, "x", "z")
        cross_finish(0, "u", "l")
        dense_to_y()
        dense_pass(0)
        final_onward(0, "x", "z")
        dense_finish(0)
        final_onward(0, "u", "l")
        pl.semaphore_wait(credit.at[2], 1)
        final_finish(0, "x", "z")
        final_finish(0, "u", "l")
        pass_finish(0)

    before, middle, after = {}, {}, {}

    def plan(table, first, *stages):
        for n, stage in enumerate(stages):
            table.setdefault(first + n, []).extend(stage)

    on, done = lambda q: lambda: reduce_onward(q), lambda q: lambda: reduce_finish(q)
    now = lambda: load(s)
    plan(before, 1, [g0.lead], [g0.follow, g0.lead_onward, g1.begin, g0.follow_onward, g0.last, g0.complete_y, now], [g0.passed_left])
    plan(before, 4, [g0.last_onward, g1.lead], [g0.complete_last, now, g0.passed_right, g1.follow], [], [g0.passed_last, now, g1.lead_onward])
    plan(before, SLOTS + 1, [g1.follow_onward, g1.last], [g1.complete_y, now], [g1.passed_left], [g1.last_onward], [g1.complete_last, now, g1.passed_right], [g1.passed_last])
    unready = (1, 4, 6, SLOTS + 1, SLOTS + 4)
    late = ("x", "z", "u", "l")
    plan(before, INPUTS1 + 5, [w_finish], [], [inner_onward])
    plan(before, WEIGHTS0, [lambda: copies.start("dense pair")], [inner_finish], [], [lambda: cross_onward("x", "z"), dense_to_x], [lambda: cross_onward("u", "l")], [dense_to_z])
    plan(middle, WEIGHTS0, [dense_sum, y_finish], [], [], [], [], [], [], [dense_to_y])
    plan(before, INPUTS0, [lambda: cross_finish(1, *late)], [], [lambda: dense_pass(1)], [], [lambda: final_onward(1, *late)], [], [lambda: final_finish(1, *late)])
    plan(before, INPUTS0 + 5, [w_finish], [], [inner_onward])
    for base in (WEIGHTS1, WEIGHTS0):
        plan(before, base + 3, [on_y["w"].start], [], [], [done(0), y_start, on_y["w"].onward])
        plan(middle, base + 4, [on(0)], [], [on(1)], [on(2)])
        plan(before, base + SLOTS, [], [done(1)], [done(2), y_onward], [on(3)], [], [], [done(3)])
        for step, q in OWN_STEPS.items():
            plan(after, base + step, [lambda q=q: reduce_start(q)])

    def hooks(table, *phases):
        for phase in phases:
            mine = {step: stages for step, stages in sorted(table.items()) if phase <= step < phase + SLOTS}
            if mine:

                @pl.when(s // SLOTS == phase // SLOTS)
                def _(mine=mine):
                    for step, stages in mine.items():

                        @pl.when(s == step)
                        def _(stages=stages):
                            for stage in stages:
                                stage()

    phase, t = s // SLOTS, s % SLOTS
    forth, back = s % 2, (s + 1) % 2

    def bring(ref, hold):
        return copy(ref, hold, keep_sem.at[1, 0])

    @pl.when(s == 0)
    def _():
        bring(x0_ref, hold_ref).start()
        load(0)
        greet(place)
        g0.begin()
        load(1)
        route(ids_ref, gate_ref, rows_ref, columns_ref, place)
        bring(x0_ref, hold_ref).wait()

    def enter(x):
        cur_ref[...] = (x.astype(F32) + dot(x, wd_ref[phase])).astype(BF16)
        acc_ref[...] = jnp.zeros_like(acc_ref)

    def leave(out_ref):
        out_ref[...] = (cur_ref[...].astype(F32) + acc_ref[...]).astype(BF16)

    @pl.when(s < WEIGHTS1)
    def _():
        hooks(before, 0, SLOTS)
        pl.when(s > 1)(lambda: wait(saves(s - 2)))
        ahead = functools.reduce(jnp.logical_and, [s != step for step in unready], (s > 0) & (s < WEIGHTS1 - 1))
        pl.when((t == 1) | (t == 2))(lambda: wait(keeps(s - 1)))
        pl.when(ahead)(lambda: load(s + 1))

        @pl.when(t < 2)
        def _():
            pl.when(s == 0)(lambda: enter(hold_ref[...]))
            pl.when(s == SLOTS)(lambda: enter(x1_ref[...]))

        layer, slot = phase, t
        come = list(weights(layer, slot, ARRAYS, forth))

        def forward_step(is_ready):
            if is_ready:
                wait(come)
            z = dot(one_hot(rows_ref, layer, slot, cap), cur_ref[...]).astype(BF16)
            z_ref[forth] = z
            if not is_ready:
                wait(come)
            a = dot(z, w1_ref[forth]).astype(BF16)
            b = dot(z, w3_ref[forth]).astype(BF16)
            a_ref[forth] = a
            b_ref[forth] = b
            h = (jax.nn.silu(a.astype(F32)) * b.astype(F32)).astype(BF16)
            o = dot(h, w2_ref[forth]).astype(BF16)
            acc_ref[...] += column(columns_ref, layer, SLOTS + slot) * dot(one_hot_t(columns_ref, layer, slot, cap), o)

        is_late = functools.reduce(jnp.logical_or, [s == step + 1 for step in unready])
        pl.when(is_late)(lambda: forward_step(False))
        pl.when(jnp.logical_not(is_late))(lambda: forward_step(True))
        pl.when(t < 2)(lambda: start(keeps(s)))
        pl.when(s < WEIGHTS1 - 1)(lambda: start(saves(s)))
        @pl.when(t == SLOTS - 1)
        def _():
            pl.when(s == SLOTS - 1)(lambda: leave(x1_ref))
            pl.when(s == WEIGHTS1 - 1)(lambda: leave(hold_ref))

    @pl.when((phase == WEIGHTS1 // SLOTS) | (phase == WEIGHTS0 // SLOTS))
    def _():
        layer, slot = layer_of(s), SLOTS - 1 - t
        hooks(before, WEIGHTS1, WEIGHTS0)

        @pl.when(s == WEIGHTS1)
        def _():
            moved = copy(hold_ref, y_ref, keep_sem.at[0, 0])
            moved.start()
            bring(dy_ref, cur_ref).start()
            wait(saves(s - 2))
            gathers.drain()
            bring(dy_ref, cur_ref).wait()
            moved.wait()
            acc_ref[...] = cur_ref[...].astype(F32)

        pl.when(s > WEIGHTS1)(lambda: wait(weights_loads(s)))
        pl.when(t > 0)(lambda: wait(defers(s - 1)))
        pl.when(t < SLOTS - 1)(lambda: start(weights_loads(s + 1)))
        pl.when(t == SLOTS - 1)(lambda: start(inputs_loads(s + 1)))

        grad_gated = (column(columns_ref, layer, SLOTS + slot) * cur_ref[...].astype(F32)).astype(BF16)
        do = dot(one_hot(rows_ref, layer, slot, cap), grad_gated).astype(BF16)
        dh = dot_nt(do, w2_ref[back])
        a = a_ref[back].astype(F32)
        b = b_ref[back].astype(F32)
        sig = jax.nn.sigmoid(a)
        act = a * sig
        h = (act * b).astype(BF16)
        db = (dh * act).astype(BF16)
        da = (dh * b * (sig + act * (1.0 - sig))).astype(BF16)
        a_ref[2] = da
        b_ref[2] = db
        z = z_ref[back]
        start(defers(s))
        hooks(middle, WEIGHTS1, WEIGHTS0)

        def weight_grads():
            return dot_tn(z, da), dot_tn(z, db), dot_tn(h, do)

        is_own = functools.reduce(jnp.logical_or, [t == step for step in OWN_STEPS])
        group = t // 4 + t // 5 + t // 7
        into = (t + t // 3 + t // 6) % 2
        turn = t + (1 - layer) * SLOTS

        @pl.when(jnp.logical_not(is_own))
        def _():
            for buf in BUFS:
                pl.when((turn >= 3) & (into == buf))(lambda: copies.sent(*[("pair", buf, n) for n in ARRAYS]))

            for ref, grad in zip(stage, weight_grads()):
                ref[into] = grad.astype(BF16)

            pl.when(turn >= 3)(lambda: pl.semaphore_wait(credit.at[into], 1))
            for buf in BUFS:
                pl.when(into == buf)(lambda: copies.start(*[("pair", buf, n) for n in ARRAYS]))

        @pl.when(is_own)
        def _():
            for buf in BUFS:
                pl.when(group % 2 == buf)(lambda: copies.arrive(*[("pair", buf, n) for n in ARRAYS]))

            for ref, add, grad in zip(mine_of, mate, weight_grads()):
                ref[group] = (grad + add[group % 2].astype(F32)).astype(BF16)

            @pl.when(turn < 2 * SLOTS - 3)
            def _():
                pl.semaphore_signal(credit.at[group % 2], inc=1, device_id=place.at("c", 0), device_id_type=MESH)

            hooks(after, WEIGHTS1, WEIGHTS0)

    def leave_back(layer, x, out_ref):
        grad = acc_ref[...]
        grad_b = grad.astype(BF16)
        dp_ref[...] = dot_tn(x, grad_b).astype(BF16)
        out_ref[...] = (grad + dot_nt(grad_b, wd_ref[layer])).astype(BF16)

    @pl.when((phase == INPUTS1 // SLOTS) | (phase == INPUTS0 // SLOTS))
    def _():
        layer, slot = layer_of(s), SLOTS - 1 - t
        hooks(before, INPUTS1, INPUTS0)
        wait(inputs_loads(s))
        pl.when(t == 0)(lambda: wait(defers(s - 1)))
        pl.when(t < SLOTS - 1)(lambda: start(inputs_loads(s + 1)))
        pl.when(s == WEIGHTS0 - 1)(lambda: start(weights_loads(s + 1)))
        dz = (dot_nt(a_ref[back], w1_ref[back]) + dot_nt(b_ref[back], w3_ref[back])).astype(BF16)
        acc_ref[...] += dot(one_hot_t(columns_ref, layer, slot, cap), dz)

        @pl.when(s == WEIGHTS0 - 1)
        def _():
            leave_back(1, x1_ref[...], cur_ref)
            acc_ref[...] = cur_ref[...].astype(F32)
            bring(x0_ref, x1_ref).start()
            bring(x0_ref, x1_ref).wait()

        @pl.when(s == STEPS - 1)
        def _():
            leave_back(0, x1_ref[...], hold_ref)
            moved = copy(hold_ref, dx_ref, keep_sem.at[0, 0])
            moved.start()
            ending()
            copies.sent(*[("pair", buf, n) for buf in BUFS for n in ARRAYS])
            moved.wait()
            dense_out(0).wait()


def step(cap, x0, dy, ids, gates, wd, w1, w3, w2):
    tokens, width = dy.shape
    layers, local, _, ff = w1.shape
    quarter, part, piece = width // SIDE, ff // 2 // SIDE, width // 2 // SIDE
    hbm = pl.BlockSpec(memory_space=pl.ANY)

    def fixed(shape):
        return pl.BlockSpec(shape, lambda s: (0,) * len(shape), pipeline_mode=pl.Buffered(1))

    def buf(*shape):
        return pltpu.VMEM(shape, BF16)

    def dma(*shape):
        return pltpu.SemaphoreType.DMA(shape)

    shape = jax.ShapeDtypeStruct
    ups, downs = [(width, ff), (width, ff), (ff, width)], [(quarter, ff), (part, width)]
    acts = [(cap, width), (cap, ff), (cap, ff)]
    scratch = [pltpu.VMEM((tokens, width), F32)] + [buf(tokens, width)] * 3 + [buf(width, width), pltpu.VMEM((layers, SLOTS, tokens), jnp.int32), pltpu.VMEM((layers, tokens, LANES), F32)]
    scratch += [buf(2, *u) for u in ups] + [buf(n, *a) for n, a in zip((2, 3, 3), acts)]
    scratch += [buf(2, *u) for u in ups] * 2 + [buf(SIDE, *u) for u in ups]
    scratch += [buf(SIDE, 2, quarter // 2, ff), buf(SIDE, 2, quarter, ff)] * 2
    scratch += [buf(SIDE, quarter, ff)] * 2
    scratch += [buf(2, quarter // 2, ff), buf(2, quarter, ff)] * 2 + [buf(2, ff // 2, width), buf(2, ff, width)]
    scratch += [buf(2, part // 2, width), buf(2, part, width)] * 2
    scratch += [buf(SIDE, quarter, ff)] * 2 + [buf(SIDE, part, width)] * 2
    scratch += [buf(quarter, ff)] * 2 + [buf(part, width)] * 2
    scratch += [buf(width, width)] + [buf(width // 2, width)] * 2 + [buf(SIDE - 1, piece, width)] + [buf(SIDE, piece, width)] * 2 + [buf(width // 2, width)] * 2
    scratch += [dma(4), dma(2, 6), dma(2, 3), dma(2, 3), dma(GATHER_COPIES), dma(GATHER_COPIES), dma(REDUCE_COPIES), dma(REDUCE_COPIES), pltpu.SemaphoreType.REGULAR((3,))]
    results = [(tokens, width), (tokens, width), (layers, width, width)]
    kept = [(layers, local, *u) for u in ups] + [(layers, SLOTS, *u) for u in ups + acts] + [(SLOTS, cap, ff)] * 2
    return pl.pallas_call(
        functools.partial(kernel, cap),
        grid=(STEPS,),
        in_specs=[hbm] * 2 + [fixed(v.shape) for v in (ids, gates, wd)] + [hbm] * 3,
        out_specs=[hbm] * len(results + kept),
        out_shape=[shape(r, BF16) for r in results + kept],
        scratch_shapes=scratch,
        compiler_params=pltpu.CompilerParams(vmem_limit_bytes=VMEM_LIMIT, collective_id=0, has_side_effects=True),
        name="step",
    )(x0, dy, ids, gates, wd, w1, w3, w2)[:6]


def take_kernel(count, *refs):
    sources, targets, holds, (come, go) = refs[:count], refs[count : 2 * count], refs[2 * count : 3 * count], refs[3 * count :]
    comes = [pltpu.make_async_copy(a, b, come.at[n]) for n, (a, b) in enumerate(zip(sources, holds))]
    goes = [pltpu.make_async_copy(a, b, go.at[n]) for n, (a, b) in enumerate(zip(holds, targets))]
    for item in comes:
        item.start()
    for first, then in zip(comes, goes):
        first.wait()
        then.start()
    for item in goes:
        item.wait()


def take(arrays):
    count = len(arrays)
    hbm = pl.BlockSpec(memory_space=pl.ANY)
    return pl.pallas_call(
        functools.partial(take_kernel, count),
        in_specs=[hbm] * count,
        out_specs=[hbm] * count,
        out_shape=[jax.ShapeDtypeStruct(a.shape, a.dtype) for a in arrays],
        scratch_shapes=[pltpu.VMEM(a.shape, a.dtype) for a in arrays] + [pltpu.SemaphoreType.DMA((count,))] * 2,
        compiler_params=pltpu.CompilerParams(vmem_limit_bytes=VMEM_LIMIT),
        name="take",
    )(*arrays)


def solution(mesh):
    tok_spec = P(TOK_AXES, None)
    route_spec = P(None, TOK_AXES, None)
    expert_spec = P(None, "ep", None, None)
    whole_spec = P(None, None, None)

    def device_step(tok_in, tok_grad, route_ids, gate_vals, *weights):
        tokens, top_k = route_ids.shape[1:]
        return tuple(take(step(2 * tokens * top_k // SLOTS, tok_in, tok_grad, jnp.swapaxes(route_ids, 1, 2), jnp.swapaxes(gate_vals, 1, 2), *weights)))

    return jax.shard_map(device_step, mesh=mesh, in_specs=(tok_spec, tok_spec, route_spec, route_spec, whole_spec, expert_spec, expert_spec, expert_spec), out_specs=(tok_spec, tok_spec, whole_spec, expert_spec, expert_spec, expert_spec), check_vma=False)
```

```python
import functools

import jax
import jax.numpy as jnp
from jax import lax
from jax.experimental import pallas as pl
from jax.experimental.pallas import tpu as pltpu
from jax.sharding import PartitionSpec as P

TOK_AXES = ("rep", "ep", "dp")
F32 = jnp.float32
BF16 = jnp.bfloat16
LANES = 128
SIDE = 4
WAYS = (1, -1)
BUFS = (0, 1)
LAYERS = (1, 0)
ARRAYS = range(3)
SLOTS = 8
MESH = pl.DeviceIdType.MESH
VMEM_LIMIT = 67_043_328


def dot(a, b):
    return jnp.dot(a, b, preferred_element_type=F32)


def sigmoid(a):
    return 0.5 + 0.5 * jnp.tanh(0.5 * a)


def dot_nt(a, b):
    return lax.dot_general(a, b, (((1,), (1,)), ((), ())), preferred_element_type=F32)


def dot_tn(a, b):
    return lax.dot_general(a, b, (((0,), (0,)), ((), ())), preferred_element_type=F32)


class Place:
    def __init__(self):
        self.z, self.y, dp = lax.axis_index("rep"), lax.axis_index("ep"), lax.axis_index("dp")
        self.x, self.c = dp // 2, dp % 2

    def at(self, axis, step):
        z, y, x, c = self.z, self.y, self.x, self.c
        if axis == "z":
            z = (z + step + SIDE) % SIDE
        elif axis == "y":
            y = (y + step + SIDE) % SIDE
        elif axis == "x":
            x = (x + step + SIDE) % SIDE
        else:
            c = 1 - c
        return (z, y, x * 2 + c)


class Copies:
    def __init__(self, place, send, recv):
        self.place, self.send, self.recv, self.made, self.number, self.count, self.over = place, send, recv, {}, {}, 0, set()

    def add(self, key, src, dst, axis, step, like=None):
        if like is None:
            n, self.count = self.count, self.count + 1
        else:
            n = self.number[like]
        self.number[key] = n
        self.made[key] = pltpu.make_async_remote_copy(src_ref=src, dst_ref=dst, send_sem=self.send.at[n], recv_sem=self.recv.at[n], device_id=self.place.at(axis, step), device_id_type=MESH)

    def start(self, *keys):
        for key in keys:
            self.made[key].start()

    def arrive(self, *keys):
        for key in keys:
            self.made[key].wait_recv()

    def sent(self, *keys):
        for key in keys:
            self.made[key].wait_send()
            self.over.add(key)

    def drain(self):
        self.sent(*[key for key in self.made if key not in self.over])


def greet(place):
    barrier = pltpu.get_barrier_semaphore()
    peers = [(axis, step) for axis in "xyz" for step in range(1, SIDE)] + [("c", 0)]
    for axis, step in peers:
        pl.semaphore_signal(barrier, inc=1, device_id=place.at(axis, step), device_id_type=MESH)
    pl.semaphore_wait(barrier, len(peers))


class Gather:
    PASS = {2: 4, 3: 6, 5: 7}

    def __init__(self, layer, copies, place, own, whole):
        self.layer, self.copies, self.place, self.own, self.whole = layer, copies, place, own, whole
        rows, ff = own[0].shape[2], own[2].shape[2]
        self.cut = {"x": ((0, 0, rows // SIDE), (2, 0, ff // 2 // SIDE)), "z": ((1, 0, rows // SIDE), (2, ff // 2, ff // 2 // SIDE))}
        mine = {"x": place.x, "z": place.z}
        for color in ("x", "z"):
            for part in BUFS:
                self._add(("y", 2, color, part), color, part, None, 2, mine[color], None, "y", 1)
                self._add(("y", 3, color, part), color, part, None, 3, mine[color], None, "y", -1)
                if color == "x":
                    self._add(("y", 5, color, part), color, part, 2, 5, mine[color], None, "y", 1)
                else:
                    self._add(("y", 5, color, part), color, part, 3, 5, mine[color], None, "y", -1)
                for slot in (2, 3, 5):
                    for step in WAYS:
                        self._add(("near", slot, color, part, step), color, part, slot, slot, mine[color], None, color, step)
                        behind = (mine[color] - step + SIDE) % SIDE
                        self._add(("far", slot, color, part, step), color, part, slot, slot, behind, (1 - step) // 2, color, step)
        for slot, to in self.PASS.items():
            for array in ARRAYS:
                copies.add((layer, "pass", slot, array), whole[array].at[layer, slot], whole[array].at[layer, to], "c", 0)

    def _view(self, refs, index, color, part, quarter, half):
        array, base, size = self.cut[color][part]
        start = base + quarter * size
        if half is not None:
            size = size // 2
            start = start + half * size
        return refs[array].at[self.layer, index, pl.ds(pl.multiple_of(start, 16), size)]

    def _add(self, key, color, part, src_slot, dst_slot, quarter, half, axis, step):
        src = self._view(self.own, self.place.c, color, part, quarter, half) if src_slot is None else self._view(self.whole, src_slot, color, part, quarter, half)
        self.copies.add((self.layer,) + key, src, self._view(self.whole, dst_slot, color, part, quarter, half), axis, step)

    def _keys(self, *key, extra=()):
        return [(self.layer,) + key + (part,) + extra for part in BUFS]

    def lead(self):
        self.spread(2, "x")
        self.spread(3, "z")

    def lead_onward(self):
        self.onward(2, "x")
        self.onward(3, "z")

    def follow(self):
        self.spread(2, "z")
        self.spread(3, "x")

    def follow_onward(self):
        self.onward(2, "z")
        self.onward(3, "x")

    def last(self):
        self.spread(5, "x")
        self.spread(5, "z")

    def last_onward(self):
        self.onward(5, "x")
        self.onward(5, "z")

    def complete_y(self):
        self.complete(2)
        self.complete(3)

    def complete_last(self):
        self.complete(5)

    def passed_left(self):
        self.passed(2)

    def passed_right(self):
        self.passed(3)

    def passed_last(self):
        self.passed(5)

    def begin(self):
        for slot, color in ((2, "x"), (3, "z"), (2, "z"), (3, "x")):
            self.copies.start(*self._keys("y", slot, color))

    def spread(self, slot, color):
        for part in BUFS:
            self.copies.arrive((self.layer, "y", slot, color, part))
            self.copies.start(*[(self.layer, "near", slot, color, part, step) for step in WAYS])
        if (slot, color) in ((2, "x"), (3, "z")):
            self.copies.start(*self._keys("y", 5, color))

    def onward(self, slot, color):
        for part in BUFS:
            for step in WAYS:
                self.copies.arrive((self.layer, "near", slot, color, part, step))
                self.copies.start((self.layer, "far", slot, color, part, step))

    def complete(self, slot):
        for color in ("x", "z"):
            for step in WAYS:
                self.copies.arrive(*self._keys("far", slot, color, extra=(step,)))
        self.copies.start(*[(self.layer, "pass", slot, array) for array in ARRAYS])

    def passed(self, slot):
        self.copies.arrive(*[(self.layer, "pass", slot, array) for array in ARRAYS])


GATHER_COPIES = 2 * (2 * 2 * (3 + 3 * 4) + 9)


def route(ids_ref, gate_ref, rows_ref, columns_ref, place):
    layers, _, tokens = ids_ref.shape
    below = lax.broadcasted_iota(jnp.int32, (tokens, tokens), 0) < lax.broadcasted_iota(jnp.int32, (tokens, tokens), 1)
    below = jnp.where(below, 1.0, 0.0).astype(BF16)
    lead = lax.broadcasted_iota(jnp.int32, (2 * SLOTS, tokens), 0)
    for layer in range(layers):
        ids, gates = ids_ref[layer], gate_ref[layer]
        off = ((ids >> 1) - place.y) & (SIDE - 1)
        odd = (ids + place.c) & 1
        slot = jnp.where(off == 0, odd, jnp.where(off == SIDE - 1, 2 + 2 * odd, jnp.where(off == 1, 3 + 3 * odd, 5 + 2 * odd)))
        hits = [slot[n : n + 1] == lead for n in BUFS]
        hit = hits[0] | hits[1]
        weight = jnp.where(hits[0], gates[0:1], 0.0) + jnp.where(hits[1], gates[1:2], 0.0)
        rank = jnp.where(hit, dot(jnp.where(hit, 1.0, 0.0).astype(BF16), below), -1.0)
        rows_ref[layer] = rank[:SLOTS].astype(jnp.int32)
        columns_ref[layer] = jnp.transpose(jnp.concatenate([rank[:SLOTS], weight[:SLOTS], jnp.zeros((LANES - 2 * SLOTS, tokens), F32)], axis=0))


def one_hot(rows_ref, layer, slot, cap):
    place = lax.broadcasted_iota(jnp.int32, (cap, rows_ref.shape[2]), 0)
    return jnp.where(rows_ref[layer, pl.ds(slot, 1), :] == place, 1.0, 0.0).astype(BF16)


def column(columns_ref, layer, index):
    lane = lax.broadcasted_iota(jnp.int32, columns_ref.shape[1:], 1)
    return jnp.sum(jnp.where(lane == index, columns_ref[layer], 0.0), axis=1, keepdims=True)


def one_hot_t(columns_ref, layer, slot, cap):
    place = lax.broadcasted_iota(jnp.int32, (columns_ref.shape[1], cap), 1)
    return jnp.where(column(columns_ref, layer, slot).astype(jnp.int32) == place, 1.0, 0.0).astype(BF16)


def add_to(dst, src):
    dst[...] = (dst[...].astype(F32) + src[...].astype(F32)).astype(BF16)


def cut(rows, half):
    first = (rows // 2 + 15) // 16 * 16
    return (half * first, first + half * (rows - 2 * first))


class RingSum:
    def __init__(self, copies, name, axis, block, first, second):
        self.copies, self.block, self.second = copies, block, second
        self.first = [first.at[half, pl.ds(0, block(2, half).shape[0])] for half in BUFS]
        self.early, self.later = ([(name, when, step) for step in WAYS] for when in ("early", "later"))
        for half, step in enumerate(WAYS):
            copies.add(self.early[half], block(2, half), self.first[half], axis, step)
            copies.add(self.later[half], block(step, None), second.at[half], axis, step)

    def start(self):
        self.copies.start(*self.early)

    def onward(self):
        self.copies.arrive(*self.early)
        for half in BUFS:
            add_to(self.block(WAYS[half], half), self.first[half])
            self.copies.start(self.later[half])
        self.copies.sent(*self.early)

    def finish(self, out):
        self.copies.arrive(*self.later)
        out[...] = (self.block(0, None)[...].astype(F32) + self.second[0].astype(F32) + self.second[1].astype(F32)).astype(BF16)
        self.copies.sent(*self.later)


class RingSpread:
    def __init__(self, copies, name, axis, me, block, source=None, like=None):
        self.copies = copies
        self.near, self.far = ([(name, when, step) for step in WAYS] for when in ("near", "far"))
        for half, step in enumerate(WAYS):
            behind = (me - step + SIDE) % SIDE
            near, far = (None, None) if like is None else (like.near[half], like.far[half])
            copies.add(self.near[half], block(me, None) if source is None else source, block(me, None), axis, step, near)
            copies.add(self.far[half], block(behind, half), block(behind, half), axis, step, far)

    def start(self):
        self.copies.start(*self.near)

    def onward(self):
        for near, far in zip(self.near, self.far):
            self.copies.arrive(near)
            self.copies.start(far)

    def finish(self):
        self.copies.arrive(*self.far)
        self.copies.sent(*self.near, *self.far)


class Direct:
    def __init__(self, copies, name, axis, source, target):
        self.copies, self.keys = copies, [(name, step) for step in range(1, SIDE)]
        for name, step in self.keys:
            copies.add((name, step), source(step), target(step), axis, step)

    def start(self):
        self.copies.start(*self.keys)

    def finish(self):
        self.copies.arrive(*self.keys)
        self.copies.sent(*self.keys)


def slices(ref, lead, base, size):
    def block(index, half):
        start, rows = base + index * size, size
        if half is not None:
            skip, rows = cut(size, half)
            start = start + skip
        return ref.at[(*lead, pl.ds(pl.multiple_of(start, 16), rows))]

    return block


def slabs(ref):
    def block(index, half):
        if half is None:
            return ref.at[index]
        return ref.at[index, pl.ds(*cut(ref.shape[1], half))]

    return block


def total(ref):
    return (ref[0].astype(F32) + ref[1].astype(F32) + ref[2].astype(F32) + ref[3].astype(F32)).astype(BF16)


OWN_STEPS = {2: 0, 4: 1, 5: 2, 7: 3}
REDUCE_COPIES = 120
WEIGHTS1, INPUTS1, WEIGHTS0, INPUTS0, STEPS = (n * SLOTS for n in range(2, 7))


def kernel(cap, x0_ref, dy_ref, ids_ref, gate_ref, wd_ref, o1_ref, o3_ref, o2_ref, y_ref, dx_ref, gdense_ref, g1_ref, g3_ref, g2_ref, h1_ref, h3_ref, h2_ref, kz_ref, ka_ref, kb_ref, kda_ref, kdb_ref, acc_ref, cur_ref, x1_ref, hold_ref, gd_ref, rows_ref, columns_ref, w1_ref, w3_ref, w2_ref, z_ref, a_ref, b_ref, m1_ref, m3_ref, m2_ref, d1_ref, d3_ref, d2_ref, s1_ref, s3_ref, s2_ref, r11_ref, r12_ref, r31_ref, r32_ref, t1_ref, t3_ref, y11_ref, y12_ref, y31_ref, y32_ref, y21_ref, y22_ref, u1_ref, u2_ref, l1_ref, l2_ref, c1_ref, c3_ref, cu_ref, cl_ref, f1_ref, f3_ref, fu_ref, fl_ref, dp_ref, dr_ref, ds_ref, e_ref, dcx_ref, dcz_ref, dcy_ref, de_ref, put_sem, load_sem, keep_sem, save_sem, gsend_sem, grecv_sem, send_sem, recv_sem, credit):
    s = pl.program_id(0)
    place = Place()
    gathers = Copies(place, gsend_sem, grecv_sem)
    copies = Copies(place, send_sem, recv_sem)
    given, whole, bufs = (o1_ref, o3_ref, o2_ref), (h1_ref, h3_ref, h2_ref), (w1_ref, w3_ref, w2_ref)
    kept, acts = (kz_ref, ka_ref, kb_ref), (z_ref, a_ref, b_ref)
    deferred = (kda_ref, kdb_ref)
    g0, g1 = (Gather(l, gathers, place, given, whole) for l in BUFS)
    rows, ff = s1_ref.shape[1], s2_ref.shape[1]
    quarter, part = rows // SIDE, ff // 2 // SIDE
    half_d = rows // 2

    stage, mate, mine_of = (m1_ref, m3_ref, m2_ref), (d1_ref, d3_ref, d2_ref), (s1_ref, s3_ref, s2_ref)
    for buf in BUFS:
        for n in ARRAYS:
            copies.add(("pair", buf, n), stage[n].at[buf], mate[n].at[buf], "c", 0)

    def ring_blocks(ref, q, me, base, size):
        block = slices(ref, (q,), base, size)
        return lambda offset, half: block((me + offset + SIDE) % SIDE, half)

    def group_blocks(ref):
        block = slabs(ref)
        return lambda offset, half: block({2: 0, 1: 1, -1: 2, 0: 3}[offset], half)

    first = {
        "x": [RingSum(copies, ("x", q), "x", ring_blocks(s1_ref, q, place.x, 0, quarter), r11_ref.at[q], r12_ref.at[q]) for q in range(SIDE)],
        "z": [RingSum(copies, ("z", q), "z", ring_blocks(s3_ref, q, place.z, 0, quarter), r31_ref.at[q], r32_ref.at[q]) for q in range(SIDE)],
    }
    mid = {"x": t1_ref, "z": t3_ref}
    on_y = {
        "x": RingSum(copies, "yx", "y", group_blocks(t1_ref), y11_ref, y12_ref),
        "z": RingSum(copies, "yz", "y", group_blocks(t3_ref), y31_ref, y32_ref),
        "w": RingSum(copies, "yw", "y", group_blocks(s2_ref), y21_ref, y22_ref),
    }
    inner = {
        "u": RingSum(copies, "u", "x", ring_blocks(s2_ref, 3, place.x, 0, part), u1_ref, u2_ref),
        "l": RingSum(copies, "l", "z", ring_blocks(s2_ref, 3, place.z, ff // 2, part), l1_ref, l2_ref),
    }
    ring_of = {"x": ("x", place.x), "u": ("x", place.x), "z": ("z", place.z), "l": ("z", place.z)}
    other_of = {"x": ("z", place.z), "u": ("z", place.z), "z": ("x", place.x), "l": ("x", place.x)}
    cross_ref = {"x": c1_ref, "z": c3_ref, "u": cu_ref, "l": cl_ref}
    done_ref = {"x": f1_ref, "z": f3_ref, "u": fu_ref, "l": fl_ref}
    out_of = {"x": (g1_ref, 0, quarter), "z": (g3_ref, 0, quarter), "u": (g2_ref, 0, part), "l": (g2_ref, ff // 2, part)}
    cross, final, puts = {}, {}, {}
    for i, k in enumerate(out_of):
        cross[k] = RingSpread(copies, ("cross", k), *other_of[k], slabs(cross_ref[k]))
        ref, base, size = out_of[k]
        for late in LAYERS:
            block = slices(ref, (late, place.c), base, size)
            final[k, late] = RingSpread(copies, ("final", k, late), *ring_of[k], block, source=done_ref[k], like=final.get((k, 1)))
            me = ring_of[k][1]
            puts[k, late] = pltpu.make_async_copy(done_ref[k], block(me, None), put_sem.at[i])
            for offset in (0, *WAYS, 2):
                quarter_at = block((me + offset) % SIDE if offset >= 0 else (me + SIDE - 1) % SIDE, None)
                copies.add(("pass", k, offset, late), quarter_at if offset else done_ref[k], quarter_at, "c", 0, None if late else ("pass", k, offset, 1))
    mine, theirs = (pl.ds(pl.multiple_of(c * half_d, 16), half_d) for c in (place.c, 1 - place.c))
    copies.add("dense pair", dp_ref.at[theirs], dr_ref, "c", 0)
    copies.add("dense pass", dcy_ref, de_ref, "c", 0)
    piece = half_d // SIDE
    dense_block = slices(ds_ref, (), 0, piece)
    dense_sums = Direct(copies, "dense sums", "y", lambda step: dense_block((place.y + step) % SIDE, None), lambda step: e_ref.at[step - 1])
    gather_block = slices(dcy_ref, (), 0, piece)(place.y, None)
    own_piece = {"x": dcx_ref.at[place.x], "z": dcz_ref.at[place.z], "y": gather_block}
    dense = {k: Direct(copies, ("dense", k), k, lambda step, k=k: own_piece[k], lambda step, k=k: own_piece[k]) for k in own_piece}

    def reduce_start(q):
        for k in ("x", "z"):
            first[k][q].start()

    def reduce_onward(q):
        for k in ("x", "z"):
            first[k][q].onward()

    def reduce_finish(q):
        for k in ("x", "z"):
            first[k][q].finish(mid[k].at[q])

    def y_start():
        for k in ("x", "z"):
            on_y[k].start()

    def y_onward():
        for k in ("x", "z"):
            on_y[k].onward()

    def y_finish():
        for k in ("x", "z"):
            on_y[k].finish(cross_ref[k].at[other_of[k][1]])
            cross[k].start()

    def w_finish():
        on_y["w"].finish(s2_ref.at[3])
        for k in ("u", "l"):
            inner[k].start()

    def inner_onward():
        for k in ("u", "l"):
            inner[k].onward()

    def inner_finish():
        for k in ("u", "l"):
            inner[k].finish(cross_ref[k].at[other_of[k][1]])
            cross[k].start()

    def cross_onward(*keys):
        for k in keys:
            cross[k].onward()

    def cross_finish(late, *keys):
        for k in keys:
            cross[k].finish()
            done_ref[k][...] = total(cross_ref[k])
            puts[k, late].start()
            final[k, late].start()
            copies.start(("pass", k, 0, late))

    def final_onward(late, *keys):
        for k in keys:
            final[k, late].onward()
            copies.start(*[("pass", k, way, late) for way in WAYS])

    def final_finish(late, *keys):
        for k in keys:
            final[k, late].finish()
            puts[k, late].wait()
            copies.start(("pass", k, 2, late))

    def pass_finish(late):
        keys = [("pass", k, offset, late) for k in out_of for offset in (0, *WAYS, 2)]
        copies.arrive(*keys)
        copies.sent(*keys)

    def dense_sum():
        copies.arrive("dense pair")
        ds_ref[...] = (dp_ref[mine].astype(F32) + dr_ref[...].astype(F32)).astype(BF16)
        copies.sent("dense pair")
        dense_sums.start()

    def dense_to_x():
        dense_sums.finish()
        mine = dense_block(place.y, None)[...].astype(F32)
        own_piece["x"][...] = (mine + e_ref[0].astype(F32) + e_ref[1].astype(F32) + e_ref[2].astype(F32)).astype(BF16)
        dense["x"].start()

    def dense_next(k, ref, follow):
        dense[k].finish()
        own_piece[follow][...] = total(ref)
        dense[follow].start()

    def dense_to_z():
        dense_next("x", dcx_ref, "z")

    def dense_to_y():
        dense_next("z", dcz_ref, "y")

    def dense_out(late):
        return pltpu.make_async_copy(gd_ref, gdense_ref.at[late], keep_sem.at[0, 1])

    def dense_pass(late):
        dense["y"].finish()
        if late == 0:
            dense_out(1).wait()
        gd_ref[mine] = dcy_ref[...]
        copies.start("dense pass")

    def dense_finish(late):
        copies.arrive("dense pass")
        gd_ref[theirs] = de_ref[...]
        copies.sent("dense pass")
        dense_out(late).start()

    def copy(src, dst, sem):
        return pltpu.make_async_copy(src, dst, sem)

    def weights(layer, slot, arrays, buf, is_given=False):
        for n in arrays:
            src = given[n].at[layer, (place.c + slot) % 2] if is_given else whole[n].at[layer, slot]
            yield copy(src, bufs[n].at[buf], load_sem.at[buf, n])

    def saved(layer, slot, buf):
        for n, (src, dst) in enumerate(zip(kept, acts)):
            yield copy(src.at[layer, slot], dst.at[buf], load_sem.at[buf, 3 + n])

    def weights_loads(step):
        layer, slot, buf = layer_of(step), SLOTS - 1 - step % SLOTS, (step + 1) % 2
        return [*weights(layer, slot, [2], buf), *saved(layer, slot, buf)]

    def inputs_loads(step):
        layer, slot, buf = layer_of(step), SLOTS - 1 - step % SLOTS, (step + 1) % 2
        return [*weights(layer, slot, BUFS, buf)] + [copy(deferred[n].at[slot], acts[n + 1].at[buf], load_sem.at[buf, 4 + n]) for n in BUFS]

    def load(step):
        slot = step % SLOTS
        for is_given in (True, False):
            pl.when((slot < 2) == is_given)(lambda: start(weights(step // SLOTS, slot, ARRAYS, step % 2, is_given)))

    def layer_of(step):
        return 1 - (step - WEIGHTS1) // (2 * SLOTS)

    def keeps(step):
        return [copy(bufs[n].at[step % 2], whole[n].at[step // SLOTS, step % SLOTS], keep_sem.at[step % 2, n]) for n in ARRAYS]

    def saves(step):
        return [copy(src.at[step % 2], dst.at[step // SLOTS, step % SLOTS], save_sem.at[step % 2, n]) for n, (src, dst) in enumerate(zip(acts, kept))]

    def defers(step):
        return [copy(acts[n + 1].at[2], deferred[n].at[SLOTS - 1 - step % SLOTS], save_sem.at[0, n]) for n in BUFS]

    def wait(items):
        for item in items:
            item.wait()

    def start(items):
        for item in items:
            item.start()

    def ending():
        dense_finish(1)
        copies.start("dense pair")
        y_finish()
        inner_finish()
        dense_sum()
        dense_to_x()
        cross_onward("x", "z")
        pass_finish(1)
        pl.semaphore_signal(credit.at[2], inc=1, device_id=place.at("c", 0), device_id_type=MESH)
        cross_onward("u", "l")
        dense_to_z()
        pl.semaphore_wait(credit.at[2], 1)
        cross_finish(0, "x", "z")
        cross_finish(0, "u", "l")
        dense_to_y()
        dense_pass(0)
        final_onward(0, "x", "z")
        dense_finish(0)
        final_onward(0, "u", "l")
        final_finish(0, "x", "z")
        final_finish(0, "u", "l")
        pass_finish(0)

    before, middle, after = {}, {}, {}

    def plan(table, first, *stages):
        for n, stage in enumerate(stages):
            table.setdefault(first + n, []).extend(stage)

    on, done = lambda q: lambda: reduce_onward(q), lambda q: lambda: reduce_finish(q)
    now = lambda: load(s)
    plan(before, 1, [g0.lead], [g0.follow, g0.lead_onward, g1.begin, g0.follow_onward, g0.last, g0.complete_y, now], [g0.passed_left])
    plan(before, 4, [g0.last_onward, g1.lead], [g0.complete_last, now, g0.passed_right, g1.follow], [], [g0.passed_last, now, g1.lead_onward])
    plan(before, SLOTS + 1, [g1.follow_onward, g1.last], [g1.complete_y, now], [g1.passed_left], [g1.last_onward], [g1.complete_last, now, g1.passed_right], [g1.passed_last])
    unready = (1, 4, 6, SLOTS + 1, SLOTS + 4)
    late = ("x", "z", "u", "l")
    plan(before, INPUTS1 + 6, [w_finish], [], [inner_onward])
    plan(before, WEIGHTS0, [lambda: copies.start("dense pair")], [], [inner_finish], [lambda: cross_onward("x", "z"), dense_to_x], [lambda: cross_onward("u", "l")], [dense_to_z])
    plan(middle, WEIGHTS0, [dense_sum, y_finish], [], [], [], [], [], [], [dense_to_y])
    plan(before, INPUTS0, [lambda: cross_finish(1, *late)], [], [], [], [lambda: final_onward(1, *late)], [], [lambda: final_finish(1, *late)], [lambda: dense_pass(1)])
    plan(before, INPUTS0 + 5, [w_finish], [], [inner_onward])
    for base in (WEIGHTS1, WEIGHTS0):
        plan(before, base + 3, [on_y["w"].start], [], [], [done(0), y_start, on_y["w"].onward])
        plan(middle, base + 4, [on(0)], [], [on(1)], [on(2)])
        plan(before, base + SLOTS, [], [done(1)], [done(2), y_onward], [on(3)], [], [], [done(3)])
        for step, q in OWN_STEPS.items():
            plan(after, base + step, [lambda q=q: reduce_start(q)])

    def hooks(table, *phases):
        for phase in phases:
            mine = {step: stages for step, stages in sorted(table.items()) if phase <= step < phase + SLOTS}
            if mine:

                @pl.when(s // SLOTS == phase // SLOTS)
                def _(mine=mine):
                    for step, stages in mine.items():

                        @pl.when(s == step)
                        def _(stages=stages):
                            for stage in stages:
                                stage()

    phase, t = s // SLOTS, s % SLOTS
    forth, back = s % 2, (s + 1) % 2

    def bring(ref, hold):
        return copy(ref, hold, keep_sem.at[1, 0])

    @pl.when(s == 0)
    def _():
        bring(x0_ref, hold_ref).start()
        load(0)
        greet(place)
        g0.begin()
        load(1)
        route(ids_ref, gate_ref, rows_ref, columns_ref, place)
        bring(x0_ref, hold_ref).wait()

    def enter(x):
        cur_ref[...] = (x.astype(F32) + dot(x, wd_ref[phase])).astype(BF16)
        acc_ref[...] = jnp.zeros_like(acc_ref)

    def leave(out_ref):
        out_ref[...] = (cur_ref[...].astype(F32) + acc_ref[...]).astype(BF16)

    @pl.when(s < WEIGHTS1)
    def _():
        hooks(before, 0, SLOTS)
        pl.when(s > 1)(lambda: wait(saves(s - 2)))
        ahead = functools.reduce(jnp.logical_and, [s != step for step in unready], (s > 0) & (s < WEIGHTS1 - 1))
        pl.when((t == 1) | (t == 2))(lambda: wait(keeps(s - 1)))
        pl.when(ahead)(lambda: load(s + 1))

        @pl.when(t < 2)
        def _():
            pl.when(s == 0)(lambda: enter(hold_ref[...]))
            pl.when(s == SLOTS)(lambda: enter(x1_ref[...]))

        layer, slot = phase, t
        come = list(weights(layer, slot, ARRAYS, forth))

        def forward_step(is_ready):
            if is_ready:
                wait(come)
            z = dot(one_hot(rows_ref, layer, slot, cap), cur_ref[...]).astype(BF16)
            z_ref[forth] = z
            if not is_ready:
                wait(come)
            a = dot(z, w1_ref[forth]).astype(BF16)
            b = dot(z, w3_ref[forth]).astype(BF16)
            a_ref[forth] = a
            b_ref[forth] = b
            a = a.astype(F32)
            h = (a * sigmoid(a) * b.astype(F32)).astype(BF16)
            o = dot(h, w2_ref[forth]).astype(BF16)
            acc_ref[...] += column(columns_ref, layer, SLOTS + slot) * dot(one_hot_t(columns_ref, layer, slot, cap), o)

        is_late = functools.reduce(jnp.logical_or, [s == step + 1 for step in unready])
        pl.when(is_late)(lambda: forward_step(False))
        pl.when(jnp.logical_not(is_late))(lambda: forward_step(True))
        pl.when(t < 2)(lambda: start(keeps(s)))
        pl.when(s < WEIGHTS1 - 1)(lambda: start(saves(s)))
        @pl.when(t == SLOTS - 1)
        def _():
            pl.when(s == SLOTS - 1)(lambda: leave(x1_ref))
            pl.when(s == WEIGHTS1 - 1)(lambda: leave(hold_ref))

    @pl.when((phase == WEIGHTS1 // SLOTS) | (phase == WEIGHTS0 // SLOTS))
    def _():
        layer, slot = layer_of(s), SLOTS - 1 - t
        hooks(before, WEIGHTS1, WEIGHTS0)

        @pl.when(s == WEIGHTS1)
        def _():
            moved = copy(hold_ref, y_ref, keep_sem.at[0, 0])
            moved.start()
            bring(dy_ref, cur_ref).start()
            wait(saves(s - 2))
            gathers.drain()
            bring(dy_ref, cur_ref).wait()
            moved.wait()
            acc_ref[...] = cur_ref[...].astype(F32)

        pl.when(s > WEIGHTS1)(lambda: wait(weights_loads(s)))
        pl.when(t > 0)(lambda: wait(defers(s - 1)))
        pl.when(t < SLOTS - 1)(lambda: start(weights_loads(s + 1)))
        pl.when(t == SLOTS - 1)(lambda: start(inputs_loads(s + 1)))

        grad_gated = (column(columns_ref, layer, SLOTS + slot) * cur_ref[...].astype(F32)).astype(BF16)
        do = dot(one_hot(rows_ref, layer, slot, cap), grad_gated).astype(BF16)
        dh = dot_nt(do, w2_ref[back])
        a = a_ref[back].astype(F32)
        b = b_ref[back].astype(F32)
        sig = sigmoid(a)
        act = a * sig
        h = (act * b).astype(BF16)
        db = (dh * act).astype(BF16)
        da = (dh * b * (sig + act * (1.0 - sig))).astype(BF16)
        a_ref[2] = da
        b_ref[2] = db
        z = z_ref[back]
        start(defers(s))
        hooks(middle, WEIGHTS1, WEIGHTS0)

        def weight_grads():
            return dot_tn(z, da), dot_tn(z, db), dot_tn(h, do)

        is_own = functools.reduce(jnp.logical_or, [t == step for step in OWN_STEPS])
        group = t // 4 + t // 5 + t // 7
        into = (t + t // 3 + t // 6) % 2
        turn = t + (1 - layer) * SLOTS

        @pl.when(jnp.logical_not(is_own))
        def _():
            for buf in BUFS:
                pl.when((turn >= 3) & (into == buf))(lambda: copies.sent(*[("pair", buf, n) for n in ARRAYS]))

            for ref, grad in zip(stage, weight_grads()):
                ref[into] = grad.astype(BF16)

            pl.when(turn >= 3)(lambda: pl.semaphore_wait(credit.at[into], 1))
            for buf in BUFS:
                pl.when(into == buf)(lambda: copies.start(*[("pair", buf, n) for n in ARRAYS]))

        @pl.when(is_own)
        def _():
            for buf in BUFS:
                pl.when(group % 2 == buf)(lambda: copies.arrive(*[("pair", buf, n) for n in ARRAYS]))

            for ref, add, grad in zip(mine_of, mate, weight_grads()):
                ref[group] = (grad + add[group % 2].astype(F32)).astype(BF16)

            @pl.when(turn < 2 * SLOTS - 3)
            def _():
                pl.semaphore_signal(credit.at[group % 2], inc=1, device_id=place.at("c", 0), device_id_type=MESH)

            hooks(after, WEIGHTS1, WEIGHTS0)

    def leave_back(layer, x, out_ref):
        grad = acc_ref[...]
        grad_b = grad.astype(BF16)
        dp_ref[...] = dot_tn(x, grad_b).astype(BF16)
        out_ref[...] = (grad + dot_nt(grad_b, wd_ref[layer])).astype(BF16)

    @pl.when((phase == INPUTS1 // SLOTS) | (phase == INPUTS0 // SLOTS))
    def _():
        layer, slot = layer_of(s), SLOTS - 1 - t
        hooks(before, INPUTS1, INPUTS0)
        wait(inputs_loads(s))
        pl.when(t == 0)(lambda: wait(defers(s - 1)))
        pl.when(t < SLOTS - 1)(lambda: start(inputs_loads(s + 1)))
        pl.when(s == WEIGHTS0 - 1)(lambda: start(weights_loads(s + 1)))
        dz = (dot_nt(a_ref[back], w1_ref[back]) + dot_nt(b_ref[back], w3_ref[back])).astype(BF16)
        acc_ref[...] += dot(one_hot_t(columns_ref, layer, slot, cap), dz)

        @pl.when(s == WEIGHTS0 - 1)
        def _():
            leave_back(1, x1_ref[...], cur_ref)
            acc_ref[...] = cur_ref[...].astype(F32)
            bring(x0_ref, x1_ref).start()
            bring(x0_ref, x1_ref).wait()

        @pl.when(s == STEPS - 1)
        def _():
            leave_back(0, x1_ref[...], hold_ref)
            moved = copy(hold_ref, dx_ref, keep_sem.at[0, 0])
            moved.start()
            ending()
            copies.sent(*[("pair", buf, n) for buf in BUFS for n in ARRAYS])
            moved.wait()
            dense_out(0).wait()


def step(cap, x0, dy, ids, gates, wd, w1, w3, w2):
    tokens, width = dy.shape
    layers, local, _, ff = w1.shape
    quarter, part, piece = width // SIDE, ff // 2 // SIDE, width // 2 // SIDE
    hbm = pl.BlockSpec(memory_space=pl.ANY)

    def fixed(shape):
        return pl.BlockSpec(shape, lambda s: (0,) * len(shape), pipeline_mode=pl.Buffered(1))

    def buf(*shape):
        return pltpu.VMEM(shape, BF16)

    def dma(*shape):
        return pltpu.SemaphoreType.DMA(shape)

    shape = jax.ShapeDtypeStruct
    ups, downs = [(width, ff), (width, ff), (ff, width)], [(quarter, ff), (part, width)]
    acts = [(cap, width), (cap, ff), (cap, ff)]
    scratch = [pltpu.VMEM((tokens, width), F32)] + [buf(tokens, width)] * 3 + [buf(width, width), pltpu.VMEM((layers, SLOTS, tokens), jnp.int32), pltpu.VMEM((layers, tokens, LANES), F32)]
    scratch += [buf(2, *u) for u in ups] + [buf(n, *a) for n, a in zip((2, 3, 3), acts)]
    scratch += [buf(2, *u) for u in ups] * 2 + [buf(SIDE, *u) for u in ups]
    scratch += [buf(SIDE, 2, quarter // 2, ff), buf(SIDE, 2, quarter, ff)] * 2
    scratch += [buf(SIDE, quarter, ff)] * 2
    scratch += [buf(2, quarter // 2, ff), buf(2, quarter, ff)] * 2 + [buf(2, ff // 2, width), buf(2, ff, width)]
    scratch += [buf(2, part // 2, width), buf(2, part, width)] * 2
    scratch += [buf(SIDE, quarter, ff)] * 2 + [buf(SIDE, part, width)] * 2
    scratch += [buf(quarter, ff)] * 2 + [buf(part, width)] * 2
    scratch += [buf(width, width)] + [buf(width // 2, width)] * 2 + [buf(SIDE - 1, piece, width)] + [buf(SIDE, piece, width)] * 2 + [buf(width // 2, width)] * 2
    scratch += [dma(4), dma(2, 6), dma(2, 3), dma(2, 3), dma(GATHER_COPIES), dma(GATHER_COPIES), dma(REDUCE_COPIES), dma(REDUCE_COPIES), pltpu.SemaphoreType.REGULAR((3,))]
    results = [(tokens, width), (tokens, width), (layers, width, width)]
    kept = [(layers, local, *u) for u in ups] + [(layers, SLOTS, *u) for u in ups + acts] + [(SLOTS, cap, ff)] * 2
    return pl.pallas_call(
        functools.partial(kernel, cap),
        grid=(STEPS,),
        in_specs=[hbm] * 2 + [fixed(v.shape) for v in (ids, gates, wd)] + [hbm] * 3,
        out_specs=[hbm] * len(results + kept),
        out_shape=[shape(r, BF16) for r in results + kept],
        scratch_shapes=scratch,
        compiler_params=pltpu.CompilerParams(vmem_limit_bytes=VMEM_LIMIT, collective_id=0, has_side_effects=True),
        name="step",
    )(x0, dy, ids, gates, wd, w1, w3, w2)[:6]


def take_kernel(count, *refs):
    sources, targets, holds, (come, go) = refs[:count], refs[count : 2 * count], refs[2 * count : 3 * count], refs[3 * count :]
    comes = [pltpu.make_async_copy(a, b, come.at[n]) for n, (a, b) in enumerate(zip(sources, holds))]
    goes = [pltpu.make_async_copy(a, b, go.at[n]) for n, (a, b) in enumerate(zip(holds, targets))]
    for item in comes:
        item.start()
    for first, then in zip(comes, goes):
        first.wait()
        then.start()
    for item in goes:
        item.wait()


def take(arrays):
    count = len(arrays)
    hbm = pl.BlockSpec(memory_space=pl.ANY)
    return pl.pallas_call(
        functools.partial(take_kernel, count),
        in_specs=[hbm] * count,
        out_specs=[hbm] * count,
        out_shape=[jax.ShapeDtypeStruct(a.shape, a.dtype) for a in arrays],
        scratch_shapes=[pltpu.VMEM(a.shape, a.dtype) for a in arrays] + [pltpu.SemaphoreType.DMA((count,))] * 2,
        compiler_params=pltpu.CompilerParams(vmem_limit_bytes=VMEM_LIMIT),
        name="take",
    )(*arrays)


def solution(mesh):
    tok_spec = P(TOK_AXES, None)
    route_spec = P(None, TOK_AXES, None)
    expert_spec = P(None, "ep", None, None)
    whole_spec = P(None, None, None)

    def device_step(tok_in, tok_grad, route_ids, gate_vals, *weights):
        tokens, top_k = route_ids.shape[1:]
        return tuple(take(step(2 * tokens * top_k // SLOTS, tok_in, tok_grad, jnp.swapaxes(route_ids, 1, 2), jnp.swapaxes(gate_vals, 1, 2), *weights)))

    return jax.shard_map(device_step, mesh=mesh, in_specs=(tok_spec, tok_spec, route_spec, route_spec, whole_spec, expert_spec, expert_spec, expert_spec), out_specs=(tok_spec, tok_spec, whole_spec, expert_spec, expert_spec, expert_spec), check_vma=False)
```

```python
import functools

import jax
import jax.numpy as jnp
from jax import lax
from jax.experimental import pallas as pl
from jax.experimental.pallas import tpu as pltpu
from jax.sharding import PartitionSpec as P

TOK_AXES = ("rep", "ep", "dp")
F32 = jnp.float32
BF16 = jnp.bfloat16
LANES = 128
SIDE = 4
WAYS = (1, -1)
BUFS = (0, 1)
LAYERS = (1, 0)
ARRAYS = range(3)
SLOTS = 8
MESH = pl.DeviceIdType.MESH
VMEM_LIMIT = 67_043_328


def dot(a, b):
    return jnp.dot(a, b, preferred_element_type=F32)


def dot_nt(a, b):
    return lax.dot_general(a, b, (((1,), (1,)), ((), ())), preferred_element_type=F32)


def dot_tn(a, b):
    return lax.dot_general(a, b, (((0,), (0,)), ((), ())), preferred_element_type=F32)


class Place:
    def __init__(self):
        self.z, self.y, dp = lax.axis_index("rep"), lax.axis_index("ep"), lax.axis_index("dp")
        self.x, self.c = dp // 2, dp % 2

    def at(self, axis, step):
        z, y, x, c = self.z, self.y, self.x, self.c
        if axis == "z":
            z = (z + step + SIDE) % SIDE
        elif axis == "y":
            y = (y + step + SIDE) % SIDE
        elif axis == "x":
            x = (x + step + SIDE) % SIDE
        else:
            c = 1 - c
        return (z, y, x * 2 + c)


class Copies:
    def __init__(self, place, send, recv):
        self.place, self.send, self.recv, self.made, self.number, self.count, self.over = place, send, recv, {}, {}, 0, set()

    def add(self, key, src, dst, axis, step, like=None):
        if like is None:
            n, self.count = self.count, self.count + 1
        else:
            n = self.number[like]
        self.number[key] = n
        self.made[key] = pltpu.make_async_remote_copy(src_ref=src, dst_ref=dst, send_sem=self.send.at[n], recv_sem=self.recv.at[n], device_id=self.place.at(axis, step), device_id_type=MESH)

    def start(self, *keys):
        for key in keys:
            self.made[key].start()

    def arrive(self, *keys):
        for key in keys:
            self.made[key].wait_recv()

    def sent(self, *keys):
        for key in keys:
            self.made[key].wait_send()
            self.over.add(key)

    def drain(self):
        self.sent(*[key for key in self.made if key not in self.over])


def greet(place):
    barrier = pltpu.get_barrier_semaphore()
    peers = [(axis, step) for axis in "xyz" for step in range(1, SIDE)] + [("c", 0)]
    for axis, step in peers:
        pl.semaphore_signal(barrier, inc=1, device_id=place.at(axis, step), device_id_type=MESH)
    pl.semaphore_wait(barrier, len(peers))


class Gather:
    PASS = {2: 4, 3: 6, 5: 7}

    def __init__(self, layer, copies, place, own, whole):
        self.layer, self.copies, self.place, self.own, self.whole = layer, copies, place, own, whole
        rows, ff = own[0].shape[2], own[2].shape[2]
        self.cut = {"x": ((0, 0, rows // SIDE), (2, 0, ff // 2 // SIDE)), "z": ((1, 0, rows // SIDE), (2, ff // 2, ff // 2 // SIDE))}
        mine = {"x": place.x, "z": place.z}
        for color in ("x", "z"):
            for part in BUFS:
                self._add(("y", 2, color, part), color, part, None, 2, mine[color], None, "y", 1)
                self._add(("y", 3, color, part), color, part, None, 3, mine[color], None, "y", -1)
                if color == "x":
                    self._add(("y", 5, color, part), color, part, 2, 5, mine[color], None, "y", 1)
                else:
                    self._add(("y", 5, color, part), color, part, 3, 5, mine[color], None, "y", -1)
                for slot in (2, 3, 5):
                    for step in WAYS:
                        self._add(("near", slot, color, part, step), color, part, slot, slot, mine[color], None, color, step)
                        behind = (mine[color] - step + SIDE) % SIDE
                        self._add(("far", slot, color, part, step), color, part, slot, slot, behind, (1 - step) // 2, color, step)
        for slot, to in self.PASS.items():
            for array in ARRAYS:
                copies.add((layer, "pass", slot, array), whole[array].at[layer, slot], whole[array].at[layer, to], "c", 0)

    def _view(self, refs, index, color, part, quarter, half):
        array, base, size = self.cut[color][part]
        start = base + quarter * size
        if half is not None:
            size = size // 2
            start = start + half * size
        return refs[array].at[self.layer, index, pl.ds(pl.multiple_of(start, 16), size)]

    def _add(self, key, color, part, src_slot, dst_slot, quarter, half, axis, step):
        src = self._view(self.own, self.place.c, color, part, quarter, half) if src_slot is None else self._view(self.whole, src_slot, color, part, quarter, half)
        self.copies.add((self.layer,) + key, src, self._view(self.whole, dst_slot, color, part, quarter, half), axis, step)

    def _keys(self, *key, extra=()):
        return [(self.layer,) + key + (part,) + extra for part in BUFS]

    def lead(self):
        self.spread(2, "x")
        self.spread(3, "z")

    def lead_onward(self):
        self.onward(2, "x")
        self.onward(3, "z")

    def follow(self):
        self.spread(2, "z")
        self.spread(3, "x")

    def follow_onward(self):
        self.onward(2, "z")
        self.onward(3, "x")

    def last(self):
        self.spread(5, "x")
        self.spread(5, "z")

    def last_onward(self):
        self.onward(5, "x")
        self.onward(5, "z")

    def complete_y(self):
        self.complete(2)
        self.complete(3)

    def complete_last(self):
        self.complete(5)

    def passed_left(self):
        self.passed(2)

    def passed_right(self):
        self.passed(3)

    def passed_last(self):
        self.passed(5)

    def begin(self):
        for slot, color in ((2, "x"), (3, "z"), (2, "z"), (3, "x")):
            self.copies.start(*self._keys("y", slot, color))

    def spread(self, slot, color):
        for part in BUFS:
            self.copies.arrive((self.layer, "y", slot, color, part))
            self.copies.start(*[(self.layer, "near", slot, color, part, step) for step in WAYS])
        if (slot, color) in ((2, "x"), (3, "z")):
            self.copies.start(*self._keys("y", 5, color))

    def onward(self, slot, color):
        for part in BUFS:
            for step in WAYS:
                self.copies.arrive((self.layer, "near", slot, color, part, step))
                self.copies.start((self.layer, "far", slot, color, part, step))

    def complete(self, slot):
        for color in ("x", "z"):
            for step in WAYS:
                self.copies.arrive(*self._keys("far", slot, color, extra=(step,)))
        self.copies.start(*[(self.layer, "pass", slot, array) for array in ARRAYS])

    def passed(self, slot):
        self.copies.arrive(*[(self.layer, "pass", slot, array) for array in ARRAYS])


GATHER_COPIES = 2 * (2 * 2 * (3 + 3 * 4) + 9)


def route(ids_ref, gate_ref, rows_ref, columns_ref, place):
    layers, _, tokens = ids_ref.shape
    below = lax.broadcasted_iota(jnp.int32, (tokens, tokens), 0) < lax.broadcasted_iota(jnp.int32, (tokens, tokens), 1)
    below = jnp.where(below, 1.0, 0.0).astype(BF16)
    lead = lax.broadcasted_iota(jnp.int32, (2 * SLOTS, tokens), 0)
    for layer in range(layers):
        ids, gates = ids_ref[layer], gate_ref[layer]
        off = ((ids >> 1) - place.y) & (SIDE - 1)
        odd = (ids + place.c) & 1
        slot = jnp.where(off == 0, odd, jnp.where(off == SIDE - 1, 2 + 2 * odd, jnp.where(off == 1, 3 + 3 * odd, 5 + 2 * odd)))
        hits = [slot[n : n + 1] == lead for n in BUFS]
        hit = hits[0] | hits[1]
        weight = jnp.where(hits[0], gates[0:1], 0.0) + jnp.where(hits[1], gates[1:2], 0.0)
        rank = jnp.where(hit, dot(jnp.where(hit, 1.0, 0.0).astype(BF16), below), -1.0)
        rows_ref[layer] = rank[:SLOTS].astype(jnp.int32)
        columns_ref[layer] = jnp.transpose(jnp.concatenate([rank[:SLOTS], weight[:SLOTS], jnp.zeros((LANES - 2 * SLOTS, tokens), F32)], axis=0))


def one_hot(rows_ref, layer, slot, cap):
    place = lax.broadcasted_iota(jnp.int32, (cap, rows_ref.shape[2]), 0)
    return jnp.where(rows_ref[layer, pl.ds(slot, 1), :] == place, 1.0, 0.0).astype(BF16)


def column(columns_ref, layer, index):
    lane = lax.broadcasted_iota(jnp.int32, columns_ref.shape[1:], 1)
    return jnp.sum(jnp.where(lane == index, columns_ref[layer], 0.0), axis=1, keepdims=True)


def one_hot_t(columns_ref, layer, slot, cap):
    place = lax.broadcasted_iota(jnp.int32, (columns_ref.shape[1], cap), 1)
    return jnp.where(column(columns_ref, layer, slot).astype(jnp.int32) == place, 1.0, 0.0).astype(BF16)


def add_to(dst, src):
    dst[...] = (dst[...].astype(F32) + src[...].astype(F32)).astype(BF16)


def cut(rows, half):
    first = (rows // 2 + 15) // 16 * 16
    return (half * first, first + half * (rows - 2 * first))


class RingSum:
    def __init__(self, copies, name, axis, block, first, second):
        self.copies, self.block, self.second = copies, block, second
        self.first = [first.at[half, pl.ds(0, block(2, half).shape[0])] for half in BUFS]
        self.early, self.later = ([(name, when, step) for step in WAYS] for when in ("early", "later"))
        for half, step in enumerate(WAYS):
            copies.add(self.early[half], block(2, half), self.first[half], axis, step)
            copies.add(self.later[half], block(step, None), second.at[half], axis, step)

    def start(self):
        self.copies.start(*self.early)

    def onward(self):
        self.copies.arrive(*self.early)
        for half in BUFS:
            add_to(self.block(WAYS[half], half), self.first[half])
            self.copies.start(self.later[half])
        self.copies.sent(*self.early)

    def finish(self, out):
        self.copies.arrive(*self.later)
        out[...] = (self.block(0, None)[...].astype(F32) + self.second[0].astype(F32) + self.second[1].astype(F32)).astype(BF16)
        self.copies.sent(*self.later)


class RingSpread:
    def __init__(self, copies, name, axis, me, block, source=None, like=None):
        self.copies = copies
        self.near, self.far = ([(name, when, step) for step in WAYS] for when in ("near", "far"))
        for half, step in enumerate(WAYS):
            behind = (me - step + SIDE) % SIDE
            near, far = (None, None) if like is None else (like.near[half], like.far[half])
            copies.add(self.near[half], block(me, None) if source is None else source, block(me, None), axis, step, near)
            copies.add(self.far[half], block(behind, half), block(behind, half), axis, step, far)

    def start(self):
        self.copies.start(*self.near)

    def onward(self):
        for near, far in zip(self.near, self.far):
            self.copies.arrive(near)
            self.copies.start(far)

    def finish(self):
        self.copies.arrive(*self.far)
        self.copies.sent(*self.near, *self.far)


class Direct:
    def __init__(self, copies, name, axis, source, target):
        self.copies, self.keys = copies, [(name, step) for step in range(1, SIDE)]
        for name, step in self.keys:
            copies.add((name, step), source(step), target(step), axis, step)

    def start(self):
        self.copies.start(*self.keys)

    def finish(self):
        self.copies.arrive(*self.keys)
        self.copies.sent(*self.keys)


def slices(ref, lead, base, size):
    def block(index, half):
        start, rows = base + index * size, size
        if half is not None:
            skip, rows = cut(size, half)
            start = start + skip
        return ref.at[(*lead, pl.ds(pl.multiple_of(start, 16), rows))]

    return block


def slabs(ref):
    def block(index, half):
        if half is None:
            return ref.at[index]
        return ref.at[index, pl.ds(*cut(ref.shape[1], half))]

    return block


def total(ref):
    return (ref[0].astype(F32) + ref[1].astype(F32) + ref[2].astype(F32) + ref[3].astype(F32)).astype(BF16)


OWN_STEPS = {2: 0, 4: 1, 5: 2, 7: 3}
REDUCE_COPIES = 120
WEIGHTS1, INPUTS1, WEIGHTS0, INPUTS0, STEPS = (n * SLOTS for n in range(2, 7))


def kernel(cap, x0_ref, dy_ref, ids_ref, gate_ref, wd_ref, o1_ref, o3_ref, o2_ref, y_ref, dx_ref, gdense_ref, g1_ref, g3_ref, g2_ref, h1_ref, h3_ref, h2_ref, kz_ref, ka_ref, kb_ref, kda_ref, kdb_ref, acc_ref, cur_ref, x1_ref, hold_ref, gd_ref, rows_ref, columns_ref, w1_ref, w3_ref, w2_ref, z_ref, a_ref, b_ref, d1_ref, d3_ref, d2_ref, s1_ref, s3_ref, s2_ref, r11_ref, r12_ref, r31_ref, r32_ref, t1_ref, t3_ref, y11_ref, y12_ref, y31_ref, y32_ref, y21_ref, y22_ref, u1_ref, u2_ref, l1_ref, l2_ref, c1_ref, c3_ref, cu_ref, cl_ref, f1_ref, f3_ref, fu_ref, fl_ref, dp_ref, dr_ref, ds_ref, e_ref, dcx_ref, dcz_ref, dcy_ref, de_ref, put_sem, load_sem, keep_sem, save_sem, gsend_sem, grecv_sem, send_sem, recv_sem, credit):
    s = pl.program_id(0)
    place = Place()
    gathers = Copies(place, gsend_sem, grecv_sem)
    copies = Copies(place, send_sem, recv_sem)
    given, whole, bufs = (o1_ref, o3_ref, o2_ref), (h1_ref, h3_ref, h2_ref), (w1_ref, w3_ref, w2_ref)
    kept, acts = (kz_ref, ka_ref, kb_ref), (z_ref, a_ref, b_ref)
    deferred = (kda_ref, kdb_ref)
    g0, g1 = (Gather(l, gathers, place, given, whole) for l in BUFS)
    rows, ff = s1_ref.shape[1], s2_ref.shape[1]
    quarter, part = rows // SIDE, ff // 2 // SIDE
    half_d = rows // 2

    mate, mine_of = (d1_ref, d3_ref, d2_ref), (s1_ref, s3_ref, s2_ref)
    for buf in BUFS:
        for n in ARRAYS:
            copies.add(("pair", buf, n), mine_of[n].at[SIDE + buf], mate[n].at[buf], "c", 0)

    def ring_blocks(ref, q, me, base, size):
        block = slices(ref, (q,), base, size)
        return lambda offset, half: block((me + offset + SIDE) % SIDE, half)

    def group_blocks(ref):
        block = slabs(ref)
        return lambda offset, half: block({2: 0, 1: 1, -1: 2, 0: 3}[offset], half)

    first = {
        "x": [RingSum(copies, ("x", q), "x", ring_blocks(s1_ref, q, place.x, 0, quarter), r11_ref.at[q], r12_ref.at[q]) for q in range(SIDE)],
        "z": [RingSum(copies, ("z", q), "z", ring_blocks(s3_ref, q, place.z, 0, quarter), r31_ref.at[q], r32_ref.at[q]) for q in range(SIDE)],
    }
    mid = {"x": t1_ref, "z": t3_ref}
    on_y = {
        "x": RingSum(copies, "yx", "y", group_blocks(t1_ref), y11_ref, y12_ref),
        "z": RingSum(copies, "yz", "y", group_blocks(t3_ref), y31_ref, y32_ref),
        "w": RingSum(copies, "yw", "y", group_blocks(s2_ref), y21_ref, y22_ref),
    }
    inner = {
        "u": RingSum(copies, "u", "x", ring_blocks(s2_ref, 3, place.x, 0, part), u1_ref, u2_ref),
        "l": RingSum(copies, "l", "z", ring_blocks(s2_ref, 3, place.z, ff // 2, part), l1_ref, l2_ref),
    }
    ring_of = {"x": ("x", place.x), "u": ("x", place.x), "z": ("z", place.z), "l": ("z", place.z)}
    other_of = {"x": ("z", place.z), "u": ("z", place.z), "z": ("x", place.x), "l": ("x", place.x)}
    cross_ref = {"x": c1_ref, "z": c3_ref, "u": cu_ref, "l": cl_ref}
    done_ref = {"x": f1_ref, "z": f3_ref, "u": fu_ref, "l": fl_ref}
    out_of = {"x": (g1_ref, 0, quarter), "z": (g3_ref, 0, quarter), "u": (g2_ref, 0, part), "l": (g2_ref, ff // 2, part)}
    cross, final, puts = {}, {}, {}
    for i, k in enumerate(out_of):
        cross[k] = RingSpread(copies, ("cross", k), *other_of[k], slabs(cross_ref[k]))
        ref, base, size = out_of[k]
        for late in LAYERS:
            block = slices(ref, (late, place.c), base, size)
            final[k, late] = RingSpread(copies, ("final", k, late), *ring_of[k], block, source=done_ref[k], like=final.get((k, 1)))
            me = ring_of[k][1]
            puts[k, late] = pltpu.make_async_copy(done_ref[k], block(me, None), put_sem.at[i])
            for offset in (0, *WAYS, 2):
                quarter_at = block((me + offset) % SIDE if offset >= 0 else (me + SIDE - 1) % SIDE, None)
                copies.add(("pass", k, offset, late), quarter_at if offset else done_ref[k], quarter_at, "c", 0, None if late else ("pass", k, offset, 1))
    mine, theirs = (pl.ds(pl.multiple_of(c * half_d, 16), half_d) for c in (place.c, 1 - place.c))
    copies.add("dense pair", dp_ref.at[theirs], dr_ref, "c", 0)
    copies.add("dense pass", dcy_ref, de_ref, "c", 0)
    piece = half_d // SIDE
    dense_block = slices(ds_ref, (), 0, piece)
    dense_sums = Direct(copies, "dense sums", "y", lambda step: dense_block((place.y + step) % SIDE, None), lambda step: e_ref.at[step - 1])
    gather_block = slices(dcy_ref, (), 0, piece)(place.y, None)
    own_piece = {"x": dcx_ref.at[place.x], "z": dcz_ref.at[place.z], "y": gather_block}
    dense = {k: Direct(copies, ("dense", k), k, lambda step, k=k: own_piece[k], lambda step, k=k: own_piece[k]) for k in own_piece}

    def reduce_start(q):
        for k in ("x", "z"):
            first[k][q].start()

    def reduce_onward(q):
        for k in ("x", "z"):
            first[k][q].onward()

    def reduce_finish(q):
        for k in ("x", "z"):
            first[k][q].finish(mid[k].at[q])

    def y_start():
        for k in ("x", "z"):
            on_y[k].start()

    def y_onward():
        for k in ("x", "z"):
            on_y[k].onward()

    def y_finish():
        for k in ("x", "z"):
            on_y[k].finish(cross_ref[k].at[other_of[k][1]])
            cross[k].start()

    def w_finish():
        on_y["w"].finish(s2_ref.at[3])
        for k in ("u", "l"):
            inner[k].start()

    def inner_onward():
        for k in ("u", "l"):
            inner[k].onward()

    def inner_finish():
        for k in ("u", "l"):
            inner[k].finish(cross_ref[k].at[other_of[k][1]])
            cross[k].start()

    def cross_onward(*keys):
        for k in keys:
            cross[k].onward()

    def cross_finish(late, *keys):
        for k in keys:
            cross[k].finish()
            done_ref[k][...] = total(cross_ref[k])
            puts[k, late].start()
            final[k, late].start()
            copies.start(("pass", k, 0, late))

    def final_onward(late, *keys):
        for k in keys:
            final[k, late].onward()
            copies.start(*[("pass", k, way, late) for way in WAYS])

    def final_finish(late, *keys):
        for k in keys:
            final[k, late].finish()
            puts[k, late].wait()
            copies.start(("pass", k, 2, late))

    def pass_finish(late):
        keys = [("pass", k, offset, late) for k in out_of for offset in (0, *WAYS, 2)]
        copies.arrive(*keys)
        copies.sent(*keys)

    def dense_sum():
        copies.arrive("dense pair")
        ds_ref[...] = (dp_ref[mine].astype(F32) + dr_ref[...].astype(F32)).astype(BF16)
        copies.sent("dense pair")
        dense_sums.start()

    def dense_to_x():
        dense_sums.finish()
        mine = dense_block(place.y, None)[...].astype(F32)
        own_piece["x"][...] = (mine + e_ref[0].astype(F32) + e_ref[1].astype(F32) + e_ref[2].astype(F32)).astype(BF16)
        dense["x"].start()

    def dense_next(k, ref, follow):
        dense[k].finish()
        own_piece[follow][...] = total(ref)
        dense[follow].start()

    def dense_to_z():
        dense_next("x", dcx_ref, "z")

    def dense_to_y():
        dense_next("z", dcz_ref, "y")

    def dense_out(late):
        return pltpu.make_async_copy(gd_ref, gdense_ref.at[late], keep_sem.at[0, 1])

    def dense_pass(late):
        dense["y"].finish()
        if late == 0:
            dense_out(1).wait()
        gd_ref[mine] = dcy_ref[...]
        copies.start("dense pass")

    def dense_finish(late):
        copies.arrive("dense pass")
        gd_ref[theirs] = de_ref[...]
        copies.sent("dense pass")
        dense_out(late).start()

    def copy(src, dst, sem):
        return pltpu.make_async_copy(src, dst, sem)

    def weights(layer, slot, arrays, buf, is_given=False):
        for n in arrays:
            src = given[n].at[layer, (place.c + slot) % 2] if is_given else whole[n].at[layer, slot]
            yield copy(src, bufs[n].at[buf], load_sem.at[buf, n])

    def saved(layer, slot, buf):
        for n, (src, dst) in enumerate(zip(kept, acts)):
            yield copy(src.at[layer, slot], dst.at[buf], load_sem.at[buf, 3 + n])

    def weights_loads(step):
        layer, slot, buf = layer_of(step), SLOTS - 1 - step % SLOTS, (step + 1) % 2
        return [*weights(layer, slot, [2], buf), *saved(layer, slot, buf)]

    def inputs_loads(step):
        layer, slot, buf = layer_of(step), SLOTS - 1 - step % SLOTS, (step + 1) % 2
        return [*weights(layer, slot, BUFS, buf)] + [copy(deferred[n].at[slot], acts[n + 1].at[buf], load_sem.at[buf, 4 + n]) for n in BUFS]

    def load(step):
        slot = step % SLOTS
        for is_given in (True, False):
            pl.when((slot < 2) == is_given)(lambda: start(weights(step // SLOTS, slot, ARRAYS, step % 2, is_given)))

    def layer_of(step):
        return 1 - (step - WEIGHTS1) // (2 * SLOTS)

    def keeps(step):
        return [copy(bufs[n].at[step % 2], whole[n].at[step // SLOTS, step % SLOTS], keep_sem.at[step % 2, n]) for n in ARRAYS]

    def saves(step):
        return [copy(src.at[step % 2], dst.at[step // SLOTS, step % SLOTS], save_sem.at[step % 2, n]) for n, (src, dst) in enumerate(zip(acts, kept))]

    def defers(step):
        return [copy(acts[n + 1].at[2], deferred[n].at[SLOTS - 1 - step % SLOTS], save_sem.at[0, n]) for n in BUFS]

    def wait(items):
        for item in items:
            item.wait()

    def start(items):
        for item in items:
            item.start()

    def ending():
        dense_finish(1)
        copies.start("dense pair")
        y_finish()
        inner_finish()
        dense_sum()
        dense_to_x()
        cross_onward("x", "z")
        pass_finish(1)
        pl.semaphore_signal(credit.at[2], inc=1, device_id=place.at("c", 0), device_id_type=MESH)
        cross_onward("u", "l")
        dense_to_z()
        pl.semaphore_wait(credit.at[2], 1)
        cross_finish(0, "x", "z")
        cross_finish(0, "u", "l")
        dense_to_y()
        dense_pass(0)
        final_onward(0, "x", "z")
        dense_finish(0)
        final_onward(0, "u", "l")
        final_finish(0, "x", "z")
        final_finish(0, "u", "l")
        pass_finish(0)

    before, middle, after = {}, {}, {}

    def plan(table, first, *stages):
        for n, stage in enumerate(stages):
            table.setdefault(first + n, []).extend(stage)

    on, done = lambda q: lambda: reduce_onward(q), lambda q: lambda: reduce_finish(q)
    now = lambda: load(s)
    plan(before, 1, [g0.lead], [g0.follow, g0.lead_onward, g1.begin, g0.follow_onward, g0.last, g0.complete_y, now], [g0.passed_left])
    plan(before, 4, [g0.last_onward, g1.lead], [g0.complete_last, now, g0.passed_right, g1.follow], [], [g0.passed_last, now, g1.lead_onward])
    plan(before, SLOTS + 1, [g1.follow_onward, g1.last], [g1.complete_y, now], [g1.passed_left], [g1.last_onward], [g1.complete_last, now, g1.passed_right], [g1.passed_last])
    unready = (1, 4, 6, SLOTS + 1, SLOTS + 4)
    late = ("x", "z", "u", "l")
    plan(before, INPUTS1 + 6, [w_finish], [], [inner_onward])
    plan(before, WEIGHTS0, [lambda: copies.start("dense pair")], [], [inner_finish], [lambda: cross_onward("x", "z"), dense_to_x], [lambda: cross_onward("u", "l")], [dense_to_z])
    plan(middle, WEIGHTS0, [dense_sum, y_finish], [], [], [], [], [], [], [dense_to_y])
    plan(before, INPUTS0, [lambda: cross_finish(1, *late)], [], [], [], [], [lambda: final_onward(1, *late)], [], [lambda: dense_pass(1), lambda: final_finish(1, *late)])
    plan(before, INPUTS0 + 5, [w_finish], [], [inner_onward])
    for base in (WEIGHTS1, WEIGHTS0):
        plan(before, base + 3, [on_y["w"].start], [], [], [done(0), y_start, on_y["w"].onward])
        plan(middle, base + 4, [on(0)], [], [on(1)], [on(2)])
        plan(before, base + SLOTS, [], [done(1)], [done(2), y_onward], [on(3)], [], [], [done(3)])
        for step, q in OWN_STEPS.items():
            plan(after, base + step, [lambda q=q: reduce_start(q)])

    def hooks(table, *phases):
        for phase in phases:
            mine = {step: stages for step, stages in sorted(table.items()) if phase <= step < phase + SLOTS}
            if mine:

                @pl.when(s // SLOTS == phase // SLOTS)
                def _(mine=mine):
                    for step, stages in mine.items():

                        @pl.when(s == step)
                        def _(stages=stages):
                            for stage in stages:
                                stage()

    phase, t = s // SLOTS, s % SLOTS
    forth, back = s % 2, (s + 1) % 2

    def bring(ref, hold):
        return copy(ref, hold, keep_sem.at[1, 0])

    @pl.when(s == 0)
    def _():
        bring(x0_ref, hold_ref).start()
        load(0)
        greet(place)
        g0.begin()
        load(1)
        route(ids_ref, gate_ref, rows_ref, columns_ref, place)
        bring(x0_ref, hold_ref).wait()

    def enter(x):
        cur_ref[...] = (x.astype(F32) + dot(x, wd_ref[phase])).astype(BF16)
        acc_ref[...] = jnp.zeros_like(acc_ref)

    def leave(out_ref):
        out_ref[...] = (cur_ref[...].astype(F32) + acc_ref[...]).astype(BF16)

    @pl.when(s < WEIGHTS1)
    def _():
        hooks(before, 0, SLOTS)
        pl.when(s > 1)(lambda: wait(saves(s - 2)))
        ahead = functools.reduce(jnp.logical_and, [s != step for step in unready], (s > 0) & (s < WEIGHTS1 - 1))
        pl.when((t == 1) | (t == 2))(lambda: wait(keeps(s - 1)))
        pl.when(ahead)(lambda: load(s + 1))

        @pl.when(t < 2)
        def _():
            pl.when(s == 0)(lambda: enter(hold_ref[...]))
            pl.when(s == SLOTS)(lambda: enter(x1_ref[...]))

        layer, slot = phase, t
        come = list(weights(layer, slot, ARRAYS, forth))

        def forward_step(is_ready):
            if is_ready:
                wait(come)
            z = dot(one_hot(rows_ref, layer, slot, cap), cur_ref[...]).astype(BF16)
            z_ref[forth] = z
            if not is_ready:
                wait(come)
            a = dot(z, w1_ref[forth]).astype(BF16)
            b = dot(z, w3_ref[forth]).astype(BF16)
            a_ref[forth] = a
            b_ref[forth] = b
            a = a.astype(F32)
            h = (a * jax.nn.sigmoid(a) * b.astype(F32)).astype(BF16)
            o = dot(h, w2_ref[forth]).astype(BF16)
            acc_ref[...] += column(columns_ref, layer, SLOTS + slot) * dot(one_hot_t(columns_ref, layer, slot, cap), o)

        is_late = functools.reduce(jnp.logical_or, [s == step + 1 for step in unready])
        pl.when(is_late)(lambda: forward_step(False))
        pl.when(jnp.logical_not(is_late))(lambda: forward_step(True))
        pl.when(t < 2)(lambda: start(keeps(s)))
        pl.when(s < WEIGHTS1 - 1)(lambda: start(saves(s)))
        @pl.when(t == SLOTS - 1)
        def _():
            pl.when(s == SLOTS - 1)(lambda: leave(x1_ref))
            pl.when(s == WEIGHTS1 - 1)(lambda: leave(hold_ref))

    @pl.when((phase == WEIGHTS1 // SLOTS) | (phase == WEIGHTS0 // SLOTS))
    def _():
        layer, slot = layer_of(s), SLOTS - 1 - t
        hooks(before, WEIGHTS1, WEIGHTS0)

        @pl.when(s == WEIGHTS1)
        def _():
            moved = copy(hold_ref, y_ref, keep_sem.at[0, 0])
            moved.start()
            bring(dy_ref, cur_ref).start()
            wait(saves(s - 2))
            gathers.drain()
            bring(dy_ref, cur_ref).wait()
            moved.wait()
            acc_ref[...] = cur_ref[...].astype(F32)

        pl.when(s > WEIGHTS1)(lambda: wait(weights_loads(s)))
        pl.when(t > 0)(lambda: wait(defers(s - 1)))
        pl.when(t < SLOTS - 1)(lambda: start(weights_loads(s + 1)))
        pl.when(t == SLOTS - 1)(lambda: start(inputs_loads(s + 1)))

        is_own = functools.reduce(jnp.logical_or, [t == step for step in OWN_STEPS])
        group = t // 4 + t // 5 + t // 7
        into = (t + t // 3 + t // 6) % 2
        turn = t + (1 - layer) * SLOTS
        for buf in BUFS:
            pl.when(is_own & (group % 2 == buf))(lambda: copies.arrive(*[("pair", buf, n) for n in ARRAYS]))
            pl.when(jnp.logical_not(is_own) & (turn >= 3) & (into == buf))(lambda: copies.sent(*[("pair", buf, n) for n in ARRAYS]))

        def back_step(adds):
            grad_gated = (column(columns_ref, layer, SLOTS + slot) * cur_ref[...].astype(F32)).astype(BF16)
            do = dot(one_hot(rows_ref, layer, slot, cap), grad_gated).astype(BF16)
            dh = dot_nt(do, w2_ref[back])
            a = a_ref[back].astype(F32)
            b = b_ref[back].astype(F32)
            sig = jax.nn.sigmoid(a)
            act = a * sig
            h = (act * b).astype(BF16)
            db = (dh * act).astype(BF16)
            da = (dh * b * (sig + act * (1.0 - sig))).astype(BF16)
            a_ref[2] = da
            b_ref[2] = db
            z = z_ref[back]
            for ref, add, grad in zip(mine_of, mate, (dot_tn(z, da), dot_tn(z, db), dot_tn(h, do))):
                if adds:
                    ref[group] = (grad + add[group % 2].astype(F32)).astype(BF16)
                else:
                    ref[SIDE + into] = grad.astype(BF16)

        pl.when(is_own)(lambda: back_step(True))
        pl.when(jnp.logical_not(is_own))(lambda: back_step(False))
        start(defers(s))

        @pl.when(jnp.logical_not(is_own))
        def _():
            pl.when(turn >= 3)(lambda: pl.semaphore_wait(credit.at[into], 1))
            for buf in BUFS:
                pl.when(into == buf)(lambda: copies.start(*[("pair", buf, n) for n in ARRAYS]))

        @pl.when(is_own)
        def _():
            @pl.when(turn < 2 * SLOTS - 3)
            def _():
                pl.semaphore_signal(credit.at[group % 2], inc=1, device_id=place.at("c", 0), device_id_type=MESH)

            hooks(after, WEIGHTS1, WEIGHTS0)

        hooks(middle, WEIGHTS1, WEIGHTS0)

    def leave_back(layer, x, out_ref):
        grad = acc_ref[...]
        grad_b = grad.astype(BF16)
        dp_ref[...] = dot_tn(x, grad_b).astype(BF16)
        out_ref[...] = (grad + dot_nt(grad_b, wd_ref[layer])).astype(BF16)

    @pl.when((phase == INPUTS1 // SLOTS) | (phase == INPUTS0 // SLOTS))
    def _():
        layer, slot = layer_of(s), SLOTS - 1 - t
        hooks(before, INPUTS1, INPUTS0)
        wait(inputs_loads(s))
        pl.when(t == 0)(lambda: wait(defers(s - 1)))
        pl.when(t < SLOTS - 1)(lambda: start(inputs_loads(s + 1)))
        pl.when(s == WEIGHTS0 - 1)(lambda: start(weights_loads(s + 1)))
        dz = (dot_nt(a_ref[back], w1_ref[back]) + dot_nt(b_ref[back], w3_ref[back])).astype(BF16)
        acc_ref[...] += dot(one_hot_t(columns_ref, layer, slot, cap), dz)

        @pl.when(s == WEIGHTS0 - 1)
        def _():
            leave_back(1, x1_ref[...], cur_ref)
            acc_ref[...] = cur_ref[...].astype(F32)
            bring(x0_ref, x1_ref).start()
            bring(x0_ref, x1_ref).wait()

        @pl.when(s == STEPS - 1)
        def _():
            leave_back(0, x1_ref[...], hold_ref)
            moved = copy(hold_ref, dx_ref, keep_sem.at[0, 0])
            moved.start()
            ending()
            copies.sent(*[("pair", buf, n) for buf in BUFS for n in ARRAYS])
            moved.wait()
            dense_out(0).wait()


def step(cap, x0, dy, ids, gates, wd, w1, w3, w2):
    tokens, width = dy.shape
    layers, local, _, ff = w1.shape
    quarter, part, piece = width // SIDE, ff // 2 // SIDE, width // 2 // SIDE
    hbm = pl.BlockSpec(memory_space=pl.ANY)

    def fixed(shape):
        return pl.BlockSpec(shape, lambda s: (0,) * len(shape), pipeline_mode=pl.Buffered(1))

    def buf(*shape):
        return pltpu.VMEM(shape, BF16)

    def dma(*shape):
        return pltpu.SemaphoreType.DMA(shape)

    shape = jax.ShapeDtypeStruct
    ups, downs = [(width, ff), (width, ff), (ff, width)], [(quarter, ff), (part, width)]
    acts = [(cap, width), (cap, ff), (cap, ff)]
    scratch = [pltpu.VMEM((tokens, width), F32)] + [buf(tokens, width)] * 3 + [buf(width, width), pltpu.VMEM((layers, SLOTS, tokens), jnp.int32), pltpu.VMEM((layers, tokens, LANES), F32)]
    scratch += [buf(2, *u) for u in ups] + [buf(n, *a) for n, a in zip((2, 3, 3), acts)]
    scratch += [buf(2, *u) for u in ups] + [buf(SIDE + 2, *u) for u in ups]
    scratch += [buf(SIDE, 2, quarter // 2, ff), buf(SIDE, 2, quarter, ff)] * 2
    scratch += [buf(SIDE, quarter, ff)] * 2
    scratch += [buf(2, quarter // 2, ff), buf(2, quarter, ff)] * 2 + [buf(2, ff // 2, width), buf(2, ff, width)]
    scratch += [buf(2, part // 2, width), buf(2, part, width)] * 2
    scratch += [buf(SIDE, quarter, ff)] * 2 + [buf(SIDE, part, width)] * 2
    scratch += [buf(quarter, ff)] * 2 + [buf(part, width)] * 2
    scratch += [buf(width, width)] + [buf(width // 2, width)] * 2 + [buf(SIDE - 1, piece, width)] + [buf(SIDE, piece, width)] * 2 + [buf(width // 2, width)] * 2
    scratch += [dma(4), dma(2, 6), dma(2, 3), dma(2, 3), dma(GATHER_COPIES), dma(GATHER_COPIES), dma(REDUCE_COPIES), dma(REDUCE_COPIES), pltpu.SemaphoreType.REGULAR((3,))]
    results = [(tokens, width), (tokens, width), (layers, width, width)]
    kept = [(layers, local, *u) for u in ups] + [(layers, SLOTS, *u) for u in ups + acts] + [(SLOTS, cap, ff)] * 2
    return pl.pallas_call(
        functools.partial(kernel, cap),
        grid=(STEPS,),
        in_specs=[hbm] * 2 + [fixed(v.shape) for v in (ids, gates, wd)] + [hbm] * 3,
        out_specs=[hbm] * len(results + kept),
        out_shape=[shape(r, BF16) for r in results + kept],
        scratch_shapes=scratch,
        compiler_params=pltpu.CompilerParams(vmem_limit_bytes=VMEM_LIMIT, collective_id=0, has_side_effects=True),
        name="step",
    )(x0, dy, ids, gates, wd, w1, w3, w2)[:6]


def take_kernel(count, *refs):
    sources, targets, holds, (come, go) = refs[:count], refs[count : 2 * count], refs[2 * count : 3 * count], refs[3 * count :]
    comes = [pltpu.make_async_copy(a, b, come.at[n]) for n, (a, b) in enumerate(zip(sources, holds))]
    goes = [pltpu.make_async_copy(a, b, go.at[n]) for n, (a, b) in enumerate(zip(holds, targets))]
    for item in comes:
        item.start()
    for first, then in zip(comes, goes):
        first.wait()
        then.start()
    for item in goes:
        item.wait()


def take(arrays):
    count = len(arrays)
    hbm = pl.BlockSpec(memory_space=pl.ANY)
    return pl.pallas_call(
        functools.partial(take_kernel, count),
        in_specs=[hbm] * count,
        out_specs=[hbm] * count,
        out_shape=[jax.ShapeDtypeStruct(a.shape, a.dtype) for a in arrays],
        scratch_shapes=[pltpu.VMEM(a.shape, a.dtype) for a in arrays] + [pltpu.SemaphoreType.DMA((count,))] * 2,
        compiler_params=pltpu.CompilerParams(vmem_limit_bytes=VMEM_LIMIT),
        name="take",
    )(*arrays)


def solution(mesh):
    tok_spec = P(TOK_AXES, None)
    route_spec = P(None, TOK_AXES, None)
    expert_spec = P(None, "ep", None, None)
    whole_spec = P(None, None, None)

    def device_step(tok_in, tok_grad, route_ids, gate_vals, *weights):
        tokens, top_k = route_ids.shape[1:]
        return tuple(take(step(2 * tokens * top_k // SLOTS, tok_in, tok_grad, jnp.swapaxes(route_ids, 1, 2), jnp.swapaxes(gate_vals, 1, 2), *weights)))

    return jax.shard_map(device_step, mesh=mesh, in_specs=(tok_spec, tok_spec, route_spec, route_spec, whole_spec, expert_spec, expert_spec, expert_spec), out_specs=(tok_spec, tok_spec, whole_spec, expert_spec, expert_spec, expert_spec), check_vma=False)
```

```python
import functools

import jax
import jax.numpy as jnp
from jax import lax
from jax.experimental import pallas as pl
from jax.experimental.pallas import tpu as pltpu
from jax.sharding import PartitionSpec as P

TOK_AXES = ("rep", "ep", "dp")
F32 = jnp.float32
BF16 = jnp.bfloat16
LANES = 128
SIDE = 4
WAYS = (1, -1)
BUFS = (0, 1)
LAYERS = (1, 0)
ARRAYS = range(3)
SLOTS = 8
MESH = pl.DeviceIdType.MESH
VMEM_LIMIT = 67_043_328


def dot(a, b):
    return jnp.dot(a, b, preferred_element_type=F32)


def dot_nt(a, b):
    return lax.dot_general(a, b, (((1,), (1,)), ((), ())), preferred_element_type=F32)


def dot_tn(a, b):
    return lax.dot_general(a, b, (((0,), (0,)), ((), ())), preferred_element_type=F32)


class Place:
    def __init__(self):
        self.z, self.y, dp = lax.axis_index("rep"), lax.axis_index("ep"), lax.axis_index("dp")
        self.x, self.c = dp // 2, dp % 2

    def at(self, axis, step):
        z, y, x, c = self.z, self.y, self.x, self.c
        if axis == "z":
            z = (z + step + SIDE) % SIDE
        elif axis == "y":
            y = (y + step + SIDE) % SIDE
        elif axis == "x":
            x = (x + step + SIDE) % SIDE
        else:
            c = 1 - c
        return (z, y, x * 2 + c)


class Copies:
    def __init__(self, place, send, recv):
        self.place, self.send, self.recv, self.made, self.number, self.count, self.over = place, send, recv, {}, {}, 0, set()

    def add(self, key, src, dst, axis, step, like=None):
        if like is None:
            n, self.count = self.count, self.count + 1
        else:
            n = self.number[like]
        self.number[key] = n
        self.made[key] = pltpu.make_async_remote_copy(src_ref=src, dst_ref=dst, send_sem=self.send.at[n], recv_sem=self.recv.at[n], device_id=self.place.at(axis, step), device_id_type=MESH)

    def start(self, *keys):
        for key in keys:
            self.made[key].start()

    def arrive(self, *keys):
        for key in keys:
            self.made[key].wait_recv()

    def sent(self, *keys):
        for key in keys:
            self.made[key].wait_send()
            self.over.add(key)

    def drain(self):
        self.sent(*[key for key in self.made if key not in self.over])


def greet(place):
    barrier = pltpu.get_barrier_semaphore()
    peers = [(axis, step) for axis in "xyz" for step in range(1, SIDE)] + [("c", 0)]
    for axis, step in peers:
        pl.semaphore_signal(barrier, inc=1, device_id=place.at(axis, step), device_id_type=MESH)
    pl.semaphore_wait(barrier, len(peers))


class Gather:
    PASS = {2: 4, 3: 6, 5: 7}

    def __init__(self, layer, copies, place, own, whole):
        self.layer, self.copies, self.place, self.own, self.whole = layer, copies, place, own, whole
        rows, ff = own[0].shape[2], own[2].shape[2]
        self.cut = {"x": ((0, 0, rows // SIDE), (2, 0, ff // 2 // SIDE)), "z": ((1, 0, rows // SIDE), (2, ff // 2, ff // 2 // SIDE))}
        mine = {"x": place.x, "z": place.z}
        for color in ("x", "z"):
            for part in BUFS:
                self._add(("y", 2, color, part), color, part, None, 2, mine[color], None, "y", 1)
                self._add(("y", 3, color, part), color, part, None, 3, mine[color], None, "y", -1)
                if color == "x":
                    self._add(("y", 5, color, part), color, part, 2, 5, mine[color], None, "y", 1)
                else:
                    self._add(("y", 5, color, part), color, part, 3, 5, mine[color], None, "y", -1)
                for slot in (2, 3, 5):
                    for step in WAYS:
                        self._add(("near", slot, color, part, step), color, part, slot, slot, mine[color], None, color, step)
                        behind = (mine[color] - step + SIDE) % SIDE
                        self._add(("far", slot, color, part, step), color, part, slot, slot, behind, (1 - step) // 2, color, step)
        for slot, to in self.PASS.items():
            for array in ARRAYS:
                copies.add((layer, "pass", slot, array), whole[array].at[layer, slot], whole[array].at[layer, to], "c", 0)

    def _view(self, refs, index, color, part, quarter, half):
        array, base, size = self.cut[color][part]
        start = base + quarter * size
        if half is not None:
            size = size // 2
            start = start + half * size
        return refs[array].at[self.layer, index, pl.ds(pl.multiple_of(start, 16), size)]

    def _add(self, key, color, part, src_slot, dst_slot, quarter, half, axis, step):
        src = self._view(self.own, self.place.c, color, part, quarter, half) if src_slot is None else self._view(self.whole, src_slot, color, part, quarter, half)
        self.copies.add((self.layer,) + key, src, self._view(self.whole, dst_slot, color, part, quarter, half), axis, step)

    def _keys(self, *key, extra=()):
        return [(self.layer,) + key + (part,) + extra for part in BUFS]

    def lead(self):
        self.spread(2, "x")
        self.spread(3, "z")

    def lead_onward(self):
        self.onward(2, "x")
        self.onward(3, "z")

    def follow(self):
        self.spread(2, "z")
        self.spread(3, "x")

    def follow_onward(self):
        self.onward(2, "z")
        self.onward(3, "x")

    def last(self):
        self.spread(5, "x")
        self.spread(5, "z")

    def last_onward(self):
        self.onward(5, "x")
        self.onward(5, "z")

    def complete_y(self):
        self.complete(2)
        self.complete(3)

    def complete_last(self):
        self.complete(5)

    def passed_left(self):
        self.passed(2)

    def passed_right(self):
        self.passed(3)

    def passed_last(self):
        self.passed(5)

    def begin(self):
        for slot, color in ((2, "x"), (3, "z"), (2, "z"), (3, "x")):
            self.copies.start(*self._keys("y", slot, color))

    def spread(self, slot, color):
        for part in BUFS:
            self.copies.arrive((self.layer, "y", slot, color, part))
            self.copies.start(*[(self.layer, "near", slot, color, part, step) for step in WAYS])
        if (slot, color) in ((2, "x"), (3, "z")):
            self.copies.start(*self._keys("y", 5, color))

    def onward(self, slot, color):
        for part in BUFS:
            for step in WAYS:
                self.copies.arrive((self.layer, "near", slot, color, part, step))
                self.copies.start((self.layer, "far", slot, color, part, step))

    def complete(self, slot):
        for color in ("x", "z"):
            for step in WAYS:
                self.copies.arrive(*self._keys("far", slot, color, extra=(step,)))
        self.copies.start(*[(self.layer, "pass", slot, array) for array in ARRAYS])

    def passed(self, slot):
        self.copies.arrive(*[(self.layer, "pass", slot, array) for array in ARRAYS])


GATHER_COPIES = 2 * (2 * 2 * (3 + 3 * 4) + 9)


def route(ids_ref, gate_ref, rows_ref, columns_ref, place):
    layers, _, tokens = ids_ref.shape
    below = lax.broadcasted_iota(jnp.int32, (tokens, tokens), 0) < lax.broadcasted_iota(jnp.int32, (tokens, tokens), 1)
    below = jnp.where(below, 1.0, 0.0).astype(BF16)
    lead = lax.broadcasted_iota(jnp.int32, (2 * SLOTS, tokens), 0)
    for layer in range(layers):
        ids, gates = ids_ref[layer], gate_ref[layer]
        off = ((ids >> 1) - place.y) & (SIDE - 1)
        odd = (ids + place.c) & 1
        slot = jnp.where(off == 0, odd, jnp.where(off == SIDE - 1, 2 + 2 * odd, jnp.where(off == 1, 3 + 3 * odd, 5 + 2 * odd)))
        hits = [slot[n : n + 1] == lead for n in BUFS]
        hit = hits[0] | hits[1]
        weight = jnp.where(hits[0], gates[0:1], 0.0) + jnp.where(hits[1], gates[1:2], 0.0)
        rank = jnp.where(hit, dot(jnp.where(hit, 1.0, 0.0).astype(BF16), below), -1.0)
        rows_ref[layer] = rank[:SLOTS].astype(jnp.int32)
        columns_ref[layer] = jnp.transpose(jnp.concatenate([rank[:SLOTS], weight[:SLOTS], jnp.zeros((LANES - 2 * SLOTS, tokens), F32)], axis=0))


def one_hot(rows_ref, layer, slot, cap):
    place = lax.broadcasted_iota(jnp.int32, (cap, rows_ref.shape[2]), 0)
    return jnp.where(rows_ref[layer, pl.ds(slot, 1), :] == place, 1.0, 0.0).astype(BF16)


def column(columns_ref, layer, index):
    lane = lax.broadcasted_iota(jnp.int32, columns_ref.shape[1:], 1)
    return jnp.sum(jnp.where(lane == index, columns_ref[layer], 0.0), axis=1, keepdims=True)


def one_hot_t(columns_ref, layer, slot, cap):
    place = lax.broadcasted_iota(jnp.int32, (columns_ref.shape[1], cap), 1)
    return jnp.where(column(columns_ref, layer, slot).astype(jnp.int32) == place, 1.0, 0.0).astype(BF16)


def add_to(dst, src):
    dst[...] = (dst[...].astype(F32) + src[...].astype(F32)).astype(BF16)


def cut(rows, half):
    first = (rows // 2 + 15) // 16 * 16
    return (half * first, first + half * (rows - 2 * first))


class RingSum:
    def __init__(self, copies, name, axis, block, first, second):
        self.copies, self.block, self.second = copies, block, second
        self.first = [first.at[half, pl.ds(0, block(2, half).shape[0])] for half in BUFS]
        self.early, self.later = ([(name, when, step) for step in WAYS] for when in ("early", "later"))
        for half, step in enumerate(WAYS):
            copies.add(self.early[half], block(2, half), self.first[half], axis, step)
            copies.add(self.later[half], block(step, None), second.at[half], axis, step)

    def start(self):
        self.copies.start(*self.early)

    def onward(self):
        self.copies.arrive(*self.early)
        for half in BUFS:
            add_to(self.block(WAYS[half], half), self.first[half])
            self.copies.start(self.later[half])
        self.copies.sent(*self.early)

    def finish(self, out):
        self.copies.arrive(*self.later)
        out[...] = (self.block(0, None)[...].astype(F32) + self.second[0].astype(F32) + self.second[1].astype(F32)).astype(BF16)
        self.copies.sent(*self.later)


class RingSpread:
    def __init__(self, copies, name, axis, me, block, source=None, like=None):
        self.copies = copies
        self.near, self.far = ([(name, when, step) for step in WAYS] for when in ("near", "far"))
        for half, step in enumerate(WAYS):
            behind = (me - step + SIDE) % SIDE
            near, far = (None, None) if like is None else (like.near[half], like.far[half])
            copies.add(self.near[half], block(me, None) if source is None else source, block(me, None), axis, step, near)
            copies.add(self.far[half], block(behind, half), block(behind, half), axis, step, far)

    def start(self):
        self.copies.start(*self.near)

    def onward(self):
        for near, far in zip(self.near, self.far):
            self.copies.arrive(near)
            self.copies.start(far)

    def finish(self):
        self.copies.arrive(*self.far)
        self.copies.sent(*self.near, *self.far)


class Direct:
    def __init__(self, copies, name, axis, source, target):
        self.copies, self.keys = copies, [(name, step) for step in range(1, SIDE)]
        for name, step in self.keys:
            copies.add((name, step), source(step), target(step), axis, step)

    def start(self):
        self.copies.start(*self.keys)

    def finish(self):
        self.copies.arrive(*self.keys)
        self.copies.sent(*self.keys)


def slices(ref, lead, base, size):
    def block(index, half):
        start, rows = base + index * size, size
        if half is not None:
            skip, rows = cut(size, half)
            start = start + skip
        return ref.at[(*lead, pl.ds(pl.multiple_of(start, 16), rows))]

    return block


def slabs(ref):
    def block(index, half):
        if half is None:
            return ref.at[index]
        return ref.at[index, pl.ds(*cut(ref.shape[1], half))]

    return block


def total(ref):
    return (ref[0].astype(F32) + ref[1].astype(F32) + ref[2].astype(F32) + ref[3].astype(F32)).astype(BF16)


OWN_STEPS = {2: 0, 4: 1, 5: 2, 7: 3}
REDUCE_COPIES = 120
WEIGHTS1, INPUTS1, WEIGHTS0, INPUTS0, STEPS = (n * SLOTS for n in range(2, 7))


def kernel(cap, x0_ref, dy_ref, ids_ref, gate_ref, wd_ref, o1_ref, o3_ref, o2_ref, y_ref, dx_ref, gdense_ref, g1_ref, g3_ref, g2_ref, h1_ref, h3_ref, h2_ref, kz_ref, ka_ref, kb_ref, kda_ref, kdb_ref, acc_ref, cur_ref, x1_ref, hold_ref, gd_ref, rows_ref, columns_ref, w1_ref, w3_ref, w2_ref, z_ref, a_ref, b_ref, m1_ref, m3_ref, m2_ref, d1_ref, d3_ref, d2_ref, s1_ref, s3_ref, s2_ref, r11_ref, r12_ref, r31_ref, r32_ref, t1_ref, t3_ref, y11_ref, y12_ref, y31_ref, y32_ref, y21_ref, y22_ref, u1_ref, u2_ref, l1_ref, l2_ref, c1_ref, c3_ref, cu_ref, cl_ref, f1_ref, f3_ref, fu_ref, fl_ref, dp_ref, dr_ref, ds_ref, e_ref, dcx_ref, dcz_ref, dcy_ref, de_ref, put_sem, load_sem, keep_sem, save_sem, gsend_sem, grecv_sem, send_sem, recv_sem, credit):
    s = pl.program_id(0)
    place = Place()
    gathers = Copies(place, gsend_sem, grecv_sem)
    copies = Copies(place, send_sem, recv_sem)
    given, whole, bufs = (o1_ref, o3_ref, o2_ref), (h1_ref, h3_ref, h2_ref), (w1_ref, w3_ref, w2_ref)
    kept, acts = (kz_ref, ka_ref, kb_ref), (z_ref, a_ref, b_ref)
    deferred = (kda_ref, kdb_ref)
    g0, g1 = (Gather(l, gathers, place, given, whole) for l in BUFS)
    rows, ff = s1_ref.shape[1], s2_ref.shape[1]
    quarter, part = rows // SIDE, ff // 2 // SIDE
    half_d = rows // 2

    stage, mate, mine_of = (m1_ref, m3_ref, m2_ref), (d1_ref, d3_ref, d2_ref), (s1_ref, s3_ref, s2_ref)
    for buf in BUFS:
        for n in ARRAYS:
            copies.add(("pair", buf, n), stage[n].at[buf], mate[n].at[buf], "c", 0)

    def ring_blocks(ref, q, me, base, size):
        block = slices(ref, (q,), base, size)
        return lambda offset, half: block((me + offset + SIDE) % SIDE, half)

    def group_blocks(ref):
        block = slabs(ref)
        return lambda offset, half: block({2: 0, 1: 1, -1: 2, 0: 3}[offset], half)

    first = {
        "x": [RingSum(copies, ("x", q), "x", ring_blocks(s1_ref, q, place.x, 0, quarter), r11_ref.at[q], r12_ref.at[q]) for q in range(SIDE)],
        "z": [RingSum(copies, ("z", q), "z", ring_blocks(s3_ref, q, place.z, 0, quarter), r31_ref.at[q], r32_ref.at[q]) for q in range(SIDE)],
    }
    mid = {"x": t1_ref, "z": t3_ref}
    on_y = {
        "x": RingSum(copies, "yx", "y", group_blocks(t1_ref), y11_ref, y12_ref),
        "z": RingSum(copies, "yz", "y", group_blocks(t3_ref), y31_ref, y32_ref),
        "w": RingSum(copies, "yw", "y", group_blocks(s2_ref), y21_ref, y22_ref),
    }
    inner = {
        "u": RingSum(copies, "u", "x", ring_blocks(s2_ref, 3, place.x, 0, part), u1_ref, u2_ref),
        "l": RingSum(copies, "l", "z", ring_blocks(s2_ref, 3, place.z, ff // 2, part), l1_ref, l2_ref),
    }
    ring_of = {"x": ("x", place.x), "u": ("x", place.x), "z": ("z", place.z), "l": ("z", place.z)}
    other_of = {"x": ("z", place.z), "u": ("z", place.z), "z": ("x", place.x), "l": ("x", place.x)}
    cross_ref = {"x": c1_ref, "z": c3_ref, "u": cu_ref, "l": cl_ref}
    done_ref = {"x": f1_ref, "z": f3_ref, "u": fu_ref, "l": fl_ref}
    out_of = {"x": (g1_ref, 0, quarter), "z": (g3_ref, 0, quarter), "u": (g2_ref, 0, part), "l": (g2_ref, ff // 2, part)}
    cross, final, puts = {}, {}, {}
    for i, k in enumerate(out_of):
        cross[k] = RingSpread(copies, ("cross", k), *other_of[k], slabs(cross_ref[k]))
        ref, base, size = out_of[k]
        for late in LAYERS:
            block = slices(ref, (late, place.c), base, size)
            final[k, late] = RingSpread(copies, ("final", k, late), *ring_of[k], block, source=done_ref[k], like=final.get((k, 1)))
            me = ring_of[k][1]
            puts[k, late] = pltpu.make_async_copy(done_ref[k], block(me, None), put_sem.at[i])
            for offset in (0, *WAYS, 2):
                quarter_at = block((me + offset) % SIDE if offset >= 0 else (me + SIDE - 1) % SIDE, None)
                copies.add(("pass", k, offset, late), quarter_at if offset else done_ref[k], quarter_at, "c", 0, None if late else ("pass", k, offset, 1))
    mine, theirs = (pl.ds(pl.multiple_of(c * half_d, 16), half_d) for c in (place.c, 1 - place.c))
    copies.add("dense pair", dp_ref.at[theirs], dr_ref, "c", 0)
    copies.add("dense pass", dcy_ref, de_ref, "c", 0)
    piece = half_d // SIDE
    dense_block = slices(ds_ref, (), 0, piece)
    dense_sums = Direct(copies, "dense sums", "y", lambda step: dense_block((place.y + step) % SIDE, None), lambda step: e_ref.at[step - 1])
    gather_block = slices(dcy_ref, (), 0, piece)(place.y, None)
    own_piece = {"x": dcx_ref.at[place.x], "z": dcz_ref.at[place.z], "y": gather_block}
    dense = {k: Direct(copies, ("dense", k), k, lambda step, k=k: own_piece[k], lambda step, k=k: own_piece[k]) for k in own_piece}

    def reduce_start(q):
        for k in ("x", "z"):
            first[k][q].start()

    def reduce_onward(q):
        for k in ("x", "z"):
            first[k][q].onward()

    def reduce_finish(q):
        for k in ("x", "z"):
            first[k][q].finish(mid[k].at[q])

    def y_start():
        for k in ("x", "z"):
            on_y[k].start()

    def y_onward():
        for k in ("x", "z"):
            on_y[k].onward()

    def y_finish():
        for k in ("x", "z"):
            on_y[k].finish(cross_ref[k].at[other_of[k][1]])
            cross[k].start()

    def w_finish():
        on_y["w"].finish(s2_ref.at[3])
        for k in ("u", "l"):
            inner[k].start()

    def inner_onward():
        for k in ("u", "l"):
            inner[k].onward()

    def inner_finish():
        for k in ("u", "l"):
            inner[k].finish(cross_ref[k].at[other_of[k][1]])
            cross[k].start()

    def cross_onward(*keys):
        for k in keys:
            cross[k].onward()

    def cross_finish(late, *keys):
        for k in keys:
            cross[k].finish()
            done_ref[k][...] = total(cross_ref[k])
            puts[k, late].start()
            final[k, late].start()
            copies.start(("pass", k, 0, late))

    def final_onward(late, *keys):
        for k in keys:
            final[k, late].onward()
            copies.start(*[("pass", k, way, late) for way in WAYS])

    def final_finish(late, *keys):
        for k in keys:
            final[k, late].finish()
            puts[k, late].wait()
            copies.start(("pass", k, 2, late))

    def pass_finish(late):
        keys = [("pass", k, offset, late) for k in out_of for offset in (0, *WAYS, 2)]
        copies.arrive(*keys)
        copies.sent(*keys)

    def dense_sum():
        copies.arrive("dense pair")
        ds_ref[...] = (dp_ref[mine].astype(F32) + dr_ref[...].astype(F32)).astype(BF16)
        copies.sent("dense pair")
        dense_sums.start()

    def dense_to_x():
        dense_sums.finish()
        mine = dense_block(place.y, None)[...].astype(F32)
        own_piece["x"][...] = (mine + e_ref[0].astype(F32) + e_ref[1].astype(F32) + e_ref[2].astype(F32)).astype(BF16)
        dense["x"].start()

    def dense_next(k, ref, follow):
        dense[k].finish()
        own_piece[follow][...] = total(ref)
        dense[follow].start()

    def dense_to_z():
        dense_next("x", dcx_ref, "z")

    def dense_to_y():
        dense_next("z", dcz_ref, "y")

    def dense_out(late):
        return pltpu.make_async_copy(gd_ref, gdense_ref.at[late], keep_sem.at[0, 1])

    def dense_pass(late):
        dense["y"].finish()
        if late == 0:
            dense_out(1).wait()
        gd_ref[mine] = dcy_ref[...]
        copies.start("dense pass")

    def dense_finish(late):
        copies.arrive("dense pass")
        gd_ref[theirs] = de_ref[...]
        copies.sent("dense pass")
        dense_out(late).start()

    def copy(src, dst, sem):
        return pltpu.make_async_copy(src, dst, sem)

    def weights(layer, slot, arrays, buf, is_given=False):
        for n in arrays:
            src = given[n].at[layer, (place.c + slot) % 2] if is_given else whole[n].at[layer, slot]
            yield copy(src, bufs[n].at[buf], load_sem.at[buf, n])

    def saved(layer, slot, buf):
        for n, (src, dst) in enumerate(zip(kept, acts)):
            yield copy(src.at[layer, slot], dst.at[buf], load_sem.at[buf, 3 + n])

    def weights_loads(step):
        layer, slot, buf = layer_of(step), SLOTS - 1 - step % SLOTS, (step + 1) % 2
        return [*weights(layer, slot, [2], buf), *saved(layer, slot, buf)]

    def inputs_loads(step):
        layer, slot, buf = layer_of(step), SLOTS - 1 - step % SLOTS, (step + 1) % 2
        return [*weights(layer, slot, BUFS, buf)] + [copy(deferred[n].at[slot], acts[n + 1].at[buf], load_sem.at[buf, 4 + n]) for n in BUFS]

    def load(step):
        slot = step % SLOTS
        for is_given in (True, False):
            pl.when((slot < 2) == is_given)(lambda: start(weights(step // SLOTS, slot, ARRAYS, step % 2, is_given)))

    def layer_of(step):
        return 1 - (step - WEIGHTS1) // (2 * SLOTS)

    def keeps(step):
        return [copy(bufs[n].at[step % 2], whole[n].at[step // SLOTS, step % SLOTS], keep_sem.at[step % 2, n]) for n in ARRAYS]

    def saves(step):
        return [copy(src.at[step % 2], dst.at[step // SLOTS, step % SLOTS], save_sem.at[step % 2, n]) for n, (src, dst) in enumerate(zip(acts, kept))]

    def defers(step):
        return [copy(acts[n + 1].at[2], deferred[n].at[SLOTS - 1 - step % SLOTS], save_sem.at[0, n]) for n in BUFS]

    def wait(items):
        for item in items:
            item.wait()

    def start(items):
        for item in items:
            item.start()

    def ending():
        dense_finish(1)
        copies.start("dense pair")
        y_finish()
        inner_finish()
        dense_sum()
        dense_to_x()
        cross_onward("x", "z")
        pass_finish(1)
        pl.semaphore_signal(credit.at[2], inc=1, device_id=place.at("c", 0), device_id_type=MESH)
        cross_onward("u", "l")
        dense_to_z()
        pl.semaphore_wait(credit.at[2], 1)
        cross_finish(0, "x", "z")
        cross_finish(0, "u", "l")
        dense_to_y()
        dense_pass(0)
        final_onward(0, "x", "z")
        dense_finish(0)
        final_onward(0, "u", "l")
        final_finish(0, "x", "z")
        final_finish(0, "u", "l")
        pass_finish(0)

    before, middle, after = {}, {}, {}

    def plan(table, first, *stages):
        for n, stage in enumerate(stages):
            table.setdefault(first + n, []).extend(stage)

    on, done = lambda q: lambda: reduce_onward(q), lambda q: lambda: reduce_finish(q)
    now = lambda: load(s)
    plan(before, 1, [g0.lead], [g0.follow, g0.lead_onward, g1.begin, g0.follow_onward, g0.last, g0.complete_y, now], [g0.passed_left])
    plan(before, 4, [g0.last_onward, g1.lead], [g0.complete_last, now, g0.passed_right, g1.follow], [], [g0.passed_last, now, g1.lead_onward])
    plan(before, SLOTS + 1, [g1.follow_onward, g1.last], [g1.complete_y, now], [g1.passed_left], [g1.last_onward], [g1.complete_last, now, g1.passed_right], [g1.passed_last])
    unready = (1, 4, 6, SLOTS + 1, SLOTS + 4)
    late = ("x", "z", "u", "l")
    plan(before, INPUTS1 + 6, [w_finish], [], [inner_onward])
    plan(before, WEIGHTS0, [lambda: copies.start("dense pair")], [], [inner_finish], [lambda: cross_onward("x", "z"), dense_to_x], [lambda: cross_onward("u", "l")], [dense_to_z])
    plan(middle, WEIGHTS0, [dense_sum, y_finish], [], [], [], [], [], [], [dense_to_y])
    plan(before, INPUTS0, [lambda: cross_finish(1, *late)], [], [], [], [], [lambda: final_onward(1, *late)], [], [lambda: dense_pass(1), lambda: final_finish(1, *late)])
    plan(before, INPUTS0 + 5, [w_finish], [], [inner_onward])
    for base in (WEIGHTS1, WEIGHTS0):
        plan(before, base + 3, [on_y["w"].start], [], [], [done(0), y_start, on_y["w"].onward])
        plan(middle, base + 4, [on(0)], [], [on(1)], [on(2)])
        plan(before, base + SLOTS, [], [done(1)], [done(2), y_onward], [on(3)], [], [], [done(3)])
        for step, q in OWN_STEPS.items():
            plan(after, base + step, [lambda q=q: reduce_start(q)])

    def hooks(table, *phases):
        for phase in phases:
            mine = {step: stages for step, stages in sorted(table.items()) if phase <= step < phase + SLOTS}
            if mine:

                @pl.when(s // SLOTS == phase // SLOTS)
                def _(mine=mine):
                    for step, stages in mine.items():

                        @pl.when(s == step)
                        def _(stages=stages):
                            for stage in stages:
                                stage()

    phase, t = s // SLOTS, s % SLOTS
    forth, back = s % 2, (s + 1) % 2

    def bring(ref, hold):
        return copy(ref, hold, keep_sem.at[1, 0])

    @pl.when(s == 0)
    def _():
        bring(x0_ref, hold_ref).start()
        load(0)
        greet(place)
        g0.begin()
        load(1)
        route(ids_ref, gate_ref, rows_ref, columns_ref, place)
        bring(x0_ref, hold_ref).wait()

    def enter(x):
        cur_ref[...] = (x.astype(F32) + dot(x, wd_ref[phase])).astype(BF16)
        acc_ref[...] = jnp.zeros_like(acc_ref)

    def leave(out_ref):
        out_ref[...] = (cur_ref[...].astype(F32) + acc_ref[...]).astype(BF16)

    @pl.when(s < WEIGHTS1)
    def _():
        hooks(before, 0, SLOTS)
        pl.when(s > 1)(lambda: wait(saves(s - 2)))
        ahead = functools.reduce(jnp.logical_and, [s != step for step in unready], (s > 0) & (s < WEIGHTS1 - 1))
        pl.when((t == 1) | (t == 2))(lambda: wait(keeps(s - 1)))
        pl.when(ahead)(lambda: load(s + 1))

        @pl.when(t < 2)
        def _():
            pl.when(s == 0)(lambda: enter(hold_ref[...]))
            pl.when(s == SLOTS)(lambda: enter(x1_ref[...]))

        layer, slot = phase, t
        come = list(weights(layer, slot, ARRAYS, forth))

        def forward_step(is_ready):
            if is_ready:
                wait(come)
            z = dot(one_hot(rows_ref, layer, slot, cap), cur_ref[...]).astype(BF16)
            z_ref[forth] = z
            if not is_ready:
                wait(come)
            a = dot(z, w1_ref[forth]).astype(BF16)
            b = dot(z, w3_ref[forth]).astype(BF16)
            a_ref[forth] = a
            b_ref[forth] = b
            a = a.astype(F32)
            h = (a * jax.nn.sigmoid(a) * b.astype(F32)).astype(BF16)
            o = dot(h, w2_ref[forth]).astype(BF16)
            acc_ref[...] += column(columns_ref, layer, SLOTS + slot) * dot(one_hot_t(columns_ref, layer, slot, cap), o)

        is_late = functools.reduce(jnp.logical_or, [s == step + 1 for step in unready])
        pl.when(is_late)(lambda: forward_step(False))
        pl.when(jnp.logical_not(is_late))(lambda: forward_step(True))
        pl.when(t < 2)(lambda: start(keeps(s)))
        pl.when(s < WEIGHTS1 - 1)(lambda: start(saves(s)))
        @pl.when(t == SLOTS - 1)
        def _():
            pl.when(s == SLOTS - 1)(lambda: leave(x1_ref))
            pl.when(s == WEIGHTS1 - 1)(lambda: leave(hold_ref))

    @pl.when((phase == WEIGHTS1 // SLOTS) | (phase == WEIGHTS0 // SLOTS))
    def _():
        layer, slot = layer_of(s), SLOTS - 1 - t
        hooks(before, WEIGHTS1, WEIGHTS0)

        @pl.when(s == WEIGHTS1)
        def _():
            moved = copy(hold_ref, y_ref, keep_sem.at[0, 0])
            moved.start()
            bring(dy_ref, cur_ref).start()
            wait(saves(s - 2))
            gathers.drain()
            bring(dy_ref, cur_ref).wait()
            moved.wait()
            acc_ref[...] = cur_ref[...].astype(F32)

        pl.when(s > WEIGHTS1)(lambda: wait(weights_loads(s)))
        pl.when(t > 0)(lambda: wait(defers(s - 1)))
        pl.when(t < SLOTS - 1)(lambda: start(weights_loads(s + 1)))
        pl.when(t == SLOTS - 1)(lambda: start(inputs_loads(s + 1)))

        grad_gated = (column(columns_ref, layer, SLOTS + slot) * cur_ref[...].astype(F32)).astype(BF16)
        do = dot(one_hot(rows_ref, layer, slot, cap), grad_gated).astype(BF16)
        dh = dot_nt(do, w2_ref[back])
        a = a_ref[back].astype(F32)
        b = b_ref[back].astype(F32)
        sig = jax.nn.sigmoid(a)
        act = a * sig
        h = (act * b).astype(BF16)
        db = (dh * act).astype(BF16)
        da = (dh * b * (sig + act * (1.0 - sig))).astype(BF16)
        a_ref[2] = da
        b_ref[2] = db
        z = z_ref[back]
        start(defers(s))
        hooks(middle, WEIGHTS1, WEIGHTS0)

        def weight_grads():
            return dot_tn(z, da), dot_tn(z, db), dot_tn(h, do)

        is_own = functools.reduce(jnp.logical_or, [t == step for step in OWN_STEPS])
        group = t // 4 + t // 5 + t // 7
        into = (t + t // 3 + t // 6) % 2
        turn = t + (1 - layer) * SLOTS

        @pl.when(jnp.logical_not(is_own))
        def _():
            for buf in BUFS:
                pl.when((turn >= 3) & (into == buf))(lambda: copies.sent(*[("pair", buf, n) for n in ARRAYS]))

            for ref, grad in zip(stage, weight_grads()):
                ref[into] = grad.astype(BF16)

            pl.when(turn >= 3)(lambda: pl.semaphore_wait(credit.at[into], 1))
            for buf in BUFS:
                pl.when(into == buf)(lambda: copies.start(*[("pair", buf, n) for n in ARRAYS]))

        @pl.when(is_own)
        def _():
            for buf in BUFS:
                pl.when(group % 2 == buf)(lambda: copies.arrive(*[("pair", buf, n) for n in ARRAYS]))

            for ref, add, grad in zip(mine_of, mate, weight_grads()):
                ref[group] = (grad + add[group % 2].astype(F32)).astype(BF16)

            @pl.when(turn < 2 * SLOTS - 3)
            def _():
                pl.semaphore_signal(credit.at[group % 2], inc=1, device_id=place.at("c", 0), device_id_type=MESH)

            hooks(after, WEIGHTS1, WEIGHTS0)

    def leave_back(layer, x, out_ref):
        grad = acc_ref[...]
        grad_b = grad.astype(BF16)
        dp_ref[...] = dot_tn(x, grad_b).astype(BF16)
        out_ref[...] = (grad + dot_nt(grad_b, wd_ref[layer])).astype(BF16)

    @pl.when((phase == INPUTS1 // SLOTS) | (phase == INPUTS0 // SLOTS))
    def _():
        layer, slot = layer_of(s), SLOTS - 1 - t
        hooks(before, INPUTS1, INPUTS0)
        wait(inputs_loads(s))
        pl.when(t == 0)(lambda: wait(defers(s - 1)))
        pl.when(t < SLOTS - 1)(lambda: start(inputs_loads(s + 1)))
        pl.when(s == WEIGHTS0 - 1)(lambda: start(weights_loads(s + 1)))
        dz = (dot_nt(a_ref[back], w1_ref[back]) + dot_nt(b_ref[back], w3_ref[back])).astype(BF16)
        acc_ref[...] += dot(one_hot_t(columns_ref, layer, slot, cap), dz)

        @pl.when(s == WEIGHTS0 - 1)
        def _():
            leave_back(1, x1_ref[...], cur_ref)
            acc_ref[...] = cur_ref[...].astype(F32)
            bring(x0_ref, x1_ref).start()
            bring(x0_ref, x1_ref).wait()

        @pl.when(s == STEPS - 1)
        def _():
            leave_back(0, x1_ref[...], hold_ref)
            moved = copy(hold_ref, dx_ref, keep_sem.at[0, 0])
            moved.start()
            ending()
            copies.sent(*[("pair", buf, n) for buf in BUFS for n in ARRAYS])
            moved.wait()
            dense_out(0).wait()


def step(cap, x0, dy, ids, gates, wd, w1, w3, w2):
    tokens, width = dy.shape
    layers, local, _, ff = w1.shape
    quarter, part, piece = width // SIDE, ff // 2 // SIDE, width // 2 // SIDE
    hbm = pl.BlockSpec(memory_space=pl.ANY)

    def fixed(shape):
        return pl.BlockSpec(shape, lambda s: (0,) * len(shape), pipeline_mode=pl.Buffered(1))

    def buf(*shape):
        return pltpu.VMEM(shape, BF16)

    def dma(*shape):
        return pltpu.SemaphoreType.DMA(shape)

    shape = jax.ShapeDtypeStruct
    ups, downs = [(width, ff), (width, ff), (ff, width)], [(quarter, ff), (part, width)]
    acts = [(cap, width), (cap, ff), (cap, ff)]
    scratch = [pltpu.VMEM((tokens, width), F32)] + [buf(tokens, width)] * 3 + [buf(width, width), pltpu.VMEM((layers, SLOTS, tokens), jnp.int32), pltpu.VMEM((layers, tokens, LANES), F32)]
    scratch += [buf(2, *u) for u in ups] + [buf(n, *a) for n, a in zip((2, 3, 3), acts)]
    scratch += [buf(2, *u) for u in ups] * 2 + [buf(SIDE, *u) for u in ups]
    scratch += [buf(SIDE, 2, quarter // 2, ff), buf(SIDE, 2, quarter, ff)] * 2
    scratch += [buf(SIDE, quarter, ff)] * 2
    scratch += [buf(2, quarter // 2, ff), buf(2, quarter, ff)] * 2 + [buf(2, ff // 2, width), buf(2, ff, width)]
    scratch += [buf(2, part // 2, width), buf(2, part, width)] * 2
    scratch += [buf(SIDE, quarter, ff)] * 2 + [buf(SIDE, part, width)] * 2
    scratch += [buf(quarter, ff)] * 2 + [buf(part, width)] * 2
    scratch += [buf(width, width)] + [buf(width // 2, width)] * 2 + [buf(SIDE - 1, piece, width)] + [buf(SIDE, piece, width)] * 2 + [buf(width // 2, width)] * 2
    scratch += [dma(4), dma(2, 6), dma(2, 3), dma(2, 3), dma(GATHER_COPIES), dma(GATHER_COPIES), dma(REDUCE_COPIES), dma(REDUCE_COPIES), pltpu.SemaphoreType.REGULAR((3,))]
    results = [(tokens, width), (tokens, width), (layers, width, width)]
    kept = [(layers, local, *u) for u in ups] + [(layers, SLOTS, *u) for u in ups + acts] + [(SLOTS, cap, ff)] * 2
    return pl.pallas_call(
        functools.partial(kernel, cap),
        grid=(STEPS,),
        in_specs=[hbm] * 2 + [fixed(v.shape) for v in (ids, gates, wd)] + [hbm] * 3,
        out_specs=[hbm] * len(results + kept),
        out_shape=[shape(r, BF16) for r in results + kept],
        scratch_shapes=scratch,
        compiler_params=pltpu.CompilerParams(vmem_limit_bytes=VMEM_LIMIT, collective_id=0, has_side_effects=True),
        name="step",
    )(x0, dy, ids, gates, wd, w1, w3, w2)[:6]


def take_kernel(count, *refs):
    sources, targets, holds, (come, go) = refs[:count], refs[count : 2 * count], refs[2 * count : 3 * count], refs[3 * count :]
    comes = [pltpu.make_async_copy(a, b, come.at[n]) for n, (a, b) in enumerate(zip(sources, holds))]
    goes = [pltpu.make_async_copy(a, b, go.at[n]) for n, (a, b) in enumerate(zip(holds, targets))]
    for item in comes:
        item.start()
    for first, then in zip(comes, goes):
        first.wait()
        then.start()
    for item in goes:
        item.wait()


def take(arrays):
    count = len(arrays)
    hbm = pl.BlockSpec(memory_space=pl.ANY)
    return pl.pallas_call(
        functools.partial(take_kernel, count),
        in_specs=[hbm] * count,
        out_specs=[hbm] * count,
        out_shape=[jax.ShapeDtypeStruct(a.shape, a.dtype) for a in arrays],
        scratch_shapes=[pltpu.VMEM(a.shape, a.dtype) for a in arrays] + [pltpu.SemaphoreType.DMA((count,))] * 2,
        compiler_params=pltpu.CompilerParams(vmem_limit_bytes=VMEM_LIMIT),
        name="take",
    )(*arrays)


def solution(mesh):
    tok_spec = P(TOK_AXES, None)
    route_spec = P(None, TOK_AXES, None)
    expert_spec = P(None, "ep", None, None)
    whole_spec = P(None, None, None)

    def device_step(tok_in, tok_grad, route_ids, gate_vals, *weights):
        tokens, top_k = route_ids.shape[1:]
        return tuple(take(step(2 * tokens * top_k // SLOTS, tok_in, tok_grad, jnp.swapaxes(route_ids, 1, 2), jnp.swapaxes(gate_vals, 1, 2), *weights)))

    return jax.shard_map(device_step, mesh=mesh, in_specs=(tok_spec, tok_spec, route_spec, route_spec, whole_spec, expert_spec, expert_spec, expert_spec), out_specs=(tok_spec, tok_spec, whole_spec, expert_spec, expert_spec, expert_spec), check_vma=False)
```

```python
import functools

import jax
import jax.numpy as jnp
from jax import lax
from jax.experimental import pallas as pl
from jax.experimental.pallas import tpu as pltpu
from jax.sharding import PartitionSpec as P

TOK_AXES = ("rep", "ep", "dp")
F32 = jnp.float32
BF16 = jnp.bfloat16
LANES = 128
SIDE = 4
WAYS = (1, -1)
BUFS = (0, 1)
LAYERS = (1, 0)
ARRAYS = range(3)
SLOTS = 8
MESH = pl.DeviceIdType.MESH
VMEM_LIMIT = 67_043_328


def dot(a, b):
    return jnp.dot(a, b, preferred_element_type=F32)


def dot_nt(a, b):
    return lax.dot_general(a, b, (((1,), (1,)), ((), ())), preferred_element_type=F32)


def dot_tn(a, b):
    return lax.dot_general(a, b, (((0,), (0,)), ((), ())), preferred_element_type=F32)


class Place:
    def __init__(self):
        self.z, self.y, dp = lax.axis_index("rep"), lax.axis_index("ep"), lax.axis_index("dp")
        self.x, self.c = dp // 2, dp % 2

    def at(self, axis, step):
        z, y, x, c = self.z, self.y, self.x, self.c
        if axis == "z":
            z = (z + step + SIDE) % SIDE
        elif axis == "y":
            y = (y + step + SIDE) % SIDE
        elif axis == "x":
            x = (x + step + SIDE) % SIDE
        else:
            c = 1 - c
        return (z, y, x * 2 + c)


class Copies:
    def __init__(self, place, send, recv):
        self.place, self.send, self.recv, self.made, self.number, self.count = place, send, recv, {}, {}, 0

    def add(self, key, src, dst, axis, step, like=None):
        if like is None:
            n, self.count = self.count, self.count + 1
        else:
            n = self.number[like]
        self.number[key] = n
        self.made[key] = pltpu.make_async_remote_copy(src_ref=src, dst_ref=dst, send_sem=self.send.at[n], recv_sem=self.recv.at[n], device_id=self.place.at(axis, step), device_id_type=MESH)

    def start(self, *keys):
        for key in keys:
            self.made[key].start()

    def arrive(self, *keys):
        for key in keys:
            self.made[key].wait_recv()

    def sent(self, *keys):
        for key in keys:
            self.made[key].wait_send()


def greet(place):
    barrier = pltpu.get_barrier_semaphore()
    peers = [(axis, step) for axis in "xyz" for step in range(1, SIDE)] + [("c", 0)]
    for axis, step in peers:
        pl.semaphore_signal(barrier, inc=1, device_id=place.at(axis, step), device_id_type=MESH)
    pl.semaphore_wait(barrier, len(peers))


class Gather:
    SECOND = {int(slot): int(second) for slot, second in ("20", "30", "41", "51", "60", "71")}
    AHEAD = {"x": {2: 6, 4: 7}, "z": {3: 6, 5: 7}}

    def __init__(self, layer, copies, place, own, whole):
        self.layer, self.copies, self.place, self.own, self.whole = layer, copies, place, own, whole
        rows, ff = own[0].shape[2], own[2].shape[2]
        half = ff // 2
        self.cut = {"x": ((0, 0, rows // SIDE), (2, 0, half // SIDE)), "z": ((1, 0, rows // SIDE), (2, half, half // SIDE))}
        mine = {"x": place.x, "z": place.z}
        for color in mine:
            back = {after: before for before, after in self.AHEAD[color].items()}
            for part in BUFS:
                for slot, second in self.SECOND.items():
                    way = WAYS[back.get(slot, slot) % 2]
                    self._add(("y", slot, part), color, part, back.get(slot), second, slot, mine[color], None, "y", way)
                    for step in WAYS:
                        behind = (mine[color] - step + SIDE) % SIDE
                        self._add(("near", slot, part, step), color, part, slot, None, slot, mine[color], None, color, step)
                        self._add(("far", slot, part, step), color, part, slot, None, slot, behind, (1 - step) // 2, color, step)
            up = whole[self.cut[color][0][0]]
            down = pl.ds(self.cut[color][1][1], half)
            for slot in self.SECOND:
                for n, view in enumerate((up.at[layer, slot], whole[2].at[layer, slot, down])):
                    self._put(("pass", slot, n), color, view, view, "c", 0)

    def _view(self, refs, index, color, part, quarter, half):
        array, base, size = self.cut[color][part]
        start = base + quarter * size
        if half is not None:
            size = size // 2
            start = start + half * size
        return refs[array].at[self.layer, index, pl.ds(pl.multiple_of(start, 16), size)]

    def _add(self, key, color, part, src_slot, second, dst_slot, quarter, half, axis, step):
        src = self._view(self.own, second, color, part, quarter, half) if src_slot is None else self._view(self.whole, src_slot, color, part, quarter, half)
        self._put(key, color, src, self._view(self.whole, dst_slot, color, part, quarter, half), axis, step)

    def _put(self, key, color, src, dst, axis, step):
        self.copies.add((self.layer, color) + key, src, dst, axis, step, None if color == "x" else (self.layer, "x") + key)

    def _stage(self, act):
        for core, color in enumerate("xz"):
            pl.when(self.place.c == core)(lambda: act(color))

    def _start(self, color, *key):
        self.copies.start((self.layer, color) + key)

    def _arrive(self, color, *key):
        self.copies.arrive((self.layer, color) + key)

    def begin(self):
        def act(color):
            for slot in (2, 3, 4, 5):
                for part in BUFS:
                    self._start(color, "y", slot, part)

        self._stage(act)

    def spread(self, slot):
        def act(color):
            for part in BUFS:
                self._arrive(color, "y", slot, part)
                for step in WAYS:
                    self._start(color, "near", slot, part, step)
            if slot in self.AHEAD[color]:
                for part in BUFS:
                    self._start(color, "y", self.AHEAD[color][slot], part)

        return lambda: self._stage(act)

    def onward(self, slot):
        def act(color):
            for part in BUFS:
                for step in WAYS:
                    self._arrive(color, "near", slot, part, step)
                    self._start(color, "far", slot, part, step)

        return lambda: self._stage(act)

    def complete(self, slot):
        def act(color):
            for part in BUFS:
                for step in WAYS:
                    self._arrive(color, "far", slot, part, step)
            for n in BUFS:
                self._start(color, "pass", slot, n)

        return lambda: self._stage(act)

    def passed(self, slot):
        def act(color):
            for n in BUFS:
                self._arrive("zx"["xz".index(color)], "pass", slot, n)

        return lambda: self._stage(act)

    def drain(self):
        self._stage(lambda color: self.copies.sent(*[key for key in self.copies.made if key[:2] == (self.layer, color)]))


GATHER_COPIES = 144


def route(ids_ref, gate_ref, rows_ref, columns_ref, place):
    layers, _, tokens = ids_ref.shape
    below = lax.broadcasted_iota(jnp.int32, (tokens, tokens), 0) < lax.broadcasted_iota(jnp.int32, (tokens, tokens), 1)
    below = jnp.where(below, 1.0, 0.0).astype(BF16)
    lead = lax.broadcasted_iota(jnp.int32, (2 * SLOTS, tokens), 0)
    for layer in range(layers):
        ids, gates = ids_ref[layer], gate_ref[layer]
        off = ((ids >> 1) - place.y) & (SIDE - 1)
        odd = ids & 1
        slot = jnp.where(off == 0, odd, jnp.where(off == SIDE - 1, 2 + 2 * odd, jnp.where(off == 1, 3 + 2 * odd, 6 + odd)))
        hits = [slot[n : n + 1] == lead for n in BUFS]
        hit = hits[0] | hits[1]
        weight = jnp.where(hits[0], gates[0:1], 0.0) + jnp.where(hits[1], gates[1:2], 0.0)
        rank = jnp.where(hit, dot(jnp.where(hit, 1.0, 0.0).astype(BF16), below), -1.0)
        rows_ref[layer] = rank[:SLOTS].astype(jnp.int32)
        columns_ref[layer] = jnp.transpose(jnp.concatenate([rank[:SLOTS], weight[:SLOTS], jnp.zeros((LANES - 2 * SLOTS, tokens), F32)], axis=0))


def one_hot(rows_ref, layer, slot, cap):
    place = lax.broadcasted_iota(jnp.int32, (cap, rows_ref.shape[2]), 0)
    return jnp.where(rows_ref[layer, pl.ds(slot, 1), :] == place, 1.0, 0.0).astype(BF16)


def column(columns_ref, layer, index):
    lane = lax.broadcasted_iota(jnp.int32, columns_ref.shape[1:], 1)
    return jnp.sum(jnp.where(lane == index, columns_ref[layer], 0.0), axis=1, keepdims=True)


def one_hot_t(columns_ref, layer, slot, cap):
    place = lax.broadcasted_iota(jnp.int32, (columns_ref.shape[1], cap), 1)
    return jnp.where(column(columns_ref, layer, slot).astype(jnp.int32) == place, 1.0, 0.0).astype(BF16)


def add_to(dst, src):
    dst[...] = (dst[...].astype(F32) + src[...].astype(F32)).astype(BF16)


def cut(rows, half):
    first = (rows // 2 + 15) // 16 * 16
    return (half * first, first + half * (rows - 2 * first))


class RingSum:
    def __init__(self, copies, name, axis, block, first, second):
        self.copies, self.block, self.second = copies, block, second
        self.first = [first.at[half, pl.ds(0, block(2, half).shape[0])] for half in BUFS]
        self.early, self.later = ([(name, when, step) for step in WAYS] for when in ("early", "later"))
        for half, step in enumerate(WAYS):
            copies.add(self.early[half], block(2, half), self.first[half], axis, step)
            copies.add(self.later[half], block(step, None), second.at[half], axis, step)

    def start(self):
        self.copies.start(*self.early)

    def onward(self):
        self.copies.arrive(*self.early)
        for half in BUFS:
            add_to(self.block(WAYS[half], half), self.first[half])
            self.copies.start(self.later[half])
        self.copies.sent(*self.early)

    def finish(self, out):
        self.copies.arrive(*self.later)
        out[...] = (self.block(0, None)[...].astype(F32) + self.second[0].astype(F32) + self.second[1].astype(F32)).astype(BF16)
        self.copies.sent(*self.later)


class RingSpread:
    def __init__(self, copies, name, axis, me, block, source=None, like=None):
        self.copies = copies
        self.near, self.far = ([(name, when, step) for step in WAYS] for when in ("near", "far"))
        for half, step in enumerate(WAYS):
            behind = (me - step + SIDE) % SIDE
            near, far = (None, None) if like is None else (like.near[half], like.far[half])
            copies.add(self.near[half], block(me, None) if source is None else source, block(me, None), axis, step, near)
            copies.add(self.far[half], block(behind, half), block(behind, half), axis, step, far)

    def start(self):
        self.copies.start(*self.near)

    def onward(self):
        for near, far in zip(self.near, self.far):
            self.copies.arrive(near)
            self.copies.start(far)

    def finish(self):
        self.copies.arrive(*self.far)
        self.copies.sent(*self.near, *self.far)


class Direct:
    def __init__(self, copies, name, axis, source, target):
        self.copies, self.keys = copies, [(name, step) for step in range(1, SIDE)]
        for name, step in self.keys:
            copies.add((name, step), source(step), target(step), axis, step)

    def start(self):
        self.copies.start(*self.keys)

    def finish(self):
        self.copies.arrive(*self.keys)
        self.copies.sent(*self.keys)


def slices(ref, lead, base, size):
    def block(index, half):
        start, rows = base + index * size, size
        if half is not None:
            skip, rows = cut(size, half)
            start = start + skip
        return ref.at[(*lead, pl.ds(pl.multiple_of(start, 16), rows))]

    return block


def slabs(ref):
    def block(index, half):
        if half is None:
            return ref.at[index]
        return ref.at[index, pl.ds(*cut(ref.shape[1], half))]

    return block


def total(ref):
    return (ref[0].astype(F32) + ref[1].astype(F32) + ref[2].astype(F32) + ref[3].astype(F32)).astype(BF16)


OWN_STEPS = {2: 0, 4: 1, 5: 2, 7: 3}
BACK_SLOTS = [int(slot) for slot in "75643210" + "63725401"]
REDUCE_COPIES = 120
WEIGHTS1, INPUTS1, WEIGHTS0, INPUTS0, STEPS = (n * SLOTS for n in range(2, 7))


def kernel(cap, x0_ref, dy_ref, ids_ref, gate_ref, wd_ref, o1_ref, o3_ref, o2_ref, y_ref, dx_ref, gdense_ref, g1_ref, g3_ref, g2_ref, h1_ref, h3_ref, h2_ref, kz_ref, ka_ref, kb_ref, kda_ref, kdb_ref, acc_ref, cur_ref, x1_ref, hold_ref, gd_ref, rows_ref, columns_ref, w1_ref, w3_ref, w2_ref, z_ref, a_ref, b_ref, m1_ref, m3_ref, m2_ref, d1_ref, d3_ref, d2_ref, s1_ref, s3_ref, s2_ref, r11_ref, r12_ref, r31_ref, r32_ref, t1_ref, t3_ref, y11_ref, y12_ref, y31_ref, y32_ref, y21_ref, y22_ref, u1_ref, u2_ref, l1_ref, l2_ref, c1_ref, c3_ref, cu_ref, cl_ref, f1_ref, f3_ref, fu_ref, fl_ref, dp_ref, dr_ref, ds_ref, e_ref, dcx_ref, dcz_ref, dcy_ref, de_ref, put_sem, load_sem, keep_sem, save_sem, gsend_sem, grecv_sem, send_sem, recv_sem, credit):
    s = pl.program_id(0)
    place = Place()
    gathers = Copies(place, gsend_sem, grecv_sem)
    copies = Copies(place, send_sem, recv_sem)
    given, whole, bufs = (o1_ref, o3_ref, o2_ref), (h1_ref, h3_ref, h2_ref), (w1_ref, w3_ref, w2_ref)
    kept, acts = (kz_ref, ka_ref, kb_ref), (z_ref, a_ref, b_ref)
    deferred = (kda_ref, kdb_ref)
    g0, g1 = (Gather(l, gathers, place, given, whole) for l in BUFS)
    rows, ff = s1_ref.shape[1], s2_ref.shape[1]
    quarter, part = rows // SIDE, ff // 2 // SIDE
    half_d = rows // 2

    stage, mate, mine_of = (m1_ref, m3_ref, m2_ref), (d1_ref, d3_ref, d2_ref), (s1_ref, s3_ref, s2_ref)
    for buf in BUFS:
        for n in ARRAYS:
            copies.add(("pair", buf, n), stage[n].at[buf], mate[n].at[buf], "c", 0)

    def ring_blocks(ref, q, me, base, size):
        block = slices(ref, (q,), base, size)
        return lambda offset, half: block((me + offset + SIDE) % SIDE, half)

    def group_blocks(ref):
        block = slabs(ref)
        return lambda offset, half: block({2: 0, 1: 1, -1: 2, 0: 3}[offset], half)

    first = {
        "x": [RingSum(copies, ("x", q), "x", ring_blocks(s1_ref, q, place.x, 0, quarter), r11_ref.at[q], r12_ref.at[q]) for q in range(SIDE)],
        "z": [RingSum(copies, ("z", q), "z", ring_blocks(s3_ref, q, place.z, 0, quarter), r31_ref.at[q], r32_ref.at[q]) for q in range(SIDE)],
    }
    mid = {"x": t1_ref, "z": t3_ref}
    on_y = {
        "x": RingSum(copies, "yx", "y", group_blocks(t1_ref), y11_ref, y12_ref),
        "z": RingSum(copies, "yz", "y", group_blocks(t3_ref), y31_ref, y32_ref),
        "w": RingSum(copies, "yw", "y", group_blocks(s2_ref), y21_ref, y22_ref),
    }
    inner = {
        "u": RingSum(copies, "u", "x", ring_blocks(s2_ref, 3, place.x, 0, part), u1_ref, u2_ref),
        "l": RingSum(copies, "l", "z", ring_blocks(s2_ref, 3, place.z, ff // 2, part), l1_ref, l2_ref),
    }
    ring_of = {"x": ("x", place.x), "u": ("x", place.x), "z": ("z", place.z), "l": ("z", place.z)}
    other_of = {"x": ("z", place.z), "u": ("z", place.z), "z": ("x", place.x), "l": ("x", place.x)}
    cross_ref = {"x": c1_ref, "z": c3_ref, "u": cu_ref, "l": cl_ref}
    done_ref = {"x": f1_ref, "z": f3_ref, "u": fu_ref, "l": fl_ref}
    out_of = {"x": (g1_ref, 0, quarter), "z": (g3_ref, 0, quarter), "u": (g2_ref, 0, part), "l": (g2_ref, ff // 2, part)}
    cross, final, puts = {}, {}, {}
    for i, k in enumerate(out_of):
        cross[k] = RingSpread(copies, ("cross", k), *other_of[k], slabs(cross_ref[k]))
        ref, base, size = out_of[k]
        for late in LAYERS:
            block = slices(ref, (late, place.c), base, size)
            final[k, late] = RingSpread(copies, ("final", k, late), *ring_of[k], block, source=done_ref[k], like=final.get((k, 1)))
            me = ring_of[k][1]
            puts[k, late] = pltpu.make_async_copy(done_ref[k], block(me, None), put_sem.at[i])
            for offset in (0, *WAYS, 2):
                quarter_at = block((me + offset) % SIDE if offset >= 0 else (me + SIDE - 1) % SIDE, None)
                copies.add(("pass", k, offset, late), quarter_at if offset else done_ref[k], quarter_at, "c", 0, None if late else ("pass", k, offset, 1))
    mine, theirs = (pl.ds(pl.multiple_of(c * half_d, 16), half_d) for c in (place.c, 1 - place.c))
    copies.add("dense pair", dp_ref.at[theirs], dr_ref, "c", 0)
    copies.add("dense pass", dcy_ref, de_ref, "c", 0)
    piece = half_d // SIDE
    dense_block = slices(ds_ref, (), 0, piece)
    dense_sums = Direct(copies, "dense sums", "y", lambda step: dense_block((place.y + step) % SIDE, None), lambda step: e_ref.at[step - 1])
    gather_block = slices(dcy_ref, (), 0, piece)(place.y, None)
    own_piece = {"x": dcx_ref.at[place.x], "z": dcz_ref.at[place.z], "y": gather_block}
    dense = {k: Direct(copies, ("dense", k), k, lambda step, k=k: own_piece[k], lambda step, k=k: own_piece[k]) for k in own_piece}

    def reduce_start(q):
        for k in ("x", "z"):
            first[k][q].start()

    def reduce_onward(q):
        for k in ("x", "z"):
            first[k][q].onward()

    def reduce_finish(q):
        for k in ("x", "z"):
            first[k][q].finish(mid[k].at[q])

    def y_start():
        for k in ("x", "z"):
            on_y[k].start()

    def y_onward():
        for k in ("x", "z"):
            on_y[k].onward()

    def y_finish():
        for k in ("x", "z"):
            on_y[k].finish(cross_ref[k].at[other_of[k][1]])
            cross[k].start()

    def w_finish():
        on_y["w"].finish(s2_ref.at[3])
        for k in ("u", "l"):
            inner[k].start()

    def inner_onward():
        for k in ("u", "l"):
            inner[k].onward()

    def inner_finish():
        for k in ("u", "l"):
            inner[k].finish(cross_ref[k].at[other_of[k][1]])
            cross[k].start()

    def cross_onward(*keys):
        for k in keys:
            cross[k].onward()

    def cross_finish(late, *keys):
        for k in keys:
            cross[k].finish()
            done_ref[k][...] = total(cross_ref[k])
            puts[k, late].start()
            final[k, late].start()
            copies.start(("pass", k, 0, late))

    def final_onward(late, *keys):
        for k in keys:
            final[k, late].onward()
            copies.start(*[("pass", k, way, late) for way in WAYS])

    def final_finish(late, *keys):
        for k in keys:
            final[k, late].finish()
            puts[k, late].wait()
            copies.start(("pass", k, 2, late))

    def pass_finish(late):
        keys = [("pass", k, offset, late) for k in out_of for offset in (0, *WAYS, 2)]
        copies.arrive(*keys)
        copies.sent(*keys)

    def dense_sum():
        copies.arrive("dense pair")
        ds_ref[...] = (dp_ref[mine].astype(F32) + dr_ref[...].astype(F32)).astype(BF16)
        copies.sent("dense pair")
        dense_sums.start()

    def dense_to_x():
        dense_sums.finish()
        mine = dense_block(place.y, None)[...].astype(F32)
        own_piece["x"][...] = (mine + e_ref[0].astype(F32) + e_ref[1].astype(F32) + e_ref[2].astype(F32)).astype(BF16)
        dense["x"].start()

    def dense_next(k, ref, follow):
        dense[k].finish()
        own_piece[follow][...] = total(ref)
        dense[follow].start()

    def dense_to_z():
        dense_next("x", dcx_ref, "z")

    def dense_to_y():
        dense_next("z", dcz_ref, "y")

    def dense_out(late):
        return pltpu.make_async_copy(gd_ref, gdense_ref.at[late], keep_sem.at[0, 1])

    def dense_pass(late):
        dense["y"].finish()
        if late == 0:
            dense_out(1).wait()
        gd_ref[mine] = dcy_ref[...]
        copies.start("dense pass")

    def dense_finish(late):
        copies.arrive("dense pass")
        gd_ref[theirs] = de_ref[...]
        copies.sent("dense pass")
        dense_out(late).start()

    def copy(src, dst, sem):
        return pltpu.make_async_copy(src, dst, sem)

    def weights(layer, slot, arrays, buf, is_given=False):
        for n in arrays:
            src = given[n].at[layer, slot] if is_given else whole[n].at[layer, slot]
            yield copy(src, bufs[n].at[buf], load_sem.at[buf, n])

    def saved(layer, slot, buf):
        for n, (src, dst) in enumerate(zip(kept, acts)):
            yield copy(src.at[layer, slot], dst.at[buf], load_sem.at[buf, 3 + n])

    def back_slot(step):
        at, size = place.c * SLOTS + step % SLOTS, len(BACK_SLOTS)
        return BACK_SLOTS[0] + sum((BACK_SLOTS[n] - BACK_SLOTS[n - 1]) * ((at + size - n) // size) for n in range(1, size))

    def weights_loads(step):
        layer, slot, buf = layer_of(step), back_slot(step), (step + 1) % 2
        return [*weights(layer, slot, [2], buf), *saved(layer, slot, buf)]

    def inputs_loads(step):
        layer, slot, buf = layer_of(step), back_slot(step), (step + 1) % 2
        return [*weights(layer, slot, BUFS, buf)] + [copy(deferred[n].at[step % SLOTS], acts[n + 1].at[buf], load_sem.at[buf, 4 + n]) for n in BUFS]

    def load(step):
        slot = step % SLOTS
        for is_given in (True, False):
            pl.when((slot < 2) == is_given)(lambda: start(weights(step // SLOTS, slot, ARRAYS, step % 2, is_given)))

    def layer_of(step):
        return 1 - (step - WEIGHTS1) // (2 * SLOTS)

    def keeps(step):
        return [copy(bufs[n].at[step % 2], whole[n].at[step // SLOTS, step % SLOTS], keep_sem.at[step % 2, n]) for n in ARRAYS]

    def saves(step):
        return [copy(src.at[step % 2], dst.at[step // SLOTS, step % SLOTS], save_sem.at[step % 2, n]) for n, (src, dst) in enumerate(zip(acts, kept))]

    def defers(step):
        return [copy(acts[n + 1].at[2], deferred[n].at[step % SLOTS], save_sem.at[0, n]) for n in BUFS]

    def wait(items):
        for item in items:
            item.wait()

    def start(items):
        for item in items:
            item.start()

    def ending():
        dense_finish(1)
        copies.start("dense pair")
        y_finish()
        inner_finish()
        dense_sum()
        dense_to_x()
        cross_onward("x", "z")
        pass_finish(1)
        pl.semaphore_signal(credit.at[2], inc=1, device_id=place.at("c", 0), device_id_type=MESH)
        cross_onward("u", "l")
        dense_to_z()
        pl.semaphore_wait(credit.at[2], 1)
        cross_finish(0, "x", "z")
        cross_finish(0, "u", "l")
        dense_to_y()
        dense_pass(0)
        final_onward(0, "x", "z")
        dense_finish(0)
        final_onward(0, "u", "l")
        final_finish(0, "x", "z")
        final_finish(0, "u", "l")
        pass_finish(0)

    before, middle, after = {}, {}, {}

    def plan(table, first, *stages):
        for n, stage in enumerate(stages):
            table.setdefault(first + n, []).extend(stage)

    on, done = lambda q: lambda: reduce_onward(q), lambda q: lambda: reduce_finish(q)
    now = lambda: load(s)
    plan(before, 2, [*(g0.spread(n) for n in (2, 3)), g0.onward(2), g0.spread(4), g0.onward(3), g0.spread(5), g0.complete(2), g0.onward(4), g0.passed(2), now])
    plan(before, 3, [g1.begin, g0.spread(6), g0.complete(3), g0.onward(5), g0.spread(7), g0.passed(3), now], [g0.complete(4), g0.onward(6), g0.passed(4), now])
    plan(before, 5, [g0.complete(5), g0.onward(7), g0.passed(5), now], [g0.complete(6), g1.spread(2), g1.spread(3), g0.passed(6), now], [g0.complete(7), g0.passed(7), now])
    plan(before, SLOTS, [g1.onward(2), g1.spread(4)], [g1.onward(3), g1.spread(5), g1.complete(2)], [g1.onward(4), g1.spread(6), g1.passed(2), now])
    plan(before, SLOTS + 3, [g1.complete(3), g1.onward(5), g1.spread(7), g1.passed(3), now], [g1.complete(4), g1.passed(4), now], [g1.complete(5), g1.onward(6), g1.passed(5), now])
    plan(before, SLOTS + 6, [g1.complete(6), g1.onward(7), g1.passed(6), now], [g1.complete(7), g1.passed(7), now])
    late = ("x", "z", "u", "l")
    plan(before, INPUTS1 + 6, [w_finish], [], [inner_onward])
    plan(before, WEIGHTS0, [lambda: copies.start("dense pair")], [], [inner_finish], [lambda: cross_onward("x", "z"), dense_to_x], [lambda: cross_onward("u", "l")], [dense_to_z])
    plan(middle, WEIGHTS0, [dense_sum, y_finish], [], [], [], [], [], [], [dense_to_y])
    plan(before, INPUTS0, [lambda: cross_finish(1, *late)], [], [], [], [], [lambda: final_onward(1, *late)], [], [lambda: dense_pass(1), lambda: final_finish(1, *late)])
    plan(before, INPUTS0 + 5, [w_finish], [], [inner_onward])
    for base in (WEIGHTS1, WEIGHTS0):
        plan(before, base + 3, [on_y["w"].start], [], [], [done(0), y_start, on_y["w"].onward])
        plan(middle, base + 4, [on(0)], [], [on(1)], [on(2)])
        plan(before, base + SLOTS, [], [done(1)], [done(2), y_onward], [on(3)], [], [], [done(3)])
        for step, q in OWN_STEPS.items():
            plan(after, base + step, [lambda q=q: reduce_start(q)])

    def hooks(table, *phases):
        for phase in phases:
            mine = {step: stages for step, stages in sorted(table.items()) if phase <= step < phase + SLOTS}
            if mine:

                @pl.when(s // SLOTS == phase // SLOTS)
                def _(mine=mine):
                    for step, stages in mine.items():

                        @pl.when(s == step)
                        def _(stages=stages):
                            for stage in stages:
                                stage()

    phase, t = s // SLOTS, s % SLOTS
    forth, back = s % 2, (s + 1) % 2

    def bring(ref, hold):
        return copy(ref, hold, keep_sem.at[1, 0])

    @pl.when(s == 0)
    def _():
        bring(x0_ref, hold_ref).start()
        load(0)
        greet(place)
        g0.begin()
        load(1)
        route(ids_ref, gate_ref, rows_ref, columns_ref, place)
        bring(x0_ref, hold_ref).wait()

    def enter(x):
        cur_ref[...] = (x.astype(F32) + dot(x, wd_ref[phase])).astype(BF16)
        acc_ref[...] = jnp.zeros_like(acc_ref)

    def leave(out_ref):
        out_ref[...] = (cur_ref[...].astype(F32) + acc_ref[...]).astype(BF16)

    @pl.when(s < WEIGHTS1)
    def _():
        hooks(before, 0, SLOTS)
        pl.when(s > 1)(lambda: wait(saves(s - 2)))
        pl.when((t == 1) | (t == 2))(lambda: wait(keeps(s - 1)))
        pl.when((s == SLOTS - 1) | (s == SLOTS))(lambda: load(s + 1))

        @pl.when(t < 2)
        def _():
            pl.when(s == 0)(lambda: enter(hold_ref[...]))
            pl.when(s == SLOTS)(lambda: enter(x1_ref[...]))

        layer, slot = phase, t
        come = list(weights(layer, slot, ARRAYS, forth))

        def forward_step(is_ready):
            if is_ready:
                wait(come)
            z = dot(one_hot(rows_ref, layer, slot, cap), cur_ref[...]).astype(BF16)
            z_ref[forth] = z
            if not is_ready:
                wait(come)
            a = dot(z, w1_ref[forth]).astype(BF16)
            b = dot(z, w3_ref[forth]).astype(BF16)
            a_ref[forth] = a
            b_ref[forth] = b
            a = a.astype(F32)
            h = (a * jax.nn.sigmoid(a) * b.astype(F32)).astype(BF16)
            o = dot(h, w2_ref[forth]).astype(BF16)
            acc_ref[...] += column(columns_ref, layer, SLOTS + slot) * dot(one_hot_t(columns_ref, layer, slot, cap), o)

        is_late = t > 1
        pl.when(is_late)(lambda: forward_step(False))
        pl.when(jnp.logical_not(is_late))(lambda: forward_step(True))
        pl.when(t < 2)(lambda: start(keeps(s)))
        start(saves(s))
        @pl.when(t == SLOTS - 1)
        def _():
            pl.when(s == SLOTS - 1)(lambda: leave(x1_ref))
            pl.when(s == WEIGHTS1 - 1)(lambda: leave(hold_ref))

    @pl.when((phase == WEIGHTS1 // SLOTS) | (phase == WEIGHTS0 // SLOTS))
    def _():
        layer, slot = layer_of(s), back_slot(s)
        hooks(before, WEIGHTS1, WEIGHTS0)

        @pl.when(s == WEIGHTS1)
        def _():
            moved = copy(hold_ref, y_ref, keep_sem.at[0, 0])
            moved.start()
            bring(dy_ref, cur_ref).start()
            wait(saves(s - 2))
            wait(saves(s - 1))
            start(weights_loads(s))
            g0.drain()
            g1.drain()
            bring(dy_ref, cur_ref).wait()
            moved.wait()
            acc_ref[...] = cur_ref[...].astype(F32)

        wait(weights_loads(s))
        pl.when(t > 0)(lambda: wait(defers(s - 1)))
        pl.when(t < SLOTS - 1)(lambda: start(weights_loads(s + 1)))
        pl.when(t == SLOTS - 1)(lambda: start(inputs_loads(s + 1)))

        grad_gated = (column(columns_ref, layer, SLOTS + slot) * cur_ref[...].astype(F32)).astype(BF16)
        do = dot(one_hot(rows_ref, layer, slot, cap), grad_gated).astype(BF16)
        dh = dot_nt(do, w2_ref[back])
        a = a_ref[back].astype(F32)
        b = b_ref[back].astype(F32)
        sig = jax.nn.sigmoid(a)
        act = a * sig
        h = (act * b).astype(BF16)
        db = (dh * act).astype(BF16)
        da = (dh * b * (sig + act * (1.0 - sig))).astype(BF16)
        a_ref[2] = da
        b_ref[2] = db
        z = z_ref[back]
        start(defers(s))
        hooks(middle, WEIGHTS1, WEIGHTS0)

        def weight_grads():
            return dot_tn(z, da), dot_tn(z, db), dot_tn(h, do)

        is_own = functools.reduce(jnp.logical_or, [t == step for step in OWN_STEPS])
        group = t // 4 + t // 5 + t // 7
        into = (t + t // 3 + t // 6) % 2
        turn = t + (1 - layer) * SLOTS

        @pl.when(jnp.logical_not(is_own))
        def _():
            for buf in BUFS:
                pl.when((turn >= 3) & (into == buf))(lambda: copies.sent(*[("pair", buf, n) for n in ARRAYS]))

            for ref, grad in zip(stage, weight_grads()):
                ref[into] = grad.astype(BF16)

            pl.when(turn >= 3)(lambda: pl.semaphore_wait(credit.at[into], 1))
            for buf in BUFS:
                pl.when(into == buf)(lambda: copies.start(*[("pair", buf, n) for n in ARRAYS]))

        @pl.when(is_own)
        def _():
            for buf in BUFS:
                pl.when(group % 2 == buf)(lambda: copies.arrive(*[("pair", buf, n) for n in ARRAYS]))

            for ref, add, grad in zip(mine_of, mate, weight_grads()):
                ref[group] = (grad + add[group % 2].astype(F32)).astype(BF16)

            @pl.when(turn < 2 * SLOTS - 3)
            def _():
                pl.semaphore_signal(credit.at[group % 2], inc=1, device_id=place.at("c", 0), device_id_type=MESH)

            hooks(after, WEIGHTS1, WEIGHTS0)

    def leave_back(layer, x, out_ref):
        grad = acc_ref[...]
        grad_b = grad.astype(BF16)
        dp_ref[...] = dot_tn(x, grad_b).astype(BF16)
        out_ref[...] = (grad + dot_nt(grad_b, wd_ref[layer])).astype(BF16)

    @pl.when((phase == INPUTS1 // SLOTS) | (phase == INPUTS0 // SLOTS))
    def _():
        layer, slot = layer_of(s), back_slot(s)
        hooks(before, INPUTS1, INPUTS0)
        wait(inputs_loads(s))
        pl.when(t == 0)(lambda: wait(defers(s - 1)))
        pl.when(t < SLOTS - 1)(lambda: start(inputs_loads(s + 1)))
        pl.when(s == WEIGHTS0 - 1)(lambda: start(weights_loads(s + 1)))
        dz = (dot_nt(a_ref[back], w1_ref[back]) + dot_nt(b_ref[back], w3_ref[back])).astype(BF16)
        acc_ref[...] += dot(one_hot_t(columns_ref, layer, slot, cap), dz)

        @pl.when(s == WEIGHTS0 - 1)
        def _():
            leave_back(1, x1_ref[...], cur_ref)
            acc_ref[...] = cur_ref[...].astype(F32)
            bring(x0_ref, x1_ref).start()
            bring(x0_ref, x1_ref).wait()

        @pl.when(s == STEPS - 1)
        def _():
            leave_back(0, x1_ref[...], hold_ref)
            moved = copy(hold_ref, dx_ref, keep_sem.at[0, 0])
            moved.start()
            ending()
            copies.sent(*[("pair", buf, n) for buf in BUFS for n in ARRAYS])
            moved.wait()
            dense_out(0).wait()


def step(cap, x0, dy, ids, gates, wd, w1, w3, w2):
    tokens, width = dy.shape
    layers, local, _, ff = w1.shape
    quarter, part, piece = width // SIDE, ff // 2 // SIDE, width // 2 // SIDE
    hbm = pl.BlockSpec(memory_space=pl.ANY)

    def fixed(shape):
        return pl.BlockSpec(shape, lambda s: (0,) * len(shape), pipeline_mode=pl.Buffered(1))

    def buf(*shape):
        return pltpu.VMEM(shape, BF16)

    def dma(*shape):
        return pltpu.SemaphoreType.DMA(shape)

    shape = jax.ShapeDtypeStruct
    ups, downs = [(width, ff), (width, ff), (ff, width)], [(quarter, ff), (part, width)]
    acts = [(cap, width), (cap, ff), (cap, ff)]
    scratch = [pltpu.VMEM((tokens, width), F32)] + [buf(tokens, width)] * 3 + [buf(width, width), pltpu.VMEM((layers, SLOTS, tokens), jnp.int32), pltpu.VMEM((layers, tokens, LANES), F32)]
    scratch += [buf(2, *u) for u in ups] + [buf(n, *a) for n, a in zip((2, 3, 3), acts)]
    scratch += [buf(2, *u) for u in ups] * 2 + [buf(SIDE, *u) for u in ups]
    scratch += [buf(SIDE, 2, quarter // 2, ff), buf(SIDE, 2, quarter, ff)] * 2
    scratch += [buf(SIDE, quarter, ff)] * 2
    scratch += [buf(2, quarter // 2, ff), buf(2, quarter, ff)] * 2 + [buf(2, ff // 2, width), buf(2, ff, width)]
    scratch += [buf(2, part // 2, width), buf(2, part, width)] * 2
    scratch += [buf(SIDE, quarter, ff)] * 2 + [buf(SIDE, part, width)] * 2
    scratch += [buf(quarter, ff)] * 2 + [buf(part, width)] * 2
    scratch += [buf(width, width)] + [buf(width // 2, width)] * 2 + [buf(SIDE - 1, piece, width)] + [buf(SIDE, piece, width)] * 2 + [buf(width // 2, width)] * 2
    scratch += [dma(4), dma(2, 6), dma(2, 3), dma(2, 3), dma(GATHER_COPIES), dma(GATHER_COPIES), dma(REDUCE_COPIES), dma(REDUCE_COPIES), pltpu.SemaphoreType.REGULAR((3,))]
    results = [(tokens, width), (tokens, width), (layers, width, width)]
    kept = [(layers, local, *u) for u in ups] + [(layers, SLOTS, *u) for u in ups + acts] + [(SLOTS, cap, ff)] * 2
    return pl.pallas_call(
        functools.partial(kernel, cap),
        grid=(STEPS,),
        in_specs=[hbm] * 2 + [fixed(v.shape) for v in (ids, gates, wd)] + [hbm] * 3,
        out_specs=[hbm] * len(results + kept),
        out_shape=[shape(r, BF16) for r in results + kept],
        scratch_shapes=scratch,
        compiler_params=pltpu.CompilerParams(vmem_limit_bytes=VMEM_LIMIT, collective_id=0, has_side_effects=True),
        name="step",
    )(x0, dy, ids, gates, wd, w1, w3, w2)[:6]


def take_kernel(count, *refs):
    sources, targets, holds, (come, go) = refs[:count], refs[count : 2 * count], refs[2 * count : 3 * count], refs[3 * count :]
    comes = [pltpu.make_async_copy(a, b, come.at[n]) for n, (a, b) in enumerate(zip(sources, holds))]
    goes = [pltpu.make_async_copy(a, b, go.at[n]) for n, (a, b) in enumerate(zip(holds, targets))]
    for item in comes:
        item.start()
    for first, then in zip(comes, goes):
        first.wait()
        then.start()
    for item in goes:
        item.wait()


def take(arrays):
    count = len(arrays)
    hbm = pl.BlockSpec(memory_space=pl.ANY)
    return pl.pallas_call(
        functools.partial(take_kernel, count),
        in_specs=[hbm] * count,
        out_specs=[hbm] * count,
        out_shape=[jax.ShapeDtypeStruct(a.shape, a.dtype) for a in arrays],
        scratch_shapes=[pltpu.VMEM(a.shape, a.dtype) for a in arrays] + [pltpu.SemaphoreType.DMA((count,))] * 2,
        compiler_params=pltpu.CompilerParams(vmem_limit_bytes=VMEM_LIMIT),
        name="take",
    )(*arrays)


def solution(mesh):
    tok_spec = P(TOK_AXES, None)
    route_spec = P(None, TOK_AXES, None)
    expert_spec = P(None, "ep", None, None)
    whole_spec = P(None, None, None)

    def device_step(tok_in, tok_grad, route_ids, gate_vals, *weights):
        tokens, top_k = route_ids.shape[1:]
        return tuple(take(step(2 * tokens * top_k // SLOTS, tok_in, tok_grad, jnp.swapaxes(route_ids, 1, 2), jnp.swapaxes(gate_vals, 1, 2), *weights)))

    return jax.shard_map(device_step, mesh=mesh, in_specs=(tok_spec, tok_spec, route_spec, route_spec, whole_spec, expert_spec, expert_spec, expert_spec), out_specs=(tok_spec, tok_spec, whole_spec, expert_spec, expert_spec, expert_spec), check_vma=False)
```

```python
import functools

import jax
import jax.numpy as jnp
from jax import lax
from jax.experimental import pallas as pl
from jax.experimental.pallas import tpu as pltpu
from jax.sharding import PartitionSpec as P

TOK_AXES = ("rep", "ep", "dp")
F32 = jnp.float32
BF16 = jnp.bfloat16
LANES = 128
SIDE = 4
WAYS = (1, -1)
BUFS = (0, 1)
LAYERS = (1, 0)
ARRAYS = range(3)
SLOTS = 8
MESH = pl.DeviceIdType.MESH
VMEM_LIMIT = 67_043_328


def dot(a, b):
    return jnp.dot(a, b, preferred_element_type=F32)


def dot_nt(a, b):
    return lax.dot_general(a, b, (((1,), (1,)), ((), ())), preferred_element_type=F32)


def dot_tn(a, b):
    return lax.dot_general(a, b, (((0,), (0,)), ((), ())), preferred_element_type=F32)


class Place:
    def __init__(self):
        self.z, self.y, dp = lax.axis_index("rep"), lax.axis_index("ep"), lax.axis_index("dp")
        self.x, self.c = dp // 2, dp % 2

    def at(self, axis, step):
        z, y, x, c = self.z, self.y, self.x, self.c
        if axis == "z":
            z = (z + step + SIDE) % SIDE
        elif axis == "y":
            y = (y + step + SIDE) % SIDE
        elif axis == "x":
            x = (x + step + SIDE) % SIDE
        else:
            c = 1 - c
        return (z, y, x * 2 + c)


class Copies:
    def __init__(self, place, send, recv):
        self.place, self.send, self.recv, self.made, self.number, self.count, self.over = place, send, recv, {}, {}, 0, set()

    def add(self, key, src, dst, axis, step, like=None):
        if like is None:
            n, self.count = self.count, self.count + 1
        else:
            n = self.number[like]
        self.number[key] = n
        self.made[key] = pltpu.make_async_remote_copy(src_ref=src, dst_ref=dst, send_sem=self.send.at[n], recv_sem=self.recv.at[n], device_id=self.place.at(axis, step), device_id_type=MESH)

    def start(self, *keys):
        for key in keys:
            self.made[key].start()

    def arrive(self, *keys):
        for key in keys:
            self.made[key].wait_recv()

    def sent(self, *keys):
        for key in keys:
            self.made[key].wait_send()
            self.over.add(key)

    def drain(self):
        self.sent(*[key for key in self.made if key not in self.over])


def greet(place):
    barrier = pltpu.get_barrier_semaphore()
    peers = [(axis, step) for axis in "xyz" for step in range(1, SIDE)] + [("c", 0)]
    for axis, step in peers:
        pl.semaphore_signal(barrier, inc=1, device_id=place.at(axis, step), device_id_type=MESH)
    pl.semaphore_wait(barrier, len(peers))


class Gather:
    PASS = {2: 4, 3: 6, 5: 7}

    def __init__(self, layer, copies, place, own, whole):
        self.layer, self.copies, self.place, self.own, self.whole = layer, copies, place, own, whole
        rows, ff = own[0].shape[2], own[2].shape[2]
        self.cut = {"x": ((0, 0, rows // SIDE), (2, 0, ff // 2 // SIDE)), "z": ((1, 0, rows // SIDE), (2, ff // 2, ff // 2 // SIDE))}
        mine = {"x": place.x, "z": place.z}
        for color in ("x", "z"):
            for part in BUFS:
                self._add(("y", 2, color, part), color, part, None, 2, mine[color], None, "y", 1)
                self._add(("y", 3, color, part), color, part, None, 3, mine[color], None, "y", -1)
                if color == "x":
                    self._add(("y", 5, color, part), color, part, 2, 5, mine[color], None, "y", 1)
                else:
                    self._add(("y", 5, color, part), color, part, 3, 5, mine[color], None, "y", -1)
                for slot in (2, 3, 5):
                    for step in WAYS:
                        self._add(("near", slot, color, part, step), color, part, slot, slot, mine[color], None, color, step)
                        behind = (mine[color] - step + SIDE) % SIDE
                        self._add(("far", slot, color, part, step), color, part, slot, slot, behind, (1 - step) // 2, color, step)
        for slot, to in self.PASS.items():
            for array in ARRAYS:
                copies.add((layer, "pass", slot, array), whole[array].at[layer, slot], whole[array].at[layer, to], "c", 0)

    def _view(self, refs, index, color, part, quarter, half):
        array, base, size = self.cut[color][part]
        start = base + quarter * size
        if half is not None:
            size = size // 2
            start = start + half * size
        return refs[array].at[self.layer, index, pl.ds(pl.multiple_of(start, 16), size)]

    def _add(self, key, color, part, src_slot, dst_slot, quarter, half, axis, step):
        src = self._view(self.own, self.place.c, color, part, quarter, half) if src_slot is None else self._view(self.whole, src_slot, color, part, quarter, half)
        self.copies.add((self.layer,) + key, src, self._view(self.whole, dst_slot, color, part, quarter, half), axis, step)

    def _keys(self, *key, extra=()):
        return [(self.layer,) + key + (part,) + extra for part in BUFS]

    def lead(self):
        self.spread(2, "x")
        self.spread(3, "z")

    def lead_onward(self):
        self.onward(2, "x")
        self.onward(3, "z")

    def follow(self):
        self.spread(2, "z")
        self.spread(3, "x")

    def follow_onward(self):
        self.onward(2, "z")
        self.onward(3, "x")

    def last(self):
        self.spread(5, "x")
        self.spread(5, "z")

    def last_onward(self):
        self.onward(5, "x")
        self.onward(5, "z")

    def complete_y(self):
        self.complete(2)
        self.complete(3)

    def complete_last(self):
        self.complete(5)

    def passed_left(self):
        self.passed(2)

    def passed_right(self):
        self.passed(3)

    def passed_last(self):
        self.passed(5)

    def begin(self):
        for slot, color in ((2, "x"), (3, "z"), (2, "z"), (3, "x")):
            self.copies.start(*self._keys("y", slot, color))

    def spread(self, slot, color):
        for part in BUFS:
            self.copies.arrive((self.layer, "y", slot, color, part))
            self.copies.start(*[(self.layer, "near", slot, color, part, step) for step in WAYS])
        if (slot, color) in ((2, "x"), (3, "z")):
            self.copies.start(*self._keys("y", 5, color))

    def onward(self, slot, color):
        for part in BUFS:
            for step in WAYS:
                self.copies.arrive((self.layer, "near", slot, color, part, step))
                self.copies.start((self.layer, "far", slot, color, part, step))

    def complete(self, slot):
        for color in ("x", "z"):
            for step in WAYS:
                self.copies.arrive(*self._keys("far", slot, color, extra=(step,)))
        self.copies.start(*[(self.layer, "pass", slot, array) for array in ARRAYS])

    def passed(self, slot):
        self.copies.arrive(*[(self.layer, "pass", slot, array) for array in ARRAYS])


GATHER_COPIES = 2 * (2 * 2 * (3 + 3 * 4) + 9)


def route(ids_ref, gate_ref, rows_ref, columns_ref, place):
    layers, _, tokens = ids_ref.shape
    below = lax.broadcasted_iota(jnp.int32, (tokens, tokens), 0) < lax.broadcasted_iota(jnp.int32, (tokens, tokens), 1)
    below = jnp.where(below, 1.0, 0.0).astype(BF16)
    lead = lax.broadcasted_iota(jnp.int32, (2 * SLOTS, tokens), 0)
    for layer in range(layers):
        ids, gates = ids_ref[layer], gate_ref[layer]
        off = ((ids >> 1) - place.y) & (SIDE - 1)
        odd = (ids + place.c) & 1
        slot = jnp.where(off == 0, odd, jnp.where(off == SIDE - 1, 2 + 2 * odd, jnp.where(off == 1, 3 + 3 * odd, 5 + 2 * odd)))
        hits = [slot[n : n + 1] == lead for n in BUFS]
        hit = hits[0] | hits[1]
        weight = jnp.where(hits[0], gates[0:1], 0.0) + jnp.where(hits[1], gates[1:2], 0.0)
        rank = jnp.where(hit, dot(jnp.where(hit, 1.0, 0.0).astype(BF16), below), -1.0)
        rows_ref[layer] = rank[:SLOTS].astype(jnp.int32)
        columns_ref[layer] = jnp.transpose(jnp.concatenate([rank[:SLOTS], weight[:SLOTS], jnp.zeros((LANES - 2 * SLOTS, tokens), F32)], axis=0))


def one_hot(rows_ref, layer, slot, cap):
    place = lax.broadcasted_iota(jnp.int32, (cap, rows_ref.shape[2]), 0)
    return jnp.where(rows_ref[layer, pl.ds(slot, 1), :] == place, 1.0, 0.0).astype(BF16)


def column(columns_ref, layer, index):
    lane = lax.broadcasted_iota(jnp.int32, columns_ref.shape[1:], 1)
    return jnp.sum(jnp.where(lane == index, columns_ref[layer], 0.0), axis=1, keepdims=True)


def one_hot_t(columns_ref, layer, slot, cap):
    place = lax.broadcasted_iota(jnp.int32, (columns_ref.shape[1], cap), 1)
    return jnp.where(column(columns_ref, layer, slot).astype(jnp.int32) == place, 1.0, 0.0).astype(BF16)


def add_to(dst, src):
    dst[...] = (dst[...].astype(F32) + src[...].astype(F32)).astype(BF16)


def cut(rows, half):
    first = (rows // 2 + 15) // 16 * 16
    return (half * first, first + half * (rows - 2 * first))


class RingSum:
    def __init__(self, copies, name, axis, block, first, second):
        self.copies, self.block, self.second = copies, block, second
        self.first = [first.at[half, pl.ds(0, block(2, half).shape[0])] for half in BUFS]
        self.early, self.later = ([(name, when, step) for step in WAYS] for when in ("early", "later"))
        for half, step in enumerate(WAYS):
            copies.add(self.early[half], block(2, half), self.first[half], axis, step)
            copies.add(self.later[half], block(step, None), second.at[half], axis, step)

    def start(self):
        self.copies.start(*self.early)

    def onward(self):
        self.copies.arrive(*self.early)
        for half in BUFS:
            add_to(self.block(WAYS[half], half), self.first[half])
            self.copies.start(self.later[half])
        self.copies.sent(*self.early)

    def finish(self, out):
        self.copies.arrive(*self.later)
        out[...] = (self.block(0, None)[...].astype(F32) + self.second[0].astype(F32) + self.second[1].astype(F32)).astype(BF16)
        self.copies.sent(*self.later)


class RingSpread:
    def __init__(self, copies, name, axis, me, block, source=None, like=None):
        self.copies = copies
        self.near, self.far = ([(name, when, step) for step in WAYS] for when in ("near", "far"))
        for half, step in enumerate(WAYS):
            behind = (me - step + SIDE) % SIDE
            near, far = (None, None) if like is None else (like.near[half], like.far[half])
            copies.add(self.near[half], block(me, None) if source is None else source, block(me, None), axis, step, near)
            copies.add(self.far[half], block(behind, half), block(behind, half), axis, step, far)

    def start(self):
        self.copies.start(*self.near)

    def onward(self):
        for near, far in zip(self.near, self.far):
            self.copies.arrive(near)
            self.copies.start(far)

    def finish(self):
        self.copies.arrive(*self.far)
        self.copies.sent(*self.near, *self.far)


class Direct:
    def __init__(self, copies, name, axis, source, target):
        self.copies, self.keys = copies, [(name, step) for step in range(1, SIDE)]
        for name, step in self.keys:
            copies.add((name, step), source(step), target(step), axis, step)

    def start(self):
        self.copies.start(*self.keys)

    def finish(self):
        self.copies.arrive(*self.keys)
        self.copies.sent(*self.keys)


def slices(ref, lead, base, size):
    def block(index, half):
        start, rows = base + index * size, size
        if half is not None:
            skip, rows = cut(size, half)
            start = start + skip
        return ref.at[(*lead, pl.ds(pl.multiple_of(start, 16), rows))]

    return block


def slabs(ref):
    def block(index, half):
        if half is None:
            return ref.at[index]
        return ref.at[index, pl.ds(*cut(ref.shape[1], half))]

    return block


def total(ref):
    return (ref[0].astype(F32) + ref[1].astype(F32) + ref[2].astype(F32) + ref[3].astype(F32)).astype(BF16)


OWN_STEPS = {2: 0, 4: 1, 5: 2, 7: 3}
REDUCE_COPIES = 120
WEIGHTS1, INPUTS1, WEIGHTS0, INPUTS0, STEPS = (n * SLOTS for n in range(2, 7))


def kernel(cap, x0_ref, dy_ref, ids_ref, gate_ref, wd_ref, o1_ref, o3_ref, o2_ref, y_ref, dx_ref, gdense_ref, g1_ref, g3_ref, g2_ref, h1_ref, h3_ref, h2_ref, kz_ref, ka_ref, kb_ref, kda_ref, kdb_ref, acc_ref, cur_ref, x1_ref, hold_ref, gd_ref, rows_ref, columns_ref, w1_ref, w3_ref, w2_ref, z_ref, a_ref, b_ref, m1_ref, m3_ref, m2_ref, d1_ref, d3_ref, d2_ref, s1_ref, s3_ref, s2_ref, r11_ref, r12_ref, r31_ref, r32_ref, t1_ref, t3_ref, y11_ref, y12_ref, y31_ref, y32_ref, y21_ref, y22_ref, u1_ref, u2_ref, l1_ref, l2_ref, c1_ref, c3_ref, cu_ref, cl_ref, f1_ref, f3_ref, fu_ref, fl_ref, dp_ref, dr_ref, ds_ref, e_ref, dcx_ref, dcz_ref, dcy_ref, de_ref, put_sem, load_sem, keep_sem, save_sem, gsend_sem, grecv_sem, send_sem, recv_sem, credit):
    s = pl.program_id(0)
    place = Place()
    gathers = Copies(place, gsend_sem, grecv_sem)
    copies = Copies(place, send_sem, recv_sem)
    given, whole, bufs = (o1_ref, o3_ref, o2_ref), (h1_ref, h3_ref, h2_ref), (w1_ref, w3_ref, w2_ref)
    kept, acts = (kz_ref, ka_ref, kb_ref), (z_ref, a_ref, b_ref)
    deferred = (kda_ref, kdb_ref)
    g0, g1 = (Gather(l, gathers, place, given, whole) for l in BUFS)
    rows, ff = s1_ref.shape[1], s2_ref.shape[1]
    quarter, part = rows // SIDE, ff // 2 // SIDE
    half_d = rows // 2

    stage, mate, mine_of = (m1_ref, m3_ref, m2_ref), (d1_ref, d3_ref, d2_ref), (s1_ref, s3_ref, s2_ref)
    for buf in BUFS:
        for n in ARRAYS:
            copies.add(("pair", buf, n), stage[n].at[buf], mate[n].at[buf], "c", 0)

    def ring_blocks(ref, q, me, base, size):
        block = slices(ref, (q,), base, size)
        return lambda offset, half: block((me + offset + SIDE) % SIDE, half)

    def group_blocks(ref):
        block = slabs(ref)
        return lambda offset, half: block({2: 0, 1: 1, -1: 2, 0: 3}[offset], half)

    first = {
        "x": [RingSum(copies, ("x", q), "x", ring_blocks(s1_ref, q, place.x, 0, quarter), r11_ref.at[q], r12_ref.at[q]) for q in range(SIDE)],
        "z": [RingSum(copies, ("z", q), "z", ring_blocks(s3_ref, q, place.z, 0, quarter), r31_ref.at[q], r32_ref.at[q]) for q in range(SIDE)],
    }
    mid = {"x": t1_ref, "z": t3_ref}
    on_y = {
        "x": RingSum(copies, "yx", "y", group_blocks(t1_ref), y11_ref, y12_ref),
        "z": RingSum(copies, "yz", "y", group_blocks(t3_ref), y31_ref, y32_ref),
        "w": RingSum(copies, "yw", "y", group_blocks(s2_ref), y21_ref, y22_ref),
    }
    inner = {
        "u": RingSum(copies, "u", "x", ring_blocks(s2_ref, 3, place.x, 0, part), u1_ref, u2_ref),
        "l": RingSum(copies, "l", "z", ring_blocks(s2_ref, 3, place.z, ff // 2, part), l1_ref, l2_ref),
    }
    ring_of = {"x": ("x", place.x), "u": ("x", place.x), "z": ("z", place.z), "l": ("z", place.z)}
    other_of = {"x": ("z", place.z), "u": ("z", place.z), "z": ("x", place.x), "l": ("x", place.x)}
    cross_ref = {"x": c1_ref, "z": c3_ref, "u": cu_ref, "l": cl_ref}
    done_ref = {"x": f1_ref, "z": f3_ref, "u": fu_ref, "l": fl_ref}
    out_of = {"x": (g1_ref, 0, quarter), "z": (g3_ref, 0, quarter), "u": (g2_ref, 0, part), "l": (g2_ref, ff // 2, part)}
    cross, final, puts = {}, {}, {}
    for i, k in enumerate(out_of):
        cross[k] = RingSpread(copies, ("cross", k), *other_of[k], slabs(cross_ref[k]))
        ref, base, size = out_of[k]
        for late in LAYERS:
            block = slices(ref, (late, place.c), base, size)
            final[k, late] = RingSpread(copies, ("final", k, late), *ring_of[k], block, source=done_ref[k], like=final.get((k, 1)))
            me = ring_of[k][1]
            puts[k, late] = pltpu.make_async_copy(done_ref[k], block(me, None), put_sem.at[i])
            for offset in (0, *WAYS, 2):
                quarter_at = block((me + offset) % SIDE if offset >= 0 else (me + SIDE - 1) % SIDE, None)
                copies.add(("pass", k, offset, late), quarter_at if offset else done_ref[k], quarter_at, "c", 0, None if late else ("pass", k, offset, 1))
    mine, theirs = (pl.ds(pl.multiple_of(c * half_d, 16), half_d) for c in (place.c, 1 - place.c))
    copies.add("dense pair", dp_ref.at[theirs], dr_ref, "c", 0)
    copies.add("dense pass", dcy_ref, de_ref, "c", 0)
    piece = half_d // SIDE
    dense_block = slices(ds_ref, (), 0, piece)
    dense_sums = Direct(copies, "dense sums", "y", lambda step: dense_block((place.y + step) % SIDE, None), lambda step: e_ref.at[step - 1])
    gather_block = slices(dcy_ref, (), 0, piece)(place.y, None)
    own_piece = {"x": dcx_ref.at[place.x], "z": dcz_ref.at[place.z], "y": gather_block}
    dense = {k: Direct(copies, ("dense", k), k, lambda step, k=k: own_piece[k], lambda step, k=k: own_piece[k]) for k in own_piece}

    def reduce_start(q):
        for k in ("x", "z"):
            first[k][q].start()

    def reduce_onward(q):
        for k in ("x", "z"):
            first[k][q].onward()

    def reduce_finish(q):
        for k in ("x", "z"):
            first[k][q].finish(mid[k].at[q])

    def y_start():
        for k in ("x", "z"):
            on_y[k].start()

    def y_onward():
        for k in ("x", "z"):
            on_y[k].onward()

    def y_finish():
        for k in ("x", "z"):
            on_y[k].finish(cross_ref[k].at[other_of[k][1]])
            cross[k].start()

    def w_finish():
        on_y["w"].finish(s2_ref.at[3])
        for k in ("u", "l"):
            inner[k].start()

    def inner_onward():
        for k in ("u", "l"):
            inner[k].onward()

    def inner_finish():
        for k in ("u", "l"):
            inner[k].finish(cross_ref[k].at[other_of[k][1]])
            cross[k].start()

    def cross_onward(*keys):
        for k in keys:
            cross[k].onward()

    def cross_finish(late, *keys):
        for k in keys:
            cross[k].finish()
            done_ref[k][...] = total(cross_ref[k])
            puts[k, late].start()
            final[k, late].start()
            copies.start(("pass", k, 0, late))

    def final_onward(late, *keys):
        for k in keys:
            final[k, late].onward()
            copies.start(*[("pass", k, way, late) for way in WAYS])

    def final_finish(late, *keys):
        for k in keys:
            final[k, late].finish()
            puts[k, late].wait()
            copies.start(("pass", k, 2, late))

    def pass_finish(late):
        keys = [("pass", k, offset, late) for k in out_of for offset in (0, *WAYS, 2)]
        copies.arrive(*keys)
        copies.sent(*keys)

    def dense_sum():
        copies.arrive("dense pair")
        ds_ref[...] = (dp_ref[mine].astype(F32) + dr_ref[...].astype(F32)).astype(BF16)
        copies.sent("dense pair")
        dense_sums.start()

    def dense_to_x():
        dense_sums.finish()
        mine = dense_block(place.y, None)[...].astype(F32)
        own_piece["x"][...] = (mine + e_ref[0].astype(F32) + e_ref[1].astype(F32) + e_ref[2].astype(F32)).astype(BF16)
        dense["x"].start()

    def dense_next(k, ref, follow):
        dense[k].finish()
        own_piece[follow][...] = total(ref)
        dense[follow].start()

    def dense_to_z():
        dense_next("x", dcx_ref, "z")

    def dense_to_y():
        dense_next("z", dcz_ref, "y")

    def dense_out(late):
        return pltpu.make_async_copy(gd_ref, gdense_ref.at[late], keep_sem.at[0, 1])

    def dense_pass(late):
        dense["y"].finish()
        if late == 0:
            dense_out(1).wait()
        gd_ref[mine] = dcy_ref[...]
        copies.start("dense pass")

    def dense_finish(late):
        copies.arrive("dense pass")
        gd_ref[theirs] = de_ref[...]
        copies.sent("dense pass")
        dense_out(late).start()

    def copy(src, dst, sem):
        return pltpu.make_async_copy(src, dst, sem)

    def weights(layer, slot, arrays, buf, is_given=False):
        for n in arrays:
            src = given[n].at[layer, (place.c + slot) % 2] if is_given else whole[n].at[layer, slot]
            yield copy(src, bufs[n].at[buf], load_sem.at[buf, n])

    def saved(layer, slot, buf):
        for n, (src, dst) in enumerate(zip(kept, acts)):
            yield copy(src.at[layer, slot], dst.at[buf], load_sem.at[buf, 3 + n])

    def weights_loads(step):
        layer, slot, buf = layer_of(step), SLOTS - 1 - step % SLOTS, (step + 1) % 2
        return [*weights(layer, slot, [2], buf), *saved(layer, slot, buf)]

    def inputs_loads(step):
        layer, slot, buf = layer_of(step), SLOTS - 1 - step % SLOTS, (step + 1) % 2
        return [*weights(layer, slot, BUFS, buf)] + [copy(deferred[n].at[slot], acts[n + 1].at[buf], load_sem.at[buf, 4 + n]) for n in BUFS]

    def load(step):
        slot = step % SLOTS
        for is_given in (True, False):
            pl.when((slot < 2) == is_given)(lambda: start(weights(step // SLOTS, slot, ARRAYS, step % 2, is_given)))

    def layer_of(step):
        return 1 - (step - WEIGHTS1) // (2 * SLOTS)

    def keeps(step):
        return [copy(bufs[n].at[step % 2], whole[n].at[step // SLOTS, step % SLOTS], keep_sem.at[step % 2, n]) for n in ARRAYS]

    def saves(step):
        return [copy(src.at[step % 2], dst.at[step // SLOTS, step % SLOTS], save_sem.at[step % 2, n]) for n, (src, dst) in enumerate(zip(acts, kept))]

    def defers(step):
        return [copy(acts[n + 1].at[2], deferred[n].at[SLOTS - 1 - step % SLOTS], save_sem.at[0, n]) for n in BUFS]

    def wait(items):
        for item in items:
            item.wait()

    def start(items):
        for item in items:
            item.start()

    def ending():
        dense_finish(1)
        copies.start("dense pair")
        y_finish()
        inner_finish()
        dense_sum()
        dense_to_x()
        cross_onward("x", "z")
        pass_finish(1)
        pl.semaphore_signal(credit.at[2], inc=1, device_id=place.at("c", 0), device_id_type=MESH)
        cross_onward("u", "l")
        dense_to_z()
        pl.semaphore_wait(credit.at[2], 1)
        cross_finish(0, "x", "z")
        cross_finish(0, "u", "l")
        dense_to_y()
        dense_pass(0)
        final_onward(0, "x", "z")
        dense_finish(0)
        final_onward(0, "u", "l")
        final_finish(0, "x", "z")
        final_finish(0, "u", "l")
        pass_finish(0)

    before, middle, after = {}, {}, {}

    def plan(table, first, *stages):
        for n, stage in enumerate(stages):
            table.setdefault(first + n, []).extend(stage)

    on, done = lambda q: lambda: reduce_onward(q), lambda q: lambda: reduce_finish(q)
    now = lambda: load(s)
    plan(before, 1, [g0.lead], [g0.follow, g0.lead_onward, g1.begin, g0.follow_onward, g0.last, g0.complete_y, now], [g0.passed_left])
    plan(before, 4, [g0.last_onward, g1.lead], [g0.complete_last, now, g0.passed_right, g1.follow], [], [g0.passed_last, now, g1.lead_onward])
    plan(before, SLOTS + 1, [g1.follow_onward, g1.last], [g1.complete_y, now], [g1.passed_left], [g1.last_onward], [g1.complete_last, now, g1.passed_right], [g1.passed_last])
    unready = (1, 4, 6, SLOTS + 1, SLOTS + 4)
    late = ("x", "z", "u", "l")
    plan(before, INPUTS1 + 7, [w_finish])
    plan(middle, WEIGHTS0, [inner_onward])
    plan(before, WEIGHTS0, [lambda: copies.start("dense pair")], [], [inner_finish], [lambda: cross_onward("x", "z"), dense_to_x], [lambda: cross_onward("u", "l")], [dense_to_z])
    plan(middle, WEIGHTS0, [dense_sum, y_finish], [], [], [], [], [], [], [dense_to_y])
    plan(before, INPUTS0, [lambda: cross_finish(1, *late)], [], [], [], [], [lambda: final_onward(1, *late)], [], [lambda: dense_pass(1), lambda: final_finish(1, *late)])
    plan(before, INPUTS0 + 5, [w_finish], [], [inner_onward])
    for base in (WEIGHTS1, WEIGHTS0):
        plan(before, base + 3, [on_y["w"].start], [], [], [done(0), y_start, on_y["w"].onward])
        plan(before, base + 4, [on(0)])
        plan(middle, base + 6, [on(1)], [on(2)])
        plan(before, base + SLOTS, [], [done(1)], [done(2), y_onward], [on(3)], [], [], [done(3)])
        for step, q in OWN_STEPS.items():
            plan(after, base + step, [lambda q=q: reduce_start(q)])

    def hooks(table, *phases):
        for phase in phases:
            mine = {step: stages for step, stages in sorted(table.items()) if phase <= step < phase + SLOTS}
            if mine:

                @pl.when(s // SLOTS == phase // SLOTS)
                def _(mine=mine):
                    for step, stages in mine.items():

                        @pl.when(s == step)
                        def _(stages=stages):
                            for stage in stages:
                                stage()

    phase, t = s // SLOTS, s % SLOTS
    forth, back = s % 2, (s + 1) % 2

    def bring(ref, hold):
        return copy(ref, hold, keep_sem.at[1, 0])

    @pl.when(s == 0)
    def _():
        bring(x0_ref, hold_ref).start()
        load(0)
        greet(place)
        g0.begin()
        load(1)
        route(ids_ref, gate_ref, rows_ref, columns_ref, place)
        bring(x0_ref, hold_ref).wait()

    def enter(x):
        cur_ref[...] = (x.astype(F32) + dot(x, wd_ref[phase])).astype(BF16)
        acc_ref[...] = jnp.zeros_like(acc_ref)

    def leave(out_ref):
        out_ref[...] = (cur_ref[...].astype(F32) + acc_ref[...]).astype(BF16)

    @pl.when(s < WEIGHTS1)
    def _():
        hooks(before, 0, SLOTS)
        pl.when(s > 1)(lambda: wait(saves(s - 2)))
        ahead = functools.reduce(jnp.logical_and, [s != step for step in unready], (s > 0) & (s < WEIGHTS1 - 1))
        pl.when((t == 1) | (t == 2))(lambda: wait(keeps(s - 1)))
        pl.when(ahead)(lambda: load(s + 1))

        @pl.when(t < 2)
        def _():
            pl.when(s == 0)(lambda: enter(hold_ref[...]))
            pl.when(s == SLOTS)(lambda: enter(x1_ref[...]))

        layer, slot = phase, t
        come = list(weights(layer, slot, ARRAYS, forth))

        def forward_step(is_ready):
            if is_ready:
                wait(come)
            z = dot(one_hot(rows_ref, layer, slot, cap), cur_ref[...]).astype(BF16)
            z_ref[forth] = z
            if not is_ready:
                wait(come)
            a = dot(z, w1_ref[forth]).astype(BF16)
            b = dot(z, w3_ref[forth]).astype(BF16)
            a_ref[forth] = a
            b_ref[forth] = b
            a = a.astype(F32)
            h = (a * jax.nn.sigmoid(a) * b.astype(F32)).astype(BF16)
            o = dot(h, w2_ref[forth]).astype(BF16)
            acc_ref[...] += column(columns_ref, layer, SLOTS + slot) * dot(one_hot_t(columns_ref, layer, slot, cap), o)

        is_late = functools.reduce(jnp.logical_or, [s == step + 1 for step in unready])
        pl.when(is_late)(lambda: forward_step(False))
        pl.when(jnp.logical_not(is_late))(lambda: forward_step(True))
        pl.when(t < 2)(lambda: start(keeps(s)))
        pl.when(s < WEIGHTS1 - 1)(lambda: start(saves(s)))
        @pl.when(t == SLOTS - 1)
        def _():
            pl.when(s == SLOTS - 1)(lambda: leave(x1_ref))
            pl.when(s == WEIGHTS1 - 1)(lambda: leave(hold_ref))

    @pl.when((phase == WEIGHTS1 // SLOTS) | (phase == WEIGHTS0 // SLOTS))
    def _():
        layer, slot = layer_of(s), SLOTS - 1 - t
        hooks(before, WEIGHTS1, WEIGHTS0)

        @pl.when(s == WEIGHTS1)
        def _():
            moved = copy(hold_ref, y_ref, keep_sem.at[0, 0])
            moved.start()
            bring(dy_ref, cur_ref).start()
            wait(saves(s - 2))
            gathers.drain()
            bring(dy_ref, cur_ref).wait()
            moved.wait()
            acc_ref[...] = cur_ref[...].astype(F32)

        pl.when(s > WEIGHTS1)(lambda: wait(weights_loads(s)))
        pl.when(t > 0)(lambda: wait(defers(s - 1)))
        pl.when(t < SLOTS - 1)(lambda: start(weights_loads(s + 1)))
        pl.when(t == SLOTS - 1)(lambda: start(inputs_loads(s + 1)))

        grad_gated = (column(columns_ref, layer, SLOTS + slot) * cur_ref[...].astype(F32)).astype(BF16)
        do = dot(one_hot(rows_ref, layer, slot, cap), grad_gated).astype(BF16)
        dh = dot_nt(do, w2_ref[back])
        a = a_ref[back].astype(F32)
        b = b_ref[back].astype(F32)
        sig = jax.nn.sigmoid(a)
        act = a * sig
        h = (act * b).astype(BF16)
        db = (dh * act).astype(BF16)
        da = (dh * b * (sig + act * (1.0 - sig))).astype(BF16)
        a_ref[2] = da
        b_ref[2] = db
        z = z_ref[back]
        start(defers(s))
        hooks(middle, WEIGHTS1, WEIGHTS0)

        def weight_grads():
            return dot_tn(z, da), dot_tn(z, db), dot_tn(h, do)

        is_own = functools.reduce(jnp.logical_or, [t == step for step in OWN_STEPS])
        group = t // 4 + t // 5 + t // 7
        into = (t + t // 3 + t // 6) % 2
        turn = t + (1 - layer) * SLOTS

        @pl.when(jnp.logical_not(is_own))
        def _():
            for buf in BUFS:
                pl.when((turn >= 3) & (into == buf))(lambda: copies.sent(*[("pair", buf, n) for n in ARRAYS]))

            for ref, grad in zip(stage, weight_grads()):
                ref[into] = grad.astype(BF16)

            pl.when(turn >= 3)(lambda: pl.semaphore_wait(credit.at[into], 1))
            for buf in BUFS:
                pl.when(into == buf)(lambda: copies.start(*[("pair", buf, n) for n in ARRAYS]))

        @pl.when(is_own)
        def _():
            for buf in BUFS:
                pl.when(group % 2 == buf)(lambda: copies.arrive(*[("pair", buf, n) for n in ARRAYS]))

            for ref, add, grad in zip(mine_of, mate, weight_grads()):
                ref[group] = (grad + add[group % 2].astype(F32)).astype(BF16)

            @pl.when(turn < 2 * SLOTS - 3)
            def _():
                pl.semaphore_signal(credit.at[group % 2], inc=1, device_id=place.at("c", 0), device_id_type=MESH)

            hooks(after, WEIGHTS1, WEIGHTS0)

    def leave_back(layer, x, out_ref):
        grad = acc_ref[...]
        grad_b = grad.astype(BF16)
        dp_ref[...] = dot_tn(x, grad_b).astype(BF16)
        out_ref[...] = (grad + dot_nt(grad_b, wd_ref[layer])).astype(BF16)

    @pl.when((phase == INPUTS1 // SLOTS) | (phase == INPUTS0 // SLOTS))
    def _():
        layer, slot = layer_of(s), SLOTS - 1 - t
        hooks(before, INPUTS1, INPUTS0)
        wait(inputs_loads(s))
        pl.when(t == 0)(lambda: wait(defers(s - 1)))
        pl.when(t < SLOTS - 1)(lambda: start(inputs_loads(s + 1)))
        pl.when(s == WEIGHTS0 - 1)(lambda: start(weights_loads(s + 1)))
        dz = (dot_nt(a_ref[back], w1_ref[back]) + dot_nt(b_ref[back], w3_ref[back])).astype(BF16)
        acc_ref[...] += dot(one_hot_t(columns_ref, layer, slot, cap), dz)

        @pl.when(s == WEIGHTS0 - 1)
        def _():
            leave_back(1, x1_ref[...], cur_ref)
            acc_ref[...] = cur_ref[...].astype(F32)
            bring(x0_ref, x1_ref).start()
            bring(x0_ref, x1_ref).wait()

        @pl.when(s == STEPS - 1)
        def _():
            leave_back(0, x1_ref[...], hold_ref)
            moved = copy(hold_ref, dx_ref, keep_sem.at[0, 0])
            moved.start()
            ending()
            copies.sent(*[("pair", buf, n) for buf in BUFS for n in ARRAYS])
            moved.wait()
            dense_out(0).wait()


def step(cap, x0, dy, ids, gates, wd, w1, w3, w2):
    tokens, width = dy.shape
    layers, local, _, ff = w1.shape
    quarter, part, piece = width // SIDE, ff // 2 // SIDE, width // 2 // SIDE
    hbm = pl.BlockSpec(memory_space=pl.ANY)

    def fixed(shape):
        return pl.BlockSpec(shape, lambda s: (0,) * len(shape), pipeline_mode=pl.Buffered(1))

    def buf(*shape):
        return pltpu.VMEM(shape, BF16)

    def dma(*shape):
        return pltpu.SemaphoreType.DMA(shape)

    shape = jax.ShapeDtypeStruct
    ups, downs = [(width, ff), (width, ff), (ff, width)], [(quarter, ff), (part, width)]
    acts = [(cap, width), (cap, ff), (cap, ff)]
    scratch = [pltpu.VMEM((tokens, width), F32)] + [buf(tokens, width)] * 3 + [buf(width, width), pltpu.VMEM((layers, SLOTS, tokens), jnp.int32), pltpu.VMEM((layers, tokens, LANES), F32)]
    scratch += [buf(2, *u) for u in ups] + [buf(n, *a) for n, a in zip((2, 3, 3), acts)]
    scratch += [buf(2, *u) for u in ups] * 2 + [buf(SIDE, *u) for u in ups]
    scratch += [buf(SIDE, 2, quarter // 2, ff), buf(SIDE, 2, quarter, ff)] * 2
    scratch += [buf(SIDE, quarter, ff)] * 2
    scratch += [buf(2, quarter // 2, ff), buf(2, quarter, ff)] * 2 + [buf(2, ff // 2, width), buf(2, ff, width)]
    scratch += [buf(2, part // 2, width), buf(2, part, width)] * 2
    scratch += [buf(SIDE, quarter, ff)] * 2 + [buf(SIDE, part, width)] * 2
    scratch += [buf(quarter, ff)] * 2 + [buf(part, width)] * 2
    scratch += [buf(width, width)] + [buf(width // 2, width)] * 2 + [buf(SIDE - 1, piece, width)] + [buf(SIDE, piece, width)] * 2 + [buf(width // 2, width)] * 2
    scratch += [dma(4), dma(2, 6), dma(2, 3), dma(2, 3), dma(GATHER_COPIES), dma(GATHER_COPIES), dma(REDUCE_COPIES), dma(REDUCE_COPIES), pltpu.SemaphoreType.REGULAR((3,))]
    results = [(tokens, width), (tokens, width), (layers, width, width)]
    kept = [(layers, local, *u) for u in ups] + [(layers, SLOTS, *u) for u in ups + acts] + [(SLOTS, cap, ff)] * 2
    return pl.pallas_call(
        functools.partial(kernel, cap),
        grid=(STEPS,),
        in_specs=[hbm] * 2 + [fixed(v.shape) for v in (ids, gates, wd)] + [hbm] * 3,
        out_specs=[hbm] * len(results + kept),
        out_shape=[shape(r, BF16) for r in results + kept],
        scratch_shapes=scratch,
        compiler_params=pltpu.CompilerParams(vmem_limit_bytes=VMEM_LIMIT, collective_id=0, has_side_effects=True),
        name="step",
    )(x0, dy, ids, gates, wd, w1, w3, w2)[:6]


def take_kernel(count, *refs):
    sources, targets, holds, (come, go) = refs[:count], refs[count : 2 * count], refs[2 * count : 3 * count], refs[3 * count :]
    comes = [pltpu.make_async_copy(a, b, come.at[n]) for n, (a, b) in enumerate(zip(sources, holds))]
    goes = [pltpu.make_async_copy(a, b, go.at[n]) for n, (a, b) in enumerate(zip(holds, targets))]
    for item in comes:
        item.start()
    for first, then in zip(comes, goes):
        first.wait()
        then.start()
    for item in goes:
        item.wait()


def take(arrays):
    count = len(arrays)
    hbm = pl.BlockSpec(memory_space=pl.ANY)
    return pl.pallas_call(
        functools.partial(take_kernel, count),
        in_specs=[hbm] * count,
        out_specs=[hbm] * count,
        out_shape=[jax.ShapeDtypeStruct(a.shape, a.dtype) for a in arrays],
        scratch_shapes=[pltpu.VMEM(a.shape, a.dtype) for a in arrays] + [pltpu.SemaphoreType.DMA((count,))] * 2,
        compiler_params=pltpu.CompilerParams(vmem_limit_bytes=VMEM_LIMIT),
        name="take",
    )(*arrays)


def solution(mesh):
    tok_spec = P(TOK_AXES, None)
    route_spec = P(None, TOK_AXES, None)
    expert_spec = P(None, "ep", None, None)
    whole_spec = P(None, None, None)

    def device_step(tok_in, tok_grad, route_ids, gate_vals, *weights):
        tokens, top_k = route_ids.shape[1:]
        return tuple(take(step(2 * tokens * top_k // SLOTS, tok_in, tok_grad, jnp.swapaxes(route_ids, 1, 2), jnp.swapaxes(gate_vals, 1, 2), *weights)))

    return jax.shard_map(device_step, mesh=mesh, in_specs=(tok_spec, tok_spec, route_spec, route_spec, whole_spec, expert_spec, expert_spec, expert_spec), out_specs=(tok_spec, tok_spec, whole_spec, expert_spec, expert_spec, expert_spec), check_vma=False)
```
